32 devices in a mesh: dp: 1 (over z), row: 4 (over y), col: 8 (over x, core).
Axes of the slice: x: 4, y: 4, z: 1, core: 2. Of those that a mesh axis runs over, the one named last changes fastest.
The devices are a block of a 4x4x8 slice.
Arguments:
- x_in: bfloat16 [16, 512, 2560], P('dp', None, ('row', 'col'))
- ln_gain: bfloat16 [2, 2560], P(None, ('row', 'col'))
- w_in: bfloat16 [2, 2560, 23040], P(None, 'row', 'col')
- w_kv: bfloat16 [2, 2560, 160], P(None, 'row', 'col')
- w_out: bfloat16 [2, 12800, 2560], P(None, 'col', 'row')
Outputs:
- output 1: bfloat16 [16, 512, 2560], P('dp', None, ('row', 'col'))
- output 2: bfloat16 [2, 2, 16, 512, 80], P(None, None, 'dp', ('row', 'col'))
All inputs are finite; a program needn't handle non-finite values.
Results may differ from the reference program's by a relative error of at most 0.0163933.
Values are sent between devices in bfloat16 or wider.
A program may use at most 768 MiB of HBM per device.

```python
import jax
import jax.numpy as jnp
from jax import lax

D_MODEL = 2560
HEADS = 32
HEAD_DIM = 80
FF_WIDTH = 10240
BATCH = 16
SEQ_LEN = 512
COL_SHARDS = 8
LAYERS = 2

LN_EPS = 1e-6
E_WIDTH = HEADS * HEAD_DIM + 2 * FF_WIDTH
R_WIDTH = HEADS * HEAD_DIM + FF_WIDTH
E_BLOCK = E_WIDTH // COL_SHARDS
Q_BLOCK = HEADS * HEAD_DIM // COL_SHARDS
F_BLOCK = FF_WIDTH // COL_SHARDS
HALF_DIM = HEAD_DIM // 2


def setup_inputs(seed: int = 0, part: int = 0) -> dict:
    root_key = jax.random.key(seed)
    shared_root, part_root = jax.random.split(root_key)
    part_key = jax.random.fold_in(part_root, part)
    key_x, key_off = jax.random.split(part_key)
    key_g, key_in, key_kv, key_out = jax.random.split(shared_root, 4)
    slope_part = 2.0 * (jnp.arange(D_MODEL, dtype=jnp.float32) / D_MODEL - 0.5)
    offset = slope_part + 0.5 * jax.random.normal(key_off, (D_MODEL,), jnp.float32)
    x_in = (jax.random.normal(key_x, (BATCH, SEQ_LEN, D_MODEL), jnp.float32) + offset).astype(jnp.bfloat16)
    ln_gain = (1.0 + 0.3 * jax.random.normal(key_g, (LAYERS, D_MODEL), jnp.float32)).astype(jnp.bfloat16)
    w_in = (jax.random.normal(key_in, (LAYERS, D_MODEL, E_WIDTH), jnp.float32) * D_MODEL ** -0.5).astype(jnp.bfloat16)
    w_kv = (jax.random.normal(key_kv, (LAYERS, D_MODEL, 2 * HEAD_DIM), jnp.float32) * D_MODEL ** -0.5).astype(jnp.bfloat16)
    w_out = (jax.random.normal(key_out, (LAYERS, R_WIDTH, D_MODEL), jnp.float32) * R_WIDTH ** -0.5).astype(jnp.bfloat16)
    return {"x_in": x_in, "ln_gain": ln_gain, "w_in": w_in, "w_kv": w_kv, "w_out": w_out}


def layer_norm(hidden, gain_row):
    hidden_f32 = hidden.astype(jnp.float32)
    mean_val = jnp.mean(hidden_f32, axis=-1, keepdims=True)
    centered = hidden_f32 - mean_val
    variance = jnp.mean(centered * centered, axis=-1, keepdims=True)
    return (centered * lax.rsqrt(variance + LN_EPS) * gain_row.astype(jnp.float32)).astype(jnp.bfloat16)


def rope_tables(positions):
    inv_freq = 1.0 / (10000.0 ** (jnp.arange(HALF_DIM, dtype=jnp.float32) * 2.0 / HEAD_DIM))
    angles = positions.astype(jnp.float32)[:, None] * inv_freq[None, :]
    return jnp.cos(angles), jnp.sin(angles)


def apply_rope(values, cos_tab, sin_tab):
    lower_half = values[..., :HALF_DIM]
    upper_half = values[..., HALF_DIM:]
    return jnp.concatenate([lower_half * cos_tab - upper_half * sin_tab, upper_half * cos_tab + lower_half * sin_tab], axis=-1)


def one_layer(hidden, params):
    gain_row, w_in_layer, w_kv_layer, w_out_layer = params
    normed = layer_norm(hidden, gain_row)
    projected = jnp.dot(normed, w_in_layer, preferred_element_type=jnp.float32).astype(jnp.bfloat16).reshape(SEQ_LEN, COL_SHARDS, E_BLOCK)
    kv_proj = jnp.dot(normed, w_kv_layer, preferred_element_type=jnp.float32).astype(jnp.bfloat16)
    query = projected[:, :, :Q_BLOCK].reshape(SEQ_LEN, HEADS, HEAD_DIM)
    gate_val = projected[:, :, Q_BLOCK:Q_BLOCK + F_BLOCK]
    up_val = projected[:, :, Q_BLOCK + F_BLOCK:]
    positions = jnp.arange(SEQ_LEN)
    cos_tab, sin_tab = rope_tables(positions)
    q_rot = (apply_rope(query.astype(jnp.float32), cos_tab[:, None, :], sin_tab[:, None, :]) * HEAD_DIM ** -0.5).astype(jnp.bfloat16)
    k_rot = apply_rope(kv_proj[:, :HEAD_DIM].astype(jnp.float32), cos_tab, sin_tab).astype(jnp.bfloat16)
    v_val = kv_proj[:, HEAD_DIM:]
    scores = jnp.einsum("qhd,kd->hqk", q_rot.astype(jnp.float32), k_rot.astype(jnp.float32))
    causal = positions[None, :] <= positions[:, None]
    scores = jnp.where(causal[None, :, :], scores, -1e30)
    attn_prob = jax.nn.softmax(scores, axis=-1).astype(jnp.bfloat16)
    attn_out = jnp.einsum("hqk,kd->qhd", attn_prob.astype(jnp.float32), v_val.astype(jnp.float32)).astype(jnp.bfloat16)
    mlp_out = (jax.nn.silu(gate_val.astype(jnp.float32)) * up_val.astype(jnp.float32)).astype(jnp.bfloat16)
    joined = jnp.concatenate([attn_out.reshape(SEQ_LEN, COL_SHARDS, Q_BLOCK), mlp_out], axis=2).reshape(SEQ_LEN, R_WIDTH)
    update = jnp.dot(joined, w_out_layer, preferred_element_type=jnp.float32).astype(jnp.bfloat16)
    return hidden + update, jnp.stack([k_rot, v_val])


def reference(x_in, ln_gain, w_in, w_kv, w_out):
    def one_sequence(seq_x):
        return lax.scan(one_layer, seq_x, (ln_gain, w_in, w_kv, w_out))
    y_out, kv_all = lax.map(one_sequence, x_in)
    return y_out, jnp.transpose(kv_all, (1, 2, 0, 3, 4))
```

```python
import functools

import jax
import jax.numpy as jnp
from jax import lax
from jax.experimental import pallas as pl
from jax.experimental.pallas import tpu as pltpu
from jax.sharding import PartitionSpec as P

LN_EPS = 1e-6
MESH = pl.DeviceIdType.MESH
ANY = pl.BlockSpec(memory_space=pl.ANY)


def rope_tables(positions, head_dim):
    half_dim = head_dim // 2
    inv_freq = 1.0 / (10000.0 ** (jnp.arange(half_dim, dtype=jnp.float32) * 2.0 / head_dim))
    angles = positions.astype(jnp.float32)[:, None] * inv_freq[None, :]
    return jnp.cos(angles), jnp.sin(angles)


def apply_rope(values, cos_tab, sin_tab):
    half_dim = values.shape[-1] // 2
    lower_half = values[..., :half_dim]
    upper_half = values[..., half_dim:]
    return jnp.concatenate([lower_half * cos_tab - upper_half * sin_tab, upper_half * cos_tab + lower_half * sin_tab], axis=-1)


def remote(src, dst, send_sem, recv_sem, **where):
    return pltpu.make_async_remote_copy(src_ref=src, dst_ref=dst, send_sem=send_sem, recv_sem=recv_sem, device_id=where, device_id_type=MESH)


def comm_params(collective_id, vmem=None):
    return pltpu.CompilerParams(collective_id=collective_id, has_side_effects=True, vmem_limit_bytes=vmem)


def exchange_kernel(n_row, n_col, with_rows, *refs):
    if with_rows:
        send, extra, out, extra_out, local_sem, ssem, rsem, local_sem2, ssem2, rsem2 = refs
    else:
        send, out, local_sem, ssem, rsem = refs
    row, col = lax.axis_index("row"), lax.axis_index("col")
    n = n_row * n_col
    me = row * n_col + col
    barrier = pltpu.get_barrier_semaphore()

    def greet(k, carry):
        dest = lax.rem(me + k, n)
        pl.semaphore_signal(barrier, inc=1, device_id={"row": dest // n_col, "col": lax.rem(dest, n_col)}, device_id_type=MESH)
        return carry

    lax.fori_loop(1, n, greet, 0)
    pl.semaphore_wait(barrier, n - 1)

    def copy_to(k):
        dest = lax.rem(me + k, n)
        return remote(send.at[dest], out.at[me], ssem.at[k], rsem.at[k], row=dest // n_col, col=lax.rem(dest, n_col))

    def copy_from(k):
        source = lax.rem(me + n - k, n)
        return remote(send.at[source], out.at[source], ssem.at[k], rsem.at[k], row=row, col=col)

    def rows_to(j):
        dest = lax.rem(row + j, n_row)
        return remote(extra.at[dest], extra_out.at[row], ssem2.at[j], rsem2.at[j], row=dest, col=col)

    def rows_from(j):
        source = lax.rem(row + n_row - j, n_row)
        return remote(extra.at[source], extra_out.at[source], ssem2.at[j], rsem2.at[j], row=row, col=col)

    local = pltpu.make_async_copy(send.at[me], out.at[me], local_sem)
    local.start()

    def start(k, carry):
        copy_to(k).start()
        return carry

    lax.fori_loop(1, n, start, 0)
    if with_rows:
        local2 = pltpu.make_async_copy(extra.at[row], extra_out.at[row], local_sem2)
        local2.start()
        for j in range(1, n_row):
            rows_to(j).start()

    def finish(k, carry):
        copy_to(k).wait_send()
        copy_from(k).wait_recv()
        return carry

    lax.fori_loop(1, n, finish, 0)
    local.wait()
    if with_rows:
        local2.wait()
        for j in range(1, n_row):
            rows_to(j).wait_send()
            rows_from(j).wait_recv()


def exchange(n_row, n_col, collective_id, send, extra=None):
    n = n_row * n_col
    with_rows = extra is not None
    args = (send, extra) if with_rows else (send,)
    sems = [pltpu.SemaphoreType.DMA, pltpu.SemaphoreType.DMA((n,)), pltpu.SemaphoreType.DMA((n,))]
    if with_rows:
        sems += [pltpu.SemaphoreType.DMA, pltpu.SemaphoreType.DMA((n_row,)), pltpu.SemaphoreType.DMA((n_row,))]
    return pl.pallas_call(
        functools.partial(exchange_kernel, n_row, n_col, with_rows),
        out_shape=tuple(jax.ShapeDtypeStruct(a.shape, a.dtype) for a in args),
        in_specs=[ANY] * len(args),
        out_specs=(ANY,) * len(args),
        scratch_shapes=sems,
        compiler_params=comm_params(collective_id),
        name="exchange",
    )(*args)


def gather_kernel(n_col, piece, out, local_sem, ssem, rsem):
    row, col = lax.axis_index("row"), lax.axis_index("col")
    n_x = n_col // 2
    x, k = col // 2, lax.rem(col, 2)
    right = lax.rem(x + 1, n_x) * 2 + k
    left = lax.rem(x + n_x - 1, n_x) * 2 + k
    far = lax.rem(x + 2, n_x) * 2 + k
    twin = x * 2 + 1 - k

    def other(c):
        return (c // 2) * 2 + 1 - k

    barrier = pltpu.get_barrier_semaphore()
    for c in (right, left, twin):
        pl.semaphore_signal(barrier, inc=1, device_id={"row": row, "col": c}, device_id_type=MESH)
    pl.semaphore_wait(barrier, 3)
    half = piece.shape[0] // 2
    low, high = pl.ds(0, half), pl.ds(half, half)

    def to(i, src, dst, c):
        return remote(src, dst, ssem.at[i], rsem.at[i], row=row, col=c)

    local = pltpu.make_async_copy(piece, out.at[col], local_sem)
    sends = [to(0, piece, out.at[col], right), to(1, piece, out.at[col], left), to(2, piece, out.at[col], twin)]
    for c in sends:
        c.start()
    local.start()

    def arrived(i, dst):
        to(i, dst, dst, col).wait_recv()

    def forward(i, src, c):
        copy = to(i, src, src, c)
        copy.start()
        sends.append(copy)

    arrived(0, out.at[left])
    forward(3, out.at[left, low], right)
    forward(4, out.at[left], twin)
    arrived(1, out.at[right])
    forward(5, out.at[right, high], left)
    forward(6, out.at[right], twin)
    arrived(3, out.at[far, low])
    forward(7, out.at[far, low], twin)
    arrived(5, out.at[far, high])
    forward(8, out.at[far, high], twin)
    arrived(2, out.at[twin])
    arrived(4, out.at[other(left)])
    arrived(6, out.at[other(right)])
    arrived(7, out.at[other(far), low])
    arrived(8, out.at[other(far), high])
    local.wait()
    for c in sends:
        c.wait_send()


def gather_cols(n_col, collective_id, piece):
    return pl.pallas_call(
        functools.partial(gather_kernel, n_col),
        out_shape=jax.ShapeDtypeStruct((n_col,) + piece.shape, piece.dtype),
        in_specs=[ANY],
        out_specs=ANY,
        scratch_shapes=[pltpu.SemaphoreType.DMA, pltpu.SemaphoreType.DMA((9,)), pltpu.SemaphoreType.DMA((9,))],
        compiler_params=comm_params(collective_id),
        name="gather_cols",
    )(piece)


def reduce_kernel(n_col, part, out, own, twin_part, from_far, from_near, local_sem, ssem, rsem):
    row, col = lax.axis_index("row"), lax.axis_index("col")
    n_x = n_col // 2
    x, k = col // 2, lax.rem(col, 2)
    xr, xl, xf = lax.rem(x + 1, n_x), lax.rem(x + n_x - 1, n_x), lax.rem(x + 2, n_x)
    right, left, twin = xr * 2 + k, xl * 2 + k, x * 2 + 1 - k
    barrier = pltpu.get_barrier_semaphore()
    for c in (right, left, twin):
        pl.semaphore_signal(barrier, inc=1, device_id={"row": row, "col": c}, device_id_type=MESH)
    pl.semaphore_wait(barrier, 3)
    rows = out.shape[0]
    half = rows // 2
    step = 16
    order = (xf, xr, xl, x)

    def to(i, src, dst, c):
        return remote(src, dst, ssem.at[i], rsem.at[i], row=row, col=c)

    sends, loads = [], []
    for j, xd in enumerate(order):
        sends.append(to(j, part.at[xd * 2 + 1 - k], twin_part.at[j], twin))
        loads.append(pltpu.make_async_copy(part.at[xd * 2 + k], own.at[j], local_sem.at[j]))
    for j in range(4):
        sends[j].start()
        loads[j].start()

    def add(dst, start, count, *srcs):
        def body(i, carry):
            at = pl.ds(pl.multiple_of(start + i * step, step), step)
            total = srcs[0][at, :].astype(jnp.float32)
            for s in srcs[1:]:
                total += s[at, :].astype(jnp.float32)
            dst[at, :] = total.astype(dst.dtype)
            return carry

        lax.fori_loop(0, count // step, body, 0)

    def arrived(i, dst):
        to(i, dst, dst, col).wait_recv()

    def send(i, src, dst, c):
        copy = to(i, src, dst, c)
        copy.start()
        sends.append(copy)

    low, high = pl.ds(0, half), pl.ds(half, half)
    for j in range(4):
        loads[j].wait()
        arrived(j, twin_part.at[j])
        if j == 0:
            add(own.at[0], 0, rows, own.at[0], twin_part.at[0])
            send(4, own.at[0, low], from_far.at[low], right)
            send(5, own.at[0, high], from_far.at[high], left)
        elif j == 1:
            arrived(4, from_far.at[low])
            add(own.at[1], 0, half, own.at[1], twin_part.at[1], from_far)
            add(own.at[1], half, half, own.at[1], twin_part.at[1])
            send(6, own.at[1], from_near.at[0], right)
        elif j == 2:
            arrived(5, from_far.at[high])
            add(own.at[2], half, half, own.at[2], twin_part.at[2], from_far)
            add(own.at[2], 0, half, own.at[2], twin_part.at[2])
            send(7, own.at[2], from_near.at[1], left)
        else:
            arrived(6, from_near.at[0])
            arrived(7, from_near.at[1])
            add(out, 0, rows, own.at[3], twin_part.at[3], from_near.at[0], from_near.at[1])
    for c in sends:
        c.wait_send()


def reduce_cols(n_col, collective_id, part):
    shape = part.shape[1:]
    return pl.pallas_call(
        functools.partial(reduce_kernel, n_col),
        out_shape=jax.ShapeDtypeStruct(shape, part.dtype),
        in_specs=[ANY],
        out_specs=pl.BlockSpec(memory_space=pltpu.VMEM),
        scratch_shapes=[
            pltpu.VMEM((4,) + shape, part.dtype),
            pltpu.VMEM((4,) + shape, part.dtype),
            pltpu.VMEM(shape, part.dtype),
            pltpu.VMEM((2,) + shape, part.dtype),
            pltpu.SemaphoreType.DMA((4,)),
            pltpu.SemaphoreType.DMA((8,)),
            pltpu.SemaphoreType.DMA((8,)),
        ],
        compiler_params=comm_params(collective_id, 40 * 2**20),
        name="reduce_cols",
    )(part)


def spread_kernel(n_col, piece, out, local_sem, ssem, rsem):
    row, col = lax.axis_index("row"), lax.axis_index("col")
    barrier = pltpu.get_barrier_semaphore()
    for j in range(1, n_col):
        pl.semaphore_signal(barrier, inc=1, device_id={"row": row, "col": lax.rem(col + j, n_col)}, device_id_type=MESH)
    pl.semaphore_wait(barrier, n_col - 1)
    local = pltpu.make_async_copy(piece, out.at[col], local_sem)
    local.start()
    sends = [remote(piece, out.at[col], ssem.at[j], rsem.at[j], row=row, col=lax.rem(col + j, n_col)) for j in range(1, n_col)]
    for c in sends:
        c.start()
    for j in range(1, n_col):
        source = lax.rem(col + n_col - j, n_col)
        remote(out.at[source], out.at[source], ssem.at[j], rsem.at[j], row=row, col=col).wait_recv()
    for c in sends:
        c.wait_send()
    local.wait()


def spread_cols(n_col, collective_id, piece):
    return pl.pallas_call(
        functools.partial(spread_kernel, n_col),
        out_shape=jax.ShapeDtypeStruct((n_col,) + piece.shape, piece.dtype),
        in_specs=[ANY],
        out_specs=ANY,
        scratch_shapes=[pltpu.SemaphoreType.DMA, pltpu.SemaphoreType.DMA((n_col,)), pltpu.SemaphoreType.DMA((n_col,))],
        compiler_params=comm_params(collective_id),
        name="spread_cols",
    )(piece)


def solution(mesh):
    row_size = mesh.shape["row"]
    col_size = mesh.shape["col"]
    group = row_size * col_size
    act_spec = P("dp", None, ("row", "col"))
    weight_spec = P(None, "row", "col")

    def device_fn(x_loc, gain_loc, w_in_loc, w_kv_loc, w_out_loc):
        n_layers = w_in_loc.shape[0]
        n_batch, seq_len, d_local = x_loc.shape
        d_model = d_local * group
        e_block = w_in_loc.shape[2]
        r_block = w_out_loc.shape[1]
        f_block = e_block - r_block
        f_half = f_block // 2
        q_block = r_block - f_block
        kv_local = w_kv_loc.shape[2]
        head_dim = kv_local * col_size // 2
        heads_local = q_block // head_dim
        n_tok = n_batch * seq_len
        tok_loc = n_tok // group
        tok_row = n_tok // row_size
        seqs = n_batch // row_size
        seq_local = seq_len // group
        cos_tab, sin_tab = rope_tables(jnp.arange(seq_len), head_dim)
        causal = jnp.arange(seq_len)[None, :] <= jnp.arange(seq_len)[:, None]

        w_a, w_b, w_o = [], [], []
        for l in range(n_layers):
            gate_up = w_in_loc[l, :, q_block:]
            first = jnp.concatenate([gate_up[:, :f_half], gate_up[:, f_block : f_block + f_half], w_in_loc[l, :, :q_block], w_kv_loc[l]], axis=1)
            second = jnp.concatenate([gate_up[:, f_half:f_block], gate_up[:, f_block + f_half :]], axis=1)
            w_a.append(lax.all_gather(first, "row", axis=0, tiled=True))
            w_b.append(lax.all_gather(second, "row", axis=0, tiled=True))
            w_o.append(lax.all_gather(w_out_loc[l], "row", axis=0))

        pieces = x_loc.reshape(group, tok_loc, d_local).transpose(0, 2, 1)
        gain_rows = jnp.pad(gain_loc, ((0, 16 - n_layers), (0, tok_loc - d_local)))
        pieces = jnp.concatenate([pieces, jnp.broadcast_to(gain_rows[None], (group,) + gain_rows.shape)], axis=1)
        (got,) = exchange(row_size, col_size, 0, pieces)
        hidden = got[:, :d_local].reshape(d_model, tok_loc).T
        gain = got[:, d_local : d_local + n_layers, :d_local].transpose(1, 0, 2).reshape(n_layers, d_model)

        kv_rows = []
        for l in range(n_layers):
            hidden_f32 = hidden.astype(jnp.float32)
            centered = hidden_f32 - jnp.mean(hidden_f32, axis=-1, keepdims=True)
            variance = jnp.mean(centered * centered, axis=-1, keepdims=True)
            normed = (centered * lax.rsqrt(variance + LN_EPS) * gain[l].astype(jnp.float32)).astype(jnp.bfloat16)
            normed_row = gather_cols(col_size, 1 + 4 * l, normed).reshape(tok_row, d_model)
            proj_a = jnp.dot(normed_row, w_a[l], preferred_element_type=jnp.float32).astype(jnp.bfloat16)
            kv_piece = jnp.pad(proj_a[:, f_block + q_block :].T, ((0, 32 - kv_local), (0, 0)))
            kv_all = spread_cols(col_size, 2 + 4 * l, kv_piece)[:, :kv_local].reshape(2, head_dim, seqs, seq_len)
            proj_b = jnp.dot(normed_row, w_b[l], preferred_element_type=jnp.float32).astype(jnp.bfloat16)
            key, v_val = (a.transpose(1, 2, 0) for a in (kv_all[0], kv_all[1]))
            query = proj_a[:, f_block : f_block + q_block].reshape(seqs, seq_len, heads_local, head_dim)
            q_rot = (apply_rope(query.astype(jnp.float32), cos_tab[:, None, :], sin_tab[:, None, :]) * head_dim ** -0.5).astype(jnp.bfloat16)
            k_rot = apply_rope(key.astype(jnp.float32), cos_tab, sin_tab).astype(jnp.bfloat16)
            scores = jnp.einsum("crie,cle->cirl", q_rot, k_rot, preferred_element_type=jnp.float32)
            scores = jnp.where(causal, scores, -1e30)
            attn_prob = jax.nn.softmax(scores, axis=-1).astype(jnp.bfloat16)
            attn_out = jnp.einsum("cirl,cle->crie", attn_prob, v_val, preferred_element_type=jnp.float32).astype(jnp.bfloat16).reshape(tok_row, q_block)

            def swish_mul(gate_val, up_val):
                return (jax.nn.silu(gate_val.astype(jnp.float32)) * up_val.astype(jnp.float32)).astype(jnp.bfloat16)

            joined = jnp.concatenate(
                [attn_out, swish_mul(proj_a[:, :f_half], proj_a[:, f_half:f_block]), swish_mul(proj_b[:, :f_half], proj_b[:, f_half:])], axis=1
            )
            part_out = jnp.einsum("tk,rkn->trn", joined, w_o[l], preferred_element_type=jnp.float32).astype(jnp.bfloat16)
            update = reduce_cols(col_size, 3 + 4 * l, part_out.reshape(col_size, tok_loc, d_model))
            hidden = hidden + update
            kv_rows.append(jnp.stack([k_rot, v_val]))

        col = lax.axis_index("col")
        kv_rows = jnp.stack(kv_rows).reshape(n_layers, 2, seqs, row_size, col_size, seq_local, head_dim)
        kv_mine = lax.dynamic_index_in_dim(kv_rows, col, axis=4, keepdims=False)
        kv_send = kv_mine.transpose(3, 5, 0, 1, 2, 4).reshape(row_size, head_dim, n_layers * 2 * seqs * seq_local)
        out_pieces, kv_got = exchange(row_size, col_size, 15, hidden.T.reshape(group, d_local, tok_loc), kv_send)
        y_out = out_pieces.transpose(0, 2, 1).reshape(n_batch, seq_len, d_local)
        kv_out = kv_got.reshape(row_size, head_dim, n_layers, 2, seqs, seq_local).transpose(2, 3, 0, 4, 5, 1)
        return y_out, kv_out.reshape(n_layers, 2, n_batch, seq_local, head_dim)

    return jax.shard_map(device_fn, mesh=mesh, in_specs=(act_spec, P(None, ("row", "col")), weight_spec, weight_spec, P(None, "col", "row")), out_specs=(act_spec, P(None, None, "dp", ("row", "col"), None)), check_vma=False)
```

```python
import functools

import numpy as np

import jax
import jax.numpy as jnp
from jax import lax
from jax.experimental import pallas as pl
from jax.experimental.pallas import tpu as pltpu
from jax.sharding import PartitionSpec as P

LN_EPS = 1e-6
MESH = pl.DeviceIdType.MESH
ANY = pl.BlockSpec(memory_space=pl.ANY)
VMEM = pl.BlockSpec(memory_space=pltpu.VMEM)
F32, BF16 = jnp.float32, jnp.bfloat16
SLOTS = 6
AHEAD = 4


def dot(a, b):
    return jnp.dot(a, b, preferred_element_type=F32)


class Dims:
    pass


def kernel(
    D,
    x_t, gains, w_t, wkv_t, wo_t, cos_ref, sin_ref, perm_ref,
    y_out, kv_out, g_w, g_kv, g_wo,
    xland, gland, gcol, hid, ht, wbuf, wobuf, qt, kvland, kn, vt, kvbuf, jt, ot, twin_in, far_in, near_in,
    xs, xr, gs, gr, ys, yr, ags, agr, kvs, kvr, rss, rsr, lsem, fs, fr, fl,
):
    row, col = lax.axis_index("row"), lax.axis_index("col")
    n_row, n_col, n = D.n_row, D.n_col, D.n_row * D.n_col
    n_x = n_col // 2
    me = row * n_col + col
    x, k = col // 2, lax.rem(col, 2)
    xr_, xl_, xf_ = lax.rem(x + 1, n_x), lax.rem(x + n_x - 1, n_x), lax.rem(x + 2, n_x)
    right, left, twin = xr_ * 2 + k, xl_ * 2 + k, x * 2 + 1 - k
    up, down, across = lax.rem(row + 1, n_row), lax.rem(row + n_row - 1, n_row), lax.rem(row + 2, n_row)
    tok, dl, dr = D.tok, D.dl, D.dr
    my_lanes = pl.ds(pl.multiple_of(k * tok, 128), tok)
    twin_lanes = pl.ds(pl.multiple_of((1 - k) * tok, 128), tok)

    def remote(src, dst, ssem, rsem, r, c):
        return pltpu.make_async_remote_copy(src_ref=src, dst_ref=dst, send_sem=ssem, recv_sem=rsem, device_id={"row": r, "col": c}, device_id_type=MESH)

    barrier = pltpu.get_barrier_semaphore()

    def greet(i, carry):
        d = lax.rem(me + i, n)
        pl.semaphore_signal(barrier, inc=1, device_id={"row": d // n_col, "col": lax.rem(d, n_col)}, device_id_type=MESH)
        return carry

    lax.fori_loop(1, n, greet, 0)
    pl.semaphore_wait(barrier, n - 1)

    def piece_of(ref, d):
        return ref.at[d // 2, :, pl.ds(pl.multiple_of(lax.rem(d, 2) * tok, 128), tok)]

    def x_copy(i):
        d = lax.rem(me + i, n)
        return remote(piece_of(x_t, d), xland.at[me], xs.at[i], xr.at[i], d // n_col, lax.rem(d, n_col))

    def g_copy(i):
        d = lax.rem(me + i, n)
        return remote(gains, gland.at[me], gs.at[i], gr.at[i], d // n_col, lax.rem(d, n_col))

    def x_start(i, carry):
        x_copy(i).start()
        g_copy(i).start()
        return carry

    own_x = pltpu.make_async_copy(piece_of(x_t, me), xland.at[me], xr.at[0])
    own_g = pltpu.make_async_copy(gains, gland.at[me], gr.at[0])
    own_x.start()
    own_g.start()
    lax.fori_loop(1, n, x_start, 0)

    def own_lanes(r):
        return pl.ds(pl.multiple_of(r * dr, 128), dr)

    half_q, fch, och = D.q // 2, D.fch, D.och

    def parts(t):
        l, s = t // D.steps, t % D.steps
        out = []

        def w_rows(a, m):
            out.append((w_t.at[l, pl.ds(a, m), :], lambda r, a=a, m=m: g_w.at[l, pl.ds(a, m), own_lanes(r)]))

        if s == 0:
            w_rows(0, half_q)
            w_rows(half_q, half_q)
            for a in (0, D.kvp // 2):
                out.append((wkv_t.at[l, pl.ds(a, D.kvp // 2), :], lambda r, a=a: g_kv.at[l, pl.ds(a, D.kvp // 2), own_lanes(r)]))
        elif s <= D.n_f:
            w_rows(D.q + (s - 1) * fch, fch)
            w_rows(D.q + D.f + (s - 1) * fch, fch)
        else:
            h = och // 2
            for a in ((s - 1 - D.n_f) * och, (s - 1 - D.n_f) * och + h):
                out.append((wo_t.at[l, pl.ds(a, h), :], lambda r, a=a: g_wo.at[l, r, pl.ds(a, h), :]))
        return out

    n_steps = D.layers * D.steps
    pending = {}

    def y_copy(t, i, kind, src, dst, r):
        return remote(src, dst, ys.at[t % SLOTS, i, kind], yr.at[t % SLOTS, i, kind], r, col)

    def drain(t):
        for c in pending.pop(t, ()):
            c.wait_send()

    def issue(t):
        if t >= n_steps:
            return
        drain(t - SLOTS)
        pending[t] = []
        for i, (src, place) in enumerate(parts(t)):
            for kind, r in ((0, up), (1, down)):
                c = y_copy(t, i, kind, src, place(row), r)
                c.start()
                pending[t].append(c)

    def relay(t):
        if t >= n_steps:
            return
        for i, (src, place) in enumerate(parts(t)):
            for kind, r, to in ((0, down, up), (1, up, down)):
                y_copy(t, i, kind, src, place(r), r).wait_recv()
                if kind == i % 2:
                    c = y_copy(t, i, 2, place(r), place(r), to)
                    c.start()
                    pending[t].append(c)

    y_next = [0]

    def advance():
        t = y_next[0]
        if t >= n_steps:
            return
        for i, (src, place) in enumerate(parts(t)):
            y_copy(t, i, 2, src, place(across), across).wait_recv()
        relay(t + 1)
        issue(t + AHEAD)
        y_next[0] = t + 1

    for t in range(AHEAD):
        issue(t)

    loaded = {}

    def load(t):
        if t in loaded or t >= n_steps:
            return
        while y_next[0] <= t:
            advance()
        l, s = t // D.steps, t % D.steps
        slot = t % 2
        copies = []

        def fetch(src, dst):
            c = pltpu.make_async_copy(src, dst, lsem.at[slot, len(copies)])
            c.start()
            copies.append(c)

        def w_rows(a, m, at):
            fetch(w_t.at[l, pl.ds(a, m), :], wbuf.at[slot, pl.ds(at, m), own_lanes(row)])
            for r in (up, down, across):
                fetch(g_w.at[l, pl.ds(a, m), own_lanes(r)], wbuf.at[slot, pl.ds(at, m), own_lanes(r)])

        if s == 0:
            w_rows(0, D.q, 0)
            kv_rows = pl.ds(D.q, D.kvp)
            fetch(wkv_t.at[l], wbuf.at[slot, kv_rows, own_lanes(row)])
            for r in (up, down, across):
                fetch(g_kv.at[l, :, own_lanes(r)], wbuf.at[slot, kv_rows, own_lanes(r)])
        elif s <= D.n_f:
            w_rows(D.q + (s - 1) * fch, fch, 0)
            w_rows(D.q + D.f + (s - 1) * fch, fch, fch)
        else:
            a = (s - 1 - D.n_f) * och
            at = lambda r: pl.ds(pl.multiple_of(r * och, 128), och)
            fetch(wo_t.at[l, pl.ds(a, och), :], wobuf.at[slot, at(row), :])
            for r in (up, down, across):
                fetch(g_wo.at[l, r, pl.ds(a, och), :], wobuf.at[slot, at(r), :])
        loaded[t] = copies

    def use(t):
        load(t)
        for c in loaded[t]:
            c.wait()
        if t + 1 < n_steps and y_next[0] > t + 1:
            load(t + 1)
        return t % 2

    own_x.wait()
    own_g.wait()

    def x_finish(i, carry):
        s = lax.rem(me + n - i, n)
        remote(xland.at[s], xland.at[s], xs.at[i], xr.at[i], row, col).wait_recv()
        remote(gland.at[s], gland.at[s], gs.at[i], gr.at[i], row, col).wait_recv()
        x_copy(i).wait_send()
        g_copy(i).wait_send()
        return carry

    lax.fori_loop(1, n, x_finish, 0)

    relay(0)

    def keep(d, carry):
        hid[pl.ds(pl.multiple_of(d * dl, 16), dl), :] = xland[d]
        return carry

    lax.fori_loop(0, n, keep, 0)
    g_all = gland[...].astype(F32)
    for l in range(D.layers):
        g_rows = g_all[:, l, :]
        g_rows = jnp.concatenate([g_rows, jnp.zeros((128 - n, 128), F32)], axis=0) if n < 128 else g_rows
        g_cols = g_rows.T
        for d in range(n):
            gcol[l, d * dl : (d + 1) * dl, :] = jnp.broadcast_to(g_cols[:dl, d : d + 1], (dl, 128))

    blk = 64
    n_blk = D.d // blk

    def layer_norm(l):
        def add_up(i, acc):
            v = hid[pl.ds(pl.multiple_of(i * blk, blk), blk), :].astype(F32)
            return acc + v.reshape(blk // 8, 8, tok).sum(axis=0)

        mean = lax.fori_loop(0, n_blk, add_up, jnp.zeros((8, tok), F32)).sum(axis=0, keepdims=True) / D.d

        def add_sq(i, acc):
            v = hid[pl.ds(pl.multiple_of(i * blk, blk), blk), :].astype(F32) - mean
            return acc + (v * v).reshape(blk // 8, 8, tok).sum(axis=0)

        var = lax.fori_loop(0, n_blk, add_sq, jnp.zeros((8, tok), F32)).sum(axis=0, keepdims=True) / D.d
        scale = lax.rsqrt(var + LN_EPS)

        def write(i, carry):
            rows = pl.ds(pl.multiple_of(i * blk, blk), blk)
            g = gcol[l, rows, :]
            g = jnp.concatenate([g] * (tok // 128), axis=1)
            v = (hid[rows, :].astype(F32) - mean) * scale * g
            ht[x, rows, my_lanes] = v.astype(BF16)
            return carry

        lax.fori_loop(0, n_blk, write, 0)

    d_low, d_high = pl.ds(0, D.d // 2), pl.ds(D.d // 2, D.d // 2)
    every = slice(None)

    class Gather:
        def __init__(self):
            self.sends = []
            mine = ht.at[x, :, my_lanes]
            for i, c in ((0, right), (1, left), (2, twin)):
                self.send(i, mine, c)

        def send(self, i, ref, c):
            copy = remote(ref, ref, ags.at[i], agr.at[i], row, c)
            copy.start()
            self.sends.append(copy)

        def arrived(self, i, ref):
            remote(ref, ref, ags.at[i], agr.at[i], row, col).wait_recv()

        def pass_on(self):
            self.arrived(0, ht.at[xl_, :, my_lanes])
            self.send(3, ht.at[xl_, d_low, my_lanes], right)
            self.send(4, ht.at[xl_, :, my_lanes], twin)
            self.arrived(1, ht.at[xr_, :, my_lanes])
            self.send(5, ht.at[xr_, d_high, my_lanes], left)
            self.send(6, ht.at[xr_, :, my_lanes], twin)

        def pass_far(self):
            self.arrived(3, ht.at[xf_, d_low, my_lanes])
            self.send(7, ht.at[xf_, d_low, my_lanes], twin)
            self.arrived(5, ht.at[xf_, d_high, my_lanes])
            self.send(8, ht.at[xf_, d_high, my_lanes], twin)

        def finish(self):
            for c in self.sends:
                c.wait_send()

    cos_t, sin_t = cos_ref, sin_ref
    half = D.hd // 2

    def rope(p):
        lo, hi = p[:half], p[half:]
        return jnp.concatenate([lo * cos_t[...] - hi * sin_t[...], hi * cos_t[...] + lo * sin_t[...]], axis=0)

    def project_q(l, slot, s):
        p = dot(wbuf[slot, : D.q + D.kvp, :], ht[s]).astype(BF16).astype(F32)
        for h in range(D.heads):
            qt[s, h * D.hd : (h + 1) * D.hd, :] = (rope(p[h * D.hd : (h + 1) * D.hd]) * D.hd**-0.5).astype(BF16)
        kvland[col, s] = p[D.q :].astype(BF16)

    def kv_copies():
        return [remote(kvland.at[col], kvland.at[col], kvs.at[j], kvr.at[j], row, lax.rem(col + j, n_col)) for j in range(1, n_col)]

    def kv_arrive(copies):
        for j in range(1, n_col):
            s = lax.rem(col + n_col - j, n_col)
            remote(kvland.at[s], kvland.at[s], kvs.at[j], kvr.at[j], row, col).wait_recv()
        for c in copies:
            c.wait_send()

    def key_value(l):
        def body(s, carry):
            raw = kvland[:, s].reshape(n_col * D.kvp, D.seq)
            both = dot(perm_ref[...], raw)
            zeros = jnp.zeros((128 - D.hd, D.seq), F32)
            k_nat = jnp.concatenate([rope(both[: D.hd]), zeros], axis=0).T.astype(BF16)
            v_nat = jnp.concatenate([both[D.hd :], zeros], axis=0).T.astype(BF16)
            kn[s] = k_nat
            vt[s] = both[D.hd :].astype(BF16)
            kvbuf[l, 0, s] = k_nat
            kvbuf[l, 1, s] = v_nat
            return carry

        lax.fori_loop(0, D.seqs, body, 0)

    qb = D.seq // 2

    def attention():
        def body(i, carry):
            s, h = i // D.heads, lax.rem(i, D.heads)
            q_rows = pl.ds(pl.multiple_of(h * D.hd, 16), D.hd)
            for b in range(2):
                ext = (b + 1) * qb
                lanes = slice(b * qb, (b + 1) * qb)
                sc = dot(kn[s, :ext, : D.hd], qt[s, q_rows, lanes])
                keys = lax.broadcasted_iota(jnp.int32, (ext, qb), 0)
                queries = lax.broadcasted_iota(jnp.int32, (ext, qb), 1) + b * qb
                sc = jnp.where(keys <= queries, sc, -1e30)
                p = jnp.exp(sc - jnp.max(sc, axis=0, keepdims=True))
                p = (p * (1.0 / jnp.sum(p, axis=0, keepdims=True))).astype(BF16)
                jt[s, q_rows, lanes] = dot(vt[s, :, :ext], p).astype(BF16)
            return carry

        lax.fori_loop(0, D.seqs * D.heads, body, 0)

    def gate_up(slot, j):
        def body(s, carry):
            p = dot(wbuf[slot, : 2 * fch, :], ht[s])
            g = p[:fch].astype(BF16).astype(F32)
            u = p[fch:].astype(BF16).astype(F32)
            jt[s, pl.ds(D.q + j * fch, fch), :] = (g * jax.nn.sigmoid(g) * u).astype(BF16)
            return carry

        lax.fori_loop(0, D.seqs, body, 0)

    order = (xf_, xr_, xl_, x)
    m = D.och * n_row
    m_low, m_high = pl.ds(0, m // 2), pl.ds(m // 2, m // 2)

    def add_into(dst, start, count, *srcs):
        step = 64

        def body(i, carry):
            at = pl.ds(pl.multiple_of(start + i * step, step), step)
            total = srcs[0](at).astype(F32)
            for f in srcs[1:]:
                total += f(at).astype(F32)
            dst[at, :] = total.astype(BF16)
            return carry

        lax.fori_loop(0, count // step, body, 0)

    class Reduce:
        def __init__(self, l):
            self.l = l
            self.sends = {j: [] for j in range(D.n_o)}

        def send(self, j, i, src, dst, c):
            copy = remote(src, dst, rss.at[j, i], rsr.at[j, i], row, c)
            copy.start()
            self.sends[j].append(copy)

        def arrived(self, j, i, ref):
            remote(ref, ref, rss.at[j, i], rsr.at[j, i], row, col).wait_recv()

        def stage_a(self, j, slot):
            if j >= 2:
                for c in self.sends[j - 2][:4]:
                    c.wait_send()
                self.sends[j - 2] = self.sends[j - 2][4:]
            for i, s in enumerate(order):
                ot[j % 2, s] = dot(wobuf[slot], jt[s]).astype(BF16)
                self.send(j, i, ot.at[j % 2, s, :, twin_lanes], twin_in.at[j, i], twin)

        def stage_b(self, j):
            for i, s in enumerate(order):
                self.arrived(j, i, twin_in.at[j, i])
                add_into(twin_in.at[j, i], 0, m, lambda at: ot[j % 2, s, at, my_lanes], lambda at: twin_in[j, i, at, :])
                if i == 0:
                    self.send(j, 4, twin_in.at[j, 0, m_low], far_in.at[j, m_low], right)
                    self.send(j, 5, twin_in.at[j, 0, m_high], far_in.at[j, m_high], left)

        def stage_c(self, j):
            self.arrived(j, 4, far_in.at[j, m_low])
            add_into(twin_in.at[j, 1], 0, m // 2, lambda at: twin_in[j, 1, at, :], lambda at: far_in[j, at, :])
            self.send(j, 6, twin_in.at[j, 1], near_in.at[j, 0], right)
            self.arrived(j, 5, far_in.at[j, m_high])
            add_into(twin_in.at[j, 2], m // 2, m // 2, lambda at: twin_in[j, 2, at, :], lambda at: far_in[j, at, :])
            self.send(j, 7, twin_in.at[j, 2], near_in.at[j, 1], left)

        def stage_d(self, j):
            self.arrived(j, 6, near_in.at[j, 0])
            self.arrived(j, 7, near_in.at[j, 1])
            for r in range(n_row):
                step = min(64, och)
                for a in range(0, och, step):
                    src = slice(r * och + a, r * och + a + step)
                    dst = slice(r * dr + j * och + a, r * dr + j * och + a + step)
                    u = twin_in[j, 3, src, :].astype(F32) + near_in[j, 0, src, :].astype(F32) + near_in[j, 1, src, :].astype(F32)
                    hid[dst, :] = (hid[dst, :].astype(F32) + u.astype(BF16).astype(F32)).astype(BF16)

        def finish(self):
            for j in range(D.n_o):
                for c in self.sends[j]:
                    c.wait_send()

    for l in range(D.layers):
        t0 = l * D.steps
        layer_norm(l)
        gather = Gather()
        if l > 0:
            advance()
        gather.pass_on()
        if l > 0:
            advance()
        slot = use(t0)
        gather.arrived(2, ht.at[x, :, twin_lanes])
        project_q(l, slot, x)
        gather.arrived(4, ht.at[xl_, :, twin_lanes])
        project_q(l, slot, xl_)
        gather.arrived(6, ht.at[xr_, :, twin_lanes])
        project_q(l, slot, xr_)
        gather.pass_far()
        gather.arrived(7, ht.at[xf_, d_low, twin_lanes])
        gather.arrived(8, ht.at[xf_, d_high, twin_lanes])
        project_q(l, slot, xf_)
        copies = kv_copies()
        for c in copies:
            c.start()
        gather.finish()
        gate_up(use(t0 + 1), 0)
        kv_arrive(copies)
        key_value(l)
        attention()
        for j in range(1, D.n_f):
            gate_up(use(t0 + 1 + j), j)
        red = Reduce(l)
        for j in range(D.n_o):
            slot = use(t0 + 1 + D.n_f + j)
            red.stage_a(j, slot)
            if j >= 1:
                red.stage_c(j - 1)
            if j >= 2:
                red.stage_d(j - 2)
            red.stage_b(j)
        if l + 1 < D.layers:
            advance()
        red.stage_c(D.n_o - 1)
        red.stage_d(D.n_o - 2)
        red.stage_d(D.n_o - 1)
        red.finish()

    def y_back(i):
        d = lax.rem(me + i, n)
        return remote(hid.at[pl.ds(pl.multiple_of(d * dl, 16), dl), :], piece_of(y_out, me), xs.at[i], xr.at[i], d // n_col, lax.rem(d, n_col))

    own_y = pltpu.make_async_copy(hid.at[pl.ds(pl.multiple_of(me * dl, 16), dl), :], piece_of(y_out, me), xr.at[0])
    own_y.start()

    def y_start(i, carry):
        y_back(i).start()
        return carry

    lax.fori_loop(1, n, y_start, 0)

    def kv_back(i):
        r = lax.rem(row + i, n_row)
        pos = pl.ds(pl.multiple_of((r * n_col + col) * D.pos, 16), D.pos)
        return kvbuf.at[:, :, :, pos, :], kv_out.at[:, :, pl.ds(row * D.seqs, D.seqs)], r

    src, dst, _ = kv_back(0)
    own_kv = pltpu.make_async_copy(src, dst, fl)
    own_kv.start()
    kv_sends = []
    for i in range(1, n_row):
        src, dst, r = kv_back(i)
        c = remote(src, dst, fs.at[i], fr.at[i], r, col)
        c.start()
        kv_sends.append(c)

    def y_finish(i, carry):
        s = lax.rem(me + n - i, n)
        remote(piece_of(y_out, s), piece_of(y_out, s), xs.at[i], xr.at[i], row, col).wait_recv()
        y_back(i).wait_send()
        return carry

    lax.fori_loop(1, n, y_finish, 0)
    own_y.wait()
    own_kv.wait()
    for i in range(1, n_row):
        r = lax.rem(row + n_row - i, n_row)
        dst = kv_out.at[:, :, pl.ds(r * D.seqs, D.seqs)]
        remote(dst, dst, fs.at[i], fr.at[i], row, col).wait_recv()
    for c in kv_sends:
        c.wait_send()
    for t in sorted(pending):
        drain(t)


def solution(mesh):
    n_row, n_col = mesh.shape["row"], mesh.shape["col"]
    group = n_row * n_col
    act_spec = P("dp", None, ("row", "col"))
    weight_spec = P(None, "row", "col")

    def device_fn(x_loc, gain_loc, w_in_loc, w_kv_loc, w_out_loc):
        D = Dims()
        D.n_row, D.n_col = n_row, n_col
        n_batch, D.seq, D.dl = x_loc.shape
        D.layers, D.dr, e = w_in_loc.shape
        D.d = D.dl * group
        r_block = w_out_loc.shape[1]
        D.f = e - r_block
        D.q = r_block - D.f
        kv_local = w_kv_loc.shape[2]
        D.hd = kv_local * n_col // 2
        D.heads = D.q // D.hd
        D.kvp = 32
        D.tok = n_batch * D.seq // group
        D.seqs = n_batch // n_row
        D.pos = D.seq // group
        D.fch = min(256, D.f)
        D.n_f = D.f // D.fch
        D.och = min(128, D.dr)
        D.n_o = D.dr // D.och
        D.steps = 1 + D.n_f + D.n_o
        assert D.seq == 2 * D.tok and D.seqs == n_col // 2

        half = D.hd // 2
        inv_freq = (np.float32(1.0) / (np.float32(10000.0) ** (np.arange(half, dtype=np.float32) * np.float32(2.0) / np.float32(D.hd)))).astype(np.float32)
        angles = (inv_freq[:, None] * np.arange(D.seq, dtype=np.float32)[None, :]).astype(np.float32)
        cos_t, sin_t = np.cos(angles).astype(np.float32), np.sin(angles).astype(np.float32)
        perm = np.zeros((2 * D.hd, n_col * D.kvp), np.float32)
        for i in range(2 * D.hd):
            perm[i, (i // kv_local) * D.kvp + i % kv_local] = 1.0

        x_t = x_loc.transpose(0, 2, 1)
        w_t = w_in_loc.transpose(0, 2, 1)
        wkv_t = jnp.pad(w_kv_loc.transpose(0, 2, 1), ((0, 0), (0, D.kvp - kv_local), (0, 0)))
        wo_t = w_out_loc.transpose(0, 2, 1)
        gains = jnp.pad(gain_loc, ((0, 16 - D.layers), (0, 128 - D.dl)))

        m = D.och * n_row
        sds = jax.ShapeDtypeStruct
        dma = pltpu.SemaphoreType.DMA
        out = pl.pallas_call(
            functools.partial(kernel, D),
            out_shape=(
                sds(x_t.shape, BF16),
                sds((D.layers, 2, n_batch, D.pos, 128), BF16),
                sds((D.layers, e, D.d), BF16),
                sds((D.layers, D.kvp, D.d), BF16),
                sds((D.layers, n_row, D.dr, r_block), BF16),
            ),
            in_specs=[ANY] * 5 + [VMEM] * 3,
            out_specs=(ANY,) * 5,
            scratch_shapes=[
                pltpu.VMEM((group, D.dl, D.tok), BF16),
                pltpu.VMEM((group, 16, 128), BF16),
                pltpu.VMEM((D.layers, D.d, 128), F32),
                pltpu.VMEM((D.d, D.tok), BF16),
                pltpu.VMEM((D.seqs, D.d, D.seq), BF16),
                pltpu.VMEM((2, max(2 * D.fch, D.q + D.kvp), D.d), BF16),
                pltpu.VMEM((2, m, r_block), BF16),
                pltpu.VMEM((D.seqs, D.q, D.seq), BF16),
                pltpu.VMEM((n_col, D.seqs, D.kvp, D.seq), BF16),
                pltpu.VMEM((D.seqs, D.seq, 128), BF16),
                pltpu.VMEM((D.seqs, D.hd, D.seq), BF16),
                pltpu.VMEM((D.layers, 2, D.seqs, D.seq, 128), BF16),
                pltpu.VMEM((D.seqs, r_block, D.seq), BF16),
                pltpu.VMEM((2, D.seqs, m, D.seq), BF16),
                pltpu.VMEM((D.n_o, 4, m, D.tok), BF16),
                pltpu.VMEM((D.n_o, m, D.tok), BF16),
                pltpu.VMEM((D.n_o, 2, m, D.tok), BF16),
                dma((group,)), dma((group,)), dma((group,)), dma((group,)),
                dma((SLOTS, 4, 3)), dma((SLOTS, 4, 3)),
                dma((9,)), dma((9,)),
                dma((n_col,)), dma((n_col,)),
                dma((D.n_o, 8)), dma((D.n_o, 8)),
                dma((2, 8)),
                dma((n_row,)), dma((n_row,)), dma,
            ],
            compiler_params=pltpu.CompilerParams(collective_id=0, has_side_effects=True, vmem_limit_bytes=67_000_000),
            name="two_layers",
        )(x_t, gains, w_t, wkv_t, wo_t, jnp.asarray(cos_t), jnp.asarray(sin_t), jnp.asarray(perm, BF16))
        return out[0].transpose(0, 2, 1), out[1][..., : D.hd]

    return jax.shard_map(device_fn, mesh=mesh, in_specs=(act_spec, P(None, ("row", "col")), weight_spec, weight_spec, P(None, "col", "row")), out_specs=(act_spec, P(None, None, "dp", ("row", "col"), None)), check_vma=False)
```

```python
import functools

import numpy as np

import jax
import jax.numpy as jnp
from jax import lax
from jax.experimental import pallas as pl
from jax.experimental.pallas import tpu as pltpu
from jax.sharding import PartitionSpec as P

LN_EPS = 1e-6
MESH = pl.DeviceIdType.MESH
ANY = pl.BlockSpec(memory_space=pl.ANY)
VMEM = pl.BlockSpec(memory_space=pltpu.VMEM)
F32, BF16 = jnp.float32, jnp.bfloat16
SLOTS = 6
AHEAD = 3
RELAY = 1


def dot(a, b):
    return jnp.dot(a, b, preferred_element_type=F32)


class Dims:
    pass


def rows_at(start, count, by=16):
    return pl.ds(start if isinstance(start, int) else pl.multiple_of(start, by), count)


def kernel(
    D,
    x_t, gains, w_t, wkv_t, w_o, cos_ref, sin_ref, perm_ref,
    y_out, kv_out, g_w, g_kv, g_wo, g_h,
    xland, gland, gcol, hid, ht, wbuf, wonat, wobuf, qt, kvland, kn, vt, kvbuf, jt, ot, twin_in, far_in, near_in, psum, pair_in,
    xs, xr, gs, gr, ys, yr, ags, agr, ps, pr_, kvs, kvr, rss, rsr, es, er, lw, lo, lh, fs, fr, fl,
):
    sc = jax.named_scope
    row, col = lax.axis_index("row"), lax.axis_index("col")
    n_row, n_col, n = D.n_row, D.n_col, D.n_row * D.n_col
    n_x = n_col // 2
    me = row * n_col + col
    x, k = col // 2, lax.rem(col, 2)
    xr_, xl_, xf_ = lax.rem(x + 1, n_x), lax.rem(x + n_x - 1, n_x), lax.rem(x + 2, n_x)
    right, left, twin = xr_ * 2 + k, xl_ * 2 + k, x * 2 + 1 - k
    up, down, across = lax.rem(row + 1, n_row), lax.rem(row + n_row - 1, n_row), lax.rem(row + 2, n_row)
    half, mate = row // 2, n_row - 1 - row
    peer = row + 1 - 2 * lax.rem(row, 2)
    tok, dl, dr = D.tok, D.dl, D.dr
    och, fch = D.och, D.fch
    my_lanes = pl.ds(pl.multiple_of(k * tok, 128), tok)
    twin_lanes = pl.ds(pl.multiple_of((1 - k) * tok, 128), tok)

    def remote(src, dst, ssem, rsem, r, c):
        return pltpu.make_async_remote_copy(src_ref=src, dst_ref=dst, send_sem=ssem, recv_sem=rsem, device_id={"row": r, "col": c}, device_id_type=MESH)

    def loop(lo_, hi_, f):
        def body(i, carry):
            f(i)
            return carry

        lax.fori_loop(lo_, hi_, body, 0)

    barrier = pltpu.get_barrier_semaphore()

    def greet(i):
        d = lax.rem(me + i, n)
        pl.semaphore_signal(barrier, inc=1, device_id={"row": d // n_col, "col": lax.rem(d, n_col)}, device_id_type=MESH)

    with sc("barrier"):
        loop(1, n, greet)
        pl.semaphore_wait(barrier, n - 1)

    def piece_of(ref, d):
        return ref.at[d // 2, :, pl.ds(pl.multiple_of(lax.rem(d, 2) * tok, 128), tok)]

    def x_copy(i):
        d = lax.rem(me + i, n)
        return remote(piece_of(x_t, d), xland.at[me], xs.at[i], xr.at[i], d // n_col, lax.rem(d, n_col))

    def g_copy(i):
        d = lax.rem(me + i, n)
        return remote(gains, gland.at[me], gs.at[i], gr.at[i], d // n_col, lax.rem(d, n_col))

    def x_start(i):
        x_copy(i).start()
        g_copy(i).start()

    own_x = pltpu.make_async_copy(piece_of(x_t, me), xland.at[me], xr.at[0])
    own_g = pltpu.make_async_copy(gains, gland.at[me], gr.at[0])
    own_x.start()
    own_g.start()
    loop(1, n, x_start)

    def own_lanes(r):
        return pl.ds(pl.multiple_of(r * dr, 128), dr)

    steps = []
    for l, C in enumerate(D.cfg):
        steps += [(l, "q", 0)] + [(l, "f", j) for j in range(C.n_f)] + [(l, "o", j) for j in range(D.n_o)]
    n_steps = len(steps)
    step_of = {s: t for t, s in enumerate(steps)}

    def blocks(t, i):
        l, kind, j = steps[t]
        C = D.cfg[l]
        out = []

        def w_rows(a, m):
            at = rows_at(a, m)
            out.append((w_t.at[l, at, :], lambda r: g_w.at[l, at, own_lanes(r)]))

        def o_rows(a, m):
            at, lanes = rows_at(a, m), pl.ds(j * och, och)
            out.append((w_o.at[l, at, lanes], lambda r: g_wo.at[l, r, at, lanes]))

        def kv_rows(a, m):
            at = pl.ds(a, m)
            out.append((wkv_t.at[l, at, :], lambda r: g_kv.at[l, at, own_lanes(r)]))

        if kind == "q":
            for a in (0, C.q // 2):
                w_rows(i * C.q + a, C.q // 2)
            for a in (0, D.kvp // 2):
                kv_rows(a, D.kvp // 2)
        elif kind == "f":
            w_rows(D.q + i * C.f + j * fch, fch)
            w_rows(D.q + D.f + i * C.f + j * fch, fch)
        elif C.split:
            o_rows(i * C.q, C.q)
            o_rows(D.q + i * C.f, C.f)
        else:
            for a in (0, (D.q + D.f) // 2):
                o_rows(a, (D.q + D.f) // 2)
        return out

    pending = {}

    def y_copy(t, i, kind, src, dst, r):
        return remote(src, dst, ys.at[t % SLOTS, i, kind], yr.at[t % SLOTS, i, kind], r, col)

    def drain(t):
        for c in pending.pop(t, ()):
            c.wait_send()

    def y_send(t, *args):
        c = y_copy(t, *args)
        c.start()
        pending[t].append(c)

    def issue(t):
        if t >= n_steps:
            return
        drain(t - SLOTS)
        pending[t] = []
        if D.cfg[steps[t][0]].split:
            for i, (src, place) in enumerate(blocks(t, 1 - half)):
                y_send(t, i, 1, src, place(row), mate)
            for i, (src, place) in enumerate(blocks(t, half)):
                y_send(t, i, 0, src, place(row), peer)
        else:
            for i, (src, place) in enumerate(blocks(t, 0)):
                y_send(t, i, 0, src, place(row), up)
                y_send(t, i, 1, src, place(row), down)

    def relay(t):
        if t >= n_steps:
            return
        if D.cfg[steps[t][0]].split:
            for i, (src, place) in enumerate(blocks(t, half)):
                y_copy(t, i, 1, src, place(mate), mate).wait_recv()
                y_send(t, i, 2, place(mate), place(mate), peer)
        else:
            for i, (src, place) in enumerate(blocks(t, 0)):
                for kind, r, to in ((0, down, up), (1, up, down)):
                    y_copy(t, i, kind, src, place(r), r).wait_recv()
                    if kind == i % 2:
                        y_send(t, i, 2, place(r), place(r), to)

    y_next = [0]

    def advance():
        t = y_next[0]
        if t >= n_steps:
            return
        with sc(f"adv{t}"):
            if D.cfg[steps[t][0]].split:
                rest = n_row - 1 - peer
                for i, (src, place) in enumerate(blocks(t, half)):
                    y_copy(t, i, 0, src, place(peer), peer).wait_recv()
                    y_copy(t, i, 2, src, place(rest), rest).wait_recv()
            else:
                for i, (src, place) in enumerate(blocks(t, 0)):
                    y_copy(t, i, 2, src, place(across), across).wait_recv()
            relay(t + RELAY)
            issue(t + AHEAD)
        y_next[0] = t + 1

    def have(*step):
        while y_next[0] <= step_of[step]:
            advance()

    for t in range(AHEAD):
        issue(t)

    def w_fetch(l, kind, j, slot):
        C = D.cfg[l]
        i = half if C.split else 0
        copies = []

        def fetch(src, dst):
            copies.append(pltpu.make_async_copy(src, dst, lw.at[slot, len(copies)]))

        def w_rows(a, m, at):
            a, at = rows_at(a, m), pl.ds(at, m)
            fetch(w_t.at[l, a, :], wbuf.at[slot, at, own_lanes(row)])
            for r in (up, down, across):
                fetch(g_w.at[l, a, own_lanes(r)], wbuf.at[slot, at, own_lanes(r)])

        if kind == "q":
            w_rows(i * C.q, C.q, 0)
            at = pl.ds(C.q, D.kvp)
            fetch(wkv_t.at[l], wbuf.at[slot, at, own_lanes(row)])
            for r in (up, down, across):
                fetch(g_kv.at[l, :, own_lanes(r)], wbuf.at[slot, at, own_lanes(r)])
        else:
            w_rows(D.q + i * C.f + j * fch, fch, 0)
            w_rows(D.q + D.f + i * C.f + j * fch, fch, fch)
        return copies

    def o_fetch(l, j, slot):
        C = D.cfg[l]
        copies = []

        def fetch(src, dst):
            copies.append(pltpu.make_async_copy(src, dst, lo.at[slot, len(copies)]))

        lanes = pl.ds(j * och, och)
        spans = ((half * C.q, 0, C.q), (D.q + half * C.f, C.q, C.f)) if C.split else ((0, 0, C.q + C.f),)
        for a, at, m in spans:
            a, at = rows_at(a, m), pl.ds(at, m)
            to = lambda r: pl.ds(pl.multiple_of(r * och, 128), och)
            fetch(w_o.at[l, a, lanes], wonat.at[slot, at, to(row)])
            for r in (up, down, across):
                fetch(g_wo.at[l, r, a, lanes], wonat.at[slot, at, to(r)])
        return copies

    def start(copies):
        for c in copies:
            c.start()

    def wait(copies):
        for c in copies:
            c.wait()

    own_x.wait()
    own_g.wait()

    def x_finish(i):
        s = lax.rem(me + n - i, n)
        remote(xland.at[s], xland.at[s], xs.at[i], xr.at[i], row, col).wait_recv()
        remote(gland.at[s], gland.at[s], gs.at[i], gr.at[i], row, col).wait_recv()
        x_copy(i).wait_send()
        g_copy(i).wait_send()

    with sc("xwait"):
        loop(1, n, x_finish)

    def keep(d):
        hid[rows_at(d * dl, dl), :] = xland[d]

    with sc("gains"):
        loop(0, n, keep)
        g_all = gland[...].astype(F32)
        for l in range(D.layers):
            g_rows = g_all[:, l, :]
            g_rows = jnp.concatenate([g_rows, jnp.zeros((128 - n, 128), F32)], axis=0) if n < 128 else g_rows
            g_cols = g_rows.T
            for d in range(n):
                gcol[l, d * dl : (d + 1) * dl, :] = jnp.broadcast_to(g_cols[:dl, d : d + 1], (dl, 128))

    blk = 64
    n_blk = D.d // blk

    def layer_norm(l):
        def add_up(i, acc):
            v = hid[rows_at(i * blk, blk), :].astype(F32)
            return acc + v.reshape(blk // 8, 8, tok).sum(axis=0)

        mean = lax.fori_loop(0, n_blk, add_up, jnp.zeros((8, tok), F32)).sum(axis=0, keepdims=True) / D.d

        def add_sq(i, acc):
            v = hid[rows_at(i * blk, blk), :].astype(F32) - mean
            return acc + (v * v).reshape(blk // 8, 8, tok).sum(axis=0)

        var = lax.fori_loop(0, n_blk, add_sq, jnp.zeros((8, tok), F32)).sum(axis=0, keepdims=True) / D.d
        scale = lax.rsqrt(var + LN_EPS)

        def write(i):
            rows = rows_at(i * blk, blk)
            g = gcol[l, rows, :]
            g = jnp.concatenate([g] * (tok // 128), axis=1)
            v = (hid[rows, :].astype(F32) - mean) * scale * g
            ht[x, rows, my_lanes] = v.astype(BF16)

        with sc(f"norm{l}"):
            loop(0, n_blk, write)

    d_low, d_high = pl.ds(0, D.d // 2), pl.ds(D.d // 2, D.d // 2)

    class Gather:
        def __init__(self, buf, a):
            self.buf, self.a, self.sends = buf, a, []
            mine = buf.at[x, :, my_lanes]
            for i, c in ((0, right), (1, left), (2, twin)):
                self.send(i, mine, c)

        def send(self, i, ref, c):
            copy = remote(ref, ref, ags.at[self.a, i], agr.at[self.a, i], row, c)
            copy.start()
            self.sends.append(copy)

        def arrived(self, i, ref):
            remote(ref, ref, ags.at[self.a, i], agr.at[self.a, i], row, col).wait_recv()

        def pass_on(self):
            b = self.buf
            with sc(f"pass_on{self.a}"):
                self.arrived(0, b.at[xl_, :, my_lanes])
                self.send(3, b.at[xl_, d_low, my_lanes], right)
                self.send(4, b.at[xl_, :, my_lanes], twin)
                self.arrived(1, b.at[xr_, :, my_lanes])
                self.send(5, b.at[xr_, d_high, my_lanes], left)
                self.send(6, b.at[xr_, :, my_lanes], twin)

        def near(self):
            b = self.buf
            with sc(f"near{self.a}"):
                self.arrived(2, b.at[x, :, twin_lanes])
                self.arrived(4, b.at[xl_, :, twin_lanes])
                self.arrived(6, b.at[xr_, :, twin_lanes])

        def pass_far(self):
            b = self.buf
            with sc(f"pass_far{self.a}"):
                self.arrived(3, b.at[xf_, d_low, my_lanes])
                self.send(7, b.at[xf_, d_low, my_lanes], twin)
                self.arrived(5, b.at[xf_, d_high, my_lanes])
                self.send(8, b.at[xf_, d_high, my_lanes], twin)

        def far(self):
            b = self.buf
            with sc(f"far{self.a}"):
                self.arrived(7, b.at[xf_, d_low, twin_lanes])
                self.arrived(8, b.at[xf_, d_high, twin_lanes])

        def finish(self):
            for c in self.sends:
                c.wait_send()

    half_dim = D.hd // 2

    def near3(i):
        return lax.rem(x + i + i // 2, n_x)

    def all4(i):
        return i

    def far1(i):
        return xf_

    def rope(p):
        lo_, hi_ = p[:half_dim], p[half_dim:]
        return jnp.concatenate([lo_ * cos_ref[...] - hi_ * sin_ref[...], hi_ * cos_ref[...] + lo_ * sin_ref[...]], axis=0)

    def project_q(l, a, seq_of, count):
        C = D.cfg[l]

        def body(i):
            s = seq_of(i)
            p = dot(wbuf[1, : C.q + D.kvp, :], ht[s]).astype(BF16).astype(F32)
            for h in range(C.heads):
                at = rows_at((a * D.seqs + s) * C.q + h * D.hd, D.hd)
                qt[at, :] = (rope(p[h * D.hd : (h + 1) * D.hd]) * D.hd**-0.5).astype(BF16)
            kvland[col, a * D.seqs + s] = p[C.q :].astype(BF16)

        with sc(f"q{l}{a}"):
            loop(0, count, body)

    def kv_send(a):
        own = kvland.at[col, pl.ds(a * D.seqs, D.seqs)]
        copies = [remote(own, own, kvs.at[a, j], kvr.at[a, j], row, lax.rem(col + j, n_col)) for j in range(1, n_col)]
        start(copies)
        return copies

    def kv_arrive(a, copies):
        with sc(f"kvwait{a}"):
            for j in range(1, n_col):
                s = lax.rem(col + n_col - j, n_col)
                ref = kvland.at[s, pl.ds(a * D.seqs, D.seqs)]
                remote(ref, ref, kvs.at[a, j], kvr.at[a, j], row, col).wait_recv()
            for c in copies:
                c.wait_send()

    def key_value(l, a):
        def body(i):
            s = a * D.seqs + i
            raw = kvland[:, s].reshape(n_col * D.kvp, D.seq)
            both = dot(perm_ref[...], raw)
            zeros = jnp.zeros((128 - D.hd, D.seq), F32)
            k_nat = jnp.concatenate([rope(both[: D.hd]), zeros], axis=0).T.astype(BF16)
            kn[s] = k_nat
            vt[s] = both[D.hd :].astype(BF16)
            if a == 0:
                kvbuf[l, 0, i] = k_nat
                kvbuf[l, 1, i] = jnp.concatenate([both[D.hd :], zeros], axis=0).T.astype(BF16)

        with sc(f"kv{l}{a}"):
            loop(0, D.seqs, body)

    qb = D.seq // 2

    def attention(l, a):
        C = D.cfg[l]

        def body(i):
            s, h = a * D.seqs + i // C.heads, lax.rem(i, C.heads)
            q_rows = rows_at(s * C.q + h * D.hd, D.hd)
            o_rows = rows_at(s * (C.q + C.f) + h * D.hd, D.hd)
            for b in range(2):
                ext = (b + 1) * qb
                lanes = slice(b * qb, (b + 1) * qb)
                score = dot(kn[s, :ext, : D.hd], qt[q_rows, lanes])
                keys = lax.broadcasted_iota(jnp.int32, (ext, qb), 0)
                queries = lax.broadcasted_iota(jnp.int32, (ext, qb), 1) + b * qb
                score = jnp.where(keys <= queries, score, -1e30)
                p = jnp.exp(score - jnp.max(score, axis=0, keepdims=True))
                p = (p * (1.0 / jnp.sum(p, axis=0, keepdims=True))).astype(BF16)
                jt[o_rows, lanes] = dot(vt[s, :, :ext], p).astype(BF16)

        with sc(f"attn{l}{a}"):
            loop(0, D.seqs * C.heads, body)

    def gate_up(l, a, slot, j, seq_of, count):
        C = D.cfg[l]

        def body(i):
            s = seq_of(i)
            p = dot(wbuf[slot, : 2 * fch, :], ht[s])
            g = p[:fch].astype(BF16).astype(F32)
            u = p[fch:].astype(BF16).astype(F32)
            jt[rows_at((a * D.seqs + s) * (C.q + C.f) + C.q + j * fch, fch), :] = (g * jax.nn.sigmoid(g) * u).astype(BF16)

        loop(0, count, body)

    def gate_up_loop(l, a, seq_of, count, first, last):
        C = D.cfg[l]
        have(l, "f", min(last, C.n_f - 1))

        def body(j):
            slot = lax.rem(j, 2)
            wait(w_fetch(l, "f", j, slot))

            @pl.when(j + 1 < C.n_f)
            def _():
                start(w_fetch(l, "f", j + 1, 1 - slot))

            gate_up(l, a, slot, j, seq_of, count)

        with sc(f"gu{l}{a}"):
            loop(first, last, body)

    def load_q(l):
        have(l, "q", 0)
        copies = w_fetch(l, "q", 0, 1)
        start(copies)
        wait(copies)

    m = och * n_row
    m_low, m_high = pl.ds(0, m // 2), pl.ds(m // 2, m // 2)
    r_slots = twin_in.shape[0]
    r_step = 64

    def order(i):
        return lax.rem(x + lax.rem(2 + 3 * i, 4), n_x)

    class Reduce:
        def __init__(self, l):
            self.l, self.C, self.sends = l, D.cfg[l], {}

        def send(self, u, i, src, dst, c):
            copy = remote(src, dst, rss.at[u % r_slots, i], rsr.at[u % r_slots, i], row, c)
            copy.start()
            self.sends[u].append(copy)

        def arrived(self, u, i, ref):
            remote(ref, ref, rss.at[u % r_slots, i], rsr.at[u % r_slots, i], row, col).wait_recv()

        def twin_copy(self, u, i):
            us = u % r_slots
            return remote(ot.at[u % 2, order(i), :, twin_lanes], twin_in.at[us, i], rss.at[us, i], rsr.at[us, i], row, twin)

        def twin_done(self, u):
            loop(0, 4, lambda i: self.twin_copy(u, i).wait_send())

        def stage_a(self, u, a):
            C = self.C
            if u >= 2:
                self.twin_done(u - 2)
            if u >= r_slots - 1:
                for c in self.sends.pop(u - r_slots + 1):
                    c.wait_send()
            self.sends[u] = []
            R = C.q + C.f

            def body(i):
                s = order(i)
                ot[u % 2, s] = dot(wobuf[:, :R], jt[rows_at((a * D.seqs + s) * R, R), :]).astype(BF16)
                self.twin_copy(u, i).start()

            with sc(f"sa{self.l}_{u}"):
                loop(0, 4, body)

        def stage_b(self, u):
            us = u % r_slots

            def body(i):
                self.arrived(u, i, twin_in.at[us, i])
                s = order(i)

                def add(b):
                    at = rows_at(b * r_step, r_step)
                    twin_in[us, i, at, :] = (ot[u % 2, s, at, my_lanes].astype(F32) + twin_in[us, i, at, :].astype(F32)).astype(BF16)

                loop(0, m // r_step, add)

            with sc(f"sb{self.l}_{u}"):
                loop(0, 1, body)
                self.send(u, 4, twin_in.at[us, 0, m_low], far_in.at[us, m_low], right)
                self.send(u, 5, twin_in.at[us, 0, m_high], far_in.at[us, m_high], left)
                loop(1, 4, body)

        def stage_c(self, u):
            us = u % r_slots

            def add_far(i, base):
                def add(b):
                    at = rows_at(base + b * r_step, r_step)
                    twin_in[us, i, at, :] = (twin_in[us, i, at, :].astype(F32) + far_in[us, at, :].astype(F32)).astype(BF16)

                loop(0, m // 2 // r_step, add)

            with sc(f"sc{self.l}_{u}"):
                self.arrived(u, 4, far_in.at[us, m_low])
                add_far(1, 0)
                self.send(u, 6, twin_in.at[us, 1], near_in.at[us, 0], right)
                self.arrived(u, 5, far_in.at[us, m_high])
                add_far(3, m // 2)
                self.send(u, 7, twin_in.at[us, 3], near_in.at[us, 1], left)

        def add_update(self, j, total):
            step = min(r_step, och)
            for r in range(n_row):

                def add(b, r=r):
                    dst = rows_at(r * dr + j * och + b * step, step)
                    u = total(rows_at(r * och + b * step, step)).astype(BF16).astype(F32)
                    hid[dst, :] = (hid[dst, :].astype(F32) + u).astype(BF16)

                loop(0, och // step, add)

        def stage_d(self, u, j, a):
            us = u % r_slots

            def total(at):
                return twin_in[us, 2, at, :].astype(F32) + near_in[us, 0, at, :].astype(F32) + near_in[us, 1, at, :].astype(F32)

            with sc(f"sd{self.l}_{u}"):
                self.arrived(u, 6, near_in.at[us, 0])
                self.arrived(u, 7, near_in.at[us, 1])
                if self.C.split:

                    def save(b):
                        at = rows_at(b * r_step, r_step)
                        psum[a, j, at, :] = total(at).astype(BF16)

                    loop(0, m // r_step, save)
                    if a == 1:
                        remote(psum.at[1, j], pair_in.at[j], es.at[j], er.at[j], mate, col).start()
                else:
                    self.add_update(j, total)

        def stage_e(self, j):
            with sc(f"se{self.l}_{j}"):
                c = remote(psum.at[1, j], pair_in.at[j], es.at[j], er.at[j], mate, col)
                c.wait_recv()
                self.add_update(j, lambda at: psum[0, j, at, :].astype(F32) + pair_in[j, at, :].astype(F32))
                c.wait_send()

        def finish(self, units):
            with sc(f"rfin{self.l}"):
                for u in range(max(0, units - 2), units):
                    self.twin_done(u)
                for u in self.sends:
                    for c in self.sends[u]:
                        c.wait_send()

    o_started = set()

    def o_load(l, j):
        if (l, j) not in o_started:
            have(l, "o", j)
            start(o_fetch(l, j, j % 2))
            o_started.add((l, j))

    def o_use(l, j):
        C = D.cfg[l]
        with sc(f"ouse{l}_{j}"):
            o_load(l, j)
            wait(o_fetch(l, j, j % 2))
            if j + 1 < D.n_o and y_next[0] > step_of[(l, "o", j + 1)]:
                o_load(l, j + 1)
            R = C.q + C.f
            for r in range(n_row):
                wobuf[r * och : (r + 1) * och, :R] = wonat[j % 2, :R, r * och : (r + 1) * och].T

    layer_norm(0)
    g0 = Gather(ht, 0)
    mine = ht.at[x, :, my_lanes]
    shared = g_h.at[x, :, my_lanes]
    to_mate = remote(mine, shared, ps, pr_, mate, col)
    to_mate.start()
    with sc("relay0"):
        for t in range(RELAY):
            relay(t)
    advance()
    advance()
    g0.pass_on()
    with sc("mate"):
        to_mate.wait_recv()
    g1 = Gather(g_h, 1)
    load_q(0)
    g0.near()
    project_q(0, 0, near3, 3)
    g0.pass_far()
    g0.far()
    project_q(0, 0, far1, 1)
    sent = kv_send(0)
    n_f = D.cfg[0].n_f
    for j in range(n_f):
        have(0, "f", j)
        copies = w_fetch(0, "f", j, j % 2)
        with sc(f"gu0_{j}"):
            start(copies)
            wait(copies)
            gate_up(0, 0, j % 2, j, all4, 4)
        if j == 0:
            kv_arrive(0, sent)
            key_value(0, 0)
            attention(0, 0)
        if j == n_f // 2:
            g1.pass_on()
    g0.finish()
    to_mate.wait_send()
    g1.near()

    def h_copy(i):
        return pltpu.make_async_copy(g_h.at[i], ht.at[i], lh.at[i])

    loop(0, 3, lambda i: h_copy(near3(i)).start())
    load_q(0)
    loop(0, 3, lambda i: h_copy(near3(i)).wait())
    project_q(0, 1, near3, 3)
    g1.pass_far()
    g1.far()
    h_copy(xf_).start()
    start(w_fetch(0, "f", 0, 0))
    h_copy(xf_).wait()
    project_q(0, 1, far1, 1)
    sent = kv_send(1)
    gate_up_loop(0, 1, all4, 4, 0, n_f)
    have(0, "o", 0)
    g1.finish()
    kv_arrive(1, sent)
    key_value(0, 1)
    attention(0, 1)

    red = Reduce(0)
    units = [(j, a) for j in range(D.n_o) for a in (1, 0)]
    done_e = 0
    for u, (j, a) in enumerate(units):
        if a == 1:
            o_use(0, j)
        red.stage_a(u, a)
        if u >= 1:
            red.stage_c(u - 1)
        if u >= 2:
            red.stage_d(u - 2, *units[u - 2])
        red.stage_b(u)
        if u >= 5 and u % 2 == 1:
            red.stage_e(done_e)
            done_e += 1
        if u >= 1 and u % 3 != 0:
            advance()
    n_u = len(units)
    red.stage_c(n_u - 1)
    red.stage_d(n_u - 2, *units[n_u - 2])
    advance()
    red.stage_d(n_u - 1, *units[n_u - 1])
    for j in range(done_e, D.n_o):
        red.stage_e(j)
    red.finish(n_u)

    def y_copy_back(i):
        d = lax.rem(me + i, n)
        return remote(hid.at[rows_at(d * dl, dl), :], piece_of(y_out, me), xs.at[i], xr.at[i], d // n_col, lax.rem(d, n_col))

    own_y = pltpu.make_async_copy(hid.at[rows_at(me * dl, dl), :], piece_of(y_out, me), xr.at[0])

    def y_send_back(c):
        def body(r):
            i = lax.rem(r * n_col + c - me + n, n)

            @pl.when(i == 0)
            def _():
                own_y.start()

            @pl.when(i != 0)
            def _():
                y_copy_back(i).start()

        loop(0, n_row, body)

    for l in range(1, D.layers):
        C = D.cfg[l]
        layer_norm(l)
        g0 = Gather(ht, 0)
        for _ in range(3):
            advance()
        g0.pass_on()
        load_q(l)
        have(l, "f", 0)
        start(w_fetch(l, "f", 0, 0))
        g0.near()
        project_q(l, 0, near3, 3)
        n_mid = C.n_f // 2
        gate_up_loop(l, 0, near3, 3, 0, n_mid)
        g0.pass_far()
        gate_up_loop(l, 0, near3, 3, n_mid, C.n_f)
        advance()
        load_q(l)
        start(w_fetch(l, "f", 0, 0))
        g0.far()
        project_q(l, 0, far1, 1)
        sent = kv_send(0)
        gate_up_loop(l, 0, far1, 1, 0, C.n_f)
        advance()
        g0.finish()
        kv_arrive(0, sent)
        key_value(l, 0)
        attention(l, 0)
        red = Reduce(l)
        last = l + 1 == D.layers
        for j in range(D.n_o):
            o_use(l, j)
            red.stage_a(j, 0)
            if j >= 1:
                red.stage_c(j - 1)
            if j >= 2:
                red.stage_d(j - 2, j - 2, 0)
            red.stage_b(j)
        red.stage_c(D.n_o - 1)
        for j in (D.n_o - 2, D.n_o - 1):
            red.stage_d(j, j, 0)
            if last:
                for c in range(n_col):
                    lo_c, hi_c = c * dl, (c + 1) * dl
                    before = j * och if j == D.n_o - 1 else 0
                    if before < hi_c <= (j + 1) * och:
                        y_send_back(c)
        red.finish(D.n_o)

    def kv_back(i):
        r = lax.rem(row + i, n_row)
        pos = rows_at((r * n_col + col) * D.pos, D.pos)
        return kvbuf.at[:, :, :, pos, :], kv_out.at[:, :, pl.ds(row * D.seqs, D.seqs)], r

    src, dst, _ = kv_back(0)
    own_kv = pltpu.make_async_copy(src, dst, fl)
    own_kv.start()
    kv_sends = []
    for i in range(1, n_row):
        src, dst, r = kv_back(i)
        c = remote(src, dst, fs.at[i], fr.at[i], r, col)
        c.start()
        kv_sends.append(c)

    def y_finish(i):
        s = lax.rem(me + n - i, n)
        remote(piece_of(y_out, s), piece_of(y_out, s), xs.at[i], xr.at[i], row, col).wait_recv()
        y_copy_back(i).wait_send()

    with sc("ywait"):
        loop(1, n, y_finish)
        own_y.wait()
        own_kv.wait()
        for i in range(1, n_row):
            r = lax.rem(row + n_row - i, n_row)
            dst = kv_out.at[:, :, pl.ds(r * D.seqs, D.seqs)]
            remote(dst, dst, fs.at[i], fr.at[i], row, col).wait_recv()
        for c in kv_sends:
            c.wait_send()
        for t in sorted(pending):
            drain(t)


def solution(mesh):
    n_row, n_col = mesh.shape["row"], mesh.shape["col"]
    group = n_row * n_col
    act_spec = P("dp", None, ("row", "col"))
    weight_spec = P(None, "row", "col")

    def device_fn(x_loc, gain_loc, w_in_loc, w_kv_loc, w_out_loc):
        D = Dims()
        D.n_row, D.n_col = n_row, n_col
        n_batch, D.seq, D.dl = x_loc.shape
        D.layers, D.dr, e = w_in_loc.shape
        D.d = D.dl * group
        r_block = w_out_loc.shape[1]
        D.f = e - r_block
        D.q = r_block - D.f
        kv_local = w_kv_loc.shape[2]
        D.hd = kv_local * n_col // 2
        D.kvp = 32
        D.tok = n_batch * D.seq // group
        D.seqs = n_batch // n_row
        D.pos = D.seq // group
        D.fch = 128
        D.och = 128
        D.n_o = D.dr // D.och
        D.cfg = []
        for l in range(D.layers):
            C = Dims()
            C.split = l == 0
            parts = 2 if C.split else 1
            C.q, C.f = D.q // parts, D.f // parts
            C.heads, C.n_f = C.q // D.hd, C.f // D.fch
            D.cfg.append(C)
        assert D.seq == 2 * D.tok and D.seqs == n_col // 2 == n_row == 4

        half = D.hd // 2
        inv_freq = (np.float32(1.0) / (np.float32(10000.0) ** (np.arange(half, dtype=np.float32) * np.float32(2.0) / np.float32(D.hd)))).astype(np.float32)
        angles = (inv_freq[:, None] * np.arange(D.seq, dtype=np.float32)[None, :]).astype(np.float32)
        cos_t, sin_t = np.cos(angles).astype(np.float32), np.sin(angles).astype(np.float32)
        perm = np.zeros((2 * D.hd, n_col * D.kvp), np.float32)
        for i in range(2 * D.hd):
            perm[i, (i // kv_local) * D.kvp + i % kv_local] = 1.0

        x_t = x_loc.transpose(0, 2, 1)
        w_t = w_in_loc.transpose(0, 2, 1)
        wkv_t = jnp.pad(w_kv_loc.transpose(0, 2, 1), ((0, 0), (0, D.kvp - kv_local), (0, 0)))
        gains = jnp.pad(gain_loc, ((0, 16 - D.layers), (0, 128 - D.dl)))

        m = D.och * n_row
        sds = jax.ShapeDtypeStruct
        dma = pltpu.SemaphoreType.DMA
        out = pl.pallas_call(
            functools.partial(kernel, D),
            out_shape=(
                sds(x_t.shape, BF16),
                sds((D.layers, 2, n_batch, D.pos, 128), BF16),
                sds((D.layers, e, D.d), BF16),
                sds((D.layers, D.kvp, D.d), BF16),
                sds((D.layers, n_row, r_block, D.dr), BF16),
                sds((D.seqs, D.d, D.seq), BF16),
            ),
            in_specs=[ANY] * 5 + [VMEM] * 3,
            out_specs=(ANY,) * 6,
            scratch_shapes=[
                pltpu.VMEM((group, D.dl, D.tok), BF16),
                pltpu.VMEM((group, 16, 128), BF16),
                pltpu.VMEM((D.layers, D.d, 128), F32),
                pltpu.VMEM((D.d, D.tok), BF16),
                pltpu.VMEM((D.seqs, D.d, D.seq), BF16),
                pltpu.VMEM((2, max(2 * D.fch, D.q + D.kvp), D.d), BF16),
                pltpu.VMEM((2, r_block, m), BF16),
                pltpu.VMEM((m, r_block), BF16),
                pltpu.VMEM((D.seqs * D.q, D.seq), BF16),
                pltpu.VMEM((n_col, 2 * D.seqs, D.kvp, D.seq), BF16),
                pltpu.VMEM((2 * D.seqs, D.seq, 128), BF16),
                pltpu.VMEM((2 * D.seqs, D.hd, D.seq), BF16),
                pltpu.VMEM((D.layers, 2, D.seqs, D.seq, 128), BF16),
                pltpu.VMEM((D.seqs * r_block, D.seq), BF16),
                pltpu.VMEM((2, D.seqs, m, D.seq), BF16),
                pltpu.VMEM((5, 4, m, D.tok), BF16),
                pltpu.VMEM((5, m, D.tok), BF16),
                pltpu.VMEM((5, 2, m, D.tok), BF16),
                pltpu.VMEM((2, D.n_o, m, D.tok), BF16),
                pltpu.VMEM((D.n_o, m, D.tok), BF16),
                dma((group,)), dma((group,)), dma((group,)), dma((group,)),
                dma((SLOTS, 4, 3)), dma((SLOTS, 4, 3)),
                dma((2, 9)), dma((2, 9)), dma, dma,
                dma((2, n_col)), dma((2, n_col)),
                dma((5, 8)), dma((5, 8)),
                dma((D.n_o,)), dma((D.n_o,)),
                dma((2, 8)), dma((2, 8)), dma((D.seqs,)),
                dma((n_row,)), dma((n_row,)), dma,
            ],
            compiler_params=pltpu.CompilerParams(collective_id=0, has_side_effects=True, vmem_limit_bytes=67_000_000),
            name="two_layers",
        )(x_t, gains, w_t, wkv_t, w_out_loc, jnp.asarray(cos_t), jnp.asarray(sin_t), jnp.asarray(perm, BF16))
        return out[0].transpose(0, 2, 1), out[1][..., : D.hd]

    return jax.shard_map(device_fn, mesh=mesh, in_specs=(act_spec, P(None, ("row", "col")), weight_spec, weight_spec, P(None, "col", "row")), out_specs=(act_spec, P(None, None, "dp", ("row", "col"), None)), check_vma=False)
```

```python
import functools

import numpy as np

import jax
import jax.numpy as jnp
from jax import lax
from jax.experimental import pallas as pl
from jax.experimental.pallas import tpu as pltpu
from jax.sharding import PartitionSpec as P

LN_EPS = 1e-6
MESH = pl.DeviceIdType.MESH
ANY = pl.BlockSpec(memory_space=pl.ANY)
VMEM = pl.BlockSpec(memory_space=pltpu.VMEM)
F32, BF16 = jnp.float32, jnp.bfloat16
SLOTS = 8
AHEAD = 4
RELAY = 2


def dot(a, b):
    return jnp.dot(a, b, preferred_element_type=F32)


class Dims:
    pass


def rows_at(start, count, by=16):
    return pl.ds(start if isinstance(start, int) else pl.multiple_of(start, by), count)


def kernel(
    D,
    x_t, gains, w_t, wkv_t, w_o, cos_ref, sin_ref, perm_ref,
    y_out, kv_out, g_w, g_kv, g_wo, g_h,
    xland, gland, gcol, hid, ht, wbuf, wonat, wobuf, qt, kvland, kn, vt, kvbuf, jt, ot, twin_in, far_in, near_in, psum, pair_in,
    xs, xr, gs, gr, ys, yr, ags, agr, ps, pr_, kvs, kvr, rss, rsr, es, er, lw, lo, lh, fs, fr, fl,
):
    sc = jax.named_scope
    row, col = lax.axis_index("row"), lax.axis_index("col")
    n_row, n_col, n = D.n_row, D.n_col, D.n_row * D.n_col
    n_x = n_col // 2
    me = row * n_col + col
    x, k = col // 2, lax.rem(col, 2)
    xr_, xl_, xf_ = lax.rem(x + 1, n_x), lax.rem(x + n_x - 1, n_x), lax.rem(x + 2, n_x)
    right, left, twin = xr_ * 2 + k, xl_ * 2 + k, x * 2 + 1 - k
    up, down, across = lax.rem(row + 1, n_row), lax.rem(row + n_row - 1, n_row), lax.rem(row + 2, n_row)
    half, mate = row // 2, n_row - 1 - row
    peer = row + 1 - 2 * lax.rem(row, 2)
    tok, dl, dr = D.tok, D.dl, D.dr
    och, fch = D.och, D.fch
    my_lanes = pl.ds(pl.multiple_of(k * tok, 128), tok)
    twin_lanes = pl.ds(pl.multiple_of((1 - k) * tok, 128), tok)

    def remote(src, dst, ssem, rsem, r, c):
        return pltpu.make_async_remote_copy(src_ref=src, dst_ref=dst, send_sem=ssem, recv_sem=rsem, device_id={"row": r, "col": c}, device_id_type=MESH)

    def loop(lo_, hi_, f):
        def body(i, carry):
            f(i)
            return carry

        lax.fori_loop(lo_, hi_, body, 0)

    barrier = pltpu.get_barrier_semaphore()

    def greet(i):
        d = lax.rem(me + i, n)
        pl.semaphore_signal(barrier, inc=1, device_id={"row": d // n_col, "col": lax.rem(d, n_col)}, device_id_type=MESH)

    with sc("barrier"):
        loop(1, n, greet)
        pl.semaphore_wait(barrier, n - 1)

    def piece_of(ref, d):
        return ref.at[d // 2, :, pl.ds(pl.multiple_of(lax.rem(d, 2) * tok, 128), tok)]

    def x_copy(i):
        d = lax.rem(me + i, n)
        return remote(piece_of(x_t, d), xland.at[me], xs.at[i], xr.at[i], d // n_col, lax.rem(d, n_col))

    def g_copy(i):
        d = lax.rem(me + i, n)
        return remote(gains, gland.at[me], gs.at[i], gr.at[i], d // n_col, lax.rem(d, n_col))

    def x_start(i):
        x_copy(i).start()
        g_copy(i).start()

    own_x = pltpu.make_async_copy(piece_of(x_t, me), xland.at[me], xr.at[0])
    own_g = pltpu.make_async_copy(gains, gland.at[me], gr.at[0])
    own_x.start()
    own_g.start()
    loop(1, n, x_start)

    def own_lanes(r):
        return pl.ds(pl.multiple_of(r * dr, 128), dr)

    steps = []
    for l, C in enumerate(D.cfg):
        steps += [(l, "q", 0)] + [(l, "f", j) for j in range(C.n_f)] + [(l, "o", j) for j in range(D.n_o)]
    n_steps = len(steps)
    step_of = {s: t for t, s in enumerate(steps)}

    def blocks(t, i):
        l, kind, j = steps[t]
        C = D.cfg[l]
        out = []

        def w_rows(a, m):
            at = rows_at(a, m)
            out.append((w_t.at[l, at, :], lambda r: g_w.at[l, at, own_lanes(r)]))

        def o_rows(a, m):
            at, lanes = rows_at(a, m), pl.ds(j * och, och)
            out.append((w_o.at[l, at, lanes], lambda r: g_wo.at[l, r, at, lanes]))

        def kv_rows(a, m):
            at = pl.ds(a, m)
            out.append((wkv_t.at[l, at, :], lambda r: g_kv.at[l, at, own_lanes(r)]))

        if kind == "q":
            for a in (0, C.q // 2):
                w_rows(i * C.q + a, C.q // 2)
            for a in (0, D.kvp // 2):
                kv_rows(a, D.kvp // 2)
        elif kind == "f":
            w_rows(D.q + i * C.f + j * fch, fch)
            w_rows(D.q + D.f + i * C.f + j * fch, fch)
        elif C.split:
            o_rows(i * C.q, C.q)
            o_rows(D.q + i * C.f, C.f)
        else:
            for a in (0, (D.q + D.f) // 2):
                o_rows(a, (D.q + D.f) // 2)
        return out

    pending = {}

    def y_copy(t, i, kind, src, dst, r):
        return remote(src, dst, ys.at[t % SLOTS, i, kind], yr.at[t % SLOTS, i, kind], r, col)

    def drain(t):
        for c in pending.pop(t, ()):
            c.wait_send()

    def y_send(t, *args):
        c = y_copy(t, *args)
        c.start()
        pending[t].append(c)

    def issue(t):
        drain(t - SLOTS)
        pending[t] = []
        if D.cfg[steps[t][0]].split:
            for i, (src, place) in enumerate(blocks(t, 1 - half)):
                y_send(t, i, 1, src, place(row), mate)
            for i, (src, place) in enumerate(blocks(t, half)):
                y_send(t, i, 0, src, place(row), peer)
        else:
            for i, (src, place) in enumerate(blocks(t, 0)):
                y_send(t, i, 0, src, place(row), up)
                y_send(t, i, 1, src, place(row), down)

    def relay(t):
        if D.cfg[steps[t][0]].split:
            for i, (src, place) in enumerate(blocks(t, half)):
                y_copy(t, i, 1, src, place(mate), mate).wait_recv()
                y_send(t, i, 2, place(mate), place(mate), peer)
        else:
            for i, (src, place) in enumerate(blocks(t, 0)):
                for kind, r, to in ((0, down, up), (1, up, down)):
                    y_copy(t, i, kind, src, place(r), r).wait_recv()
                    if kind == i % 2:
                        y_send(t, i, 2, place(r), place(r), to)

    y_next, issued, ahead, relayed, lead = [0], [0], [AHEAD], [0], [RELAY]

    def relay_to(t):
        while relayed[0] <= min(t, n_steps - 1):
            relay(relayed[0])
            relayed[0] += 1

    def issue_to(t):
        while issued[0] <= min(t, n_steps - 1):
            issue(issued[0])
            issued[0] += 1

    def advance():
        t = y_next[0]
        if t >= n_steps:
            return
        with sc(f"adv{t}"):
            if D.cfg[steps[t][0]].split:
                rest = n_row - 1 - peer
                for i, (src, place) in enumerate(blocks(t, half)):
                    y_copy(t, i, 0, src, place(peer), peer).wait_recv()
                    y_copy(t, i, 2, src, place(rest), rest).wait_recv()
            else:
                for i, (src, place) in enumerate(blocks(t, 0)):
                    y_copy(t, i, 2, src, place(across), across).wait_recv()
            relay_to(t + lead[0])
            issue_to(t + ahead[0])
        y_next[0] = t + 1

    def have(*step):
        while y_next[0] <= step_of[step]:
            advance()

    issue_to(AHEAD - 1)

    def w_fetch(l, kind, j, slot):
        C = D.cfg[l]
        i = half if C.split else 0
        copies = []

        def fetch(src, dst):
            copies.append(pltpu.make_async_copy(src, dst, lw.at[slot, len(copies)]))

        def w_rows(a, m, at):
            a, at = rows_at(a, m), pl.ds(at, m)
            fetch(w_t.at[l, a, :], wbuf.at[slot, at, own_lanes(row)])
            for r in (up, down, across):
                fetch(g_w.at[l, a, own_lanes(r)], wbuf.at[slot, at, own_lanes(r)])

        if kind == "q":
            w_rows(i * C.q, C.q, 0)
            at = pl.ds(C.q, D.kvp)
            fetch(wkv_t.at[l], wbuf.at[slot, at, own_lanes(row)])
            for r in (up, down, across):
                fetch(g_kv.at[l, :, own_lanes(r)], wbuf.at[slot, at, own_lanes(r)])
        else:
            w_rows(D.q + i * C.f + j * C.cw, C.cw, 0)
            w_rows(D.q + D.f + i * C.f + j * C.cw, C.cw, C.cw)
        return copies

    def o_fetch(l, j, slot):
        C = D.cfg[l]
        copies = []

        def fetch(src, dst):
            copies.append(pltpu.make_async_copy(src, dst, lo.at[slot, len(copies)]))

        lanes = pl.ds(j * och, och)
        spans = ((half * C.q, 0, C.q), (D.q + half * C.f, C.q, C.f)) if C.split else ((0, 0, C.q + C.f),)
        for a, at, m in spans:
            a, at = rows_at(a, m), pl.ds(at, m)
            to = lambda r: pl.ds(pl.multiple_of(r * och, 128), och)
            fetch(w_o.at[l, a, lanes], wonat.at[slot, at, to(row)])
            for r in (up, down, across):
                fetch(g_wo.at[l, r, a, lanes], wonat.at[slot, at, to(r)])
        return copies

    def start(copies):
        for c in copies:
            c.start()

    def wait(copies):
        for c in copies:
            c.wait()

    own_x.wait()
    own_g.wait()

    def x_finish(i):
        s = lax.rem(me + n - i, n)
        remote(xland.at[s], xland.at[s], xs.at[i], xr.at[i], row, col).wait_recv()
        remote(gland.at[s], gland.at[s], gs.at[i], gr.at[i], row, col).wait_recv()
        x_copy(i).wait_send()
        g_copy(i).wait_send()

    with sc("xwait"):
        loop(1, n, x_finish)

    def keep(d):
        hid[rows_at(d * dl, dl), :] = xland[d]

    with sc("gains"):
        loop(0, n, keep)
        g_all = gland[...].astype(F32)
        for l in range(D.layers):
            g_rows = g_all[:, l, :]
            g_rows = jnp.concatenate([g_rows, jnp.zeros((128 - n, 128), F32)], axis=0) if n < 128 else g_rows
            g_cols = g_rows.T
            for d in range(n):
                gcol[l, d * dl : (d + 1) * dl, :] = jnp.broadcast_to(g_cols[:dl, d : d + 1], (dl, 128))

    blk = 64
    n_blk = D.d // blk

    def layer_norm(l):
        def add_up(i, acc):
            v = hid[rows_at(i * blk, blk), :].astype(F32)
            return acc + v.reshape(blk // 8, 8, tok).sum(axis=0)

        mean = lax.fori_loop(0, n_blk, add_up, jnp.zeros((8, tok), F32)).sum(axis=0, keepdims=True) / D.d

        def add_sq(i, acc):
            v = hid[rows_at(i * blk, blk), :].astype(F32) - mean
            return acc + (v * v).reshape(blk // 8, 8, tok).sum(axis=0)

        var = lax.fori_loop(0, n_blk, add_sq, jnp.zeros((8, tok), F32)).sum(axis=0, keepdims=True) / D.d
        scale = lax.rsqrt(var + LN_EPS)

        def write(i):
            rows = rows_at(i * blk, blk)
            g = gcol[l, rows, :]
            g = jnp.concatenate([g] * (tok // 128), axis=1)
            v = (hid[rows, :].astype(F32) - mean) * scale * g
            ht[x, rows, my_lanes] = v.astype(BF16)

        with sc(f"norm{l}"):
            loop(0, n_blk, write)

    d_low, d_high = pl.ds(0, D.d // 2), pl.ds(D.d // 2, D.d // 2)

    class Gather:
        def __init__(self, buf, a):
            self.buf, self.a, self.sends = buf, a, []
            mine = buf.at[x, :, my_lanes]
            for i, c in ((0, right), (1, left), (2, twin)):
                self.send(i, mine, c)

        def send(self, i, ref, c):
            copy = remote(ref, ref, ags.at[self.a, i], agr.at[self.a, i], row, c)
            copy.start()
            self.sends.append(copy)

        def arrived(self, i, ref):
            remote(ref, ref, ags.at[self.a, i], agr.at[self.a, i], row, col).wait_recv()

        def pass_on(self):
            b = self.buf
            with sc(f"pass_on{self.a}"):
                self.arrived(0, b.at[xl_, :, my_lanes])
                self.send(3, b.at[xl_, d_low, my_lanes], right)
                self.send(4, b.at[xl_, :, my_lanes], twin)
                self.arrived(1, b.at[xr_, :, my_lanes])
                self.send(5, b.at[xr_, d_high, my_lanes], left)
                self.send(6, b.at[xr_, :, my_lanes], twin)

        def near(self):
            b = self.buf
            with sc(f"near{self.a}"):
                self.arrived(2, b.at[x, :, twin_lanes])
                self.arrived(4, b.at[xl_, :, twin_lanes])
                self.arrived(6, b.at[xr_, :, twin_lanes])

        def pass_far(self):
            b = self.buf
            with sc(f"pass_far{self.a}"):
                self.arrived(3, b.at[xf_, d_low, my_lanes])
                self.send(7, b.at[xf_, d_low, my_lanes], twin)
                self.arrived(5, b.at[xf_, d_high, my_lanes])
                self.send(8, b.at[xf_, d_high, my_lanes], twin)

        def far(self):
            b = self.buf
            with sc(f"far{self.a}"):
                self.arrived(7, b.at[xf_, d_low, twin_lanes])
                self.arrived(8, b.at[xf_, d_high, twin_lanes])

        def finish(self):
            for c in self.sends:
                c.wait_send()

    half_dim = D.hd // 2

    def near3(i):
        return lax.rem(x + i + i // 2, n_x)

    def all4(i):
        return i

    def far1(i):
        return xf_

    def rope(p):
        lo_, hi_ = p[:half_dim], p[half_dim:]
        return jnp.concatenate([lo_ * cos_ref[...] - hi_ * sin_ref[...], hi_ * cos_ref[...] + lo_ * sin_ref[...]], axis=0)

    def project_q(l, a, seq_of, count):
        C = D.cfg[l]

        def body(i):
            s = seq_of(i)
            p = dot(wbuf[1, : C.q + D.kvp, :], ht[s]).astype(BF16).astype(F32)
            for h in range(C.heads):
                at = rows_at((a * D.seqs + s) * C.q + h * D.hd, D.hd)
                qt[at, :] = (rope(p[h * D.hd : (h + 1) * D.hd]) * D.hd**-0.5).astype(BF16)
            kvland[col, a * D.seqs + s] = p[C.q :].astype(BF16)

        with sc(f"q{l}{a}"):
            loop(0, count, body)

    def kv_send(a):
        own = kvland.at[col, pl.ds(a * D.seqs, D.seqs)]
        copies = [remote(own, own, kvs.at[a, j], kvr.at[a, j], row, lax.rem(col + j, n_col)) for j in range(1, n_col)]
        start(copies)
        return copies

    def kv_arrive(a, copies):
        with sc(f"kvwait{a}"):
            for j in range(1, n_col):
                s = lax.rem(col + n_col - j, n_col)
                ref = kvland.at[s, pl.ds(a * D.seqs, D.seqs)]
                remote(ref, ref, kvs.at[a, j], kvr.at[a, j], row, col).wait_recv()
            for c in copies:
                c.wait_send()

    def key_value(l, a):
        def body(i):
            s = a * D.seqs + i
            raw = kvland[:, s].reshape(n_col * D.kvp, D.seq)
            both = dot(perm_ref[...], raw)
            zeros = jnp.zeros((128 - D.hd, D.seq), F32)
            k_nat = jnp.concatenate([rope(both[: D.hd]), zeros], axis=0).T.astype(BF16)
            kn[s] = k_nat
            vt[s] = both[D.hd :].astype(BF16)
            if a == 0:
                kvbuf[l, 0, i] = k_nat
                kvbuf[l, 1, i] = jnp.concatenate([both[D.hd :], zeros], axis=0).T.astype(BF16)

        with sc(f"kv{l}{a}"):
            loop(0, D.seqs, body)

    qb = D.seq // 2

    def attention(l, a):
        C = D.cfg[l]

        def body(i):
            s, h = a * D.seqs + i // C.heads, lax.rem(i, C.heads)
            q_rows = rows_at(s * C.q + h * D.hd, D.hd)
            o_rows = rows_at(s * (C.q + C.f) + h * D.hd, D.hd)
            for b in range(2):
                ext = (b + 1) * qb
                lanes = slice(b * qb, (b + 1) * qb)
                score = dot(kn[s, :ext, : D.hd], qt[q_rows, lanes])
                keys = lax.broadcasted_iota(jnp.int32, (ext, qb), 0)
                queries = lax.broadcasted_iota(jnp.int32, (ext, qb), 1) + b * qb
                score = jnp.where(keys <= queries, score, -1e30)
                p = jnp.exp(score - jnp.max(score, axis=0, keepdims=True))
                p = (p * (1.0 / jnp.sum(p, axis=0, keepdims=True))).astype(BF16)
                jt[o_rows, lanes] = dot(vt[s, :, :ext], p).astype(BF16)

        with sc(f"attn{l}{a}"):
            loop(0, D.seqs * C.heads, body)

    def gate_up(l, a, slot, j, seq_of, count):
        C = D.cfg[l]

        def body(i):
            s = seq_of(i)
            p = dot(wbuf[slot, : 2 * C.cw, :], ht[s])
            g = p[: C.cw].astype(BF16).astype(F32)
            u = p[C.cw :].astype(BF16).astype(F32)
            jt[rows_at((a * D.seqs + s) * (C.q + C.f) + C.q + j * C.cw, C.cw), :] = (g * jax.nn.sigmoid(g) * u).astype(BF16)

        loop(0, count, body)

    def gate_up_loop(l, a, seq_of, count, first, last):
        C = D.cfg[l]
        have_chunk(l, min(last, C.n_c - 1))

        def body(j):
            slot = lax.rem(j, 2)
            wait(w_fetch(l, "f", j, slot))

            @pl.when(j + 1 < C.n_c)
            def _():
                start(w_fetch(l, "f", j + 1, 1 - slot))

            gate_up(l, a, slot, j, seq_of, count)

        with sc(f"gu{l}{a}"):
            loop(first, last, body)

    def have_chunk(l, j):
        C = D.cfg[l]
        have(l, "f", (j + 1) * C.cw // fch - 1)

    def load_q(l):
        have(l, "q", 0)
        copies = w_fetch(l, "q", 0, 1)
        start(copies)
        wait(copies)

    m = och * n_row
    m_low, m_high = pl.ds(0, m // 2), pl.ds(m // 2, m // 2)
    r_slots = twin_in.shape[0]
    r_step = 64

    def order(i):
        return lax.rem(x + lax.rem(2 + 3 * i, 4), n_x)

    class Reduce:
        def __init__(self, l):
            self.l, self.C, self.sends = l, D.cfg[l], {}

        def send(self, u, i, src, dst, c):
            copy = remote(src, dst, rss.at[u % r_slots, i], rsr.at[u % r_slots, i], row, c)
            copy.start()
            self.sends[u].append(copy)

        def arrived(self, u, i, ref):
            remote(ref, ref, rss.at[u % r_slots, i], rsr.at[u % r_slots, i], row, col).wait_recv()

        def twin_copy(self, u, i):
            us = u % r_slots
            return remote(ot.at[u % 2, order(i), :, twin_lanes], twin_in.at[us, i], rss.at[us, i], rsr.at[us, i], row, twin)

        def twin_done(self, u):
            loop(0, 4, lambda i: self.twin_copy(u, i).wait_send())

        def stage_a(self, u, a):
            C = self.C
            if u >= 2:
                self.twin_done(u - 2)
            if u >= r_slots - 1:
                for c in self.sends.pop(u - r_slots + 1):
                    c.wait_send()
            self.sends[u] = []
            R = C.q + C.f

            def body(i):
                s = order(i)
                ot[u % 2, s] = dot(wobuf[:, :R], jt[rows_at((a * D.seqs + s) * R, R), :]).astype(BF16)
                self.twin_copy(u, i).start()

            with sc(f"sa{self.l}_{u}"):
                loop(0, 4, body)

        def stage_b(self, u):
            us = u % r_slots

            def body(i):
                self.arrived(u, i, twin_in.at[us, i])
                s = order(i)

                def add(b):
                    at = rows_at(b * r_step, r_step)
                    twin_in[us, i, at, :] = (ot[u % 2, s, at, my_lanes].astype(F32) + twin_in[us, i, at, :].astype(F32)).astype(BF16)

                loop(0, m // r_step, add)

            with sc(f"sb{self.l}_{u}"):
                loop(0, 1, body)
                self.send(u, 4, twin_in.at[us, 0, m_low], far_in.at[us, m_low], right)
                self.send(u, 5, twin_in.at[us, 0, m_high], far_in.at[us, m_high], left)
                loop(1, 4, body)

        def stage_c(self, u):
            us = u % r_slots

            def add_far(i, base):
                def add(b):
                    at = rows_at(base + b * r_step, r_step)
                    twin_in[us, i, at, :] = (twin_in[us, i, at, :].astype(F32) + far_in[us, at, :].astype(F32)).astype(BF16)

                loop(0, m // 2 // r_step, add)

            with sc(f"sc{self.l}_{u}"):
                self.arrived(u, 4, far_in.at[us, m_low])
                add_far(1, 0)
                self.send(u, 6, twin_in.at[us, 1], near_in.at[us, 0], right)
                self.arrived(u, 5, far_in.at[us, m_high])
                add_far(3, m // 2)
                self.send(u, 7, twin_in.at[us, 3], near_in.at[us, 1], left)

        def add_update(self, j, total):
            step = min(r_step, och)
            for r in range(n_row):

                def add(b, r=r):
                    dst = rows_at(r * dr + j * och + b * step, step)
                    u = total(rows_at(r * och + b * step, step)).astype(BF16).astype(F32)
                    hid[dst, :] = (hid[dst, :].astype(F32) + u).astype(BF16)

                loop(0, och // step, add)

        def stage_d(self, u, j, a):
            us = u % r_slots

            def total(at):
                return twin_in[us, 2, at, :].astype(F32) + near_in[us, 0, at, :].astype(F32) + near_in[us, 1, at, :].astype(F32)

            with sc(f"sd{self.l}_{u}"):
                self.arrived(u, 6, near_in.at[us, 0])
                self.arrived(u, 7, near_in.at[us, 1])
                if self.C.split:

                    def save(b):
                        at = rows_at(b * r_step, r_step)
                        psum[a, j, at, :] = total(at).astype(BF16)

                    loop(0, m // r_step, save)
                    if a == 1:
                        remote(psum.at[1, j], pair_in.at[j], es.at[j], er.at[j], mate, col).start()
                else:
                    self.add_update(j, total)

        def stage_e(self, j):
            with sc(f"se{self.l}_{j}"):
                c = remote(psum.at[1, j], pair_in.at[j], es.at[j], er.at[j], mate, col)
                c.wait_recv()
                self.add_update(j, lambda at: psum[0, j, at, :].astype(F32) + pair_in[j, at, :].astype(F32))
                c.wait_send()

        def finish(self, units):
            with sc(f"rfin{self.l}"):
                for u in range(max(0, units - 2), units):
                    self.twin_done(u)
                for u in self.sends:
                    for c in self.sends[u]:
                        c.wait_send()

    o_started = set()

    def o_load(l, j, a):
        if (l, j, a) not in o_started:
            have(l, "o", j)
            start(o_fetch(l, j, j % 2))
            o_started.add((l, j, a))

    def o_use(l, j, a):
        C = D.cfg[l]
        with sc(f"ouse{l}_{j}"):
            o_load(l, j, a)
            wait(o_fetch(l, j, j % 2))
            if j + 1 < D.n_o and y_next[0] > step_of[(l, "o", j + 1)]:
                o_load(l, j + 1, a)
            R = C.q + C.f
            for r in range(n_row):
                wobuf[r * och : (r + 1) * och, :R] = wonat[j % 2, :R, r * och : (r + 1) * och].T

    layer_norm(0)
    g0 = Gather(ht, 0)
    mine = ht.at[x, :, my_lanes]
    shared = g_h.at[x, :, my_lanes]
    to_mate = remote(mine, shared, ps, pr_, mate, col)
    to_mate.start()
    with sc("relay0"):
        relay_to(RELAY - 1)
    advance()
    advance()
    g0.pass_on()
    with sc("mate"):
        to_mate.wait_recv()
    g1 = Gather(g_h, 1)
    load_q(0)
    g0.near()
    project_q(0, 0, near3, 3)
    g0.pass_far()
    g0.far()
    project_q(0, 0, far1, 1)
    sent = kv_send(0)
    n_f = D.cfg[0].n_f
    f_started = set()

    def f_load(j):
        if j not in f_started:
            f_started.add(j)
            start(w_fetch(0, "f", j, j % 2))

    for j in range(n_f):
        have(0, "f", j)
        f_load(j)
        if j == n_f - 2:
            g1.pass_on()
        with sc(f"gu0_{j}"):
            wait(w_fetch(0, "f", j, j % 2))
            if j + 1 < n_f and y_next[0] > step_of[(0, "f", j + 1)]:
                f_load(j + 1)
            gate_up(0, 0, j % 2, j, all4, 4)
        if j == n_f - 2:
            kv_arrive(0, sent)
            key_value(0, 0)
            attention(0, 0)
    g0.finish()
    to_mate.wait_send()
    g1.near()

    def h_copy(i):
        return pltpu.make_async_copy(g_h.at[i], ht.at[i], lh.at[i])

    loop(0, 3, lambda i: h_copy(near3(i)).start())
    load_q(0)
    g1.pass_far()
    loop(0, 3, lambda i: h_copy(near3(i)).wait())
    project_q(0, 1, near3, 3)
    g1.far()
    h_copy(xf_).start()
    start(w_fetch(0, "f", 0, 0))
    h_copy(xf_).wait()
    project_q(0, 1, far1, 1)
    sent = kv_send(1)

    red = Reduce(0)
    units = [(j, a) for a in (0, 1) for j in range(D.n_o)]
    n_u = len(units)
    state = {"e": 0}

    def unit(u):
        j, a = units[u]
        o_use(0, j, a)
        red.stage_a(u, a)
        if u >= 1:
            red.stage_c(u - 1)
        if u >= 2:
            red.stage_d(u - 2, *units[u - 2])
        red.stage_b(u)
        if u >= D.n_o + 3:
            red.stage_e(state["e"])
            state["e"] += 1

    cuts = [n_f * i // 3 for i in range(4)]
    unit(0)
    gate_up_loop(0, 1, all4, 4, cuts[0], cuts[1])
    unit(1)
    gate_up_loop(0, 1, all4, 4, cuts[1], cuts[2])
    unit(2)
    gate_up_loop(0, 1, all4, 4, cuts[2], cuts[3])
    kv_arrive(1, sent)
    key_value(0, 1)
    for u in range(3, D.n_o):
        unit(u)
        if u == 3:
            attention(0, 1)
    g1.finish()
    if D.n_o <= 3:
        attention(0, 1)
    for u in range(D.n_o, n_u):
        unit(u)
        if u >= n_u - 3:
            ahead[0], lead[0] = 2, 1
        if u < n_u - 1:
            advance()
    red.stage_c(n_u - 1)
    red.stage_d(n_u - 2, *units[n_u - 2])
    red.stage_d(n_u - 1, *units[n_u - 1])
    ahead[0], lead[0] = AHEAD, RELAY
    issue_to(y_next[0] - 1 + AHEAD)
    for j in range(state["e"], D.n_o):
        red.stage_e(j)
    red.finish(n_u)

    def y_copy_back(i):
        d = lax.rem(me + i, n)
        return remote(hid.at[rows_at(d * dl, dl), :], piece_of(y_out, me), xs.at[i], xr.at[i], d // n_col, lax.rem(d, n_col))

    own_y = pltpu.make_async_copy(hid.at[rows_at(me * dl, dl), :], piece_of(y_out, me), xr.at[0])

    def y_send_back(c):
        def body(r):
            i = lax.rem(r * n_col + c - me + n, n)

            @pl.when(i == 0)
            def _():
                own_y.start()

            @pl.when(i != 0)
            def _():
                y_copy_back(i).start()

        loop(0, n_row, body)

    for l in range(1, D.layers):
        C = D.cfg[l]
        layer_norm(l)
        g0 = Gather(ht, 0)
        for _ in range(3):
            advance()
        g0.pass_on()
        load_q(l)
        have_chunk(l, 0)
        start(w_fetch(l, "f", 0, 0))
        g0.near()
        project_q(l, 0, near3, 3)
        n_mid = C.n_c // 2
        gate_up_loop(l, 0, near3, 3, 0, n_mid)
        g0.pass_far()
        gate_up_loop(l, 0, near3, 3, n_mid, C.n_c)
        load_q(l)
        start(w_fetch(l, "f", 0, 0))
        g0.far()
        project_q(l, 0, far1, 1)
        sent = kv_send(0)
        gate_up_loop(l, 0, far1, 1, 0, C.n_c)
        have(l, "o", 0)
        o_load(l, 0, 0)
        g0.finish()
        kv_arrive(0, sent)
        key_value(l, 0)
        attention(l, 0)
        red = Reduce(l)
        last = l + 1 == D.layers

        def final(j):
            red.stage_d(j, j, 0)
            if last:
                for c in range(n_col):
                    if j * och < (c + 1) * dl <= (j + 1) * och:
                        y_send_back(c)

        for j in range(D.n_o):
            o_use(l, j, 0)
            red.stage_a(j, 0)
            red.stage_b(j)
            if j >= 1:
                final(j - 1)
            red.stage_c(j)
        final(D.n_o - 1)
        red.finish(D.n_o)

    def kv_back(i):
        r = lax.rem(row + i, n_row)
        pos = rows_at((r * n_col + col) * D.pos, D.pos)
        return kvbuf.at[:, :, :, pos, :], kv_out.at[:, :, pl.ds(row * D.seqs, D.seqs)], r

    src, dst, _ = kv_back(0)
    own_kv = pltpu.make_async_copy(src, dst, fl)
    own_kv.start()
    kv_sends = []
    for i in range(1, n_row):
        src, dst, r = kv_back(i)
        c = remote(src, dst, fs.at[i], fr.at[i], r, col)
        c.start()
        kv_sends.append(c)

    def y_finish(i):
        s = lax.rem(me + n - i, n)
        remote(piece_of(y_out, s), piece_of(y_out, s), xs.at[i], xr.at[i], row, col).wait_recv()
        y_copy_back(i).wait_send()

    with sc("ywait"):
        loop(1, n, y_finish)
        own_y.wait()
        own_kv.wait()
        for i in range(1, n_row):
            r = lax.rem(row + n_row - i, n_row)
            dst = kv_out.at[:, :, pl.ds(r * D.seqs, D.seqs)]
            remote(dst, dst, fs.at[i], fr.at[i], row, col).wait_recv()
        for c in kv_sends:
            c.wait_send()
        for t in sorted(pending):
            drain(t)


def solution(mesh):
    n_row, n_col = mesh.shape["row"], mesh.shape["col"]
    group = n_row * n_col
    act_spec = P("dp", None, ("row", "col"))
    weight_spec = P(None, "row", "col")

    def device_fn(x_loc, gain_loc, w_in_loc, w_kv_loc, w_out_loc):
        D = Dims()
        D.n_row, D.n_col = n_row, n_col
        n_batch, D.seq, D.dl = x_loc.shape
        D.layers, D.dr, e = w_in_loc.shape
        D.d = D.dl * group
        r_block = w_out_loc.shape[1]
        D.f = e - r_block
        D.q = r_block - D.f
        kv_local = w_kv_loc.shape[2]
        D.hd = kv_local * n_col // 2
        D.kvp = 32
        D.tok = n_batch * D.seq // group
        D.seqs = n_batch // n_row
        D.pos = D.seq // group
        D.fch = 128
        D.och = 128
        D.n_o = D.dr // D.och
        D.cfg = []
        for l in range(D.layers):
            C = Dims()
            C.split = l == 0
            parts = 2 if C.split else 1
            C.q, C.f = D.q // parts, D.f // parts
            C.heads, C.n_f = C.q // D.hd, C.f // D.fch
            C.cw = D.fch if C.split else 2 * D.fch
            C.n_c = C.f // C.cw
            D.cfg.append(C)
        assert D.seq == 2 * D.tok and D.seqs == n_col // 2 == n_row == 4

        half = D.hd // 2
        inv_freq = (np.float32(1.0) / (np.float32(10000.0) ** (np.arange(half, dtype=np.float32) * np.float32(2.0) / np.float32(D.hd)))).astype(np.float32)
        angles = (inv_freq[:, None] * np.arange(D.seq, dtype=np.float32)[None, :]).astype(np.float32)
        cos_t, sin_t = np.cos(angles).astype(np.float32), np.sin(angles).astype(np.float32)
        perm = np.zeros((2 * D.hd, n_col * D.kvp), np.float32)
        for i in range(2 * D.hd):
            perm[i, (i // kv_local) * D.kvp + i % kv_local] = 1.0

        x_t = x_loc.transpose(0, 2, 1)
        w_t = w_in_loc.transpose(0, 2, 1)
        wkv_t = jnp.pad(w_kv_loc.transpose(0, 2, 1), ((0, 0), (0, D.kvp - kv_local), (0, 0)))
        gains = jnp.pad(gain_loc, ((0, 16 - D.layers), (0, 128 - D.dl)))

        m = D.och * n_row
        sds = jax.ShapeDtypeStruct
        dma = pltpu.SemaphoreType.DMA
        out = pl.pallas_call(
            functools.partial(kernel, D),
            out_shape=(
                sds(x_t.shape, BF16),
                sds((D.layers, 2, n_batch, D.pos, 128), BF16),
                sds((D.layers, e, D.d), BF16),
                sds((D.layers, D.kvp, D.d), BF16),
                sds((D.layers, n_row, r_block, D.dr), BF16),
                sds((D.seqs, D.d, D.seq), BF16),
            ),
            in_specs=[ANY] * 5 + [VMEM] * 3,
            out_specs=(ANY,) * 6,
            scratch_shapes=[
                pltpu.VMEM((group, D.dl, D.tok), BF16),
                pltpu.VMEM((group, 16, 128), BF16),
                pltpu.VMEM((D.layers, D.d, 128), F32),
                pltpu.VMEM((D.d, D.tok), BF16),
                pltpu.VMEM((D.seqs, D.d, D.seq), BF16),
                pltpu.VMEM((2, max(4 * D.fch, D.q + D.kvp), D.d), BF16),
                pltpu.VMEM((2, r_block, m), BF16),
                pltpu.VMEM((m, r_block), BF16),
                pltpu.VMEM((D.seqs * D.q, D.seq), BF16),
                pltpu.VMEM((n_col, 2 * D.seqs, D.kvp, D.seq), BF16),
                pltpu.VMEM((2 * D.seqs, D.seq, 128), BF16),
                pltpu.VMEM((2 * D.seqs, D.hd, D.seq), BF16),
                pltpu.VMEM((D.layers, 2, D.seqs, D.seq, 128), BF16),
                pltpu.VMEM((D.seqs * r_block, D.seq), BF16),
                pltpu.VMEM((2, D.seqs, m, D.seq), BF16),
                pltpu.VMEM((5, 4, m, D.tok), BF16),
                pltpu.VMEM((5, m, D.tok), BF16),
                pltpu.VMEM((5, 2, m, D.tok), BF16),
                pltpu.VMEM((2, D.n_o, m, D.tok), BF16),
                pltpu.VMEM((D.n_o, m, D.tok), BF16),
                dma((group,)), dma((group,)), dma((group,)), dma((group,)),
                dma((SLOTS, 4, 3)), dma((SLOTS, 4, 3)),
                dma((2, 9)), dma((2, 9)), dma, dma,
                dma((2, n_col)), dma((2, n_col)),
                dma((5, 8)), dma((5, 8)),
                dma((D.n_o,)), dma((D.n_o,)),
                dma((2, 8)), dma((2, 8)), dma((D.seqs,)),
                dma((n_row,)), dma((n_row,)), dma,
            ],
            compiler_params=pltpu.CompilerParams(collective_id=0, has_side_effects=True, vmem_limit_bytes=67_000_000),
            name="two_layers",
        )(x_t, gains, w_t, wkv_t, w_out_loc, jnp.asarray(cos_t), jnp.asarray(sin_t), jnp.asarray(perm, BF16))
        return out[0].transpose(0, 2, 1), out[1][..., : D.hd]

    return jax.shard_map(device_fn, mesh=mesh, in_specs=(act_spec, P(None, ("row", "col")), weight_spec, weight_spec, P(None, "col", "row")), out_specs=(act_spec, P(None, None, "dp", ("row", "col"), None)), check_vma=False)
```

```python
import functools

import numpy as np

import jax
import jax.numpy as jnp
from jax import lax
from jax.experimental import pallas as pl
from jax.experimental.pallas import tpu as pltpu
from jax.sharding import PartitionSpec as P

LN_EPS = 1e-6
MESH = pl.DeviceIdType.MESH
ANY = pl.BlockSpec(memory_space=pl.ANY)
VMEM = pl.BlockSpec(memory_space=pltpu.VMEM)
F32, BF16 = jnp.float32, jnp.bfloat16
SLOTS = 8
AHEAD = 4
RELAY = 2


def dot(a, b):
    return jnp.dot(a, b, preferred_element_type=F32)


class Dims:
    pass


def rows_at(start, count, by=16):
    return pl.ds(start if isinstance(start, int) else pl.multiple_of(start, by), count)


def kernel(
    D,
    x_t, gains, w_t, wkv_t, w_o, cos_ref, sin_ref, perm_ref,
    y_out, kv_out, g_w, g_kv, g_wo, g_h,
    xland, gland, gcol, hid, ht, wbuf, wonat, wobuf, qt, kvland, kn, vt, kvbuf, jt, ot, twin_in, far_in, near_in, psum, pair_in,
    xs, xr, gs, gr, ys, yr, ags, agr, ps, pr_, kvs, kvr, rss, rsr, es, er, lw, lo, lh, fs, fr, fl,
):
    sc = jax.named_scope
    row, col = lax.axis_index("row"), lax.axis_index("col")
    n_row, n_col, n = D.n_row, D.n_col, D.n_row * D.n_col
    n_x = n_col // 2
    me = row * n_col + col
    x, k = col // 2, lax.rem(col, 2)
    xr_, xl_, xf_ = lax.rem(x + 1, n_x), lax.rem(x + n_x - 1, n_x), lax.rem(x + 2, n_x)
    right, left, twin = xr_ * 2 + k, xl_ * 2 + k, x * 2 + 1 - k
    up, down, across = lax.rem(row + 1, n_row), lax.rem(row + n_row - 1, n_row), lax.rem(row + 2, n_row)
    half, mate = row // 2, n_row - 1 - row
    peer = row + 1 - 2 * lax.rem(row, 2)
    tok, dl, dr = D.tok, D.dl, D.dr
    och, fch = D.och, D.fch
    my_lanes = pl.ds(pl.multiple_of(k * tok, 128), tok)
    twin_lanes = pl.ds(pl.multiple_of((1 - k) * tok, 128), tok)

    def remote(src, dst, ssem, rsem, r, c):
        return pltpu.make_async_remote_copy(src_ref=src, dst_ref=dst, send_sem=ssem, recv_sem=rsem, device_id={"row": r, "col": c}, device_id_type=MESH)

    def loop(lo_, hi_, f):
        def body(i, carry):
            f(i)
            return carry

        lax.fori_loop(lo_, hi_, body, 0)

    barrier = pltpu.get_barrier_semaphore()

    def greet(i):
        d = lax.rem(me + i, n)
        pl.semaphore_signal(barrier, inc=1, device_id={"row": d // n_col, "col": lax.rem(d, n_col)}, device_id_type=MESH)

    with sc("barrier"):
        loop(1, n, greet)
        pl.semaphore_wait(barrier, n - 1)

    def piece_of(ref, d):
        return ref.at[d // 2, :, pl.ds(pl.multiple_of(lax.rem(d, 2) * tok, 128), tok)]

    def x_copy(i):
        d = lax.rem(me + i, n)
        return remote(piece_of(x_t, d), xland.at[me], xs.at[i], xr.at[i], d // n_col, lax.rem(d, n_col))

    def g_copy(i):
        d = lax.rem(me + i, n)
        return remote(gains, gland.at[me], gs.at[i], gr.at[i], d // n_col, lax.rem(d, n_col))

    def x_start(i):
        x_copy(i).start()
        g_copy(i).start()

    own_x = pltpu.make_async_copy(piece_of(x_t, me), xland.at[me], xr.at[0])
    own_g = pltpu.make_async_copy(gains, gland.at[me], gr.at[0])
    own_x.start()
    own_g.start()
    loop(1, n, x_start)

    def own_lanes(r):
        return pl.ds(pl.multiple_of(r * dr, 128), dr)

    def o_lanes(j, r):
        return pl.ds(pl.multiple_of(lax.rem(r + j, D.n_o) * och, 128), och)

    steps = []
    for l, C in enumerate(D.cfg):
        steps += [(l, "q", 0)] + [(l, "f", j) for j in range(C.n_f)] + [(l, "o", j) for j in range(D.n_o)]
    n_steps = len(steps)
    step_of = {s: t for t, s in enumerate(steps)}

    def blocks(t, i):
        l, kind, j = steps[t]
        C = D.cfg[l]
        out = []

        def w_rows(a, m):
            at = rows_at(a, m)
            out.append((w_t.at[l, at, :], lambda r: g_w.at[l, at, own_lanes(r)]))

        def o_rows(a, m):
            at = rows_at(a, m)
            out.append((w_o.at[l, at, o_lanes(j, row)], lambda r: g_wo.at[l, r, at, o_lanes(j, r)]))

        def kv_rows(a, m):
            at = pl.ds(a, m)
            out.append((wkv_t.at[l, at, :], lambda r: g_kv.at[l, at, own_lanes(r)]))

        if kind == "q":
            for a in (0, C.q // 2):
                w_rows(i * C.q + a, C.q // 2)
            for a in (0, D.kvp // 2):
                kv_rows(a, D.kvp // 2)
        elif kind == "f":
            w_rows(D.q + i * C.f + j * fch, fch)
            w_rows(D.q + D.f + i * C.f + j * fch, fch)
        elif C.split:
            o_rows(i * C.q, C.q)
            o_rows(D.q + i * C.f, C.f)
        else:
            for a in (0, (D.q + D.f) // 2):
                o_rows(a, (D.q + D.f) // 2)
        return out

    pending = {}

    def y_copy(t, i, kind, src, dst, r):
        return remote(src, dst, ys.at[t % SLOTS, i, kind], yr.at[t % SLOTS, i, kind], r, col)

    def drain(t):
        for c in pending.pop(t, ()):
            c.wait_send()

    def y_send(t, *args):
        c = y_copy(t, *args)
        c.start()
        pending[t].append(c)

    def issue(t):
        drain(t - SLOTS)
        pending[t] = []
        if D.cfg[steps[t][0]].split:
            for i, (src, place) in enumerate(blocks(t, 1 - half)):
                y_send(t, i, 1, src, place(row), mate)
            for i, (src, place) in enumerate(blocks(t, half)):
                y_send(t, i, 0, src, place(row), peer)
        else:
            for i, (src, place) in enumerate(blocks(t, 0)):
                y_send(t, i, 0, src, place(row), up)
                y_send(t, i, 1, src, place(row), down)

    def relay(t):
        if D.cfg[steps[t][0]].split:
            for i, (src, place) in enumerate(blocks(t, half)):
                y_copy(t, i, 1, src, place(mate), mate).wait_recv()
                y_send(t, i, 2, place(mate), place(mate), peer)
        else:
            for i, (src, place) in enumerate(blocks(t, 0)):
                for kind, r, to in ((0, down, up), (1, up, down)):
                    y_copy(t, i, kind, src, place(r), r).wait_recv()
                    if kind == i % 2:
                        y_send(t, i, 2, place(r), place(r), to)

    y_next, issued, ahead, relayed, lead = [0], [0], [AHEAD], [0], [RELAY]

    def relay_to(t):
        while relayed[0] <= min(t, n_steps - 1):
            relay(relayed[0])
            relayed[0] += 1

    def issue_to(t):
        while issued[0] <= min(t, n_steps - 1):
            issue(issued[0])
            issued[0] += 1

    def advance():
        t = y_next[0]
        if t >= n_steps:
            return
        with sc(f"adv{t}"):
            if D.cfg[steps[t][0]].split:
                rest = n_row - 1 - peer
                for i, (src, place) in enumerate(blocks(t, half)):
                    y_copy(t, i, 0, src, place(peer), peer).wait_recv()
                    y_copy(t, i, 2, src, place(rest), rest).wait_recv()
            else:
                for i, (src, place) in enumerate(blocks(t, 0)):
                    y_copy(t, i, 2, src, place(across), across).wait_recv()
            relay_to(t + lead[0])
            issue_to(t + ahead[0])
        y_next[0] = t + 1

    def have(*step):
        while y_next[0] <= step_of[step]:
            advance()

    issue_to(1)

    def w_fetch(l, kind, j, slot):
        C = D.cfg[l]
        i = half if C.split else 0
        copies = []

        def fetch(src, dst):
            copies.append(pltpu.make_async_copy(src, dst, lw.at[slot, len(copies)]))

        def w_rows(a, m, at):
            a, at = rows_at(a, m), pl.ds(at, m)
            fetch(w_t.at[l, a, :], wbuf.at[slot, at, own_lanes(row)])
            for r in (up, down, across):
                fetch(g_w.at[l, a, own_lanes(r)], wbuf.at[slot, at, own_lanes(r)])

        if kind == "q":
            w_rows(i * C.q, C.q, 0)
            at = pl.ds(C.q, D.kvp)
            fetch(wkv_t.at[l], wbuf.at[slot, at, own_lanes(row)])
            for r in (up, down, across):
                fetch(g_kv.at[l, :, own_lanes(r)], wbuf.at[slot, at, own_lanes(r)])
        else:
            w_rows(D.q + i * C.f + j * C.cw, C.cw, 0)
            w_rows(D.q + D.f + i * C.f + j * C.cw, C.cw, C.cw)
        return copies

    def o_fetch(l, j, slot):
        C = D.cfg[l]
        copies = []

        def fetch(src, dst):
            copies.append(pltpu.make_async_copy(src, dst, lo.at[slot, len(copies)]))

        spans = ((half * C.q, 0, C.q), (D.q + half * C.f, C.q, C.f)) if C.split else ((0, 0, C.q + C.f),)
        for a, at, m in spans:
            a, at = rows_at(a, m), pl.ds(at, m)
            to = lambda r: pl.ds(pl.multiple_of(r * och, 128), och)
            fetch(w_o.at[l, a, o_lanes(j, row)], wonat.at[slot, at, to(row)])
            for r in (up, down, across):
                fetch(g_wo.at[l, r, a, o_lanes(j, r)], wonat.at[slot, at, to(r)])
        return copies

    def start(copies):
        for c in copies:
            c.start()

    def wait(copies):
        for c in copies:
            c.wait()

    own_x.wait()
    own_g.wait()

    def x_finish(i):
        s = lax.rem(me + n - i, n)
        remote(xland.at[s], xland.at[s], xs.at[i], xr.at[i], row, col).wait_recv()
        remote(gland.at[s], gland.at[s], gs.at[i], gr.at[i], row, col).wait_recv()
        x_copy(i).wait_send()
        g_copy(i).wait_send()

    with sc("xwait"):
        loop(1, n, x_finish)

    def keep(d):
        hid[rows_at(d * dl, dl), :] = xland[d]

    with sc("gains"):
        loop(0, n, keep)
        g_all = gland[...].astype(F32)
        for l in range(D.layers):
            g_rows = g_all[:, l, :]
            g_rows = jnp.concatenate([g_rows, jnp.zeros((128 - n, 128), F32)], axis=0) if n < 128 else g_rows
            g_cols = g_rows.T
            for d in range(n):
                gcol[l, d * dl : (d + 1) * dl, :] = jnp.broadcast_to(g_cols[:dl, d : d + 1], (dl, 128))

    blk = 64
    n_blk = D.d // blk

    def layer_norm(l):
        def add_up(i, acc):
            v = hid[rows_at(i * blk, blk), :].astype(F32)
            return acc + v.reshape(blk // 8, 8, tok).sum(axis=0)

        mean = lax.fori_loop(0, n_blk, add_up, jnp.zeros((8, tok), F32)).sum(axis=0, keepdims=True) / D.d

        def add_sq(i, acc):
            v = hid[rows_at(i * blk, blk), :].astype(F32) - mean
            return acc + (v * v).reshape(blk // 8, 8, tok).sum(axis=0)

        var = lax.fori_loop(0, n_blk, add_sq, jnp.zeros((8, tok), F32)).sum(axis=0, keepdims=True) / D.d
        scale = lax.rsqrt(var + LN_EPS)

        def write(i):
            rows = rows_at(i * blk, blk)
            g = gcol[l, rows, :]
            g = jnp.concatenate([g] * (tok // 128), axis=1)
            v = (hid[rows, :].astype(F32) - mean) * scale * g
            ht[x, rows, my_lanes] = v.astype(BF16)

        with sc(f"norm{l}"):
            loop(0, n_blk, write)

    d_low, d_high = pl.ds(0, D.d // 2), pl.ds(D.d // 2, D.d // 2)

    class Gather:
        def __init__(self, buf, a):
            self.buf, self.a, self.sends = buf, a, []
            mine = buf.at[x, :, my_lanes]
            for i, c in ((0, right), (1, left), (2, twin)):
                self.send(i, mine, c)

        def send(self, i, ref, c):
            copy = remote(ref, ref, ags.at[self.a, i], agr.at[self.a, i], row, c)
            copy.start()
            self.sends.append(copy)

        def arrived(self, i, ref):
            remote(ref, ref, ags.at[self.a, i], agr.at[self.a, i], row, col).wait_recv()

        def pass_on(self):
            b = self.buf
            with sc(f"pass_on{self.a}"):
                self.arrived(0, b.at[xl_, :, my_lanes])
                self.send(3, b.at[xl_, d_low, my_lanes], right)
                self.send(4, b.at[xl_, :, my_lanes], twin)
                self.arrived(1, b.at[xr_, :, my_lanes])
                self.send(5, b.at[xr_, d_high, my_lanes], left)
                self.send(6, b.at[xr_, :, my_lanes], twin)

        def near(self):
            b = self.buf
            with sc(f"near{self.a}"):
                self.arrived(2, b.at[x, :, twin_lanes])
                self.arrived(4, b.at[xl_, :, twin_lanes])
                self.arrived(6, b.at[xr_, :, twin_lanes])

        def pass_far(self):
            b = self.buf
            with sc(f"pass_far{self.a}"):
                self.arrived(3, b.at[xf_, d_low, my_lanes])
                self.send(7, b.at[xf_, d_low, my_lanes], twin)
                self.arrived(5, b.at[xf_, d_high, my_lanes])
                self.send(8, b.at[xf_, d_high, my_lanes], twin)

        def far(self):
            b = self.buf
            with sc(f"far{self.a}"):
                self.arrived(7, b.at[xf_, d_low, twin_lanes])
                self.arrived(8, b.at[xf_, d_high, twin_lanes])

        def finish(self):
            for c in self.sends:
                c.wait_send()

    half_dim = D.hd // 2

    def near3(i):
        return lax.rem(x + i + i // 2, n_x)

    def all4(i):
        return i

    def far1(i):
        return xf_

    def rope(p):
        lo_, hi_ = p[:half_dim], p[half_dim:]
        return jnp.concatenate([lo_ * cos_ref[...] - hi_ * sin_ref[...], hi_ * cos_ref[...] + lo_ * sin_ref[...]], axis=0)

    def project_q(l, a, seq_of, count):
        C = D.cfg[l]

        def body(i):
            s = seq_of(i)
            p = dot(wbuf[1, : C.q + D.kvp, :], ht[s]).astype(BF16).astype(F32)
            for h in range(C.heads):
                at = rows_at((a * D.seqs + s) * C.q + h * D.hd, D.hd)
                qt[at, :] = (rope(p[h * D.hd : (h + 1) * D.hd]) * D.hd**-0.5).astype(BF16)
            kvland[col, a * D.seqs + s] = p[C.q :].astype(BF16)

        with sc(f"q{l}{a}"):
            loop(0, count, body)

    def kv_send(a):
        own = kvland.at[col, pl.ds(a * D.seqs, D.seqs)]
        copies = [remote(own, own, kvs.at[a, j], kvr.at[a, j], row, lax.rem(col + j, n_col)) for j in range(1, n_col)]
        start(copies)
        return copies

    def kv_arrive(a, copies):
        with sc(f"kvwait{a}"):
            for j in range(1, n_col):
                s = lax.rem(col + n_col - j, n_col)
                ref = kvland.at[s, pl.ds(a * D.seqs, D.seqs)]
                remote(ref, ref, kvs.at[a, j], kvr.at[a, j], row, col).wait_recv()
            for c in copies:
                c.wait_send()

    def key_value(l, a):
        def body(i):
            s = a * D.seqs + i
            raw = kvland[:, s].reshape(n_col * D.kvp, D.seq)
            both = dot(perm_ref[...], raw)
            zeros = jnp.zeros((128 - D.hd, D.seq), F32)
            k_nat = jnp.concatenate([rope(both[: D.hd]), zeros], axis=0).T.astype(BF16)
            kn[s] = k_nat
            vt[s] = both[D.hd :].astype(BF16)
            if a == 0:
                kvbuf[l, 0, i] = k_nat
                kvbuf[l, 1, i] = jnp.concatenate([both[D.hd :], zeros], axis=0).T.astype(BF16)

        with sc(f"kv{l}{a}"):
            loop(0, D.seqs, body)

    qb = D.seq // 2

    def attention(l, a):
        C = D.cfg[l]

        def body(i):
            s, h = a * D.seqs + i // C.heads, lax.rem(i, C.heads)
            q_rows = rows_at(s * C.q + h * D.hd, D.hd)
            o_rows = rows_at(s * (C.q + C.f) + h * D.hd, D.hd)
            for b in range(2):
                ext = (b + 1) * qb
                lanes = slice(b * qb, (b + 1) * qb)
                score = dot(kn[s, :ext, : D.hd], qt[q_rows, lanes])
                keys = lax.broadcasted_iota(jnp.int32, (ext, qb), 0)
                queries = lax.broadcasted_iota(jnp.int32, (ext, qb), 1) + b * qb
                score = jnp.where(keys <= queries, score, -1e30)
                p = jnp.exp(score - jnp.max(score, axis=0, keepdims=True))
                p = (p * (1.0 / jnp.sum(p, axis=0, keepdims=True))).astype(BF16)
                jt[o_rows, lanes] = dot(vt[s, :, :ext], p).astype(BF16)

        with sc(f"attn{l}{a}"):
            loop(0, D.seqs * C.heads, body)

    def gate_up(l, a, slot, j, seq_of, count):
        C = D.cfg[l]

        def body(i):
            s = seq_of(i)
            p = dot(wbuf[slot, : 2 * C.cw, :], ht[s])
            g = p[: C.cw].astype(BF16).astype(F32)
            u = p[C.cw :].astype(BF16).astype(F32)
            jt[rows_at((a * D.seqs + s) * (C.q + C.f) + C.q + j * C.cw, C.cw), :] = (g * jax.nn.sigmoid(g) * u).astype(BF16)

        loop(0, count, body)

    def gate_up_loop(l, a, seq_of, count, first, last):
        C = D.cfg[l]
        have_chunk(l, min(last, C.n_c - 1))

        def body(j):
            slot = lax.rem(j, 2)
            wait(w_fetch(l, "f", j, slot))

            @pl.when(j + 1 < C.n_c)
            def _():
                start(w_fetch(l, "f", j + 1, 1 - slot))

            gate_up(l, a, slot, j, seq_of, count)

        with sc(f"gu{l}{a}"):
            loop(first, last, body)

    def have_chunk(l, j):
        C = D.cfg[l]
        have(l, "f", (j + 1) * C.cw // fch - 1)

    def load_q(l):
        have(l, "q", 0)
        copies = w_fetch(l, "q", 0, 1)
        start(copies)
        wait(copies)

    m = och * n_row
    m_low, m_high = pl.ds(0, m // 2), pl.ds(m // 2, m // 2)
    r_slots = twin_in.shape[0]
    r_step = 64

    def order(i):
        return lax.rem(x + lax.rem(2 + 3 * i, 4), n_x)

    class Reduce:
        def __init__(self, l):
            self.l, self.C, self.sends = l, D.cfg[l], {}

        def send(self, u, i, src, dst, c):
            copy = remote(src, dst, rss.at[u % r_slots, i], rsr.at[u % r_slots, i], row, c)
            copy.start()
            self.sends[u].append(copy)

        def arrived(self, u, i, ref):
            remote(ref, ref, rss.at[u % r_slots, i], rsr.at[u % r_slots, i], row, col).wait_recv()

        def twin_copy(self, u, i):
            us = u % r_slots
            return remote(ot.at[u % 2, order(i), :, twin_lanes], twin_in.at[us, i], rss.at[us, i], rsr.at[us, i], row, twin)

        def twin_done(self, u):
            loop(0, 4, lambda i: self.twin_copy(u, i).wait_send())

        def stage_a(self, u, a):
            C = self.C
            if u >= 2:
                self.twin_done(u - 2)
            if u >= r_slots - 1:
                for c in self.sends.pop(u - r_slots + 1):
                    c.wait_send()
            self.sends[u] = []
            R = C.q + C.f

            def body(i):
                s = order(i)
                ot[u % 2, s] = dot(wobuf[:, :R], jt[rows_at((a * D.seqs + s) * R, R), :]).astype(BF16)
                self.twin_copy(u, i).start()

            with sc(f"sa{self.l}_{u}"):
                loop(0, 4, body)

        def stage_b(self, u):
            us = u % r_slots

            def body(i):
                self.arrived(u, i, twin_in.at[us, i])
                s = order(i)

                def add(b):
                    at = rows_at(b * r_step, r_step)
                    twin_in[us, i, at, :] = (ot[u % 2, s, at, my_lanes].astype(F32) + twin_in[us, i, at, :].astype(F32)).astype(BF16)

                loop(0, m // r_step, add)

            with sc(f"sb{self.l}_{u}"):
                loop(0, 1, body)
                self.send(u, 4, twin_in.at[us, 0, m_low], far_in.at[us, m_low], right)
                self.send(u, 5, twin_in.at[us, 0, m_high], far_in.at[us, m_high], left)
                loop(1, 4, body)

        def stage_c(self, u):
            us = u % r_slots

            def add_far(i, base):
                def add(b):
                    at = rows_at(base + b * r_step, r_step)
                    twin_in[us, i, at, :] = (twin_in[us, i, at, :].astype(F32) + far_in[us, at, :].astype(F32)).astype(BF16)

                loop(0, m // 2 // r_step, add)

            with sc(f"sc{self.l}_{u}"):
                self.arrived(u, 4, far_in.at[us, m_low])
                add_far(1, 0)
                self.send(u, 6, twin_in.at[us, 1], near_in.at[us, 0], right)
                self.arrived(u, 5, far_in.at[us, m_high])
                add_far(3, m // 2)
                self.send(u, 7, twin_in.at[us, 3], near_in.at[us, 1], left)

        def add_update(self, j, total):
            step = min(r_step, och)
            for r in range(n_row):

                def add(b, r=r):
                    dst = rows_at(r * dr + (r + j) % D.n_o * och + b * step, step)
                    u = total(rows_at(r * och + b * step, step)).astype(BF16).astype(F32)
                    hid[dst, :] = (hid[dst, :].astype(F32) + u).astype(BF16)

                loop(0, och // step, add)

        def stage_d(self, u, j, a):
            us = u % r_slots

            def total(at):
                return twin_in[us, 2, at, :].astype(F32) + near_in[us, 0, at, :].astype(F32) + near_in[us, 1, at, :].astype(F32)

            with sc(f"sd{self.l}_{u}"):
                self.arrived(u, 6, near_in.at[us, 0])
                self.arrived(u, 7, near_in.at[us, 1])
                if self.C.split:

                    def save(b):
                        at = rows_at(b * r_step, r_step)
                        psum[a, j, at, :] = total(at).astype(BF16)

                    loop(0, m // r_step, save)
                    if a == 1:
                        remote(psum.at[1, j], pair_in.at[j], es.at[j], er.at[j], mate, col).start()
                else:
                    self.add_update(j, total)

        def stage_e(self, j):
            with sc(f"se{self.l}_{j}"):
                c = remote(psum.at[1, j], pair_in.at[j], es.at[j], er.at[j], mate, col)
                c.wait_recv()
                self.add_update(j, lambda at: psum[0, j, at, :].astype(F32) + pair_in[j, at, :].astype(F32))
                c.wait_send()

        def finish(self, units):
            with sc(f"rfin{self.l}"):
                for u in range(max(0, units - 2), units):
                    self.twin_done(u)
                for u in self.sends:
                    for c in self.sends[u]:
                        c.wait_send()

    o_started = set()

    def o_load(l, j, a):
        if (l, j, a) not in o_started:
            have(l, "o", j)
            start(o_fetch(l, j, j % 2))
            o_started.add((l, j, a))

    def o_use(l, j, a):
        C = D.cfg[l]
        with sc(f"ouse{l}_{j}"):
            o_load(l, j, a)
            wait(o_fetch(l, j, j % 2))
            if j + 1 < D.n_o and y_next[0] > step_of[(l, "o", j + 1)]:
                o_load(l, j + 1, a)
            R = C.q + C.f
            for r in range(n_row):
                wobuf[r * och : (r + 1) * och, :R] = wonat[j % 2, :R, r * och : (r + 1) * och].T

    layer_norm(0)
    g0 = Gather(ht, 0)
    mine = ht.at[x, :, my_lanes]
    shared = g_h.at[x, :, my_lanes]
    to_mate = remote(mine, shared, ps, pr_, mate, col)
    to_mate.start()
    with sc("relay0"):
        relay_to(RELAY - 1)
    issue_to(AHEAD - 1)
    advance()
    advance()
    g0.pass_on()
    with sc("mate"):
        to_mate.wait_recv()
    g1 = Gather(g_h, 1)
    load_q(0)
    g0.near()
    project_q(0, 0, near3, 3)
    g0.pass_far()
    g0.far()
    project_q(0, 0, far1, 1)
    sent = kv_send(0)
    n_f = D.cfg[0].n_f
    f_started = set()

    def f_load(j):
        if j not in f_started:
            f_started.add(j)
            start(w_fetch(0, "f", j, j % 2))

    def h_copy(i):
        return pltpu.make_async_copy(g_h.at[i], ht.at[i], lh.at[i])

    for j in range(n_f):
        if j == n_f - 1:
            g1.pass_on()
        have(0, "f", j)
        f_load(j)
        with sc(f"gu0_{j}"):
            wait(w_fetch(0, "f", j, j % 2))
            if j + 1 < n_f and y_next[0] > step_of[(0, "f", j + 1)]:
                f_load(j + 1)
            gate_up(0, 0, j % 2, j, all4, 4)
    g0.finish()
    to_mate.wait_send()
    g1.near()
    loop(0, 3, lambda i: h_copy(near3(i)).start())
    kv_arrive(0, sent)
    key_value(0, 0)
    attention(0, 0)
    g1.pass_far()

    red = Reduce(0)
    units = [(j, a) for a in (0, 1) for j in range(D.n_o)]
    n_u = len(units)
    state = {"e": 0}

    def unit(u):
        j, a = units[u]
        o_use(0, j, a)
        red.stage_a(u, a)
        if u >= 2:
            red.stage_c(u - 2)
        if u >= 3:
            red.stage_d(u - 3, *units[u - 3])
        red.stage_b(u)
        if u >= D.n_o + 4:
            red.stage_e(state["e"])
            state["e"] += 1

    unit(0)
    load_q(0)
    loop(0, 3, lambda i: h_copy(near3(i)).wait())
    project_q(0, 1, near3, 3)
    g1.far()
    h_copy(xf_).start()
    start(w_fetch(0, "f", 0, 0))
    h_copy(xf_).wait()
    project_q(0, 1, far1, 1)
    sent = kv_send(1)
    cuts = [n_f * i // D.n_o for i in range(D.n_o + 1)]
    for u in range(1, D.n_o):
        unit(u)
        if cuts[u] > cuts[u - 1]:
            gate_up_loop(0, 1, all4, 4, cuts[u - 1], cuts[u])
    gate_up_loop(0, 1, all4, 4, cuts[-2], n_f)
    advance()
    kv_arrive(1, sent)
    key_value(0, 1)
    attention(0, 1)
    g1.finish()
    for u in range(D.n_o, n_u):
        unit(u)
        if u >= n_u - 3:
            ahead[0], lead[0] = 2, 1
        advance()
    red.stage_c(n_u - 2)
    red.stage_d(n_u - 3, *units[n_u - 3])
    red.stage_c(n_u - 1)
    red.stage_d(n_u - 2, *units[n_u - 2])
    red.stage_d(n_u - 1, *units[n_u - 1])
    ahead[0], lead[0] = AHEAD, RELAY
    issue_to(y_next[0] - 1 + AHEAD)
    for j in range(state["e"], D.n_o):
        red.stage_e(j)
    red.finish(n_u)

    def y_copy_back(i):
        d = lax.rem(me + i, n)
        return remote(hid.at[rows_at(d * dl, dl), :], piece_of(y_out, me), xs.at[i], xr.at[i], d // n_col, lax.rem(d, n_col))

    own_y = pltpu.make_async_copy(hid.at[rows_at(me * dl, dl), :], piece_of(y_out, me), xr.at[0])

    def y_send_back(d):
        i = lax.rem(d - me + n, n)

        @pl.when(i == 0)
        def _():
            own_y.start()

        @pl.when(i != 0)
        def _():
            y_copy_back(i).start()

    def y_ready(j):
        out = []
        for d in range(n):
            r, a = d // n_col, d % n_col * dl
            last_j = max((b - r) % D.n_o for b in range(a // och, (a + dl - 1) // och + 1))
            if last_j == j:
                out.append(d)
        return out

    for l in range(1, D.layers):
        C = D.cfg[l]
        layer_norm(l)
        g0 = Gather(ht, 0)
        for _ in range(4):
            advance()
        g0.pass_on()
        load_q(l)
        have_chunk(l, 0)
        start(w_fetch(l, "f", 0, 0))
        g0.near()
        project_q(l, 0, near3, 3)
        n_mid = C.n_c // 2
        gate_up_loop(l, 0, near3, 3, 0, n_mid)
        g0.pass_far()
        gate_up_loop(l, 0, near3, 3, n_mid, C.n_c)
        load_q(l)
        start(w_fetch(l, "f", 0, 0))
        g0.far()
        project_q(l, 0, far1, 1)
        sent = kv_send(0)
        gate_up_loop(l, 0, far1, 1, 0, C.n_c)
        have(l, "o", 0)
        o_load(l, 0, 0)
        g0.finish()
        kv_arrive(0, sent)
        key_value(l, 0)
        attention(l, 0)
        red = Reduce(l)
        last = l + 1 == D.layers

        def send_final(j):
            if last:
                for d in y_ready(j):
                    y_send_back(d)

        end = D.n_o - 1
        for j in range(D.n_o):
            if j == end:
                red.stage_c(j - 1)
                red.stage_d(j - 2, j - 2, 0)
                send_final(j - 2)
            o_use(l, j, 0)
            red.stage_a(j, 0)
            if 1 <= j < end:
                red.stage_c(j - 1)
            if 2 <= j < end:
                red.stage_d(j - 2, j - 2, 0)
                send_final(j - 2)
            red.stage_b(j)
        red.stage_d(end - 1, end - 1, 0)
        red.stage_c(end)
        send_final(end - 1)
        red.stage_d(end, end, 0)
        send_final(end)
        red.finish(D.n_o)

    def kv_back(i):
        r = lax.rem(row + i, n_row)
        pos = rows_at((r * n_col + col) * D.pos, D.pos)
        return kvbuf.at[:, :, :, pos, :], kv_out.at[:, :, pl.ds(row * D.seqs, D.seqs)], r

    src, dst, _ = kv_back(0)
    own_kv = pltpu.make_async_copy(src, dst, fl)
    own_kv.start()
    kv_sends = []
    for i in range(1, n_row):
        src, dst, r = kv_back(i)
        c = remote(src, dst, fs.at[i], fr.at[i], r, col)
        c.start()
        kv_sends.append(c)

    def y_finish(i):
        s = lax.rem(me + n - i, n)
        remote(piece_of(y_out, s), piece_of(y_out, s), xs.at[i], xr.at[i], row, col).wait_recv()
        y_copy_back(i).wait_send()

    with sc("ywait"):
        loop(1, n, y_finish)
        own_y.wait()
        own_kv.wait()
        for i in range(1, n_row):
            r = lax.rem(row + n_row - i, n_row)
            dst = kv_out.at[:, :, pl.ds(r * D.seqs, D.seqs)]
            remote(dst, dst, fs.at[i], fr.at[i], row, col).wait_recv()
        for c in kv_sends:
            c.wait_send()
        for t in sorted(pending):
            drain(t)


def solution(mesh):
    n_row, n_col = mesh.shape["row"], mesh.shape["col"]
    group = n_row * n_col
    act_spec = P("dp", None, ("row", "col"))
    weight_spec = P(None, "row", "col")

    def device_fn(x_loc, gain_loc, w_in_loc, w_kv_loc, w_out_loc):
        D = Dims()
        D.n_row, D.n_col = n_row, n_col
        n_batch, D.seq, D.dl = x_loc.shape
        D.layers, D.dr, e = w_in_loc.shape
        D.d = D.dl * group
        r_block = w_out_loc.shape[1]
        D.f = e - r_block
        D.q = r_block - D.f
        kv_local = w_kv_loc.shape[2]
        D.hd = kv_local * n_col // 2
        D.kvp = 32
        D.tok = n_batch * D.seq // group
        D.seqs = n_batch // n_row
        D.pos = D.seq // group
        D.fch = 128
        D.och = 128
        D.n_o = D.dr // D.och
        D.cfg = []
        for l in range(D.layers):
            C = Dims()
            C.split = l == 0
            parts = 2 if C.split else 1
            C.q, C.f = D.q // parts, D.f // parts
            C.heads, C.n_f = C.q // D.hd, C.f // D.fch
            C.cw = D.fch if C.split else 2 * D.fch
            C.n_c = C.f // C.cw
            D.cfg.append(C)
        assert D.seq == 2 * D.tok and D.seqs == n_col // 2 == n_row == 4

        half = D.hd // 2
        inv_freq = (np.float32(1.0) / (np.float32(10000.0) ** (np.arange(half, dtype=np.float32) * np.float32(2.0) / np.float32(D.hd)))).astype(np.float32)
        angles = (inv_freq[:, None] * np.arange(D.seq, dtype=np.float32)[None, :]).astype(np.float32)
        cos_t, sin_t = np.cos(angles).astype(np.float32), np.sin(angles).astype(np.float32)
        perm = np.zeros((2 * D.hd, n_col * D.kvp), np.float32)
        for i in range(2 * D.hd):
            perm[i, (i // kv_local) * D.kvp + i % kv_local] = 1.0

        x_t = x_loc.transpose(0, 2, 1)
        w_t = w_in_loc.transpose(0, 2, 1)
        wkv_t = jnp.pad(w_kv_loc.transpose(0, 2, 1), ((0, 0), (0, D.kvp - kv_local), (0, 0)))
        gains = jnp.pad(gain_loc, ((0, 16 - D.layers), (0, 128 - D.dl)))

        m = D.och * n_row
        sds = jax.ShapeDtypeStruct
        dma = pltpu.SemaphoreType.DMA
        out = pl.pallas_call(
            functools.partial(kernel, D),
            out_shape=(
                sds(x_t.shape, BF16),
                sds((D.layers, 2, n_batch, D.pos, 128), BF16),
                sds((D.layers, e, D.d), BF16),
                sds((D.layers, D.kvp, D.d), BF16),
                sds((D.layers, n_row, r_block, D.dr), BF16),
                sds((D.seqs, D.d, D.seq), BF16),
            ),
            in_specs=[ANY] * 5 + [VMEM] * 3,
            out_specs=(ANY,) * 6,
            scratch_shapes=[
                pltpu.VMEM((group, D.dl, D.tok), BF16),
                pltpu.VMEM((group, 16, 128), BF16),
                pltpu.VMEM((D.layers, D.d, 128), F32),
                pltpu.VMEM((D.d, D.tok), BF16),
                pltpu.VMEM((D.seqs, D.d, D.seq), BF16),
                pltpu.VMEM((2, max(4 * D.fch, D.q + D.kvp), D.d), BF16),
                pltpu.VMEM((2, r_block, m), BF16),
                pltpu.VMEM((m, r_block), BF16),
                pltpu.VMEM((D.seqs * D.q, D.seq), BF16),
                pltpu.VMEM((n_col, 2 * D.seqs, D.kvp, D.seq), BF16),
                pltpu.VMEM((2 * D.seqs, D.seq, 128), BF16),
                pltpu.VMEM((2 * D.seqs, D.hd, D.seq), BF16),
                pltpu.VMEM((D.layers, 2, D.seqs, D.seq, 128), BF16),
                pltpu.VMEM((D.seqs * r_block, D.seq), BF16),
                pltpu.VMEM((2, D.seqs, m, D.seq), BF16),
                pltpu.VMEM((5, 4, m, D.tok), BF16),
                pltpu.VMEM((5, m, D.tok), BF16),
                pltpu.VMEM((5, 2, m, D.tok), BF16),
                pltpu.VMEM((2, D.n_o, m, D.tok), BF16),
                pltpu.VMEM((D.n_o, m, D.tok), BF16),
                dma((group,)), dma((group,)), dma((group,)), dma((group,)),
                dma((SLOTS, 4, 3)), dma((SLOTS, 4, 3)),
                dma((2, 9)), dma((2, 9)), dma, dma,
                dma((2, n_col)), dma((2, n_col)),
                dma((5, 8)), dma((5, 8)),
                dma((D.n_o,)), dma((D.n_o,)),
                dma((2, 8)), dma((2, 8)), dma((D.seqs,)),
                dma((n_row,)), dma((n_row,)), dma,
            ],
            compiler_params=pltpu.CompilerParams(collective_id=0, has_side_effects=True, vmem_limit_bytes=67_000_000),
            name="two_layers",
        )(x_t, gains, w_t, wkv_t, w_out_loc, jnp.asarray(cos_t), jnp.asarray(sin_t), jnp.asarray(perm, BF16))
        return out[0].transpose(0, 2, 1), out[1][..., : D.hd]

    return jax.shard_map(device_fn, mesh=mesh, in_specs=(act_spec, P(None, ("row", "col")), weight_spec, weight_spec, P(None, "col", "row")), out_specs=(act_spec, P(None, None, "dp", ("row", "col"), None)), check_vma=False)
```

```python
import functools

import numpy as np

import jax
import jax.numpy as jnp
from jax import lax
from jax.experimental import pallas as pl
from jax.experimental.pallas import tpu as pltpu
from jax.sharding import PartitionSpec as P

LN_EPS = 1e-6
MESH = pl.DeviceIdType.MESH
ANY = pl.BlockSpec(memory_space=pl.ANY)
VMEM = pl.BlockSpec(memory_space=pltpu.VMEM)
F32, BF16 = jnp.float32, jnp.bfloat16
SLOTS = 16
AHEAD = 4
FAR_AHEAD = 9
RELAY = 2


def dot(a, b):
    return jnp.dot(a, b, preferred_element_type=F32)


class Dims:
    pass


def rows_at(start, count, by=16):
    return pl.ds(start if isinstance(start, int) else pl.multiple_of(start, by), count)


def kernel(
    D,
    x_t, gains, w_t, wkv_t, w_o, cos_ref, sin_ref, perm_ref,
    y_out, kv_out, g_w, g_kv, g_wo, g_h,
    xland, gland, gcol, hid, ht, wbuf, wonat, wobuf, qt, kvland, kn, vt, kvbuf, jt, ot, twin_in, far_in, near_in, psum, pair_in,
    xs, xr, gs, gr, ys, yr, ags, agr, ps, pr_, kvs, kvr, rss, rsr, es, er, lw, lo, lh, fs, fr, fl,
):
    sc = jax.named_scope
    row, col = lax.axis_index("row"), lax.axis_index("col")
    n_row, n_col, n = D.n_row, D.n_col, D.n_row * D.n_col
    n_x = n_col // 2
    me = row * n_col + col
    x, k = col // 2, lax.rem(col, 2)
    xr_, xl_, xf_ = lax.rem(x + 1, n_x), lax.rem(x + n_x - 1, n_x), lax.rem(x + 2, n_x)
    right, left, twin = xr_ * 2 + k, xl_ * 2 + k, x * 2 + 1 - k
    up, down, across = lax.rem(row + 1, n_row), lax.rem(row + n_row - 1, n_row), lax.rem(row + 2, n_row)
    half, mate = row // 2, n_row - 1 - row
    peer = row + 1 - 2 * lax.rem(row, 2)
    tok, dl, dr = D.tok, D.dl, D.dr
    och, fch = D.och, D.fch
    my_lanes = pl.ds(pl.multiple_of(k * tok, 128), tok)
    twin_lanes = pl.ds(pl.multiple_of((1 - k) * tok, 128), tok)

    def remote(src, dst, ssem, rsem, r, c):
        return pltpu.make_async_remote_copy(src_ref=src, dst_ref=dst, send_sem=ssem, recv_sem=rsem, device_id={"row": r, "col": c}, device_id_type=MESH)

    def loop(lo_, hi_, f):
        def body(i, carry):
            f(i)
            return carry

        lax.fori_loop(lo_, hi_, body, 0)

    barrier = pltpu.get_barrier_semaphore()

    def greet(i):
        d = lax.rem(me + i, n)
        pl.semaphore_signal(barrier, inc=1, device_id={"row": d // n_col, "col": lax.rem(d, n_col)}, device_id_type=MESH)

    with sc("barrier"):
        loop(1, n, greet)
        pl.semaphore_wait(barrier, n - 1)

    def piece_of(ref, d):
        return ref.at[d // 2, :, pl.ds(pl.multiple_of(lax.rem(d, 2) * tok, 128), tok)]

    def x_copy(i):
        d = lax.rem(me + i, n)
        return remote(piece_of(x_t, d), xland.at[me], xs.at[i], xr.at[i], d // n_col, lax.rem(d, n_col))

    def g_copy(i):
        d = lax.rem(me + i, n)
        return remote(gains, gland.at[me], gs.at[i], gr.at[i], d // n_col, lax.rem(d, n_col))

    def x_start(i):
        x_copy(i).start()
        g_copy(i).start()

    own_x = pltpu.make_async_copy(piece_of(x_t, me), xland.at[me], xr.at[0])
    own_g = pltpu.make_async_copy(gains, gland.at[me], gr.at[0])
    own_x.start()
    own_g.start()
    loop(1, n, x_start)

    def own_lanes(r):
        return pl.ds(pl.multiple_of(r * dr, 128), dr)

    def o_lanes(j, r):
        return pl.ds(pl.multiple_of(lax.rem(r + j, D.n_o) * och, 128), och)

    steps = []
    for l, C in enumerate(D.cfg):
        steps += [(l, "q", 0)] + [(l, "f", j) for j in range(C.n_f)] + [(l, "o", j) for j in range(D.n_o)]
    n_steps = len(steps)
    step_of = {s: t for t, s in enumerate(steps)}

    def blocks(t, i):
        l, kind, j = steps[t]
        C = D.cfg[l]
        out = []

        def w_rows(a, m):
            at = rows_at(a, m)
            out.append((w_t.at[l, at, :], lambda r: g_w.at[l, at, own_lanes(r)]))

        def o_rows(a, m):
            at = rows_at(a, m)
            out.append((w_o.at[l, at, o_lanes(j, row)], lambda r: g_wo.at[l, r, at, o_lanes(j, r)]))

        def kv_rows(a, m):
            at = pl.ds(a, m)
            out.append((wkv_t.at[l, at, :], lambda r: g_kv.at[l, at, own_lanes(r)]))

        if kind == "q":
            for a in (0, C.q // 2):
                w_rows(i * C.q + a, C.q // 2)
            for a in (0, D.kvp // 2):
                kv_rows(a, D.kvp // 2)
        elif kind == "f":
            w_rows(D.q + i * C.f + j * fch, fch)
            w_rows(D.q + D.f + i * C.f + j * fch, fch)
        elif C.split:
            o_rows(i * C.q, C.q)
            o_rows(D.q + i * C.f, C.f)
        else:
            for a in (0, (D.q + D.f) // 2):
                o_rows(a, (D.q + D.f) // 2)
        return out

    pending = {}

    def y_copy(t, i, kind, src, dst, r):
        return remote(src, dst, ys.at[t % SLOTS, i, kind], yr.at[t % SLOTS, i, kind], r, col)

    def drain(t):
        for c in pending.pop(t, ()):
            c.wait_send()

    def y_send(t, *args):
        c = y_copy(t, *args)
        c.start()
        pending[t].append(c)

    def issue_peer(t):
        for i, (src, place) in enumerate(blocks(t, half if D.cfg[steps[t][0]].split else 0)):
            y_send(t, i, 0, src, place(row), peer)

    def issue_mate(t):
        drain(t - SLOTS)
        pending[t] = []
        for i, (src, place) in enumerate(blocks(t, 1 - half if D.cfg[steps[t][0]].split else 0)):
            y_send(t, i, 1, src, place(row), mate)

    def relay(t):
        split = D.cfg[steps[t][0]].split
        for i, (src, place) in enumerate(blocks(t, half if split else 0)):
            y_copy(t, i, 1, src, place(mate), mate).wait_recv()
            if split or i % 2 == 0:
                y_send(t, i, 2, place(mate), place(mate), peer)
            if not split:
                y_copy(t, i, 0, src, place(peer), peer).wait_recv()
                if i % 2 == 1:
                    y_send(t, i, 2, place(peer), place(peer), mate)

    at, lead = {"next": 0, "peer": 0, "mate": 0, "relay": 0}, {"peer": AHEAD, "mate": AHEAD, "relay": 0}

    def run_to(kind, t):
        while at[kind] <= min(t, n_steps - 1):
            {"peer": issue_peer, "mate": issue_mate, "relay": relay}[kind](at[kind])
            at[kind] += 1

    def catch_up():
        for kind in ("mate", "relay", "peer"):
            run_to(kind, at["next"] - 1 + lead[kind])

    def advance():
        t = at["next"]
        if t >= n_steps:
            return
        rest = n_row - 1 - peer
        with sc(f"adv{t}"):
            split = D.cfg[steps[t][0]].split
            for i, (src, place) in enumerate(blocks(t, half if split else 0)):
                if split:
                    y_copy(t, i, 0, src, place(peer), peer).wait_recv()
                y_copy(t, i, 2, src, place(rest), rest).wait_recv()
            at["next"] = t + 1
            catch_up()

    def have(*step):
        while at["next"] <= step_of[step]:
            advance()

    for t in range(2):
        run_to("mate", t)
        run_to("peer", t)

    def w_fetch(l, kind, j, slot):
        C = D.cfg[l]
        i = half if C.split else 0
        copies = []

        def fetch(src, dst):
            copies.append(pltpu.make_async_copy(src, dst, lw.at[slot, len(copies)]))

        def w_rows(a, m, at):
            a, at = rows_at(a, m), pl.ds(at, m)
            fetch(w_t.at[l, a, :], wbuf.at[slot, at, own_lanes(row)])
            for r in (up, down, across):
                fetch(g_w.at[l, a, own_lanes(r)], wbuf.at[slot, at, own_lanes(r)])

        if kind == "q":
            w_rows(i * C.q, C.q, 0)
            at = pl.ds(C.q, D.kvp)
            fetch(wkv_t.at[l], wbuf.at[slot, at, own_lanes(row)])
            for r in (up, down, across):
                fetch(g_kv.at[l, :, own_lanes(r)], wbuf.at[slot, at, own_lanes(r)])
        else:
            w_rows(D.q + i * C.f + j * C.cw, C.cw, 0)
            w_rows(D.q + D.f + i * C.f + j * C.cw, C.cw, C.cw)
        return copies

    def o_fetch(l, j, slot):
        C = D.cfg[l]
        copies = []

        def fetch(src, dst):
            copies.append(pltpu.make_async_copy(src, dst, lo.at[slot, len(copies)]))

        spans = ((half * C.q, 0, C.q), (D.q + half * C.f, C.q, C.f)) if C.split else ((0, 0, C.q + C.f),)
        for a, at, m in spans:
            a, at = rows_at(a, m), pl.ds(at, m)
            to = lambda r: pl.ds(pl.multiple_of(r * och, 128), och)
            fetch(w_o.at[l, a, o_lanes(j, row)], wonat.at[slot, at, to(row)])
            for r in (up, down, across):
                fetch(g_wo.at[l, r, a, o_lanes(j, r)], wonat.at[slot, at, to(r)])
        return copies

    def start(copies):
        for c in copies:
            c.start()

    def wait(copies):
        for c in copies:
            c.wait()

    own_x.wait()
    own_g.wait()

    def x_finish(i):
        s = lax.rem(me + n - i, n)
        remote(xland.at[s], xland.at[s], xs.at[i], xr.at[i], row, col).wait_recv()
        remote(gland.at[s], gland.at[s], gs.at[i], gr.at[i], row, col).wait_recv()
        x_copy(i).wait_send()
        g_copy(i).wait_send()

    with sc("xwait"):
        loop(1, n, x_finish)

    def keep(d):
        hid[rows_at(d * dl, dl), :] = xland[d]

    with sc("gains"):
        loop(0, n, keep)
        g_all = gland[...].astype(F32)
        for l in range(D.layers):
            g_rows = g_all[:, l, :]
            g_rows = jnp.concatenate([g_rows, jnp.zeros((128 - n, 128), F32)], axis=0) if n < 128 else g_rows
            g_cols = g_rows.T
            for d in range(n):
                gcol[l, d * dl : (d + 1) * dl, :] = jnp.broadcast_to(g_cols[:dl, d : d + 1], (dl, 128))

    blk = 64
    n_blk = D.d // blk

    def layer_norm(l):
        def add_up(i, acc):
            v = hid[rows_at(i * blk, blk), :].astype(F32)
            return acc + v.reshape(blk // 8, 8, tok).sum(axis=0)

        mean = lax.fori_loop(0, n_blk, add_up, jnp.zeros((8, tok), F32)).sum(axis=0, keepdims=True) / D.d

        def add_sq(i, acc):
            v = hid[rows_at(i * blk, blk), :].astype(F32) - mean
            return acc + (v * v).reshape(blk // 8, 8, tok).sum(axis=0)

        var = lax.fori_loop(0, n_blk, add_sq, jnp.zeros((8, tok), F32)).sum(axis=0, keepdims=True) / D.d
        scale = lax.rsqrt(var + LN_EPS)

        def write(i):
            rows = rows_at(i * blk, blk)
            g = gcol[l, rows, :]
            g = jnp.concatenate([g] * (tok // 128), axis=1)
            v = (hid[rows, :].astype(F32) - mean) * scale * g
            ht[x, rows, my_lanes] = v.astype(BF16)

        with sc(f"norm{l}"):
            loop(0, n_blk, write)

    d_low, d_high = pl.ds(0, D.d // 2), pl.ds(D.d // 2, D.d // 2)

    class Gather:
        def __init__(self, buf, a):
            self.buf, self.a, self.sends = buf, a, []
            mine = buf.at[x, :, my_lanes]
            for i, c in ((0, right), (1, left), (2, twin)):
                self.send(i, mine, c)

        def send(self, i, ref, c):
            copy = remote(ref, ref, ags.at[self.a, i], agr.at[self.a, i], row, c)
            copy.start()
            self.sends.append(copy)

        def arrived(self, i, ref):
            remote(ref, ref, ags.at[self.a, i], agr.at[self.a, i], row, col).wait_recv()

        def pass_on(self):
            b = self.buf
            with sc(f"pass_on{self.a}"):
                self.arrived(0, b.at[xl_, :, my_lanes])
                self.send(3, b.at[xl_, d_low, my_lanes], right)
                self.send(4, b.at[xl_, :, my_lanes], twin)
                self.arrived(1, b.at[xr_, :, my_lanes])
                self.send(5, b.at[xr_, d_high, my_lanes], left)
                self.send(6, b.at[xr_, :, my_lanes], twin)

        def own(self):
            self.arrived(2, self.buf.at[x, :, twin_lanes])

        def near(self):
            b = self.buf
            with sc(f"near{self.a}"):
                self.arrived(4, b.at[xl_, :, twin_lanes])
                self.arrived(6, b.at[xr_, :, twin_lanes])

        def pass_far(self):
            b = self.buf
            with sc(f"pass_far{self.a}"):
                self.arrived(3, b.at[xf_, d_low, my_lanes])
                self.send(7, b.at[xf_, d_low, my_lanes], twin)
                self.arrived(5, b.at[xf_, d_high, my_lanes])
                self.send(8, b.at[xf_, d_high, my_lanes], twin)

        def far(self):
            b = self.buf
            with sc(f"far{self.a}"):
                self.arrived(7, b.at[xf_, d_low, twin_lanes])
                self.arrived(8, b.at[xf_, d_high, twin_lanes])

        def finish(self):
            for c in self.sends:
                c.wait_send()

    half_dim = D.hd // 2

    def near3(i):
        return lax.rem(x + i + i // 2, n_x)

    def all4(i):
        return i

    def far1(i):
        return xf_

    def rope(p):
        lo_, hi_ = p[:half_dim], p[half_dim:]
        return jnp.concatenate([lo_ * cos_ref[...] - hi_ * sin_ref[...], hi_ * cos_ref[...] + lo_ * sin_ref[...]], axis=0)

    def project_q(l, a, seq_of, count):
        C = D.cfg[l]

        def body(i):
            s = seq_of(i)
            p = dot(wbuf[1, : C.q + D.kvp, :], ht[s]).astype(BF16).astype(F32)
            for h in range(C.heads):
                at = rows_at((a * D.seqs + s) * C.q + h * D.hd, D.hd)
                qt[at, :] = (rope(p[h * D.hd : (h + 1) * D.hd]) * D.hd**-0.5).astype(BF16)
            kvland[col, a * D.seqs + s] = p[C.q :].astype(BF16)

        with sc(f"q{l}{a}"):
            loop(0, count, body)

    def kv_send(a):
        own = kvland.at[col, pl.ds(a * D.seqs, D.seqs)]
        copies = [remote(own, own, kvs.at[a, j], kvr.at[a, j], row, lax.rem(col + j, n_col)) for j in range(1, n_col)]
        start(copies)
        return copies

    def kv_arrive(a, copies):
        with sc(f"kvwait{a}"):
            for j in range(1, n_col):
                s = lax.rem(col + n_col - j, n_col)
                ref = kvland.at[s, pl.ds(a * D.seqs, D.seqs)]
                remote(ref, ref, kvs.at[a, j], kvr.at[a, j], row, col).wait_recv()
            for c in copies:
                c.wait_send()

    def key_value(l, a):
        def body(i):
            s = a * D.seqs + i
            raw = kvland[:, s].reshape(n_col * D.kvp, D.seq)
            both = dot(perm_ref[...], raw)
            zeros = jnp.zeros((128 - D.hd, D.seq), F32)
            k_nat = jnp.concatenate([rope(both[: D.hd]), zeros], axis=0).T.astype(BF16)
            kn[s] = k_nat
            vt[s] = both[D.hd :].astype(BF16)
            if a == 0:
                kvbuf[l, 0, i] = k_nat
                kvbuf[l, 1, i] = jnp.concatenate([both[D.hd :], zeros], axis=0).T.astype(BF16)

        with sc(f"kv{l}{a}"):
            loop(0, D.seqs, body)

    qb = D.seq // 2

    def attention(l, a):
        C = D.cfg[l]

        def body(i):
            s, h = a * D.seqs + i // C.heads, lax.rem(i, C.heads)
            q_rows = rows_at(s * C.q + h * D.hd, D.hd)
            o_rows = rows_at(s * (C.q + C.f) + h * D.hd, D.hd)
            for b in range(2):
                ext = (b + 1) * qb
                lanes = slice(b * qb, (b + 1) * qb)
                score = dot(kn[s, :ext, : D.hd], qt[q_rows, lanes])
                keys = lax.broadcasted_iota(jnp.int32, (ext, qb), 0)
                queries = lax.broadcasted_iota(jnp.int32, (ext, qb), 1) + b * qb
                score = jnp.where(keys <= queries, score, -1e30)
                p = jnp.exp(score - jnp.max(score, axis=0, keepdims=True))
                p = (p * (1.0 / jnp.sum(p, axis=0, keepdims=True))).astype(BF16)
                jt[o_rows, lanes] = dot(vt[s, :, :ext], p).astype(BF16)

        with sc(f"attn{l}{a}"):
            loop(0, D.seqs * C.heads, body)

    def gate_up(l, a, slot, j, seq_of, count):
        C = D.cfg[l]

        def body(i):
            s = seq_of(i)
            p = dot(wbuf[slot, : 2 * C.cw, :], ht[s])
            g = p[: C.cw].astype(BF16).astype(F32)
            u = p[C.cw :].astype(BF16).astype(F32)
            jt[rows_at((a * D.seqs + s) * (C.q + C.f) + C.q + j * C.cw, C.cw), :] = (g * jax.nn.sigmoid(g) * u).astype(BF16)

        loop(0, count, body)

    def gate_up_loop(l, a, seq_of, count, first, last, stop=None):
        C = D.cfg[l]
        stop = C.n_c if stop is None else stop
        have_chunk(l, min(last, stop - 1))

        def body(j):
            slot = lax.rem(j, 2)
            wait(w_fetch(l, "f", j, slot))

            @pl.when(j + 1 < stop)
            def _():
                start(w_fetch(l, "f", j + 1, 1 - slot))

            gate_up(l, a, slot, j, seq_of, count)

        with sc(f"gu{l}{a}"):
            loop(first, last, body)

    def have_chunk(l, j):
        C = D.cfg[l]
        have(l, "f", (j + 1) * C.cw // fch - 1)

    def load_q(l):
        have(l, "q", 0)
        copies = w_fetch(l, "q", 0, 1)
        start(copies)
        wait(copies)

    m = och * n_row
    m_low, m_high = pl.ds(0, m // 2), pl.ds(m // 2, m // 2)
    r_slots = twin_in.shape[0]
    r_step = 64

    def order(i):
        return lax.rem(x + lax.rem(2 + 3 * i, 4), n_x)

    class Reduce:
        def __init__(self, l):
            self.l, self.C, self.sends = l, D.cfg[l], {}

        def send(self, u, i, src, dst, c):
            copy = remote(src, dst, rss.at[u % r_slots, i], rsr.at[u % r_slots, i], row, c)
            copy.start()
            self.sends[u].append(copy)

        def arrived(self, u, i, ref):
            remote(ref, ref, rss.at[u % r_slots, i], rsr.at[u % r_slots, i], row, col).wait_recv()

        def twin_copy(self, u, i):
            us = u % r_slots
            return remote(ot.at[u % 2, order(i), :, twin_lanes], twin_in.at[us, i], rss.at[us, i], rsr.at[us, i], row, twin)

        def twin_done(self, u):
            loop(0, 4, lambda i: self.twin_copy(u, i).wait_send())

        def stage_a(self, u, a):
            C = self.C
            if u >= 2:
                self.twin_done(u - 2)
            if u >= r_slots - 1:
                for c in self.sends.pop(u - r_slots + 1):
                    c.wait_send()
            self.sends[u] = []
            R = C.q + C.f

            def body(i):
                s = order(i)
                ot[u % 2, s] = dot(wobuf[:, :R], jt[rows_at((a * D.seqs + s) * R, R), :]).astype(BF16)
                self.twin_copy(u, i).start()

            with sc(f"sa{self.l}_{u}"):
                loop(0, 4, body)

        def stage_b(self, u):
            us = u % r_slots

            def body(i):
                self.arrived(u, i, twin_in.at[us, i])
                s = order(i)

                def add(b):
                    at = rows_at(b * r_step, r_step)
                    twin_in[us, i, at, :] = (ot[u % 2, s, at, my_lanes].astype(F32) + twin_in[us, i, at, :].astype(F32)).astype(BF16)

                loop(0, m // r_step, add)

            with sc(f"sb{self.l}_{u}"):
                loop(0, 1, body)
                self.send(u, 4, twin_in.at[us, 0, m_low], far_in.at[us, m_low], right)
                self.send(u, 5, twin_in.at[us, 0, m_high], far_in.at[us, m_high], left)
                loop(1, 4, body)

        def stage_c(self, u):
            us = u % r_slots

            def add_far(i, base):
                def add(b):
                    at = rows_at(base + b * r_step, r_step)
                    twin_in[us, i, at, :] = (twin_in[us, i, at, :].astype(F32) + far_in[us, at, :].astype(F32)).astype(BF16)

                loop(0, m // 2 // r_step, add)

            with sc(f"sc{self.l}_{u}"):
                self.arrived(u, 4, far_in.at[us, m_low])
                add_far(1, 0)
                self.send(u, 6, twin_in.at[us, 1], near_in.at[us, 0], right)
                self.arrived(u, 5, far_in.at[us, m_high])
                add_far(3, m // 2)
                self.send(u, 7, twin_in.at[us, 3], near_in.at[us, 1], left)

        def add_update(self, j, total):
            step = min(r_step, och)
            for r in range(n_row):

                def add(b, r=r):
                    dst = rows_at(r * dr + (r + j) % D.n_o * och + b * step, step)
                    u = total(rows_at(r * och + b * step, step)).astype(BF16).astype(F32)
                    hid[dst, :] = (hid[dst, :].astype(F32) + u).astype(BF16)

                loop(0, och // step, add)

        def stage_d(self, u, j, a):
            us = u % r_slots

            def total(at):
                return twin_in[us, 2, at, :].astype(F32) + near_in[us, 0, at, :].astype(F32) + near_in[us, 1, at, :].astype(F32)

            with sc(f"sd{self.l}_{u}"):
                self.arrived(u, 6, near_in.at[us, 0])
                self.arrived(u, 7, near_in.at[us, 1])
                if self.C.split:

                    def save(b):
                        at = rows_at(b * r_step, r_step)
                        psum[a, j, at, :] = total(at).astype(BF16)

                    loop(0, m // r_step, save)
                    if a == 1:
                        remote(psum.at[1, j], pair_in.at[j], es.at[j], er.at[j], mate, col).start()
                else:
                    self.add_update(j, total)

        def stage_e(self, j):
            with sc(f"se{self.l}_{j}"):
                c = remote(psum.at[1, j], pair_in.at[j], es.at[j], er.at[j], mate, col)
                c.wait_recv()
                self.add_update(j, lambda at: psum[0, j, at, :].astype(F32) + pair_in[j, at, :].astype(F32))
                c.wait_send()

        def finish(self, units):
            with sc(f"rfin{self.l}"):
                for u in range(max(0, units - 2), units):
                    self.twin_done(u)
                for u in self.sends:
                    for c in self.sends[u]:
                        c.wait_send()

    o_started = set()

    def o_load(l, j, a):
        if (l, j, a) not in o_started:
            have(l, "o", j)
            start(o_fetch(l, j, j % 2))
            o_started.add((l, j, a))

    def o_use(l, j, a):
        C = D.cfg[l]
        with sc(f"ouse{l}_{j}"):
            o_load(l, j, a)
            wait(o_fetch(l, j, j % 2))
            R = C.q + C.f
            for r in range(n_row):
                wobuf[r * och : (r + 1) * och, :R] = wonat[j % 2, :R, r * och : (r + 1) * och].T

    layer_norm(0)
    g0 = Gather(ht, 0)
    mine = ht.at[x, :, my_lanes]
    shared = g_h.at[x, :, my_lanes]
    to_mate = remote(mine, shared, ps, pr_, mate, col)
    to_mate.start()
    with sc("relay0"):
        run_to("relay", 1)
    catch_up()
    advance()
    advance()
    g0.pass_on()
    with sc("mate"):
        to_mate.wait_recv()
    g1 = Gather(g_h, 1)
    load_q(0)
    g0.own()
    g0.near()
    project_q(0, 0, near3, 3)
    with sc("relay2"):
        run_to("relay", 2)
    g0.pass_far()
    g0.far()
    project_q(0, 0, far1, 1)
    sent = kv_send(0)
    lead["relay"], lead["mate"] = RELAY, FAR_AHEAD
    with sc("relay3"):
        catch_up()
    n_f = D.cfg[0].n_f
    f_started = set()

    def f_load(j):
        if j not in f_started:
            f_started.add(j)
            start(w_fetch(0, "f", j, j % 2))

    def h_copy(i):
        return pltpu.make_async_copy(g_h.at[i], ht.at[i], lh.at[i])

    for j in range(n_f):
        if j == n_f - 2:
            g1.pass_on()
        have(0, "f", j)
        f_load(j)
        with sc(f"gu0_{j}"):
            wait(w_fetch(0, "f", j, j % 2))
            if j + 1 < n_f and at["next"] > step_of[(0, "f", j + 1)]:
                f_load(j + 1)
            gate_up(0, 0, j % 2, j, all4, 4)
    g0.finish()
    to_mate.wait_send()
    g1.own()
    g1.near()
    loop(0, 3, lambda i: h_copy(near3(i)).start())
    kv_arrive(0, sent)
    key_value(0, 0)
    attention(0, 0)
    g1.pass_far()

    red = Reduce(0)
    units = [(j, a) for a in (0, 1) for j in range(D.n_o)]
    n_u = len(units)
    state = {"e": 0}

    def unit(u):
        j, a = units[u]
        o_use(0, j, a)
        red.stage_a(u, a)
        if u + 1 < n_u:
            o_load(0, *units[u + 1])
        if u >= 2:
            red.stage_c(u - 2)
        if u >= 3:
            red.stage_d(u - 3, *units[u - 3])
        red.stage_b(u)
        if u >= D.n_o + 4:
            red.stage_e(state["e"])
            state["e"] += 1
        if u == D.n_o:
            lead["mate"] = 0

    unit(0)
    load_q(0)
    loop(0, 3, lambda i: h_copy(near3(i)).wait())
    project_q(0, 1, near3, 3)
    g1.far()
    h_copy(xf_).start()
    start(w_fetch(0, "f", 0, 0))
    h_copy(xf_).wait()
    project_q(0, 1, far1, 1)
    sent = kv_send(1)
    parts = D.n_o - 2
    cuts = [n_f * i // parts for i in range(parts + 1)]
    for u in range(1, D.n_o):
        unit(u)
        if 1 < u and cuts[u - 2] < cuts[u - 1]:
            gate_up_loop(0, 1, all4, 4, cuts[u - 2], cuts[u - 1])
    advance()
    kv_arrive(1, sent)
    key_value(0, 1)
    attention(0, 1)
    g1.finish()
    for u in range(D.n_o, n_u):
        unit(u)
        advance()
    red.stage_c(n_u - 2)
    red.stage_d(n_u - 3, *units[n_u - 3])
    red.stage_c(n_u - 1)
    red.stage_d(n_u - 2, *units[n_u - 2])
    red.stage_d(n_u - 1, *units[n_u - 1])
    lead["mate"] = AHEAD
    catch_up()
    for j in range(state["e"], D.n_o):
        red.stage_e(j)
    red.finish(n_u)

    def y_copy_back(i):
        d = lax.rem(me + i, n)
        return remote(hid.at[rows_at(d * dl, dl), :], piece_of(y_out, me), xs.at[i], xr.at[i], d // n_col, lax.rem(d, n_col))

    own_y = pltpu.make_async_copy(hid.at[rows_at(me * dl, dl), :], piece_of(y_out, me), xr.at[0])

    def y_send_back(d):
        i = lax.rem(d - me + n, n)

        @pl.when(i == 0)
        def _():
            own_y.start()

        @pl.when(i != 0)
        def _():
            y_copy_back(i).start()

    def y_ready(j):
        def body(d):
            r, a = d // n_col, lax.rem(d, n_col) * dl
            first = lax.rem(a // och + D.n_o - lax.rem(r, D.n_o), D.n_o)
            second = lax.rem((a + dl - 1) // och + D.n_o - lax.rem(r, D.n_o), D.n_o)

            @pl.when(jnp.maximum(first, second) == j)
            def _():
                y_send_back(d)

        loop(0, n, body)

    for l in range(1, D.layers):
        C = D.cfg[l]
        layer_norm(l)
        g0 = Gather(ht, 0)
        for _ in range(3):
            advance()
        own1, near2 = (lambda i: x), (lambda i: lax.rem(x + 1 + 2 * i, n_x))
        n_mid = min(3, C.n_c - 1)

        def begin(seq_of, count):
            load_q(l)
            have_chunk(l, 0)
            start(w_fetch(l, "f", 0, 0))
            project_q(l, 0, seq_of, count)

        g0.own()
        begin(own1, 1)
        gate_up_loop(l, 0, own1, 1, 0, n_mid, n_mid)
        advance()
        g0.pass_on()
        g0.near()
        begin(near2, 2)
        gate_up_loop(l, 0, near2, 2, 0, n_mid)
        g0.pass_far()
        gate_up_loop(l, 0, near3, 3, n_mid, C.n_c)
        g0.far()
        begin(far1, 1)
        sent = kv_send(0)
        gate_up_loop(l, 0, far1, 1, 0, C.n_c)
        have(l, "o", 0)
        o_load(l, 0, 0)
        g0.finish()
        kv_arrive(0, sent)
        key_value(l, 0)
        attention(l, 0)
        red = Reduce(l)
        last = l + 1 == D.layers

        def send_final(j):
            if last:
                y_ready(j)

        end = D.n_o - 1
        for j in range(D.n_o):
            if j == end:
                red.stage_c(j - 1)
                red.stage_d(j - 2, j - 2, 0)
                send_final(j - 2)
            o_use(l, j, 0)
            red.stage_a(j, 0)
            if j < end:
                o_load(l, j + 1, 0)
            if 1 <= j < end:
                red.stage_c(j - 1)
            if 2 <= j < end:
                red.stage_d(j - 2, j - 2, 0)
                send_final(j - 2)
            red.stage_b(j)
        red.stage_d(end - 1, end - 1, 0)
        red.stage_c(end)
        send_final(end - 1)
        red.stage_d(end, end, 0)
        send_final(end)
        red.finish(D.n_o)

    def kv_back(i):
        r = lax.rem(row + i, n_row)
        pos = rows_at((r * n_col + col) * D.pos, D.pos)
        return kvbuf.at[:, :, :, pos, :], kv_out.at[:, :, pl.ds(row * D.seqs, D.seqs)], r

    src, dst, _ = kv_back(0)
    own_kv = pltpu.make_async_copy(src, dst, fl)
    own_kv.start()
    kv_sends = []
    for i in range(1, n_row):
        src, dst, r = kv_back(i)
        c = remote(src, dst, fs.at[i], fr.at[i], r, col)
        c.start()
        kv_sends.append(c)

    def y_finish(i):
        s = lax.rem(me + n - i, n)
        remote(piece_of(y_out, s), piece_of(y_out, s), xs.at[i], xr.at[i], row, col).wait_recv()
        y_copy_back(i).wait_send()

    with sc("ywait"):
        loop(1, n, y_finish)
        own_y.wait()
        own_kv.wait()
        for i in range(1, n_row):
            r = lax.rem(row + n_row - i, n_row)
            dst = kv_out.at[:, :, pl.ds(r * D.seqs, D.seqs)]
            remote(dst, dst, fs.at[i], fr.at[i], row, col).wait_recv()
        for c in kv_sends:
            c.wait_send()
        for t in sorted(pending):
            drain(t)


def solution(mesh):
    n_row, n_col = mesh.shape["row"], mesh.shape["col"]
    group = n_row * n_col
    act_spec = P("dp", None, ("row", "col"))
    weight_spec = P(None, "row", "col")

    def device_fn(x_loc, gain_loc, w_in_loc, w_kv_loc, w_out_loc):
        D = Dims()
        D.n_row, D.n_col = n_row, n_col
        n_batch, D.seq, D.dl = x_loc.shape
        D.layers, D.dr, e = w_in_loc.shape
        D.d = D.dl * group
        r_block = w_out_loc.shape[1]
        D.f = e - r_block
        D.q = r_block - D.f
        kv_local = w_kv_loc.shape[2]
        D.hd = kv_local * n_col // 2
        D.kvp = 32
        D.tok = n_batch * D.seq // group
        D.seqs = n_batch // n_row
        D.pos = D.seq // group
        D.fch = 128
        D.och = 128
        D.n_o = D.dr // D.och
        D.cfg = []
        for l in range(D.layers):
            C = Dims()
            C.split = l == 0
            parts = 2 if C.split else 1
            C.q, C.f = D.q // parts, D.f // parts
            C.heads, C.n_f = C.q // D.hd, C.f // D.fch
            C.cw = D.fch if C.split else 2 * D.fch
            C.n_c = C.f // C.cw
            D.cfg.append(C)
        assert D.seq == 2 * D.tok and D.seqs == n_col // 2 == n_row == 4

        half = D.hd // 2
        inv_freq = (np.float32(1.0) / (np.float32(10000.0) ** (np.arange(half, dtype=np.float32) * np.float32(2.0) / np.float32(D.hd)))).astype(np.float32)
        angles = (inv_freq[:, None] * np.arange(D.seq, dtype=np.float32)[None, :]).astype(np.float32)
        cos_t, sin_t = np.cos(angles).astype(np.float32), np.sin(angles).astype(np.float32)
        perm = np.zeros((2 * D.hd, n_col * D.kvp), np.float32)
        for i in range(2 * D.hd):
            perm[i, (i // kv_local) * D.kvp + i % kv_local] = 1.0

        x_t = x_loc.transpose(0, 2, 1)
        w_t = w_in_loc.transpose(0, 2, 1)
        wkv_t = jnp.pad(w_kv_loc.transpose(0, 2, 1), ((0, 0), (0, D.kvp - kv_local), (0, 0)))
        gains = jnp.pad(gain_loc, ((0, 16 - D.layers), (0, 128 - D.dl)))

        m = D.och * n_row
        sds = jax.ShapeDtypeStruct
        dma = pltpu.SemaphoreType.DMA
        out = pl.pallas_call(
            functools.partial(kernel, D),
            out_shape=(
                sds(x_t.shape, BF16),
                sds((D.layers, 2, n_batch, D.pos, 128), BF16),
                sds((D.layers, e, D.d), BF16),
                sds((D.layers, D.kvp, D.d), BF16),
                sds((D.layers, n_row, r_block, D.dr), BF16),
                sds((D.seqs, D.d, D.seq), BF16),
            ),
            in_specs=[ANY] * 5 + [VMEM] * 3,
            out_specs=(ANY,) * 6,
            scratch_shapes=[
                pltpu.VMEM((group, D.dl, D.tok), BF16),
                pltpu.VMEM((group, 16, 128), BF16),
                pltpu.VMEM((D.layers, D.d, 128), F32),
                pltpu.VMEM((D.d, D.tok), BF16),
                pltpu.VMEM((D.seqs, D.d, D.seq), BF16),
                pltpu.VMEM((2, max(4 * D.fch, D.q + D.kvp), D.d), BF16),
                pltpu.VMEM((2, r_block, m), BF16),
                pltpu.VMEM((m, r_block), BF16),
                pltpu.VMEM((D.seqs * D.q, D.seq), BF16),
                pltpu.VMEM((n_col, 2 * D.seqs, D.kvp, D.seq), BF16),
                pltpu.VMEM((2 * D.seqs, D.seq, 128), BF16),
                pltpu.VMEM((2 * D.seqs, D.hd, D.seq), BF16),
                pltpu.VMEM((D.layers, 2, D.seqs, D.seq, 128), BF16),
                pltpu.VMEM((D.seqs * r_block, D.seq), BF16),
                pltpu.VMEM((2, D.seqs, m, D.seq), BF16),
                pltpu.VMEM((5, 4, m, D.tok), BF16),
                pltpu.VMEM((5, m, D.tok), BF16),
                pltpu.VMEM((5, 2, m, D.tok), BF16),
                pltpu.VMEM((2, D.n_o, m, D.tok), BF16),
                pltpu.VMEM((D.n_o, m, D.tok), BF16),
                dma((group,)), dma((group,)), dma((group,)), dma((group,)),
                dma((SLOTS, 4, 3)), dma((SLOTS, 4, 3)),
                dma((2, 9)), dma((2, 9)), dma, dma,
                dma((2, n_col)), dma((2, n_col)),
                dma((5, 8)), dma((5, 8)),
                dma((D.n_o,)), dma((D.n_o,)),
                dma((2, 8)), dma((2, 8)), dma((D.seqs,)),
                dma((n_row,)), dma((n_row,)), dma,
            ],
            compiler_params=pltpu.CompilerParams(collective_id=0, has_side_effects=True, vmem_limit_bytes=67_000_000),
            name="two_layers",
        )(x_t, gains, w_t, wkv_t, w_out_loc, jnp.asarray(cos_t), jnp.asarray(sin_t), jnp.asarray(perm, BF16))
        return out[0].transpose(0, 2, 1), out[1][..., : D.hd]

    return jax.shard_map(device_fn, mesh=mesh, in_specs=(act_spec, P(None, ("row", "col")), weight_spec, weight_spec, P(None, "col", "row")), out_specs=(act_spec, P(None, None, "dp", ("row", "col"), None)), check_vma=False)
```

```python
import functools

import numpy as np

import jax
import jax.numpy as jnp
from jax import lax
from jax.experimental import pallas as pl
from jax.experimental.pallas import tpu as pltpu
from jax.sharding import PartitionSpec as P

LN_EPS = 1e-6
MESH = pl.DeviceIdType.MESH
ANY = pl.BlockSpec(memory_space=pl.ANY)
VMEM = pl.BlockSpec(memory_space=pltpu.VMEM)
F32, BF16 = jnp.float32, jnp.bfloat16
SLOTS = 16
AHEAD = 4
FAR_AHEAD = 9
RELAY = 2


def dot(a, b):
    return jnp.dot(a, b, preferred_element_type=F32)


class Dims:
    pass


def rows_at(start, count, by=16):
    return pl.ds(start if isinstance(start, int) else pl.multiple_of(start, by), count)


def kernel(
    D,
    x_t, gains, w_t, wkv_t, w_o, cos_ref, sin_ref, perm_ref,
    y_out, kv_out, g_w, g_kv, g_wo, g_h,
    xland, gland, gcol, hid, ht, wbuf, wonat, wobuf, qt, kvland, kn, vt, kvbuf, jt, ot, twin_in, far_in, near_in, psum, pair_in,
    xs, xr, gs, gr, ys, yr, ags, agr, ps, pr_, kvs, kvr, rss, rsr, es, er, lw, lo, lh, fs, fr, fl,
):
    sc = jax.named_scope
    row, col = lax.axis_index("row"), lax.axis_index("col")
    n_row, n_col, n = D.n_row, D.n_col, D.n_row * D.n_col
    n_x = n_col // 2
    me = row * n_col + col
    x, k = col // 2, lax.rem(col, 2)
    xr_, xl_, xf_ = lax.rem(x + 1, n_x), lax.rem(x + n_x - 1, n_x), lax.rem(x + 2, n_x)
    right, left, twin = xr_ * 2 + k, xl_ * 2 + k, x * 2 + 1 - k
    up, down, across = lax.rem(row + 1, n_row), lax.rem(row + n_row - 1, n_row), lax.rem(row + 2, n_row)
    half, mate = row // 2, n_row - 1 - row
    peer = row + 1 - 2 * lax.rem(row, 2)
    tok, dl, dr = D.tok, D.dl, D.dr
    och, fch = D.och, D.fch
    my_lanes = pl.ds(pl.multiple_of(k * tok, 128), tok)
    twin_lanes = pl.ds(pl.multiple_of((1 - k) * tok, 128), tok)

    def remote(src, dst, ssem, rsem, r, c):
        return pltpu.make_async_remote_copy(src_ref=src, dst_ref=dst, send_sem=ssem, recv_sem=rsem, device_id={"row": r, "col": c}, device_id_type=MESH)

    def loop(lo_, hi_, f):
        def body(i, carry):
            f(i)
            return carry

        lax.fori_loop(lo_, hi_, body, 0)

    barrier = pltpu.get_barrier_semaphore()

    def greet(i):
        d = lax.rem(me + i, n)
        pl.semaphore_signal(barrier, inc=1, device_id={"row": d // n_col, "col": lax.rem(d, n_col)}, device_id_type=MESH)

    with sc("barrier"):
        loop(1, n, greet)
        pl.semaphore_wait(barrier, n - 1)

    def piece_of(ref, d):
        return ref.at[d // 2, :, pl.ds(pl.multiple_of(lax.rem(d, 2) * tok, 128), tok)]

    def x_copy(i):
        d = lax.rem(me + i, n)
        return remote(piece_of(x_t, d), xland.at[me], xs.at[i], xr.at[i], d // n_col, lax.rem(d, n_col))

    def g_copy(i):
        d = lax.rem(me + i, n)
        return remote(gains, gland.at[me], gs.at[i], gr.at[i], d // n_col, lax.rem(d, n_col))

    def x_start(i):
        x_copy(i).start()
        g_copy(i).start()

    own_x = pltpu.make_async_copy(piece_of(x_t, me), xland.at[me], xr.at[0])
    own_g = pltpu.make_async_copy(gains, gland.at[me], gr.at[0])
    own_x.start()
    own_g.start()
    loop(1, n, x_start)

    def own_lanes(r):
        return pl.ds(pl.multiple_of(r * dr, 128), dr)

    def o_lanes(j, r):
        return pl.ds(pl.multiple_of(lax.rem(r + j, D.n_o) * och, 128), och)

    steps = []
    for l, C in enumerate(D.cfg):
        steps += [(l, "q", 0)] + [(l, "f", j) for j in range(C.n_f)] + [(l, "o", j) for j in range(D.n_o)]
    n_steps = len(steps)
    step_of = {s: t for t, s in enumerate(steps)}

    def blocks(t, i):
        l, kind, j = steps[t]
        C = D.cfg[l]
        out = []

        def w_rows(a, m):
            at = rows_at(a, m)
            out.append((w_t.at[l, at, :], lambda r: g_w.at[l, at, own_lanes(r)]))

        def o_rows(a, m):
            at = rows_at(a, m)
            out.append((w_o.at[l, at, o_lanes(j, row)], lambda r: g_wo.at[l, r, at, o_lanes(j, r)]))

        def kv_rows(a, m):
            at = pl.ds(a, m)
            out.append((wkv_t.at[l, at, :], lambda r: g_kv.at[l, at, own_lanes(r)]))

        if kind == "q":
            for a in (0, C.q // 2):
                w_rows(i * C.q + a, C.q // 2)
            for a in (0, D.kvp // 2):
                kv_rows(a, D.kvp // 2)
        elif kind == "f":
            w_rows(D.q + i * C.f + j * fch, fch)
            w_rows(D.q + D.f + i * C.f + j * fch, fch)
        elif C.split:
            o_rows(i * C.q, C.q)
            o_rows(D.q + i * C.f, C.f)
        else:
            for a in (0, (D.q + D.f) // 2):
                o_rows(a, (D.q + D.f) // 2)
        return out

    pending = {}

    def y_copy(t, i, kind, src, dst, r):
        return remote(src, dst, ys.at[t % SLOTS, i, kind], yr.at[t % SLOTS, i, kind], r, col)

    def drain(t):
        for c in pending.pop(t, ()):
            c.wait_send()

    def y_send(t, *args):
        c = y_copy(t, *args)
        c.start()
        pending[t].append(c)

    def issue_peer(t):
        for i, (src, place) in enumerate(blocks(t, half if D.cfg[steps[t][0]].split else 0)):
            y_send(t, i, 0, src, place(row), peer)

    def issue_mate(t):
        drain(t - SLOTS)
        pending[t] = []
        for i, (src, place) in enumerate(blocks(t, 1 - half if D.cfg[steps[t][0]].split else 0)):
            y_send(t, i, 1, src, place(row), mate)

    def relay(t):
        split = D.cfg[steps[t][0]].split
        for i, (src, place) in enumerate(blocks(t, half if split else 0)):
            y_copy(t, i, 1, src, place(mate), mate).wait_recv()
            if split or i % 2 == 0:
                y_send(t, i, 2, place(mate), place(mate), peer)
            if not split:
                y_copy(t, i, 0, src, place(peer), peer).wait_recv()
                if i % 2 == 1:
                    y_send(t, i, 2, place(peer), place(peer), mate)

    at, lead = {"next": 0, "peer": 0, "mate": 0, "relay": 0}, {"peer": AHEAD, "mate": AHEAD, "relay": 0}

    def run_to(kind, t):
        while at[kind] <= min(t, n_steps - 1):
            {"peer": issue_peer, "mate": issue_mate, "relay": relay}[kind](at[kind])
            at[kind] += 1

    def catch_up():
        for kind in ("mate", "relay", "peer"):
            run_to(kind, at["next"] - 1 + lead[kind])

    def advance():
        t = at["next"]
        if t >= n_steps:
            return
        rest = n_row - 1 - peer
        with sc(f"adv{t}"):
            split = D.cfg[steps[t][0]].split
            for i, (src, place) in enumerate(blocks(t, half if split else 0)):
                if split:
                    y_copy(t, i, 0, src, place(peer), peer).wait_recv()
                y_copy(t, i, 2, src, place(rest), rest).wait_recv()
            at["next"] = t + 1
            catch_up()

    def have(*step):
        while at["next"] <= step_of[step]:
            advance()

    for t in range(2):
        run_to("mate", t)
        run_to("peer", t)

    def w_fetch(l, kind, j, slot):
        C = D.cfg[l]
        i = half if C.split else 0
        copies = []

        def fetch(src, dst):
            copies.append(pltpu.make_async_copy(src, dst, lw.at[slot, len(copies)]))

        def w_rows(a, m, at):
            a, at = rows_at(a, m), pl.ds(at, m)
            fetch(w_t.at[l, a, :], wbuf.at[slot, at, own_lanes(row)])
            for r in (up, down, across):
                fetch(g_w.at[l, a, own_lanes(r)], wbuf.at[slot, at, own_lanes(r)])

        if kind == "q":
            w_rows(i * C.q, C.q, 0)
            at = pl.ds(C.q, D.kvp)
            fetch(wkv_t.at[l], wbuf.at[slot, at, own_lanes(row)])
            for r in (up, down, across):
                fetch(g_kv.at[l, :, own_lanes(r)], wbuf.at[slot, at, own_lanes(r)])
        else:
            w_rows(D.q + i * C.f + j * C.cw, C.cw, 0)
            w_rows(D.q + D.f + i * C.f + j * C.cw, C.cw, C.cw)
        return copies

    def o_fetch(l, j, slot):
        C = D.cfg[l]
        copies = []

        def fetch(src, dst):
            copies.append(pltpu.make_async_copy(src, dst, lo.at[slot, len(copies)]))

        spans = ((half * C.q, 0, C.q), (D.q + half * C.f, C.q, C.f)) if C.split else ((0, 0, C.q + C.f),)
        for a, at, m in spans:
            a, at = rows_at(a, m), pl.ds(at, m)
            to = lambda r: pl.ds(pl.multiple_of(r * och, 128), och)
            fetch(w_o.at[l, a, o_lanes(j, row)], wonat.at[slot, at, to(row)])
            for r in (up, down, across):
                fetch(g_wo.at[l, r, a, o_lanes(j, r)], wonat.at[slot, at, to(r)])
        return copies

    def start(copies):
        for c in copies:
            c.start()

    def wait(copies):
        for c in copies:
            c.wait()

    own_x.wait()
    own_g.wait()

    def x_finish(i):
        s = lax.rem(me + n - i, n)
        remote(xland.at[s], xland.at[s], xs.at[i], xr.at[i], row, col).wait_recv()
        remote(gland.at[s], gland.at[s], gs.at[i], gr.at[i], row, col).wait_recv()
        x_copy(i).wait_send()
        g_copy(i).wait_send()

    with sc("xwait"):
        loop(1, n, x_finish)

    def keep(d):
        hid[rows_at(d * dl, dl), :] = xland[d]

    with sc("gains"):
        loop(0, n, keep)
        g_all = gland[...].astype(F32)
        for l in range(D.layers):
            g_rows = g_all[:, l, :]
            g_rows = jnp.concatenate([g_rows, jnp.zeros((128 - n, 128), F32)], axis=0) if n < 128 else g_rows
            g_cols = g_rows.T
            for d in range(n):
                gcol[l, d * dl : (d + 1) * dl, :] = jnp.broadcast_to(g_cols[:dl, d : d + 1], (dl, 128))

    blk = 64
    n_blk = D.d // blk

    def layer_norm(l):
        def add_up(i, acc):
            v = hid[rows_at(i * blk, blk), :].astype(F32)
            return acc + v.reshape(blk // 8, 8, tok).sum(axis=0)

        mean = lax.fori_loop(0, n_blk, add_up, jnp.zeros((8, tok), F32)).sum(axis=0, keepdims=True) / D.d

        def add_sq(i, acc):
            v = hid[rows_at(i * blk, blk), :].astype(F32) - mean
            return acc + (v * v).reshape(blk // 8, 8, tok).sum(axis=0)

        var = lax.fori_loop(0, n_blk, add_sq, jnp.zeros((8, tok), F32)).sum(axis=0, keepdims=True) / D.d
        scale = lax.rsqrt(var + LN_EPS)

        def write(i):
            rows = rows_at(i * blk, blk)
            g = gcol[l, rows, :]
            g = jnp.concatenate([g] * (tok // 128), axis=1)
            v = (hid[rows, :].astype(F32) - mean) * scale * g
            ht[x, rows, my_lanes] = v.astype(BF16)

        with sc(f"norm{l}"):
            loop(0, n_blk, write)

    d_low, d_high = pl.ds(0, D.d // 2), pl.ds(D.d // 2, D.d // 2)

    class Gather:
        def __init__(self, ref, tag):
            self.ref, self.tag, self.sends = ref, tag, []
            for i, c in ((0, right), (1, left), (2, twin)):
                self.send(i, ref(x, False, None), c)

        def send(self, i, ref, c):
            copy = remote(ref, ref, ags.at[self.tag, i], agr.at[self.tag, i], row, c)
            copy.start()
            self.sends.append(copy)

        def arrived(self, i, ref):
            remote(ref, ref, ags.at[self.tag, i], agr.at[self.tag, i], row, col).wait_recv()

        def pass_on(self):
            with sc(f"pass_on{self.tag}"):
                self.arrived(0, self.ref(xl_, False, None))
                self.send(3, self.ref(xl_, False, 0), right)
                self.send(4, self.ref(xl_, False, None), twin)
                self.arrived(1, self.ref(xr_, False, None))
                self.send(5, self.ref(xr_, False, 1), left)
                self.send(6, self.ref(xr_, False, None), twin)

        def own(self):
            self.arrived(2, self.ref(x, True, None))

        def near(self):
            with sc(f"near{self.tag}"):
                self.arrived(4, self.ref(xl_, True, None))
                self.arrived(6, self.ref(xr_, True, None))

        def pass_far(self):
            with sc(f"pass_far{self.tag}"):
                for part, i, j in ((0, 3, 7), (1, 5, 8)):
                    self.arrived(i, self.ref(xf_, False, part))
                    self.send(j, self.ref(xf_, False, part), twin)

        def far(self):
            with sc(f"far{self.tag}"):
                self.arrived(7, self.ref(xf_, True, 0))
                self.arrived(8, self.ref(xf_, True, 1))

        def finish(self):
            for c in self.sends:
                c.wait_send()

    def normed_of(buf):
        def ref(chip, other, part):
            rows = slice(None) if part is None else (d_low, d_high)[part]
            return buf.at[chip, rows, twin_lanes if other else my_lanes]

        return ref

    def kv_of(a):
        def ref(chip, other, part):
            h = D.seqs // 2
            span = pl.ds(a * D.seqs, D.seqs) if part is None else pl.ds(a * D.seqs + part * h, h)
            return kvland.at[chip * 2 + (1 - k if other else k), span]

        return ref

    half_dim = D.hd // 2

    def near3(i):
        return lax.rem(x + i + i // 2, n_x)

    def all4(i):
        return i

    def far1(i):
        return xf_

    def rope(p):
        lo_, hi_ = p[:half_dim], p[half_dim:]
        return jnp.concatenate([lo_ * cos_ref[...] - hi_ * sin_ref[...], hi_ * cos_ref[...] + lo_ * sin_ref[...]], axis=0)

    def project_q(l, a, seq_of, count):
        C = D.cfg[l]

        def body(i):
            s = seq_of(i)
            p = dot(wbuf[1, : C.q + D.kvp, :], ht[s]).astype(BF16).astype(F32)
            for h in range(C.heads):
                at = rows_at((a * D.seqs + s) * C.q + h * D.hd, D.hd)
                qt[at, :] = (rope(p[h * D.hd : (h + 1) * D.hd]) * D.hd**-0.5).astype(BF16)
            kvland[col, a * D.seqs + s] = p[C.q :].astype(BF16)

        with sc(f"q{l}{a}"):
            loop(0, count, body)

    def kv_copy(s, j, source):
        ref = kvland.at[source, s]
        return remote(ref, ref, kvs.at[s, j], kvr.at[s, j], row, lax.rem(col + j, n_col))

    def kv_send(seq_of, count):
        def body(i):
            s = seq_of(i)
            loop(1, n_col, lambda j: kv_copy(s, j, col).start())

        loop(0, count, body)

    def kv_arrive():
        def body(i):
            j = i // D.seqs + 1
            s = lax.rem(i, D.seqs)
            kv_copy(s, j, lax.rem(col + n_col - j, n_col)).wait_recv()
            kv_copy(s, j, col).wait_send()

        with sc("kvwait"):
            loop(0, D.seqs * (n_col - 1), body)

    def key_value(l, a):
        def body(i):
            s = a * D.seqs + i
            raw = kvland[:, s].reshape(n_col * D.kvp, D.seq)
            both = dot(perm_ref[...], raw)
            zeros = jnp.zeros((128 - D.hd, D.seq), F32)
            k_nat = jnp.concatenate([rope(both[: D.hd]), zeros], axis=0).T.astype(BF16)
            kn[s] = k_nat
            vt[s] = both[D.hd :].astype(BF16)
            if a == 0:
                kvbuf[l, 0, i] = k_nat
                kvbuf[l, 1, i] = jnp.concatenate([both[D.hd :], zeros], axis=0).T.astype(BF16)

        with sc(f"kv{l}{a}"):
            loop(0, D.seqs, body)

    qb = D.seq // 2

    def attention(l, a):
        C = D.cfg[l]

        def body(i):
            s, h = a * D.seqs + i // C.heads, lax.rem(i, C.heads)
            q_rows = rows_at(s * C.q + h * D.hd, D.hd)
            o_rows = rows_at(s * (C.q + C.f) + h * D.hd, D.hd)
            for b in range(2):
                ext = (b + 1) * qb
                lanes = slice(b * qb, (b + 1) * qb)
                score = dot(kn[s, :ext, : D.hd], qt[q_rows, lanes])
                keys = lax.broadcasted_iota(jnp.int32, (ext, qb), 0)
                queries = lax.broadcasted_iota(jnp.int32, (ext, qb), 1) + b * qb
                score = jnp.where(keys <= queries, score, -1e30)
                p = jnp.exp(score - jnp.max(score, axis=0, keepdims=True))
                p = (p * (1.0 / jnp.sum(p, axis=0, keepdims=True))).astype(BF16)
                jt[o_rows, lanes] = dot(vt[s, :, :ext], p).astype(BF16)

        with sc(f"attn{l}{a}"):
            loop(0, D.seqs * C.heads, body)

    def gate_up(l, a, slot, j, seq_of, count):
        C = D.cfg[l]

        def body(i):
            s = seq_of(i)
            p = dot(wbuf[slot, : 2 * C.cw, :], ht[s])
            g = p[: C.cw].astype(BF16).astype(F32)
            u = p[C.cw :].astype(BF16).astype(F32)
            jt[rows_at((a * D.seqs + s) * (C.q + C.f) + C.q + j * C.cw, C.cw), :] = (g * jax.nn.sigmoid(g) * u).astype(BF16)

        loop(0, count, body)

    def gate_up_loop(l, a, seq_of, count, first, last, stop=None):
        C = D.cfg[l]
        stop = C.n_c if stop is None else stop
        have_chunk(l, min(last, stop - 1))

        def body(j):
            slot = lax.rem(j, 2)
            wait(w_fetch(l, "f", j, slot))

            @pl.when(j + 1 < stop)
            def _():
                start(w_fetch(l, "f", j + 1, 1 - slot))

            gate_up(l, a, slot, j, seq_of, count)

        with sc(f"gu{l}{a}"):
            loop(first, last, body)

    def have_chunk(l, j):
        C = D.cfg[l]
        have(l, "f", (j + 1) * C.cw // fch - 1)

    def load_q(l):
        have(l, "q", 0)
        copies = w_fetch(l, "q", 0, 1)
        start(copies)
        wait(copies)

    m = och * n_row
    m_low, m_high = pl.ds(0, m // 2), pl.ds(m // 2, m // 2)
    r_slots = twin_in.shape[0]
    r_step = 64

    def order(i):
        return lax.rem(x + lax.rem(2 + 3 * i, 4), n_x)

    class Reduce:
        def __init__(self, l):
            self.l, self.C, self.sends = l, D.cfg[l], {}

        def send(self, u, i, src, dst, c):
            copy = remote(src, dst, rss.at[u % r_slots, i], rsr.at[u % r_slots, i], row, c)
            copy.start()
            self.sends[u].append(copy)

        def arrived(self, u, i, ref):
            remote(ref, ref, rss.at[u % r_slots, i], rsr.at[u % r_slots, i], row, col).wait_recv()

        def twin_copy(self, u, i):
            us = u % r_slots
            return remote(ot.at[u % 2, order(i), :, twin_lanes], twin_in.at[us, i], rss.at[us, i], rsr.at[us, i], row, twin)

        def twin_done(self, u):
            loop(0, 4, lambda i: self.twin_copy(u, i).wait_send())

        def stage_a(self, u, a):
            C = self.C
            if u >= 2:
                self.twin_done(u - 2)
            if u >= r_slots - 1:
                for c in self.sends.pop(u - r_slots + 1):
                    c.wait_send()
            self.sends[u] = []
            R = C.q + C.f

            def body(i):
                s = order(i)
                ot[u % 2, s] = dot(wobuf[:, :R], jt[rows_at((a * D.seqs + s) * R, R), :]).astype(BF16)
                self.twin_copy(u, i).start()

            with sc(f"sa{self.l}_{u}"):
                loop(0, 4, body)

        def stage_b(self, u):
            us = u % r_slots

            def body(i):
                self.arrived(u, i, twin_in.at[us, i])
                s = order(i)

                def add(b):
                    at = rows_at(b * r_step, r_step)
                    twin_in[us, i, at, :] = (ot[u % 2, s, at, my_lanes].astype(F32) + twin_in[us, i, at, :].astype(F32)).astype(BF16)

                loop(0, m // r_step, add)

            with sc(f"sb{self.l}_{u}"):
                loop(0, 1, body)
                self.send(u, 4, twin_in.at[us, 0, m_low], far_in.at[us, m_low], right)
                self.send(u, 5, twin_in.at[us, 0, m_high], far_in.at[us, m_high], left)
                loop(1, 4, body)

        def stage_c(self, u):
            us = u % r_slots

            def add_far(i, base):
                def add(b):
                    at = rows_at(base + b * r_step, r_step)
                    twin_in[us, i, at, :] = (twin_in[us, i, at, :].astype(F32) + far_in[us, at, :].astype(F32)).astype(BF16)

                loop(0, m // 2 // r_step, add)

            with sc(f"sc{self.l}_{u}"):
                self.arrived(u, 4, far_in.at[us, m_low])
                add_far(1, 0)
                self.send(u, 6, twin_in.at[us, 1], near_in.at[us, 0], right)
                self.arrived(u, 5, far_in.at[us, m_high])
                add_far(3, m // 2)
                self.send(u, 7, twin_in.at[us, 3], near_in.at[us, 1], left)

        def add_update(self, j, total):
            step = min(r_step, och)
            for r in range(n_row):

                def add(b, r=r):
                    dst = rows_at(r * dr + (r + j) % D.n_o * och + b * step, step)
                    u = total(rows_at(r * och + b * step, step)).astype(BF16).astype(F32)
                    hid[dst, :] = (hid[dst, :].astype(F32) + u).astype(BF16)

                loop(0, och // step, add)

        def stage_d(self, u, j, a):
            us = u % r_slots

            def total(at):
                return twin_in[us, 2, at, :].astype(F32) + near_in[us, 0, at, :].astype(F32) + near_in[us, 1, at, :].astype(F32)

            with sc(f"sd{self.l}_{u}"):
                self.arrived(u, 6, near_in.at[us, 0])
                self.arrived(u, 7, near_in.at[us, 1])
                if self.C.split:

                    def save(b):
                        at = rows_at(b * r_step, r_step)
                        psum[a, j, at, :] = total(at).astype(BF16)

                    loop(0, m // r_step, save)
                    if a == 1:
                        remote(psum.at[1, j], pair_in.at[j], es.at[j], er.at[j], mate, col).start()
                else:
                    self.add_update(j, total)

        def stage_e(self, j):
            with sc(f"se{self.l}_{j}"):
                c = remote(psum.at[1, j], pair_in.at[j], es.at[j], er.at[j], mate, col)
                c.wait_recv()
                self.add_update(j, lambda at: psum[0, j, at, :].astype(F32) + pair_in[j, at, :].astype(F32))
                c.wait_send()

        def finish(self, units):
            with sc(f"rfin{self.l}"):
                for u in range(max(0, units - 2), units):
                    self.twin_done(u)
                for u in self.sends:
                    for c in self.sends[u]:
                        c.wait_send()

    o_started = set()

    def o_load(l, j, a):
        if (l, j, a) not in o_started:
            have(l, "o", j)
            start(o_fetch(l, j, j % 2))
            o_started.add((l, j, a))

    def o_use(l, j, a):
        C = D.cfg[l]
        with sc(f"ouse{l}_{j}"):
            o_load(l, j, a)
            wait(o_fetch(l, j, j % 2))
            R = C.q + C.f
            for r in range(n_row):
                wobuf[r * och : (r + 1) * och, :R] = wonat[j % 2, :R, r * och : (r + 1) * och].T

    layer_norm(0)
    g0 = Gather(normed_of(ht), 0)
    mine = ht.at[x, :, my_lanes]
    shared = g_h.at[x, :, my_lanes]
    to_mate = remote(mine, shared, ps, pr_, mate, col)
    to_mate.start()
    with sc("relay0"):
        run_to("relay", 1)
    catch_up()
    advance()
    advance()
    g0.pass_on()
    with sc("mate"):
        to_mate.wait_recv()
    g1 = Gather(normed_of(g_h), 1)
    load_q(0)
    g0.own()
    g0.near()
    project_q(0, 0, near3, 3)
    with sc("relay2"):
        run_to("relay", 2)
    g0.pass_far()
    g0.far()
    project_q(0, 0, far1, 1)
    kv0 = Gather(kv_of(0), 2)
    lead["relay"], lead["mate"], lead["peer"] = RELAY, FAR_AHEAD, RELAY + 1
    with sc("relay3"):
        catch_up()
    n_f = D.cfg[0].n_f
    f_started = set()

    def f_load(j):
        if j not in f_started:
            f_started.add(j)
            start(w_fetch(0, "f", j, j % 2))

    def h_copy(i):
        return pltpu.make_async_copy(g_h.at[i], ht.at[i], lh.at[i])

    for j in range(n_f):
        if j == n_f - 2:
            kv0.pass_on()
            g1.pass_on()
        have(0, "f", j)
        f_load(j)
        with sc(f"gu0_{j}"):
            wait(w_fetch(0, "f", j, j % 2))
            if j + 1 < n_f and at["next"] > step_of[(0, "f", j + 1)]:
                f_load(j + 1)
            gate_up(0, 0, j % 2, j, all4, 4)
    g0.finish()
    to_mate.wait_send()
    g1.own()
    g1.near()
    loop(0, 3, lambda i: h_copy(near3(i)).start())
    kv0.pass_far()
    with sc("kv0wait"):
        kv0.own()
        kv0.near()
        kv0.far()
        kv0.finish()
    key_value(0, 0)
    attention(0, 0)

    red = Reduce(0)
    units = [(j, 0) for j in range(D.n_o - 1)] + [(j, 1) for j in range(D.n_o)] + [(D.n_o - 1, 0)]
    n_u = len(units)
    first = D.n_o - 1
    state = {"e": 0}

    def settle(count):
        while state["e"] < count:
            red.stage_e(state["e"])
            state["e"] += 1

    def unit(u):
        j, a = units[u]
        if u == 0 or units[u - 1][0] != j:
            o_use(0, j, a)
        red.stage_a(u, a)
        if u + 1 < n_u and units[u + 1][0] != j:
            o_load(0, *units[u + 1])
        if u >= 2:
            red.stage_c(u - 2)
        if u >= 3:
            red.stage_d(u - 3, *units[u - 3])
        red.stage_b(u)

    unit(0)
    g1.pass_far()
    g1.far()
    h_copy(xf_).start()
    load_q(0)
    start(w_fetch(0, "f", 0, 0))
    loop(0, 3, lambda i: h_copy(near3(i)).wait())
    h_copy(xf_).wait()
    project_q(0, 1, all4, 4)
    kv1 = Gather(kv_of(1), 3)
    parts = first - 2
    cuts = [n_f * i // parts for i in range(parts + 1)]
    for u in range(1, first):
        unit(u)
        if u == 2:
            kv1.pass_on()
        if 1 < u:
            gate_up_loop(0, 1, all4, 4, cuts[u - 2], cuts[u - 1])
    kv1.pass_far()
    advance()
    with sc("kv1wait"):
        kv1.own()
        kv1.near()
        kv1.far()
        kv1.finish()
    key_value(0, 1)
    attention(0, 1)
    g1.finish()
    lead["mate"] = 0
    for u in range(first, n_u):
        unit(u)
        if u == n_u - 1:
            settle(1)
        advance()
    red.stage_c(n_u - 2)
    red.stage_d(n_u - 3, *units[n_u - 3])
    red.stage_c(n_u - 1)
    red.stage_d(n_u - 2, *units[n_u - 2])
    lead["mate"] = AHEAD
    catch_up()
    settle(D.n_o - 1)
    red.stage_d(n_u - 1, *units[n_u - 1])
    settle(D.n_o)
    red.finish(n_u)

    def y_copy_back(i):
        d = lax.rem(me + i, n)
        return remote(hid.at[rows_at(d * dl, dl), :], piece_of(y_out, me), xs.at[i], xr.at[i], d // n_col, lax.rem(d, n_col))

    own_y = pltpu.make_async_copy(hid.at[rows_at(me * dl, dl), :], piece_of(y_out, me), xr.at[0])

    def y_send_back(d):
        i = lax.rem(d - me + n, n)

        @pl.when(i == 0)
        def _():
            own_y.start()

        @pl.when(i != 0)
        def _():
            y_copy_back(i).start()

    def y_ready(j):
        def body(d):
            r, a = d // n_col, lax.rem(d, n_col) * dl
            first = lax.rem(a // och + D.n_o - lax.rem(r, D.n_o), D.n_o)
            second = lax.rem((a + dl - 1) // och + D.n_o - lax.rem(r, D.n_o), D.n_o)

            @pl.when(jnp.maximum(first, second) == j)
            def _():
                y_send_back(d)

        loop(0, n, body)

    for l in range(1, D.layers):
        C = D.cfg[l]
        layer_norm(l)
        g0 = Gather(normed_of(ht), 0)
        advance()
        own1, near2 = (lambda i: x), (lambda i: lax.rem(x + 1 + 2 * i, n_x))
        n_mid = min(3, C.n_c - 1)

        def begin(seq_of, count):
            load_q(l)
            have_chunk(l, 0)
            start(w_fetch(l, "f", 0, 0))
            project_q(l, 0, seq_of, count)

        g0.own()
        begin(own1, 1)
        kv_send(own1, 1)
        gate_up_loop(l, 0, own1, 1, 0, n_mid, n_mid)
        for _ in range(3):
            advance()
        g0.pass_on()
        g0.near()
        begin(near2, 2)
        kv_send(near2, 2)
        gate_up_loop(l, 0, near2, 2, 0, n_mid)
        g0.pass_far()
        gate_up_loop(l, 0, near3, 3, n_mid, C.n_c)
        g0.far()
        begin(far1, 1)
        kv_send(far1, 1)
        gate_up_loop(l, 0, far1, 1, 0, C.n_c)
        have(l, "o", 0)
        o_load(l, 0, 0)
        g0.finish()
        kv_arrive()
        key_value(l, 0)
        attention(l, 0)
        red = Reduce(l)
        last = l + 1 == D.layers

        def send_final(j):
            if last:
                y_ready(j)

        end = D.n_o - 1
        for j in range(D.n_o):
            o_use(l, j, 0)
            red.stage_a(j, 0)
            if j < end:
                o_load(l, j + 1, 0)
            if 1 <= j:
                red.stage_c(j - 1)
            if 2 <= j:
                red.stage_d(j - 2, j - 2, 0)
            red.stage_b(j)
        red.stage_c(end)
        red.stage_d(end - 1, end - 1, 0)
        for j in range(end):
            send_final(j)
        red.stage_d(end, end, 0)
        send_final(end)
        red.finish(D.n_o)

    def kv_back(i):
        r = lax.rem(row + i, n_row)
        pos = rows_at((r * n_col + col) * D.pos, D.pos)
        return kvbuf.at[:, :, :, pos, :], kv_out.at[:, :, pl.ds(row * D.seqs, D.seqs)], r

    src, dst, _ = kv_back(0)
    own_kv = pltpu.make_async_copy(src, dst, fl)
    own_kv.start()
    kv_sends = []
    for i in range(1, n_row):
        src, dst, r = kv_back(i)
        c = remote(src, dst, fs.at[i], fr.at[i], r, col)
        c.start()
        kv_sends.append(c)

    def y_finish(i):
        s = lax.rem(me + n - i, n)
        remote(piece_of(y_out, s), piece_of(y_out, s), xs.at[i], xr.at[i], row, col).wait_recv()
        y_copy_back(i).wait_send()

    with sc("ywait"):
        loop(1, n, y_finish)
        own_y.wait()
        own_kv.wait()
        for i in range(1, n_row):
            r = lax.rem(row + n_row - i, n_row)
            dst = kv_out.at[:, :, pl.ds(r * D.seqs, D.seqs)]
            remote(dst, dst, fs.at[i], fr.at[i], row, col).wait_recv()
        for c in kv_sends:
            c.wait_send()
        for t in sorted(pending):
            drain(t)


def solution(mesh):
    n_row, n_col = mesh.shape["row"], mesh.shape["col"]
    group = n_row * n_col
    act_spec = P("dp", None, ("row", "col"))
    weight_spec = P(None, "row", "col")

    def device_fn(x_loc, gain_loc, w_in_loc, w_kv_loc, w_out_loc):
        D = Dims()
        D.n_row, D.n_col = n_row, n_col
        n_batch, D.seq, D.dl = x_loc.shape
        D.layers, D.dr, e = w_in_loc.shape
        D.d = D.dl * group
        r_block = w_out_loc.shape[1]
        D.f = e - r_block
        D.q = r_block - D.f
        kv_local = w_kv_loc.shape[2]
        D.hd = kv_local * n_col // 2
        D.kvp = 32
        D.tok = n_batch * D.seq // group
        D.seqs = n_batch // n_row
        D.pos = D.seq // group
        D.fch = 128
        D.och = 128
        D.n_o = D.dr // D.och
        D.cfg = []
        for l in range(D.layers):
            C = Dims()
            C.split = l == 0
            parts = 2 if C.split else 1
            C.q, C.f = D.q // parts, D.f // parts
            C.heads, C.n_f = C.q // D.hd, C.f // D.fch
            C.cw = D.fch if C.split else 2 * D.fch
            C.n_c = C.f // C.cw
            D.cfg.append(C)
        assert D.seq == 2 * D.tok and D.seqs == n_col // 2 == n_row == 4

        half = D.hd // 2
        inv_freq = (np.float32(1.0) / (np.float32(10000.0) ** (np.arange(half, dtype=np.float32) * np.float32(2.0) / np.float32(D.hd)))).astype(np.float32)
        angles = (inv_freq[:, None] * np.arange(D.seq, dtype=np.float32)[None, :]).astype(np.float32)
        cos_t, sin_t = np.cos(angles).astype(np.float32), np.sin(angles).astype(np.float32)
        perm = np.zeros((2 * D.hd, n_col * D.kvp), np.float32)
        for i in range(2 * D.hd):
            perm[i, (i // kv_local) * D.kvp + i % kv_local] = 1.0

        x_t = x_loc.transpose(0, 2, 1)
        w_t = w_in_loc.transpose(0, 2, 1)
        wkv_t = jnp.pad(w_kv_loc.transpose(0, 2, 1), ((0, 0), (0, D.kvp - kv_local), (0, 0)))
        gains = jnp.pad(gain_loc, ((0, 16 - D.layers), (0, 128 - D.dl)))

        m = D.och * n_row
        sds = jax.ShapeDtypeStruct
        dma = pltpu.SemaphoreType.DMA
        out = pl.pallas_call(
            functools.partial(kernel, D),
            out_shape=(
                sds(x_t.shape, BF16),
                sds((D.layers, 2, n_batch, D.pos, 128), BF16),
                sds((D.layers, e, D.d), BF16),
                sds((D.layers, D.kvp, D.d), BF16),
                sds((D.layers, n_row, r_block, D.dr), BF16),
                sds((D.seqs, D.d, D.seq), BF16),
            ),
            in_specs=[ANY] * 5 + [VMEM] * 3,
            out_specs=(ANY,) * 6,
            scratch_shapes=[
                pltpu.VMEM((group, D.dl, D.tok), BF16),
                pltpu.VMEM((group, 16, 128), BF16),
                pltpu.VMEM((D.layers, D.d, 128), F32),
                pltpu.VMEM((D.d, D.tok), BF16),
                pltpu.VMEM((D.seqs, D.d, D.seq), BF16),
                pltpu.VMEM((2, max(4 * D.fch, D.q + D.kvp), D.d), BF16),
                pltpu.VMEM((2, r_block, m), BF16),
                pltpu.VMEM((m, r_block), BF16),
                pltpu.VMEM((D.seqs * D.q, D.seq), BF16),
                pltpu.VMEM((n_col, 2 * D.seqs, D.kvp, D.seq), BF16),
                pltpu.VMEM((2 * D.seqs, D.seq, 128), BF16),
                pltpu.VMEM((2 * D.seqs, D.hd, D.seq), BF16),
                pltpu.VMEM((D.layers, 2, D.seqs, D.seq, 128), BF16),
                pltpu.VMEM((D.seqs * r_block, D.seq), BF16),
                pltpu.VMEM((2, D.seqs, m, D.seq), BF16),
                pltpu.VMEM((5, 4, m, D.tok), BF16),
                pltpu.VMEM((5, m, D.tok), BF16),
                pltpu.VMEM((5, 2, m, D.tok), BF16),
                pltpu.VMEM((2, D.n_o, m, D.tok), BF16),
                pltpu.VMEM((D.n_o, m, D.tok), BF16),
                dma((group,)), dma((group,)), dma((group,)), dma((group,)),
                dma((SLOTS, 4, 3)), dma((SLOTS, 4, 3)),
                dma((4, 9)), dma((4, 9)), dma, dma,
                dma((D.seqs, n_col)), dma((D.seqs, n_col)),
                dma((5, 8)), dma((5, 8)),
                dma((D.n_o,)), dma((D.n_o,)),
                dma((2, 8)), dma((2, 8)), dma((D.seqs,)),
                dma((n_row,)), dma((n_row,)), dma,
            ],
            compiler_params=pltpu.CompilerParams(collective_id=0, has_side_effects=True, vmem_limit_bytes=67_000_000),
            name="two_layers",
        )(x_t, gains, w_t, wkv_t, w_out_loc, jnp.asarray(cos_t), jnp.asarray(sin_t), jnp.asarray(perm, BF16))
        return out[0].transpose(0, 2, 1), out[1][..., : D.hd]

    return jax.shard_map(device_fn, mesh=mesh, in_specs=(act_spec, P(None, ("row", "col")), weight_spec, weight_spec, P(None, "col", "row")), out_specs=(act_spec, P(None, None, "dp", ("row", "col"), None)), check_vma=False)
```

```python
import functools

import numpy as np

import jax
import jax.numpy as jnp
from jax import lax
from jax.experimental import pallas as pl
from jax.experimental.pallas import tpu as pltpu
from jax.sharding import PartitionSpec as P

LN_EPS = 1e-6
MESH = pl.DeviceIdType.MESH
ANY = pl.BlockSpec(memory_space=pl.ANY)
VMEM = pl.BlockSpec(memory_space=pltpu.VMEM)
F32, BF16 = jnp.float32, jnp.bfloat16


def dot(a, b):
    return jnp.dot(a, b, preferred_element_type=F32)


class Dims:
    pass


def rows_at(start, count, by=16):
    return pl.ds(start if isinstance(start, int) else pl.multiple_of(start, by), count)


def kernel(
    D,
    x_t, gains, w_t, wkv_t, w_o, cos_ref, sin_ref, perm_ref,
    y_out, kv_out, g_w, g_kv, g_wo, g_h,
    xland, gland, gcol, hid, ht, wbuf, wonat, wobuf, qt, kvland, kn, vt, kvbuf, jt, ot, twin_in, far_in, near_in, psum, pair_in,
    xs, xr, gs, gr, ys, yr, ags, agr, ps, pr_, kvs, kvr, rss, rsr, es, er, lw, lo, lh, fs, fr, fl,
):
    sc = jax.named_scope
    row, col = lax.axis_index("row"), lax.axis_index("col")
    n_row, n_col, n = D.n_row, D.n_col, D.n_row * D.n_col
    n_x = n_col // 2
    me = row * n_col + col
    x, k = col // 2, lax.rem(col, 2)
    xr_, xl_, xf_ = lax.rem(x + 1, n_x), lax.rem(x + n_x - 1, n_x), lax.rem(x + 2, n_x)
    right, left, twin = xr_ * 2 + k, xl_ * 2 + k, x * 2 + 1 - k
    up, down, across = lax.rem(row + 1, n_row), lax.rem(row + n_row - 1, n_row), lax.rem(row + 2, n_row)
    half, mate = row // 2, n_row - 1 - row
    peer = row + 1 - 2 * lax.rem(row, 2)
    tok, dl, dr = D.tok, D.dl, D.dr
    och, fch = D.och, D.fch
    my_lanes = pl.ds(pl.multiple_of(k * tok, 128), tok)
    twin_lanes = pl.ds(pl.multiple_of((1 - k) * tok, 128), tok)

    def remote(src, dst, ssem, rsem, r, c):
        return pltpu.make_async_remote_copy(src_ref=src, dst_ref=dst, send_sem=ssem, recv_sem=rsem, device_id={"row": r, "col": c}, device_id_type=MESH)

    def loop(lo_, hi_, f):
        def body(i, carry):
            f(i)
            return carry

        lax.fori_loop(lo_, hi_, body, 0)

    barrier = pltpu.get_barrier_semaphore()

    def greet(i):
        d = lax.rem(me + i, n)
        pl.semaphore_signal(barrier, inc=1, device_id={"row": d // n_col, "col": lax.rem(d, n_col)}, device_id_type=MESH)

    with sc("barrier"):
        loop(1, n, greet)
        pl.semaphore_wait(barrier, n - 1)

    def piece_of(ref, d):
        return ref.at[d // 2, :, pl.ds(pl.multiple_of(lax.rem(d, 2) * tok, 128), tok)]

    def x_copy(i):
        d = lax.rem(me + i, n)
        return remote(piece_of(x_t, d), xland.at[me], xs.at[i], xr.at[i], d // n_col, lax.rem(d, n_col))

    def g_copy(i):
        d = lax.rem(me + i, n)
        return remote(gains, gland.at[me], gs.at[i], gr.at[i], d // n_col, lax.rem(d, n_col))

    def x_start(i):
        x_copy(i).start()
        g_copy(i).start()

    own_x = pltpu.make_async_copy(piece_of(x_t, me), xland.at[me], xr.at[0])
    own_g = pltpu.make_async_copy(gains, gland.at[me], gr.at[0])
    own_x.start()
    own_g.start()
    loop(1, n, x_start)

    def own_lanes(r):
        return pl.ds(pl.multiple_of(r * dr, 128), dr)

    def o_lanes(j, r):
        return pl.ds(pl.multiple_of(lax.rem(r + j, D.n_o) * och, 128), och)

    steps = []
    for l, C in enumerate(D.cfg):
        steps += [(l, "q", 0)] + [(l, "f", j) for j in range(C.n_f)] + [(l, "o", j) for j in range(D.n_o)]
    n_steps = len(steps)
    step_of = {s: t for t, s in enumerate(steps)}

    def blocks(t, i):
        l, kind, j = steps[t]
        C = D.cfg[l]
        out = []

        def w_rows(a, m):
            at = rows_at(a, m)
            out.append((w_t.at[l, at, :], lambda r: g_w.at[l, at, own_lanes(r)]))

        def o_rows(a, m):
            at = rows_at(a, m)
            out.append((w_o.at[l, at, o_lanes(j, row)], lambda r: g_wo.at[l, r, at, o_lanes(j, r)]))

        def kv_rows(a, m):
            at = pl.ds(a, m)
            out.append((wkv_t.at[l, at, :], lambda r: g_kv.at[l, at, own_lanes(r)]))

        if kind == "q":
            for a in (0, C.q // 2):
                w_rows(i * C.q + a, C.q // 2)
            for a in (0, D.kvp // 2):
                kv_rows(a, D.kvp // 2)
        elif kind == "f":
            w_rows(D.q + i * C.f + j * fch, fch)
            w_rows(D.q + D.f + i * C.f + j * fch, fch)
        elif C.split:
            o_rows(i * C.q, C.q)
            o_rows(D.q + i * C.f, C.f)
        else:
            for a in (0, (D.q + D.f) // 2):
                o_rows(a, (D.q + D.f) // 2)
        return out

    base, n_sems = [], 0
    for l, kind, j in steps:
        base.append(n_sems)
        n_sems += 12 if kind == "q" else 6
    assert n_sems == ys.shape[0]
    y_sent = []

    def y_copy(t, i, kind, src, dst, r):
        at = base[t] + 3 * i + kind
        return remote(src, dst, ys.at[at], yr.at[at], r, col)

    def y_send(*args):
        c = y_copy(*args)
        c.start()
        y_sent.append(c)

    def issue_peer(t):
        for i, (src, place) in enumerate(blocks(t, half if D.cfg[steps[t][0]].split else 0)):
            y_send(t, i, 0, src, place(row), peer)

    def issue_mate(t):
        for i, (src, place) in enumerate(blocks(t, 1 - half if D.cfg[steps[t][0]].split else 0)):
            y_send(t, i, 1, src, place(row), mate)

    def relay(t):
        split = D.cfg[steps[t][0]].split
        with sc(f"relay{t}"):
            for i, (src, place) in enumerate(blocks(t, half if split else 0)):
                y_copy(t, i, 1, src, place(mate), mate).wait_recv()
                if split or i % 2 == 0:
                    y_send(t, i, 2, place(mate), place(mate), peer)
                if not split:
                    y_copy(t, i, 0, src, place(peer), peer).wait_recv()
                    if i % 2 == 1:
                        y_send(t, i, 2, place(peer), place(peer), mate)

    at = {"next": 0, "peer": 0, "mate": 0, "relay": 0}
    first_of = {l: min(t for t, st in enumerate(steps) if st[0] == l) for l in range(D.layers)}

    def step(l, j):
        return min(first_of[l] + j, first_of.get(l + 1, n_steps) - 1)

    def peer_to(t):
        while at["peer"] <= t:
            issue_peer(at["peer"])
            at["peer"] += 1

    def mate_to(t):
        while at["mate"] <= t:
            issue_mate(at["mate"])
            at["mate"] += 1

    def relay_to(t):
        assert t < at["peer"] and t < at["mate"]
        while at["relay"] <= t:
            relay(at["relay"])
            at["relay"] += 1

    def advance():
        t = at["next"]
        assert t < at["relay"], t
        rest = n_row - 1 - peer
        with sc(f"adv{t}"):
            split = D.cfg[steps[t][0]].split
            for i, (src, place) in enumerate(blocks(t, half if split else 0)):
                if split:
                    y_copy(t, i, 0, src, place(peer), peer).wait_recv()
                y_copy(t, i, 2, src, place(rest), rest).wait_recv()
            at["next"] = t + 1

    def have(*which):
        while at["next"] <= step_of[which]:
            advance()

    mate_to(1)
    peer_to(step(0, 3))

    def w_fetch(l, kind, j, slot):
        C = D.cfg[l]
        i = half if C.split else 0
        copies = []

        def fetch(src, dst):
            copies.append(pltpu.make_async_copy(src, dst, lw.at[slot, len(copies)]))

        def w_rows(a, m, at):
            a, at = rows_at(a, m), pl.ds(at, m)
            fetch(w_t.at[l, a, :], wbuf.at[slot, at, own_lanes(row)])
            for r in (up, down, across):
                fetch(g_w.at[l, a, own_lanes(r)], wbuf.at[slot, at, own_lanes(r)])

        if kind == "q":
            w_rows(i * C.q, C.q, 0)
            at = pl.ds(C.q, D.kvp)
            fetch(wkv_t.at[l], wbuf.at[slot, at, own_lanes(row)])
            for r in (up, down, across):
                fetch(g_kv.at[l, :, own_lanes(r)], wbuf.at[slot, at, own_lanes(r)])
        else:
            w_rows(D.q + i * C.f + j * C.cw, C.cw, 0)
            w_rows(D.q + D.f + i * C.f + j * C.cw, C.cw, C.cw)
        return copies

    def o_fetch(l, j, slot):
        C = D.cfg[l]
        copies = []

        def fetch(src, dst):
            copies.append(pltpu.make_async_copy(src, dst, lo.at[slot, len(copies)]))

        spans = ((half * C.q, 0, C.q), (D.q + half * C.f, C.q, C.f)) if C.split else ((0, 0, C.q + C.f),)
        for a, at, m in spans:
            a, at = rows_at(a, m), pl.ds(at, m)
            to = lambda r: pl.ds(pl.multiple_of(r * och, 128), och)
            fetch(w_o.at[l, a, o_lanes(j, row)], wonat.at[slot, at, to(row)])
            for r in (up, down, across):
                fetch(g_wo.at[l, r, a, o_lanes(j, r)], wonat.at[slot, at, to(r)])
        return copies

    def start(copies):
        for c in copies:
            c.start()

    def wait(copies):
        for c in copies:
            c.wait()

    own_x.wait()
    own_g.wait()

    def x_finish(i):
        s = lax.rem(me + n - i, n)
        remote(xland.at[s], xland.at[s], xs.at[i], xr.at[i], row, col).wait_recv()
        remote(gland.at[s], gland.at[s], gs.at[i], gr.at[i], row, col).wait_recv()
        x_copy(i).wait_send()
        g_copy(i).wait_send()

    with sc("xwait"):
        loop(1, n, x_finish)

    def keep(d):
        hid[rows_at(d * dl, dl), :] = xland[d]

    with sc("gains"):
        loop(0, n, keep)
        g_all = gland[...].astype(F32)
        for l in range(D.layers):
            g_rows = g_all[:, l, :]
            g_rows = jnp.concatenate([g_rows, jnp.zeros((128 - n, 128), F32)], axis=0) if n < 128 else g_rows
            g_cols = g_rows.T
            for d in range(n):
                gcol[l, d * dl : (d + 1) * dl, :] = jnp.broadcast_to(g_cols[:dl, d : d + 1], (dl, 128))

    blk = 64
    n_blk = D.d // blk

    def layer_norm(l):
        def add_up(i, acc):
            v = hid[rows_at(i * blk, blk), :].astype(F32)
            return acc + v.reshape(blk // 8, 8, tok).sum(axis=0)

        mean = lax.fori_loop(0, n_blk, add_up, jnp.zeros((8, tok), F32)).sum(axis=0, keepdims=True) / D.d

        def add_sq(i, acc):
            v = hid[rows_at(i * blk, blk), :].astype(F32) - mean
            return acc + (v * v).reshape(blk // 8, 8, tok).sum(axis=0)

        var = lax.fori_loop(0, n_blk, add_sq, jnp.zeros((8, tok), F32)).sum(axis=0, keepdims=True) / D.d
        scale = lax.rsqrt(var + LN_EPS)

        def write(i):
            rows = rows_at(i * blk, blk)
            g = gcol[l, rows, :]
            g = jnp.concatenate([g] * (tok // 128), axis=1)
            v = (hid[rows, :].astype(F32) - mean) * scale * g
            ht[x, rows, my_lanes] = v.astype(BF16)

        with sc(f"norm{l}"):
            loop(0, n_blk, write)

    d_low, d_high = pl.ds(0, D.d // 2), pl.ds(D.d // 2, D.d // 2)

    class Gather:
        def __init__(self, ref, tag):
            self.ref, self.tag, self.sends = ref, tag, []
            for i, c in ((0, right), (1, left), (2, twin)):
                self.send(i, ref(x, False, None), c)

        def send(self, i, ref, c):
            copy = remote(ref, ref, ags.at[self.tag, i], agr.at[self.tag, i], row, c)
            copy.start()
            self.sends.append(copy)

        def arrived(self, i, ref):
            remote(ref, ref, ags.at[self.tag, i], agr.at[self.tag, i], row, col).wait_recv()

        def pass_on(self):
            with sc(f"pass_on{self.tag}"):
                self.arrived(0, self.ref(xl_, False, None))
                self.send(3, self.ref(xl_, False, 0), right)
                self.send(4, self.ref(xl_, False, None), twin)
                self.arrived(1, self.ref(xr_, False, None))
                self.send(5, self.ref(xr_, False, 1), left)
                self.send(6, self.ref(xr_, False, None), twin)

        def own(self):
            self.arrived(2, self.ref(x, True, None))

        def near(self):
            with sc(f"near{self.tag}"):
                self.arrived(4, self.ref(xl_, True, None))
                self.arrived(6, self.ref(xr_, True, None))

        def pass_far(self):
            with sc(f"pass_far{self.tag}"):
                for part, i, j in ((0, 3, 7), (1, 5, 8)):
                    self.arrived(i, self.ref(xf_, False, part))
                    self.send(j, self.ref(xf_, False, part), twin)

        def far(self):
            with sc(f"far{self.tag}"):
                self.arrived(7, self.ref(xf_, True, 0))
                self.arrived(8, self.ref(xf_, True, 1))

        def finish(self):
            for c in self.sends:
                c.wait_send()

    def normed_of(buf):
        def ref(chip, other, part):
            rows = slice(None) if part is None else (d_low, d_high)[part]
            return buf.at[chip, rows, twin_lanes if other else my_lanes]

        return ref

    def kv_of(a):
        def ref(chip, other, part):
            h = D.seqs // 2
            span = pl.ds(a * D.seqs, D.seqs) if part is None else pl.ds(a * D.seqs + part * h, h)
            return kvland.at[chip * 2 + (1 - k if other else k), span]

        return ref

    half_dim = D.hd // 2

    def near3(i):
        return lax.rem(x + i + i // 2, n_x)

    def all4(i):
        return i

    def far1(i):
        return xf_

    def rope(p):
        lo_, hi_ = p[:half_dim], p[half_dim:]
        return jnp.concatenate([lo_ * cos_ref[...] - hi_ * sin_ref[...], hi_ * cos_ref[...] + lo_ * sin_ref[...]], axis=0)

    def project_q(l, a, seq_of, count):
        C = D.cfg[l]

        def body(i):
            s = seq_of(i)
            p = dot(wbuf[1, : C.q + D.kvp, :], ht[s]).astype(BF16).astype(F32)
            for h in range(C.heads):
                at = rows_at((a * D.seqs + s) * C.q + h * D.hd, D.hd)
                qt[at, :] = (rope(p[h * D.hd : (h + 1) * D.hd]) * D.hd**-0.5).astype(BF16)
            kvland[col, a * D.seqs + s] = p[C.q :].astype(BF16)

        with sc(f"q{l}{a}"):
            loop(0, count, body)

    def kv_copy(s, j, source):
        ref = kvland.at[source, s]
        return remote(ref, ref, kvs.at[s, j], kvr.at[s, j], row, lax.rem(col + j, n_col))

    def kv_send(seq_of, count):
        def body(i):
            s = seq_of(i)
            loop(1, n_col, lambda j: kv_copy(s, j, col).start())

        loop(0, count, body)

    def kv_arrive():
        def body(i):
            j = i // D.seqs + 1
            s = lax.rem(i, D.seqs)
            kv_copy(s, j, lax.rem(col + n_col - j, n_col)).wait_recv()
            kv_copy(s, j, col).wait_send()

        with sc("kvwait"):
            loop(0, D.seqs * (n_col - 1), body)

    def key_value(l, a):
        def body(i):
            s = a * D.seqs + i
            raw = kvland[:, s].reshape(n_col * D.kvp, D.seq)
            both = dot(perm_ref[...], raw)
            zeros = jnp.zeros((128 - D.hd, D.seq), F32)
            k_nat = jnp.concatenate([rope(both[: D.hd]), zeros], axis=0).T.astype(BF16)
            kn[s] = k_nat
            vt[s] = both[D.hd :].astype(BF16)
            if a == 0:
                kvbuf[l, 0, i] = k_nat
                kvbuf[l, 1, i] = jnp.concatenate([both[D.hd :], zeros], axis=0).T.astype(BF16)

        with sc(f"kv{l}{a}"):
            loop(0, D.seqs, body)

    qb = D.seq // 2

    def attention(l, a):
        C = D.cfg[l]

        def body(i):
            s, h = a * D.seqs + i // C.heads, lax.rem(i, C.heads)
            q_rows = rows_at(s * C.q + h * D.hd, D.hd)
            o_rows = rows_at(s * (C.q + C.f) + h * D.hd, D.hd)
            for b in range(2):
                ext = (b + 1) * qb
                lanes = slice(b * qb, (b + 1) * qb)
                score = dot(kn[s, :ext, : D.hd], qt[q_rows, lanes])
                keys = lax.broadcasted_iota(jnp.int32, (ext, qb), 0)
                queries = lax.broadcasted_iota(jnp.int32, (ext, qb), 1) + b * qb
                score = jnp.where(keys <= queries, score, -1e30)
                p = jnp.exp(score - jnp.max(score, axis=0, keepdims=True))
                p = (p * (1.0 / jnp.sum(p, axis=0, keepdims=True))).astype(BF16)
                jt[o_rows, lanes] = dot(vt[s, :, :ext], p).astype(BF16)

        with sc(f"attn{l}{a}"):
            loop(0, D.seqs * C.heads, body)

    def gate_up(l, a, slot, j, seq_of, count):
        C = D.cfg[l]

        def body(i):
            s = seq_of(i)
            p = dot(wbuf[slot, : 2 * C.cw, :], ht[s])
            g = p[: C.cw].astype(BF16).astype(F32)
            u = p[C.cw :].astype(BF16).astype(F32)
            jt[rows_at((a * D.seqs + s) * (C.q + C.f) + C.q + j * C.cw, C.cw), :] = (g * jax.nn.sigmoid(g) * u).astype(BF16)

        loop(0, count, body)

    def gate_up_loop(l, a, seq_of, count, first, last, stop=None):
        C = D.cfg[l]
        stop = C.n_c if stop is None else stop
        have_chunk(l, min(last, stop - 1))

        def body(j):
            slot = lax.rem(j, 2)
            wait(w_fetch(l, "f", j, slot))

            @pl.when(j + 1 < stop)
            def _():
                start(w_fetch(l, "f", j + 1, 1 - slot))

            gate_up(l, a, slot, j, seq_of, count)

        with sc(f"gu{l}{a}"):
            loop(first, last, body)

    def have_chunk(l, j):
        C = D.cfg[l]
        have(l, "f", (j + 1) * C.cw // fch - 1)

    def load_q(l):
        have(l, "q", 0)
        copies = w_fetch(l, "q", 0, 1)
        start(copies)
        wait(copies)

    m = och * n_row
    m_low, m_high = pl.ds(0, m // 2), pl.ds(m // 2, m // 2)
    r_slots = twin_in.shape[0]
    r_step = 64

    def order(i):
        return lax.rem(x + lax.rem(2 + 3 * i, 4), n_x)

    class Reduce:
        def __init__(self, l):
            self.l, self.C, self.sends = l, D.cfg[l], {}

        def send(self, u, i, src, dst, c):
            copy = remote(src, dst, rss.at[u % r_slots, i], rsr.at[u % r_slots, i], row, c)
            copy.start()
            self.sends[u].append(copy)

        def arrived(self, u, i, ref):
            remote(ref, ref, rss.at[u % r_slots, i], rsr.at[u % r_slots, i], row, col).wait_recv()

        def twin_copy(self, u, i):
            us = u % r_slots
            return remote(ot.at[u % 2, order(i), :, twin_lanes], twin_in.at[us, i], rss.at[us, i], rsr.at[us, i], row, twin)

        def twin_done(self, u):
            loop(0, 4, lambda i: self.twin_copy(u, i).wait_send())

        def stage_a(self, u, a):
            C = self.C
            if u >= 2:
                self.twin_done(u - 2)
            if u >= r_slots - 1:
                for c in self.sends.pop(u - r_slots + 1):
                    c.wait_send()
            self.sends[u] = []
            R = C.q + C.f

            def body(i):
                s = order(i)
                ot[u % 2, s] = dot(wobuf[:, :R], jt[rows_at((a * D.seqs + s) * R, R), :]).astype(BF16)
                self.twin_copy(u, i).start()

            with sc(f"sa{self.l}_{u}"):
                loop(0, 4, body)

        def stage_b(self, u):
            us = u % r_slots

            def body(i):
                self.arrived(u, i, twin_in.at[us, i])
                s = order(i)

                def add(b):
                    at = rows_at(b * r_step, r_step)
                    twin_in[us, i, at, :] = (ot[u % 2, s, at, my_lanes].astype(F32) + twin_in[us, i, at, :].astype(F32)).astype(BF16)

                loop(0, m // r_step, add)

            with sc(f"sb{self.l}_{u}"):
                loop(0, 1, body)
                self.send(u, 4, twin_in.at[us, 0, m_low], far_in.at[us, m_low], right)
                self.send(u, 5, twin_in.at[us, 0, m_high], far_in.at[us, m_high], left)
                loop(1, 4, body)

        def stage_c(self, u):
            us = u % r_slots

            def add_far(i, base):
                def add(b):
                    at = rows_at(base + b * r_step, r_step)
                    twin_in[us, i, at, :] = (twin_in[us, i, at, :].astype(F32) + far_in[us, at, :].astype(F32)).astype(BF16)

                loop(0, m // 2 // r_step, add)

            with sc(f"sc{self.l}_{u}"):
                self.arrived(u, 4, far_in.at[us, m_low])
                add_far(1, 0)
                self.send(u, 6, twin_in.at[us, 1], near_in.at[us, 0], right)
                self.arrived(u, 5, far_in.at[us, m_high])
                add_far(3, m // 2)
                self.send(u, 7, twin_in.at[us, 3], near_in.at[us, 1], left)

        def add_update(self, j, total):
            step = min(r_step, och)
            for r in range(n_row):

                def add(b, r=r):
                    dst = rows_at(r * dr + (r + j) % D.n_o * och + b * step, step)
                    u = total(rows_at(r * och + b * step, step)).astype(BF16).astype(F32)
                    hid[dst, :] = (hid[dst, :].astype(F32) + u).astype(BF16)

                loop(0, och // step, add)

        def stage_d(self, u, j, a):
            us = u % r_slots

            def total(at):
                return twin_in[us, 2, at, :].astype(F32) + near_in[us, 0, at, :].astype(F32) + near_in[us, 1, at, :].astype(F32)

            with sc(f"sd{self.l}_{u}"):
                self.arrived(u, 6, near_in.at[us, 0])
                self.arrived(u, 7, near_in.at[us, 1])
                if self.C.split:

                    def save(b):
                        at = rows_at(b * r_step, r_step)
                        psum[a, j, at, :] = total(at).astype(BF16)

                    loop(0, m // r_step, save)
                    if a == 1:
                        remote(psum.at[1, j], pair_in.at[j], es.at[j], er.at[j], mate, col).start()
                else:
                    self.add_update(j, total)

        def stage_e(self, j):
            with sc(f"se{self.l}_{j}"):
                c = remote(psum.at[1, j], pair_in.at[j], es.at[j], er.at[j], mate, col)
                c.wait_recv()
                self.add_update(j, lambda at: psum[0, j, at, :].astype(F32) + pair_in[j, at, :].astype(F32))
                c.wait_send()

        def finish(self, units):
            with sc(f"rfin{self.l}"):
                for u in range(max(0, units - 2), units):
                    self.twin_done(u)
                for u in self.sends:
                    for c in self.sends[u]:
                        c.wait_send()

    o_started = set()

    def o_load(l, j, a):
        if (l, j, a) not in o_started:
            have(l, "o", j)
            start(o_fetch(l, j, j % 2))
            o_started.add((l, j, a))

    def o_use(l, j, a):
        C = D.cfg[l]
        with sc(f"ouse{l}_{j}"):
            o_load(l, j, a)
            wait(o_fetch(l, j, j % 2))
            R = C.q + C.f
            for r in range(n_row):
                wobuf[r * och : (r + 1) * och, :R] = wonat[j % 2, :R, r * och : (r + 1) * och].T

    layer_norm(0)
    g0 = Gather(normed_of(ht), 0)
    mine = ht.at[x, :, my_lanes]
    shared = g_h.at[x, :, my_lanes]
    to_mate = remote(mine, shared, ps, pr_, mate, col)
    to_mate.start()
    relay_to(1)
    mate_to(step(0, 5))
    peer_to(step(0, 5))
    g0.pass_on()
    with sc("mate"):
        to_mate.wait_recv()
    g1 = Gather(normed_of(g_h), 1)
    load_q(0)
    g0.own()
    g0.near()
    project_q(0, 0, near3, 3)
    relay_to(2)
    mate_to(step(0, 10))
    g0.pass_far()
    g0.far()
    project_q(0, 0, far1, 1)
    kv0 = Gather(kv_of(0), 2)
    relay_to(3)
    n_f = D.cfg[0].n_f
    f_started = set()

    def f_load(j):
        if j not in f_started:
            f_started.add(j)
            start(w_fetch(0, "f", j, j % 2))

    def h_copy(i):
        return pltpu.make_async_copy(g_h.at[i], ht.at[i], lh.at[i])

    for j in range(n_f):
        if j == n_f - 1:
            kv0.pass_on()
            g1.pass_on()
            for t in (7, 8):
                relay_to(step(0, t))
                peer_to(step(0, t + 1))
        have(0, "f", j)
        f_load(j)
        with sc(f"gu0_{j}"):
            wait(w_fetch(0, "f", j, j % 2))
            gate_up(0, 0, j % 2, j, all4, 4)
        if j == 0:
            relay_to(step(0, 4))
        elif j == n_f - 3:
            relay_to(step(0, 5))
            peer_to(step(0, 6))
            relay_to(step(0, 6))
            peer_to(step(0, 7))
    relay_to(step(0, 9))
    peer_to(step(0, 10))
    relay_to(step(0, 10))
    peer_to(step(1, 5))
    mate_to(step(1, D.cfg[1].n_f))
    g0.finish()
    to_mate.wait_send()
    g1.own()
    g1.near()
    loop(0, 3, lambda i: h_copy(near3(i)).start())
    kv0.pass_far()
    with sc("kv0wait"):
        kv0.own()
        kv0.near()
        kv0.far()
        kv0.finish()
    key_value(0, 0)
    attention(0, 0)

    red = Reduce(0)
    units = [(j, 0) for j in range(D.n_o - 1)] + [(j, 1) for j in range(D.n_o)] + [(D.n_o - 1, 0)]
    n_u = len(units)
    first = D.n_o - 1
    state = {"e": 0}

    def settle(count):
        while state["e"] < count:
            red.stage_e(state["e"])
            state["e"] += 1

    def unit(u):
        j, a = units[u]
        if u == 0 or units[u - 1][0] != j:
            o_use(0, j, a)
        red.stage_a(u, a)
        if u + 1 < n_u and units[u + 1][0] != j:
            o_load(0, *units[u + 1])
        if u >= 2:
            red.stage_c(u - 2)
        if u >= 3:
            red.stage_d(u - 3, *units[u - 3])
        red.stage_b(u)

    unit(0)
    g1.pass_far()
    g1.far()
    h_copy(xf_).start()
    load_q(0)
    start(w_fetch(0, "f", 0, 0))
    loop(0, 3, lambda i: h_copy(near3(i)).wait())
    h_copy(xf_).wait()
    project_q(0, 1, all4, 4)
    kv1 = Gather(kv_of(1), 3)
    parts = first - 2
    cuts = [n_f * i // parts for i in range(parts + 1)]
    for u in range(1, first):
        unit(u)
        if u == 2:
            kv1.pass_on()
        if 1 < u:
            gate_up_loop(0, 1, all4, 4, cuts[u - 2], cuts[u - 1])
    kv1.pass_far()
    relay_to(step(1, 1))
    with sc("kv1wait"):
        kv1.own()
        kv1.near()
        kv1.far()
        kv1.finish()
    key_value(0, 1)
    attention(0, 1)
    g1.finish()
    relay_to(step(1, 2))
    peer_to(step(1, 7))
    n_f1 = D.cfg[1].n_f
    for u in range(first, n_u):
        unit(u)
        if u == n_u - 1:
            settle(1)
        v = u - first
        if v in (0, 1, 2):
            relay_to(step(1, min(v + 3, n_f1)))
            peer_to(step(1, min(v + 8, n_f1)))
        elif v == 4:
            relay_to(step(1, min(6, n_f1)))
            peer_to(step(1, n_f1))
    red.stage_c(n_u - 2)
    red.stage_d(n_u - 3, *units[n_u - 3])
    red.stage_c(n_u - 1)
    red.stage_d(n_u - 2, *units[n_u - 2])
    relay_to(step(1, min(7, n_f1)))
    settle(D.n_o - 1)
    red.stage_d(n_u - 1, *units[n_u - 1])
    settle(D.n_o)
    red.finish(n_u)

    def y_copy_back(i):
        d = lax.rem(me + i, n)
        return remote(hid.at[rows_at(d * dl, dl), :], piece_of(y_out, me), xs.at[i], xr.at[i], d // n_col, lax.rem(d, n_col))

    own_y = pltpu.make_async_copy(hid.at[rows_at(me * dl, dl), :], piece_of(y_out, me), xr.at[0])

    def y_send_back(d):
        i = lax.rem(d - me + n, n)

        @pl.when(i == 0)
        def _():
            own_y.start()

        @pl.when(i != 0)
        def _():
            y_copy_back(i).start()

    def y_ready(j):
        def body(d):
            r, a = d // n_col, lax.rem(d, n_col) * dl
            first = lax.rem(a // och + D.n_o - lax.rem(r, D.n_o), D.n_o)
            second = lax.rem((a + dl - 1) // och + D.n_o - lax.rem(r, D.n_o), D.n_o)

            @pl.when(jnp.maximum(first, second) == j)
            def _():
                y_send_back(d)

        loop(0, n, body)

    for l in range(1, D.layers):
        C = D.cfg[l]
        layer_norm(l)
        g0 = Gather(normed_of(ht), 0)
        peer_to(step(l, C.n_f))
        mate_to(step(l, C.n_f))
        relay_to(step(l, min(8, C.n_f)))
        own1, near2 = (lambda i: x), (lambda i: lax.rem(x + 1 + 2 * i, n_x))
        n_mid = min(3, C.n_c - 1)

        def begin(seq_of, count):
            load_q(l)
            have_chunk(l, 0)
            start(w_fetch(l, "f", 0, 0))
            project_q(l, 0, seq_of, count)

        g0.own()
        begin(own1, 1)
        kv_send(own1, 1)
        gate_up_loop(l, 0, own1, 1, 0, n_mid, n_mid)
        peer_to(step(l, C.n_f + 1))
        mate_to(step(l, C.n_f + 1))
        relay_to(step(l, C.n_f))
        g0.pass_on()
        peer_to(step(l, C.n_f + D.n_o))
        mate_to(step(l, C.n_f + D.n_o))
        g0.near()
        begin(near2, 2)
        kv_send(near2, 2)
        gate_up_loop(l, 0, near2, 2, 0, n_mid)
        g0.pass_far()
        relay_to(step(l, C.n_f + 1))
        gate_up_loop(l, 0, near3, 3, n_mid, C.n_c)
        relay_to(step(l, C.n_f + 2))
        g0.far()
        begin(far1, 1)
        kv_send(far1, 1)
        gate_up_loop(l, 0, far1, 1, 0, C.n_c)
        relay_to(step(l, C.n_f + 3))
        o_load(l, 0, 0)
        g0.finish()
        kv_arrive()
        key_value(l, 0)
        attention(l, 0)
        relay_to(step(l, C.n_f + 4))
        red = Reduce(l)
        last = l + 1 == D.layers

        def send_final(j):
            if last:
                y_ready(j)

        end = D.n_o - 1
        for j in range(D.n_o):
            o_use(l, j, 0)
            red.stage_a(j, 0)
            if j == 0:
                relay_to(step(l, C.n_f + D.n_o))
            if j < end:
                o_load(l, j + 1, 0)
            if 1 <= j:
                red.stage_c(j - 1)
            if 2 <= j:
                red.stage_d(j - 2, j - 2, 0)
            red.stage_b(j)
        red.stage_c(end)
        red.stage_d(end - 1, end - 1, 0)
        for j in range(end):
            send_final(j)
        red.stage_d(end, end, 0)
        send_final(end)
        red.finish(D.n_o)

    def kv_back(i):
        r = lax.rem(row + i, n_row)
        pos = rows_at((r * n_col + col) * D.pos, D.pos)
        return kvbuf.at[:, :, :, pos, :], kv_out.at[:, :, pl.ds(row * D.seqs, D.seqs)], r

    src, dst, _ = kv_back(0)
    own_kv = pltpu.make_async_copy(src, dst, fl)
    own_kv.start()
    kv_sends = []
    for i in range(1, n_row):
        src, dst, r = kv_back(i)
        c = remote(src, dst, fs.at[i], fr.at[i], r, col)
        c.start()
        kv_sends.append(c)

    def y_finish(i):
        s = lax.rem(me + n - i, n)
        remote(piece_of(y_out, s), piece_of(y_out, s), xs.at[i], xr.at[i], row, col).wait_recv()
        y_copy_back(i).wait_send()

    with sc("ywait"):
        loop(1, n, y_finish)
        own_y.wait()
        own_kv.wait()
        for i in range(1, n_row):
            r = lax.rem(row + n_row - i, n_row)
            dst = kv_out.at[:, :, pl.ds(r * D.seqs, D.seqs)]
            remote(dst, dst, fs.at[i], fr.at[i], row, col).wait_recv()
        for c in kv_sends:
            c.wait_send()
        for c in y_sent:
            c.wait_send()


def solution(mesh):
    n_row, n_col = mesh.shape["row"], mesh.shape["col"]
    group = n_row * n_col
    act_spec = P("dp", None, ("row", "col"))
    weight_spec = P(None, "row", "col")

    def device_fn(x_loc, gain_loc, w_in_loc, w_kv_loc, w_out_loc):
        D = Dims()
        D.n_row, D.n_col = n_row, n_col
        n_batch, D.seq, D.dl = x_loc.shape
        D.layers, D.dr, e = w_in_loc.shape
        D.d = D.dl * group
        r_block = w_out_loc.shape[1]
        D.f = e - r_block
        D.q = r_block - D.f
        kv_local = w_kv_loc.shape[2]
        D.hd = kv_local * n_col // 2
        D.kvp = 32
        D.tok = n_batch * D.seq // group
        D.seqs = n_batch // n_row
        D.pos = D.seq // group
        D.fch = 128
        D.och = 128
        D.n_o = D.dr // D.och
        D.cfg = []
        for l in range(D.layers):
            C = Dims()
            C.split = l == 0
            parts = 2 if C.split else 1
            C.q, C.f = D.q // parts, D.f // parts
            C.heads, C.n_f = C.q // D.hd, C.f // D.fch
            C.cw = D.fch if C.split else 2 * D.fch
            C.n_c = C.f // C.cw
            D.cfg.append(C)
        assert D.seq == 2 * D.tok and D.seqs == n_col // 2 == n_row == 4

        half = D.hd // 2
        inv_freq = (np.float32(1.0) / (np.float32(10000.0) ** (np.arange(half, dtype=np.float32) * np.float32(2.0) / np.float32(D.hd)))).astype(np.float32)
        angles = (inv_freq[:, None] * np.arange(D.seq, dtype=np.float32)[None, :]).astype(np.float32)
        cos_t, sin_t = np.cos(angles).astype(np.float32), np.sin(angles).astype(np.float32)
        perm = np.zeros((2 * D.hd, n_col * D.kvp), np.float32)
        for i in range(2 * D.hd):
            perm[i, (i // kv_local) * D.kvp + i % kv_local] = 1.0

        x_t = x_loc.transpose(0, 2, 1)
        w_t = w_in_loc.transpose(0, 2, 1)
        wkv_t = jnp.pad(w_kv_loc.transpose(0, 2, 1), ((0, 0), (0, D.kvp - kv_local), (0, 0)))
        gains = jnp.pad(gain_loc, ((0, 16 - D.layers), (0, 128 - D.dl)))

        n_y = sum(12 + 6 * (C.n_f + D.n_o) for C in D.cfg)
        m = D.och * n_row
        sds = jax.ShapeDtypeStruct
        dma = pltpu.SemaphoreType.DMA
        out = pl.pallas_call(
            functools.partial(kernel, D),
            out_shape=(
                sds(x_t.shape, BF16),
                sds((D.layers, 2, n_batch, D.pos, 128), BF16),
                sds((D.layers, e, D.d), BF16),
                sds((D.layers, D.kvp, D.d), BF16),
                sds((D.layers, n_row, r_block, D.dr), BF16),
                sds((D.seqs, D.d, D.seq), BF16),
            ),
            in_specs=[ANY] * 5 + [VMEM] * 3,
            out_specs=(ANY,) * 6,
            scratch_shapes=[
                pltpu.VMEM((group, D.dl, D.tok), BF16),
                pltpu.VMEM((group, 16, 128), BF16),
                pltpu.VMEM((D.layers, D.d, 128), F32),
                pltpu.VMEM((D.d, D.tok), BF16),
                pltpu.VMEM((D.seqs, D.d, D.seq), BF16),
                pltpu.VMEM((2, max(4 * D.fch, D.q + D.kvp), D.d), BF16),
                pltpu.VMEM((2, r_block, m), BF16),
                pltpu.VMEM((m, r_block), BF16),
                pltpu.VMEM((D.seqs * D.q, D.seq), BF16),
                pltpu.VMEM((n_col, 2 * D.seqs, D.kvp, D.seq), BF16),
                pltpu.VMEM((2 * D.seqs, D.seq, 128), BF16),
                pltpu.VMEM((2 * D.seqs, D.hd, D.seq), BF16),
                pltpu.VMEM((D.layers, 2, D.seqs, D.seq, 128), BF16),
                pltpu.VMEM((D.seqs * r_block, D.seq), BF16),
                pltpu.VMEM((2, D.seqs, m, D.seq), BF16),
                pltpu.VMEM((5, 4, m, D.tok), BF16),
                pltpu.VMEM((5, m, D.tok), BF16),
                pltpu.VMEM((5, 2, m, D.tok), BF16),
                pltpu.VMEM((2, D.n_o, m, D.tok), BF16),
                pltpu.VMEM((D.n_o, m, D.tok), BF16),
                dma((group,)), dma((group,)), dma((group,)), dma((group,)),
                dma((n_y,)), dma((n_y,)),
                dma((4, 9)), dma((4, 9)), dma, dma,
                dma((D.seqs, n_col)), dma((D.seqs, n_col)),
                dma((5, 8)), dma((5, 8)),
                dma((D.n_o,)), dma((D.n_o,)),
                dma((2, 8)), dma((2, 8)), dma((D.seqs,)),
                dma((n_row,)), dma((n_row,)), dma,
            ],
            compiler_params=pltpu.CompilerParams(collective_id=0, has_side_effects=True, vmem_limit_bytes=67_000_000),
            name="two_layers",
        )(x_t, gains, w_t, wkv_t, w_out_loc, jnp.asarray(cos_t), jnp.asarray(sin_t), jnp.asarray(perm, BF16))
        return out[0].transpose(0, 2, 1), out[1][..., : D.hd]

    return jax.shard_map(device_fn, mesh=mesh, in_specs=(act_spec, P(None, ("row", "col")), weight_spec, weight_spec, P(None, "col", "row")), out_specs=(act_spec, P(None, None, "dp", ("row", "col"), None)), check_vma=False)
```

```python
import functools

import numpy as np

import jax
import jax.numpy as jnp
from jax import lax
from jax.experimental import pallas as pl
from jax.experimental.pallas import tpu as pltpu
from jax.sharding import PartitionSpec as P

LN_EPS = 1e-6
MESH = pl.DeviceIdType.MESH
ANY = pl.BlockSpec(memory_space=pl.ANY)
VMEM = pl.BlockSpec(memory_space=pltpu.VMEM)
F32, BF16 = jnp.float32, jnp.bfloat16


def dot(a, b):
    return jnp.dot(a, b, preferred_element_type=F32)


class Dims:
    pass


def rows_at(start, count, by=16):
    return pl.ds(start if isinstance(start, int) else pl.multiple_of(start, by), count)


def kernel(
    D,
    x_t, gains, w_t, wkv_t, w_o, cos_ref, sin_ref, perm_ref,
    y_out, kv_out, g_w, g_kv, g_wo, g_h,
    xland, gland, gcol, hid, ht, wbuf, wonat, wobuf, qt, kvland, kn, vt, kvbuf, jt, ot, twin_in, far_in, near_in, psum, pair_in,
    xs, xr, gs, gr, ys, yr, ags, agr, ps, pr_, kvs, kvr, rss, rsr, es, er, lw, lo, lh, fs, fr, fl,
):
    sc = jax.named_scope
    row, col = lax.axis_index("row"), lax.axis_index("col")
    n_row, n_col, n = D.n_row, D.n_col, D.n_row * D.n_col
    n_x = n_col // 2
    me = row * n_col + col
    x, k = col // 2, lax.rem(col, 2)
    xr_, xl_, xf_ = lax.rem(x + 1, n_x), lax.rem(x + n_x - 1, n_x), lax.rem(x + 2, n_x)
    right, left, twin = xr_ * 2 + k, xl_ * 2 + k, x * 2 + 1 - k
    up, down, across = lax.rem(row + 1, n_row), lax.rem(row + n_row - 1, n_row), lax.rem(row + 2, n_row)
    half, mate = row // 2, n_row - 1 - row
    peer = row + 1 - 2 * lax.rem(row, 2)
    tok, dl, dr = D.tok, D.dl, D.dr
    och, fch = D.och, D.fch
    my_lanes = pl.ds(pl.multiple_of(k * tok, 128), tok)
    twin_lanes = pl.ds(pl.multiple_of((1 - k) * tok, 128), tok)

    def remote(src, dst, ssem, rsem, r, c):
        return pltpu.make_async_remote_copy(src_ref=src, dst_ref=dst, send_sem=ssem, recv_sem=rsem, device_id={"row": r, "col": c}, device_id_type=MESH)

    def loop(lo_, hi_, f):
        def body(i, carry):
            f(i)
            return carry

        lax.fori_loop(lo_, hi_, body, 0)

    barrier = pltpu.get_barrier_semaphore()

    def greet(i):
        d = lax.rem(me + i, n)
        pl.semaphore_signal(barrier, inc=1, device_id={"row": d // n_col, "col": lax.rem(d, n_col)}, device_id_type=MESH)

    with sc("barrier"):
        loop(1, n, greet)
        pl.semaphore_wait(barrier, n - 1)

    def piece_of(ref, d):
        return ref.at[d // 2, :, pl.ds(pl.multiple_of(lax.rem(d, 2) * tok, 128), tok)]

    def x_copy(i):
        d = lax.rem(me + i, n)
        return remote(piece_of(x_t, d), xland.at[me], xs.at[i], xr.at[i], d // n_col, lax.rem(d, n_col))

    def g_copy(i):
        d = lax.rem(me + i, n)
        return remote(gains, gland.at[me], gs.at[i], gr.at[i], d // n_col, lax.rem(d, n_col))

    def x_start(i):
        x_copy(i).start()
        g_copy(i).start()

    own_x = pltpu.make_async_copy(piece_of(x_t, me), xland.at[me], xr.at[0])
    own_g = pltpu.make_async_copy(gains, gland.at[me], gr.at[0])
    own_x.start()
    own_g.start()
    loop(1, n, x_start)

    def own_lanes(r):
        return pl.ds(pl.multiple_of(r * dr, 128), dr)

    def o_lanes(j, r):
        return pl.ds(pl.multiple_of(lax.rem(r + j, D.n_o) * och, 128), och)

    steps = []
    for l, C in enumerate(D.cfg):
        steps += [(l, "q", 0)] + [(l, "f", j) for j in range(C.n_f)] + [(l, "o", j) for j in range(D.n_o)]
    n_steps = len(steps)
    step_of = {s: t for t, s in enumerate(steps)}

    def blocks(t, i):
        l, kind, j = steps[t]
        C = D.cfg[l]
        out = []

        def w_rows(a, m):
            at = rows_at(a, m)
            out.append((w_t.at[l, at, :], lambda r: g_w.at[l, at, own_lanes(r)]))

        def o_rows(a, m):
            at = rows_at(a, m)
            out.append((w_o.at[l, at, o_lanes(j, row)], lambda r: g_wo.at[l, r, at, o_lanes(j, r)]))

        def kv_rows(a, m):
            at = pl.ds(a, m)
            out.append((wkv_t.at[l, at, :], lambda r: g_kv.at[l, at, own_lanes(r)]))

        if kind == "q":
            for a in (0, C.q // 2):
                w_rows(i * C.q + a, C.q // 2)
            for a in (0, D.kvp // 2):
                kv_rows(a, D.kvp // 2)
        elif kind == "f":
            w_rows(D.q + i * C.f + j * fch, fch)
            w_rows(D.q + D.f + i * C.f + j * fch, fch)
        elif C.split:
            o_rows(i * C.q, C.q)
            o_rows(D.q + i * C.f, C.f)
        else:
            for a in (0, (D.q + D.f) // 2):
                o_rows(a, (D.q + D.f) // 2)
        return out

    base, n_sems = [], 0
    for l, kind, j in steps:
        base.append(n_sems)
        n_sems += 12 if kind == "q" else 6
    assert n_sems == ys.shape[0]
    y_sent = []

    def y_copy(t, i, kind, src, dst, r):
        at = base[t] + 3 * i + kind
        return remote(src, dst, ys.at[at], yr.at[at], r, col)

    def y_send(*args):
        c = y_copy(*args)
        c.start()
        y_sent.append(c)

    def issue_peer(t):
        for i, (src, place) in enumerate(blocks(t, half if D.cfg[steps[t][0]].split else 0)):
            y_send(t, i, 0, src, place(row), peer)

    def issue_mate(t):
        for i, (src, place) in enumerate(blocks(t, 1 - half if D.cfg[steps[t][0]].split else 0)):
            y_send(t, i, 1, src, place(row), mate)

    def relay(t):
        split = D.cfg[steps[t][0]].split
        with sc(f"relay{t}"):
            for i, (src, place) in enumerate(blocks(t, half if split else 0)):
                y_copy(t, i, 1, src, place(mate), mate).wait_recv()
                if split or i % 2 == 0:
                    y_send(t, i, 2, place(mate), place(mate), peer)
                if not split:
                    y_copy(t, i, 0, src, place(peer), peer).wait_recv()
                    if i % 2 == 1:
                        y_send(t, i, 2, place(peer), place(peer), mate)

    at = {"next": 0, "peer": 0, "mate": 0, "relay": 0}
    first_of = {l: min(t for t, st in enumerate(steps) if st[0] == l) for l in range(D.layers)}

    def step(l, j):
        return min(first_of[l] + j, first_of.get(l + 1, n_steps) - 1)

    def peer_to(t):
        while at["peer"] <= t:
            issue_peer(at["peer"])
            at["peer"] += 1

    def mate_to(t):
        while at["mate"] <= t:
            issue_mate(at["mate"])
            at["mate"] += 1

    def relay_to(t):
        assert t < at["peer"] and t < at["mate"]
        while at["relay"] <= t:
            relay(at["relay"])
            at["relay"] += 1

    def advance():
        t = at["next"]
        assert t < at["relay"], t
        rest = n_row - 1 - peer
        with sc(f"adv{t}"):
            split = D.cfg[steps[t][0]].split
            for i, (src, place) in enumerate(blocks(t, half if split else 0)):
                if split:
                    y_copy(t, i, 0, src, place(peer), peer).wait_recv()
                y_copy(t, i, 2, src, place(rest), rest).wait_recv()
            at["next"] = t + 1

    def have(*which):
        while at["next"] <= step_of[which]:
            advance()

    mate_to(1)
    peer_to(step(0, 3))

    def w_fetch(l, kind, j, slot):
        C = D.cfg[l]
        i = half if C.split else 0
        copies = []

        def fetch(src, dst):
            copies.append(pltpu.make_async_copy(src, dst, lw.at[slot, len(copies)]))

        def w_rows(a, m, at):
            a, at = rows_at(a, m), pl.ds(at, m)
            fetch(w_t.at[l, a, :], wbuf.at[slot, at, own_lanes(row)])
            for r in (up, down, across):
                fetch(g_w.at[l, a, own_lanes(r)], wbuf.at[slot, at, own_lanes(r)])

        if kind == "q":
            w_rows(i * C.q, C.q, 0)
            at = pl.ds(C.q, D.kvp)
            fetch(wkv_t.at[l], wbuf.at[slot, at, own_lanes(row)])
            for r in (up, down, across):
                fetch(g_kv.at[l, :, own_lanes(r)], wbuf.at[slot, at, own_lanes(r)])
        else:
            w_rows(D.q + i * C.f + j * C.cw, C.cw, 0)
            w_rows(D.q + D.f + i * C.f + j * C.cw, C.cw, C.cw)
        return copies

    def o_fetch(l, j, slot):
        C = D.cfg[l]
        copies = []

        def fetch(src, dst):
            copies.append(pltpu.make_async_copy(src, dst, lo.at[slot, len(copies)]))

        spans = ((half * C.q, 0, C.q), (D.q + half * C.f, C.q, C.f)) if C.split else ((0, 0, C.q + C.f),)
        for a, at, m in spans:
            a, at = rows_at(a, m), pl.ds(at, m)
            to = lambda r: pl.ds(pl.multiple_of(r * och, 128), och)
            fetch(w_o.at[l, a, o_lanes(j, row)], wonat.at[slot, at, to(row)])
            for r in (up, down, across):
                fetch(g_wo.at[l, r, a, o_lanes(j, r)], wonat.at[slot, at, to(r)])
        return copies

    def start(copies):
        for c in copies:
            c.start()

    def wait(copies):
        for c in copies:
            c.wait()

    own_x.wait()
    own_g.wait()

    def x_finish(i):
        s = lax.rem(me + n - i, n)
        remote(xland.at[s], xland.at[s], xs.at[i], xr.at[i], row, col).wait_recv()
        remote(gland.at[s], gland.at[s], gs.at[i], gr.at[i], row, col).wait_recv()
        x_copy(i).wait_send()
        g_copy(i).wait_send()

    with sc("xwait"):
        loop(1, n, x_finish)

    def keep(d):
        hid[rows_at(d * dl, dl), :] = xland[d]

    with sc("gains"):
        loop(0, n, keep)
        g_all = gland[...].astype(F32)
        for l in range(D.layers):
            g_rows = g_all[:, l, :]
            g_rows = jnp.concatenate([g_rows, jnp.zeros((128 - n, 128), F32)], axis=0) if n < 128 else g_rows
            g_cols = g_rows.T
            for d in range(n):
                gcol[l, d * dl : (d + 1) * dl, :] = jnp.broadcast_to(g_cols[:dl, d : d + 1], (dl, 128))

    blk = 64
    n_blk = D.d // blk

    def layer_norm(l):
        def add_up(i, acc):
            v = hid[rows_at(i * blk, blk), :].astype(F32)
            return acc + v.reshape(blk // 8, 8, tok).sum(axis=0)

        mean = lax.fori_loop(0, n_blk, add_up, jnp.zeros((8, tok), F32)).sum(axis=0, keepdims=True) / D.d

        def add_sq(i, acc):
            v = hid[rows_at(i * blk, blk), :].astype(F32) - mean
            return acc + (v * v).reshape(blk // 8, 8, tok).sum(axis=0)

        var = lax.fori_loop(0, n_blk, add_sq, jnp.zeros((8, tok), F32)).sum(axis=0, keepdims=True) / D.d
        scale = lax.rsqrt(var + LN_EPS)

        def write(i):
            rows = rows_at(i * blk, blk)
            g = gcol[l, rows, :]
            g = jnp.concatenate([g] * (tok // 128), axis=1)
            v = (hid[rows, :].astype(F32) - mean) * scale * g
            ht[x, rows, my_lanes] = v.astype(BF16)

        with sc(f"norm{l}"):
            loop(0, n_blk, write)

    d_low, d_high = pl.ds(0, D.d // 2), pl.ds(D.d // 2, D.d // 2)

    class Gather:
        def __init__(self, ref, tag):
            self.ref, self.tag, self.sends = ref, tag, []
            for i, c in ((0, right), (1, left), (2, twin)):
                self.send(i, ref(x, False, None), c)

        def send(self, i, ref, c):
            copy = remote(ref, ref, ags.at[self.tag, i], agr.at[self.tag, i], row, c)
            copy.start()
            self.sends.append(copy)

        def arrived(self, i, ref):
            remote(ref, ref, ags.at[self.tag, i], agr.at[self.tag, i], row, col).wait_recv()

        def pass_on(self):
            with sc(f"pass_on{self.tag}"):
                self.arrived(0, self.ref(xl_, False, None))
                self.send(3, self.ref(xl_, False, 0), right)
                self.send(4, self.ref(xl_, False, None), twin)
                self.arrived(1, self.ref(xr_, False, None))
                self.send(5, self.ref(xr_, False, 1), left)
                self.send(6, self.ref(xr_, False, None), twin)

        def own(self):
            self.arrived(2, self.ref(x, True, None))

        def near(self):
            with sc(f"near{self.tag}"):
                self.arrived(4, self.ref(xl_, True, None))
                self.arrived(6, self.ref(xr_, True, None))

        def pass_far(self):
            with sc(f"pass_far{self.tag}"):
                for part, i, j in ((0, 3, 7), (1, 5, 8)):
                    self.arrived(i, self.ref(xf_, False, part))
                    self.send(j, self.ref(xf_, False, part), twin)

        def far(self):
            with sc(f"far{self.tag}"):
                self.arrived(7, self.ref(xf_, True, 0))
                self.arrived(8, self.ref(xf_, True, 1))

        def finish(self):
            for c in self.sends:
                c.wait_send()

    def normed_of(buf):
        def ref(chip, other, part):
            rows = slice(None) if part is None else (d_low, d_high)[part]
            return buf.at[chip, rows, twin_lanes if other else my_lanes]

        return ref

    def kv_of(a):
        def ref(chip, other, part):
            h = D.seqs // 2
            span = pl.ds(a * D.seqs, D.seqs) if part is None else pl.ds(a * D.seqs + part * h, h)
            return kvland.at[chip * 2 + (1 - k if other else k), span]

        return ref

    half_dim = D.hd // 2

    def near3(i):
        return lax.rem(x + i + i // 2, n_x)

    def all4(i):
        return i

    def far1(i):
        return xf_

    def rope(p):
        lo_, hi_ = p[:half_dim], p[half_dim:]
        return jnp.concatenate([lo_ * cos_ref[...] - hi_ * sin_ref[...], hi_ * cos_ref[...] + lo_ * sin_ref[...]], axis=0)

    def project_q(l, a, seq_of, count):
        C = D.cfg[l]

        def body(i):
            s = seq_of(i)
            p = dot(wbuf[1, : C.q + D.kvp, :], ht[s]).astype(BF16).astype(F32)
            for h in range(C.heads):
                at = rows_at((a * D.seqs + s) * C.q + h * D.hd, D.hd)
                qt[at, :] = (rope(p[h * D.hd : (h + 1) * D.hd]) * D.hd**-0.5).astype(BF16)
            kvland[col, a * D.seqs + s] = p[C.q :].astype(BF16)

        with sc(f"q{l}{a}"):
            loop(0, count, body)

    def kv_copy(s, j, source):
        ref = kvland.at[source, s]
        return remote(ref, ref, kvs.at[s, j], kvr.at[s, j], row, lax.rem(col + j, n_col))

    def kv_send(seq_of, count):
        def body(i):
            s = seq_of(i)
            loop(1, n_col, lambda j: kv_copy(s, j, col).start())

        loop(0, count, body)

    def kv_arrive():
        def body(i):
            j = i // D.seqs + 1
            s = lax.rem(i, D.seqs)
            kv_copy(s, j, lax.rem(col + n_col - j, n_col)).wait_recv()
            kv_copy(s, j, col).wait_send()

        with sc("kvwait"):
            loop(0, D.seqs * (n_col - 1), body)

    def key_value(l, a):
        def body(i):
            s = a * D.seqs + i
            raw = kvland[:, s].reshape(n_col * D.kvp, D.seq)
            both = dot(perm_ref[...], raw)
            zeros = jnp.zeros((128 - D.hd, D.seq), F32)
            k_nat = jnp.concatenate([rope(both[: D.hd]), zeros], axis=0).T.astype(BF16)
            kn[s] = k_nat
            vt[s] = both[D.hd :].astype(BF16)
            if a == 0:
                kvbuf[l, 0, i] = k_nat
                kvbuf[l, 1, i] = jnp.concatenate([both[D.hd :], zeros], axis=0).T.astype(BF16)

        with sc(f"kv{l}{a}"):
            loop(0, D.seqs, body)

    qb = D.seq // 2

    def attention(l, a):
        C = D.cfg[l]

        def body(i):
            s, h = a * D.seqs + i // C.heads, lax.rem(i, C.heads)
            q_rows = rows_at(s * C.q + h * D.hd, D.hd)
            o_rows = rows_at(s * (C.q + C.f) + h * D.hd, D.hd)
            for b in range(2):
                ext = (b + 1) * qb
                lanes = slice(b * qb, (b + 1) * qb)
                score = dot(kn[s, :ext, : D.hd], qt[q_rows, lanes])
                keys = lax.broadcasted_iota(jnp.int32, (ext, qb), 0)
                queries = lax.broadcasted_iota(jnp.int32, (ext, qb), 1) + b * qb
                score = jnp.where(keys <= queries, score, -1e30)
                p = jnp.exp(score - jnp.max(score, axis=0, keepdims=True))
                p = (p * (1.0 / jnp.sum(p, axis=0, keepdims=True))).astype(BF16)
                jt[o_rows, lanes] = dot(vt[s, :, :ext], p).astype(BF16)

        with sc(f"attn{l}{a}"):
            loop(0, D.seqs * C.heads, body)

    def gate_up(l, a, slot, j, seq_of, count):
        C = D.cfg[l]

        def body(i):
            s = seq_of(i)
            p = dot(wbuf[slot, : 2 * C.cw, :], ht[s])
            g = p[: C.cw].astype(BF16).astype(F32)
            u = p[C.cw :].astype(BF16).astype(F32)
            jt[rows_at((a * D.seqs + s) * (C.q + C.f) + C.q + j * C.cw, C.cw), :] = (g * jax.nn.sigmoid(g) * u).astype(BF16)

        loop(0, count, body)

    def gate_up_loop(l, a, seq_of, count, first, last, stop=None):
        C = D.cfg[l]
        stop = C.n_c if stop is None else stop
        have_chunk(l, min(last, stop - 1))

        def body(j):
            slot = lax.rem(j, 2)
            wait(w_fetch(l, "f", j, slot))

            @pl.when(j + 1 < stop)
            def _():
                start(w_fetch(l, "f", j + 1, 1 - slot))

            gate_up(l, a, slot, j, seq_of, count)

        with sc(f"gu{l}{a}"):
            loop(first, last, body)

    def have_chunk(l, j):
        C = D.cfg[l]
        have(l, "f", (j + 1) * C.cw // fch - 1)

    def load_q(l):
        have(l, "q", 0)
        copies = w_fetch(l, "q", 0, 1)
        start(copies)
        wait(copies)

    m = och * n_row
    m_low, m_high = pl.ds(0, m // 2), pl.ds(m // 2, m // 2)
    r_slots = twin_in.shape[0]
    r_step = 64

    def order(i):
        return lax.rem(x + lax.rem(2 + 3 * i, 4), n_x)

    class Reduce:
        def __init__(self, l):
            self.l, self.C, self.sends = l, D.cfg[l], {}

        def send(self, u, i, src, dst, c):
            copy = remote(src, dst, rss.at[u % r_slots, i], rsr.at[u % r_slots, i], row, c)
            copy.start()
            self.sends[u].append(copy)

        def arrived(self, u, i, ref):
            remote(ref, ref, rss.at[u % r_slots, i], rsr.at[u % r_slots, i], row, col).wait_recv()

        def twin_copy(self, u, i):
            us = u % r_slots
            return remote(ot.at[u % 2, order(i), :, twin_lanes], twin_in.at[us, i], rss.at[us, i], rsr.at[us, i], row, twin)

        def twin_done(self, u):
            loop(0, 4, lambda i: self.twin_copy(u, i).wait_send())

        def stage_a(self, u, a):
            C = self.C
            if u >= 2:
                self.twin_done(u - 2)
            if u >= r_slots - 1:
                for c in self.sends.pop(u - r_slots + 1):
                    c.wait_send()
            self.sends[u] = []
            R = C.q + C.f

            def body(i):
                s = order(i)
                ot[u % 2, s] = dot(wobuf[:, :R], jt[rows_at((a * D.seqs + s) * R, R), :]).astype(BF16)
                self.twin_copy(u, i).start()

            with sc(f"sa{self.l}_{u}"):
                loop(0, 4, body)

        def stage_b(self, u):
            us = u % r_slots

            def body(i):
                self.arrived(u, i, twin_in.at[us, i])
                s = order(i)

                def add(b):
                    at = rows_at(b * r_step, r_step)
                    twin_in[us, i, at, :] = (ot[u % 2, s, at, my_lanes].astype(F32) + twin_in[us, i, at, :].astype(F32)).astype(BF16)

                loop(0, m // r_step, add)

            with sc(f"sb{self.l}_{u}"):
                loop(0, 1, body)
                self.send(u, 4, twin_in.at[us, 0, m_low], far_in.at[us, m_low], right)
                self.send(u, 5, twin_in.at[us, 0, m_high], far_in.at[us, m_high], left)
                loop(1, 4, body)

        def stage_c(self, u):
            us = u % r_slots

            def add_far(i, base):
                def add(b):
                    at = rows_at(base + b * r_step, r_step)
                    twin_in[us, i, at, :] = (twin_in[us, i, at, :].astype(F32) + far_in[us, at, :].astype(F32)).astype(BF16)

                loop(0, m // 2 // r_step, add)

            with sc(f"sc{self.l}_{u}"):
                self.arrived(u, 4, far_in.at[us, m_low])
                add_far(1, 0)
                self.send(u, 6, twin_in.at[us, 1], near_in.at[us, 0], right)
                self.arrived(u, 5, far_in.at[us, m_high])
                add_far(3, m // 2)
                self.send(u, 7, twin_in.at[us, 3], near_in.at[us, 1], left)

        def add_update(self, j, total):
            step = min(r_step, och)
            for r in range(n_row):

                def add(b, r=r):
                    dst = rows_at(r * dr + (r + j) % D.n_o * och + b * step, step)
                    u = total(rows_at(r * och + b * step, step)).astype(BF16).astype(F32)
                    hid[dst, :] = (hid[dst, :].astype(F32) + u).astype(BF16)

                loop(0, och // step, add)

        def stage_d(self, u, j, a):
            us = u % r_slots

            def total(at):
                return twin_in[us, 2, at, :].astype(F32) + near_in[us, 0, at, :].astype(F32) + near_in[us, 1, at, :].astype(F32)

            with sc(f"sd{self.l}_{u}"):
                self.arrived(u, 6, near_in.at[us, 0])
                self.arrived(u, 7, near_in.at[us, 1])
                if self.C.split:

                    def save(b):
                        at = rows_at(b * r_step, r_step)
                        psum[a, j, at, :] = total(at).astype(BF16)

                    loop(0, m // r_step, save)
                    if a == 1:
                        remote(psum.at[1, j], pair_in.at[j], es.at[j], er.at[j], mate, col).start()
                else:
                    self.add_update(j, total)

        def stage_e(self, j):
            with sc(f"se{self.l}_{j}"):
                c = remote(psum.at[1, j], pair_in.at[j], es.at[j], er.at[j], mate, col)
                c.wait_recv()
                self.add_update(j, lambda at: psum[0, j, at, :].astype(F32) + pair_in[j, at, :].astype(F32))
                c.wait_send()

        def finish(self, units):
            with sc(f"rfin{self.l}"):
                for u in range(max(0, units - 2), units):
                    self.twin_done(u)
                for u in self.sends:
                    for c in self.sends[u]:
                        c.wait_send()

    o_started = set()

    def o_load(l, j, a):
        if (l, j, a) not in o_started:
            have(l, "o", j)
            start(o_fetch(l, j, j % 2))
            o_started.add((l, j, a))

    def o_use(l, j, a):
        C = D.cfg[l]
        with sc(f"ouse{l}_{j}"):
            o_load(l, j, a)
            wait(o_fetch(l, j, j % 2))
            R = C.q + C.f
            for r in range(n_row):
                wobuf[r * och : (r + 1) * och, :R] = wonat[j % 2, :R, r * och : (r + 1) * och].T

    layer_norm(0)
    g0 = Gather(normed_of(ht), 0)
    mine = ht.at[x, :, my_lanes]
    shared = g_h.at[x, :, my_lanes]
    to_mate = remote(mine, shared, ps, pr_, mate, col)
    to_mate.start()
    relay_to(1)
    mate_to(step(0, 5))
    peer_to(step(0, 5))
    g0.pass_on()
    with sc("mate"):
        to_mate.wait_recv()
    g1 = Gather(normed_of(g_h), 1)
    load_q(0)
    g0.own()
    g0.near()
    project_q(0, 0, near3, 3)
    relay_to(2)
    mate_to(step(0, 10))
    g0.pass_far()
    g0.far()
    project_q(0, 0, far1, 1)
    kv0 = Gather(kv_of(0), 2)
    relay_to(3)
    n_f = D.cfg[0].n_f
    f_started = set()

    def f_load(j):
        if j not in f_started:
            f_started.add(j)
            start(w_fetch(0, "f", j, j % 2))

    def h_copy(i):
        return pltpu.make_async_copy(g_h.at[i], ht.at[i], lh.at[i])

    for j in range(n_f):
        have(0, "f", j)
        f_load(j)
        with sc(f"gu0_{j}"):
            wait(w_fetch(0, "f", j, j % 2))
            gate_up(0, 0, j % 2, j, all4, 4)
        if j == 0:
            relay_to(step(0, 4))
        elif j == n_f - 3:
            relay_to(step(0, 5))
            peer_to(step(0, 6))
            relay_to(step(0, 6))
            peer_to(step(0, 7))
    kv0.pass_on()
    g1.pass_on()
    for t in (7, 8):
        relay_to(step(0, t))
        peer_to(step(0, t + 1))
    relay_to(step(0, 9))
    peer_to(step(0, 10))
    relay_to(step(0, 10))
    peer_to(step(1, 5))
    mate_to(step(1, D.cfg[1].n_f - 2))
    g0.finish()
    to_mate.wait_send()
    g1.own()
    g1.near()
    loop(0, 3, lambda i: h_copy(near3(i)).start())
    kv0.pass_far()
    with sc("kv0wait"):
        kv0.own()
        kv0.near()
        kv0.far()
        kv0.finish()
    key_value(0, 0)
    attention(0, 0)

    red = Reduce(0)
    units = [(j, 0) for j in range(D.n_o - 1)] + [(j, 1) for j in range(D.n_o)] + [(D.n_o - 1, 0)]
    n_u = len(units)
    first = D.n_o - 1
    state = {"e": 0}

    def settle(count):
        while state["e"] < count:
            red.stage_e(state["e"])
            state["e"] += 1

    def unit(u):
        j, a = units[u]
        if u == 0 or units[u - 1][0] != j:
            o_use(0, j, a)
        red.stage_a(u, a)
        if u + 1 < n_u and units[u + 1][0] != j:
            o_load(0, *units[u + 1])
        if u >= 2:
            red.stage_c(u - 2)
        if u >= 3:
            red.stage_d(u - 3, *units[u - 3])
        red.stage_b(u)

    unit(0)
    g1.pass_far()
    unit(1)
    g1.far()
    h_copy(xf_).start()
    load_q(0)
    start(w_fetch(0, "f", 0, 0))
    loop(0, 3, lambda i: h_copy(near3(i)).wait())
    h_copy(xf_).wait()
    project_q(0, 1, all4, 4)
    kv1 = Gather(kv_of(1), 3)
    parts = first - 2
    cuts = [n_f * i // parts for i in range(parts + 1)]
    for u in range(2, first):
        unit(u)
        if u == 2:
            kv1.pass_on()
        gate_up_loop(0, 1, all4, 4, cuts[u - 2], cuts[u - 1])
    kv1.pass_far()
    relay_to(step(1, 1))
    with sc("kv1wait"):
        kv1.own()
        kv1.near()
        kv1.far()
        kv1.finish()
    key_value(0, 1)
    attention(0, 1)
    g1.finish()
    relay_to(step(1, 2))
    peer_to(step(1, 7))
    n_f1 = D.cfg[1].n_f
    for u in range(first, n_u):
        unit(u)
        v = u - first
        if v in (0, 1, 2):
            relay_to(step(1, min(v + 3, n_f1 - 2)))
            peer_to(step(1, min(v + 8, n_f1)))
        elif v == 4:
            relay_to(step(1, min(6, n_f1 - 2)))
            peer_to(step(1, n_f1))
    red.stage_c(n_u - 2)
    red.stage_d(n_u - 3, *units[n_u - 3])
    red.stage_c(n_u - 1)
    red.stage_d(n_u - 2, *units[n_u - 2])
    relay_to(step(1, min(7, n_f1 - 2)))
    settle(D.n_o - 1)
    red.stage_d(n_u - 1, *units[n_u - 1])
    settle(D.n_o)
    red.finish(n_u)

    def y_copy_back(i):
        d = lax.rem(me + i, n)
        return remote(hid.at[rows_at(d * dl, dl), :], piece_of(y_out, me), xs.at[i], xr.at[i], d // n_col, lax.rem(d, n_col))

    own_y = pltpu.make_async_copy(hid.at[rows_at(me * dl, dl), :], piece_of(y_out, me), xr.at[0])

    def y_send_back(d):
        i = lax.rem(d - me + n, n)

        @pl.when(i == 0)
        def _():
            own_y.start()

        @pl.when(i != 0)
        def _():
            y_copy_back(i).start()

    def y_ready(low, high):
        def body(d):
            r, a = d // n_col, lax.rem(d, n_col) * dl
            first = lax.rem(a // och + D.n_o - lax.rem(r, D.n_o), D.n_o)
            second = lax.rem((a + dl - 1) // och + D.n_o - lax.rem(r, D.n_o), D.n_o)

            done = jnp.maximum(first, second)

            @pl.when((low <= done) & (done < high))
            def _():
                y_send_back(d)

        loop(0, n, body)

    for l in range(1, D.layers):
        C = D.cfg[l]
        layer_norm(l)
        g0 = Gather(normed_of(ht), 0)
        peer_to(step(l, C.n_f))
        mate_to(step(l, C.n_f))
        relay_to(step(l, min(8, C.n_f)))
        own1, near2 = (lambda i: x), (lambda i: lax.rem(x + 1 + 2 * i, n_x))
        n_mid = min(3, C.n_c - 1)

        def begin(seq_of, count):
            load_q(l)
            have_chunk(l, 0)
            start(w_fetch(l, "f", 0, 0))
            project_q(l, 0, seq_of, count)

        g0.own()
        begin(own1, 1)
        kv_send(own1, 1)
        gate_up_loop(l, 0, own1, 1, 0, n_mid, n_mid)
        peer_to(step(l, C.n_f + 1))
        mate_to(step(l, C.n_f + 1))
        relay_to(step(l, C.n_f))
        g0.pass_on()
        peer_to(step(l, C.n_f + D.n_o))
        mate_to(step(l, C.n_f + D.n_o))
        g0.near()
        begin(near2, 2)
        kv_send(near2, 2)
        gate_up_loop(l, 0, near2, 2, 0, n_mid)
        g0.pass_far()
        relay_to(step(l, C.n_f + 1))
        gate_up_loop(l, 0, near3, 3, n_mid, C.n_c)
        relay_to(step(l, C.n_f + 2))
        g0.far()
        begin(far1, 1)
        kv_send(far1, 1)
        gate_up_loop(l, 0, far1, 1, 0, C.n_c)
        relay_to(step(l, C.n_f + 3))
        o_load(l, 0, 0)
        g0.finish()
        kv_arrive()
        key_value(l, 0)
        attention(l, 0)
        relay_to(step(l, C.n_f + 4))
        red = Reduce(l)
        last = l + 1 == D.layers

        end = D.n_o - 1
        for j in range(D.n_o):
            o_use(l, j, 0)
            red.stage_a(j, 0)
            if j == 0:
                relay_to(step(l, C.n_f + D.n_o))
            if j < end:
                o_load(l, j + 1, 0)
            if 2 <= j:
                red.stage_c(j - 2)
            if 3 <= j:
                red.stage_d(j - 3, j - 3, 0)
            red.stage_b(j)
        red.stage_c(end - 1)
        red.stage_d(end - 2, end - 2, 0)
        red.stage_c(end)
        red.stage_d(end - 1, end - 1, 0)
        if last:
            with sc("send"):
                y_ready(0, end)
        red.stage_d(end, end, 0)
        if last:
            y_ready(end, end + 1)
        red.finish(D.n_o)

    def kv_back(i):
        r = lax.rem(row + i, n_row)
        pos = rows_at((r * n_col + col) * D.pos, D.pos)
        return kvbuf.at[:, :, :, pos, :], kv_out.at[:, :, pl.ds(row * D.seqs, D.seqs)], r

    src, dst, _ = kv_back(0)
    own_kv = pltpu.make_async_copy(src, dst, fl)
    own_kv.start()
    kv_sends = []
    for i in range(1, n_row):
        src, dst, r = kv_back(i)
        c = remote(src, dst, fs.at[i], fr.at[i], r, col)
        c.start()
        kv_sends.append(c)

    def y_finish(i):
        s = lax.rem(me + n - i, n)
        remote(piece_of(y_out, s), piece_of(y_out, s), xs.at[i], xr.at[i], row, col).wait_recv()
        y_copy_back(i).wait_send()

    with sc("ywait"):
        loop(1, n, y_finish)
        own_y.wait()
        own_kv.wait()
        for i in range(1, n_row):
            r = lax.rem(row + n_row - i, n_row)
            dst = kv_out.at[:, :, pl.ds(r * D.seqs, D.seqs)]
            remote(dst, dst, fs.at[i], fr.at[i], row, col).wait_recv()
        for c in kv_sends:
            c.wait_send()
        for c in y_sent:
            c.wait_send()


def solution(mesh):
    n_row, n_col = mesh.shape["row"], mesh.shape["col"]
    group = n_row * n_col
    act_spec = P("dp", None, ("row", "col"))
    weight_spec = P(None, "row", "col")

    def device_fn(x_loc, gain_loc, w_in_loc, w_kv_loc, w_out_loc):
        D = Dims()
        D.n_row, D.n_col = n_row, n_col
        n_batch, D.seq, D.dl = x_loc.shape
        D.layers, D.dr, e = w_in_loc.shape
        D.d = D.dl * group
        r_block = w_out_loc.shape[1]
        D.f = e - r_block
        D.q = r_block - D.f
        kv_local = w_kv_loc.shape[2]
        D.hd = kv_local * n_col // 2
        D.kvp = 32
        D.tok = n_batch * D.seq // group
        D.seqs = n_batch // n_row
        D.pos = D.seq // group
        D.fch = 128
        D.och = 128
        D.n_o = D.dr // D.och
        D.cfg = []
        for l in range(D.layers):
            C = Dims()
            C.split = l == 0
            parts = 2 if C.split else 1
            C.q, C.f = D.q // parts, D.f // parts
            C.heads, C.n_f = C.q // D.hd, C.f // D.fch
            C.cw = D.fch if C.split else 2 * D.fch
            C.n_c = C.f // C.cw
            D.cfg.append(C)
        assert D.seq == 2 * D.tok and D.seqs == n_col // 2 == n_row == 4

        half = D.hd // 2
        inv_freq = (np.float32(1.0) / (np.float32(10000.0) ** (np.arange(half, dtype=np.float32) * np.float32(2.0) / np.float32(D.hd)))).astype(np.float32)
        angles = (inv_freq[:, None] * np.arange(D.seq, dtype=np.float32)[None, :]).astype(np.float32)
        cos_t, sin_t = np.cos(angles).astype(np.float32), np.sin(angles).astype(np.float32)
        perm = np.zeros((2 * D.hd, n_col * D.kvp), np.float32)
        for i in range(2 * D.hd):
            perm[i, (i // kv_local) * D.kvp + i % kv_local] = 1.0

        x_t = x_loc.transpose(0, 2, 1)
        w_t = w_in_loc.transpose(0, 2, 1)
        wkv_t = jnp.pad(w_kv_loc.transpose(0, 2, 1), ((0, 0), (0, D.kvp - kv_local), (0, 0)))
        gains = jnp.pad(gain_loc, ((0, 16 - D.layers), (0, 128 - D.dl)))

        n_y = sum(12 + 6 * (C.n_f + D.n_o) for C in D.cfg)
        m = D.och * n_row
        sds = jax.ShapeDtypeStruct
        dma = pltpu.SemaphoreType.DMA
        out = pl.pallas_call(
            functools.partial(kernel, D),
            out_shape=(
                sds(x_t.shape, BF16),
                sds((D.layers, 2, n_batch, D.pos, 128), BF16),
                sds((D.layers, e, D.d), BF16),
                sds((D.layers, D.kvp, D.d), BF16),
                sds((D.layers, n_row, r_block, D.dr), BF16),
                sds((D.seqs, D.d, D.seq), BF16),
            ),
            in_specs=[ANY] * 5 + [VMEM] * 3,
            out_specs=(ANY,) * 6,
            scratch_shapes=[
                pltpu.VMEM((group, D.dl, D.tok), BF16),
                pltpu.VMEM((group, 16, 128), BF16),
                pltpu.VMEM((D.layers, D.d, 128), F32),
                pltpu.VMEM((D.d, D.tok), BF16),
                pltpu.VMEM((D.seqs, D.d, D.seq), BF16),
                pltpu.VMEM((2, max(4 * D.fch, D.q + D.kvp), D.d), BF16),
                pltpu.VMEM((2, r_block, m), BF16),
                pltpu.VMEM((m, r_block), BF16),
                pltpu.VMEM((D.seqs * D.q, D.seq), BF16),
                pltpu.VMEM((n_col, 2 * D.seqs, D.kvp, D.seq), BF16),
                pltpu.VMEM((2 * D.seqs, D.seq, 128), BF16),
                pltpu.VMEM((2 * D.seqs, D.hd, D.seq), BF16),
                pltpu.VMEM((D.layers, 2, D.seqs, D.seq, 128), BF16),
                pltpu.VMEM((D.seqs * r_block, D.seq), BF16),
                pltpu.VMEM((2, D.seqs, m, D.seq), BF16),
                pltpu.VMEM((5, 4, m, D.tok), BF16),
                pltpu.VMEM((5, m, D.tok), BF16),
                pltpu.VMEM((5, 2, m, D.tok), BF16),
                pltpu.VMEM((2, D.n_o, m, D.tok), BF16),
                pltpu.VMEM((D.n_o, m, D.tok), BF16),
                dma((group,)), dma((group,)), dma((group,)), dma((group,)),
                dma((n_y,)), dma((n_y,)),
                dma((4, 9)), dma((4, 9)), dma, dma,
                dma((D.seqs, n_col)), dma((D.seqs, n_col)),
                dma((5, 8)), dma((5, 8)),
                dma((D.n_o,)), dma((D.n_o,)),
                dma((2, 8)), dma((2, 8)), dma((D.seqs,)),
                dma((n_row,)), dma((n_row,)), dma,
            ],
            compiler_params=pltpu.CompilerParams(collective_id=0, has_side_effects=True, vmem_limit_bytes=67_000_000),
            name="two_layers",
        )(x_t, gains, w_t, wkv_t, w_out_loc, jnp.asarray(cos_t), jnp.asarray(sin_t), jnp.asarray(perm, BF16))
        return out[0].transpose(0, 2, 1), out[1][..., : D.hd]

    return jax.shard_map(device_fn, mesh=mesh, in_specs=(act_spec, P(None, ("row", "col")), weight_spec, weight_spec, P(None, "col", "row")), out_specs=(act_spec, P(None, None, "dp", ("row", "col"), None)), check_vma=False)
```

```python
import functools

import numpy as np

import jax
import jax.numpy as jnp
from jax import lax
from jax.experimental import pallas as pl
from jax.experimental.pallas import tpu as pltpu
from jax.sharding import PartitionSpec as P

LN_EPS = 1e-6
MESH = pl.DeviceIdType.MESH
ANY = pl.BlockSpec(memory_space=pl.ANY)
VMEM = pl.BlockSpec(memory_space=pltpu.VMEM)
F32, BF16 = jnp.float32, jnp.bfloat16


def dot(a, b):
    return jnp.dot(a, b, preferred_element_type=F32)


class Dims:
    pass


def rows_at(start, count, by=16):
    return pl.ds(start if isinstance(start, int) else pl.multiple_of(start, by), count)


def kernel(
    D,
    x_t, gains, w_t, wkv_t, w_o, cos_ref, sin_ref, perm_ref,
    y_out, kv_out, g_w, g_kv, g_wo, g_h,
    xland, gland, gcol, hid, ht, wbuf, wonat, wobuf, qt, kvland, kn, vt, kvbuf, jt, ot, twin_in, far_in, near_in, psum, pair_in,
    xs, xr, gs, gr, ys, yr, ags, agr, ps, pr_, kvs, kvr, rss, rsr, es, er, lw, lo, lh, fs, fr, fl,
):
    sc = jax.named_scope
    row, col = lax.axis_index("row"), lax.axis_index("col")
    n_row, n_col, n = D.n_row, D.n_col, D.n_row * D.n_col
    n_x = n_col // 2
    me = row * n_col + col
    x, k = col // 2, lax.rem(col, 2)
    xr_, xl_, xf_ = lax.rem(x + 1, n_x), lax.rem(x + n_x - 1, n_x), lax.rem(x + 2, n_x)
    right, left, twin = xr_ * 2 + k, xl_ * 2 + k, x * 2 + 1 - k
    up, down, across = lax.rem(row + 1, n_row), lax.rem(row + n_row - 1, n_row), lax.rem(row + 2, n_row)
    half, mate = row // 2, n_row - 1 - row
    peer = row + 1 - 2 * lax.rem(row, 2)
    tok, dl, dr = D.tok, D.dl, D.dr
    och, fch = D.och, D.fch
    my_lanes = pl.ds(pl.multiple_of(k * tok, 128), tok)
    twin_lanes = pl.ds(pl.multiple_of((1 - k) * tok, 128), tok)

    def remote(src, dst, ssem, rsem, r, c):
        return pltpu.make_async_remote_copy(src_ref=src, dst_ref=dst, send_sem=ssem, recv_sem=rsem, device_id={"row": r, "col": c}, device_id_type=MESH)

    def loop(lo_, hi_, f):
        def body(i, carry):
            f(i)
            return carry

        lax.fori_loop(lo_, hi_, body, 0)

    barrier = pltpu.get_barrier_semaphore()

    def greet(i):
        d = lax.rem(me + i, n)
        pl.semaphore_signal(barrier, inc=1, device_id={"row": d // n_col, "col": lax.rem(d, n_col)}, device_id_type=MESH)

    with sc("barrier"):
        loop(1, n, greet)
        pl.semaphore_wait(barrier, n - 1)

    def piece_of(ref, d):
        return ref.at[d // 2, :, pl.ds(pl.multiple_of(lax.rem(d, 2) * tok, 128), tok)]

    def x_copy(i):
        d = lax.rem(me + i, n)
        return remote(piece_of(x_t, d), xland.at[me], xs.at[i], xr.at[i], d // n_col, lax.rem(d, n_col))

    def g_copy(i):
        d = lax.rem(me + i, n)
        return remote(gains, gland.at[me], gs.at[i], gr.at[i], d // n_col, lax.rem(d, n_col))

    def x_start(i):
        x_copy(i).start()
        g_copy(i).start()

    own_x = pltpu.make_async_copy(piece_of(x_t, me), xland.at[me], xr.at[0])
    own_g = pltpu.make_async_copy(gains, gland.at[me], gr.at[0])
    own_x.start()
    own_g.start()
    loop(1, n, x_start)

    def own_lanes(r):
        return pl.ds(pl.multiple_of(r * dr, 128), dr)

    def o_lanes(j, r):
        return pl.ds(pl.multiple_of(lax.rem(r + j, D.n_o) * och, 128), och)

    steps = []
    for l, C in enumerate(D.cfg):
        steps += [(l, "q", 0)] + [(l, "f", j) for j in range(C.n_f)] + [(l, "o", j) for j in range(D.n_o)]
    n_steps = len(steps)
    step_of = {s: t for t, s in enumerate(steps)}

    def blocks(t, i):
        l, kind, j = steps[t]
        C = D.cfg[l]
        out = []

        def w_rows(a, m):
            at = rows_at(a, m)
            out.append((w_t.at[l, at, :], lambda r: g_w.at[l, at, own_lanes(r)]))

        def o_rows(a, m):
            at = rows_at(a, m)
            out.append((w_o.at[l, at, o_lanes(j, row)], lambda r: g_wo.at[l, r, at, o_lanes(j, r)]))

        def kv_rows(a, m):
            at = pl.ds(a, m)
            out.append((wkv_t.at[l, at, :], lambda r: g_kv.at[l, at, own_lanes(r)]))

        if kind == "q":
            for a in (0, C.q // 2):
                w_rows(i * C.q + a, C.q // 2)
            for a in (0, D.kvp // 2):
                kv_rows(a, D.kvp // 2)
        elif kind == "f":
            w_rows(D.q + i * C.f + j * fch, fch)
            w_rows(D.q + D.f + i * C.f + j * fch, fch)
        elif C.split:
            o_rows(i * C.q, C.q)
            o_rows(D.q + i * C.f, C.f)
        else:
            for a in (0, (D.q + D.f) // 2):
                o_rows(a, (D.q + D.f) // 2)
        return out

    base, n_sems = [], 0
    for l, kind, j in steps:
        base.append(n_sems)
        n_sems += 12 if kind == "q" else 6
    assert n_sems == ys.shape[0]
    y_sent = []

    def y_copy(t, i, kind, src, dst, r):
        at = base[t] + 3 * i + kind
        return remote(src, dst, ys.at[at], yr.at[at], r, col)

    def y_send(*args):
        c = y_copy(*args)
        c.start()
        y_sent.append(c)

    def issue_peer(t):
        for i, (src, place) in enumerate(blocks(t, half if D.cfg[steps[t][0]].split else 0)):
            y_send(t, i, 0, src, place(row), peer)

    def issue_mate(t):
        for i, (src, place) in enumerate(blocks(t, 1 - half if D.cfg[steps[t][0]].split else 0)):
            y_send(t, i, 1, src, place(row), mate)

    def relay(t):
        split = D.cfg[steps[t][0]].split
        with sc(f"relay{t}"):
            for i, (src, place) in enumerate(blocks(t, half if split else 0)):
                y_copy(t, i, 1, src, place(mate), mate).wait_recv()
                if split or i % 2 == 0:
                    y_send(t, i, 2, place(mate), place(mate), peer)
                if not split:
                    y_copy(t, i, 0, src, place(peer), peer).wait_recv()
                    if i % 2 == 1:
                        y_send(t, i, 2, place(peer), place(peer), mate)

    at = {"next": 0, "peer": 0, "mate": 0, "relay": 0}
    first_of = {l: min(t for t, st in enumerate(steps) if st[0] == l) for l in range(D.layers)}

    def step(l, j):
        return min(first_of[l] + j, first_of.get(l + 1, n_steps) - 1)

    def peer_to(t):
        while at["peer"] <= t:
            issue_peer(at["peer"])
            at["peer"] += 1

    def mate_to(t):
        while at["mate"] <= t:
            issue_mate(at["mate"])
            at["mate"] += 1

    def relay_to(t):
        assert t < at["peer"] and t < at["mate"]
        while at["relay"] <= t:
            relay(at["relay"])
            at["relay"] += 1

    def advance():
        t = at["next"]
        assert t < at["relay"], t
        rest = n_row - 1 - peer
        with sc(f"adv{t}"):
            split = D.cfg[steps[t][0]].split
            for i, (src, place) in enumerate(blocks(t, half if split else 0)):
                if split:
                    y_copy(t, i, 0, src, place(peer), peer).wait_recv()
                y_copy(t, i, 2, src, place(rest), rest).wait_recv()
            at["next"] = t + 1

    def have(*which):
        while at["next"] <= step_of[which]:
            advance()

    mate_to(1)
    peer_to(step(0, 3))

    def w_fetch(l, kind, j, slot):
        C = D.cfg[l]
        i = half if C.split else 0
        copies = []

        def fetch(src, dst):
            copies.append(pltpu.make_async_copy(src, dst, lw.at[slot, len(copies)]))

        def w_rows(a, m, at):
            a, at = rows_at(a, m), pl.ds(at, m)
            fetch(w_t.at[l, a, :], wbuf.at[slot, at, own_lanes(row)])
            for r in (up, down, across):
                fetch(g_w.at[l, a, own_lanes(r)], wbuf.at[slot, at, own_lanes(r)])

        if kind == "q":
            w_rows(i * C.q, C.q, 0)
            at = pl.ds(C.q, D.kvp)
            fetch(wkv_t.at[l], wbuf.at[slot, at, own_lanes(row)])
            for r in (up, down, across):
                fetch(g_kv.at[l, :, own_lanes(r)], wbuf.at[slot, at, own_lanes(r)])
        else:
            w_rows(D.q + i * C.f + j * C.cw, C.cw, 0)
            w_rows(D.q + D.f + i * C.f + j * C.cw, C.cw, C.cw)
        return copies

    def o_fetch(l, j, slot):
        C = D.cfg[l]
        copies = []

        def fetch(src, dst):
            copies.append(pltpu.make_async_copy(src, dst, lo.at[slot, len(copies)]))

        spans = ((half * C.q, 0, C.q), (D.q + half * C.f, C.q, C.f)) if C.split else ((0, 0, C.q + C.f),)
        for a, at, m in spans:
            a, at = rows_at(a, m), pl.ds(at, m)
            to = lambda r: pl.ds(pl.multiple_of(r * och, 128), och)
            fetch(w_o.at[l, a, o_lanes(j, row)], wonat.at[slot, at, to(row)])
            for r in (up, down, across):
                fetch(g_wo.at[l, r, a, o_lanes(j, r)], wonat.at[slot, at, to(r)])
        return copies

    def start(copies):
        for c in copies:
            c.start()

    def wait(copies):
        for c in copies:
            c.wait()

    own_x.wait()
    own_g.wait()

    def x_finish(i):
        s = lax.rem(me + n - i, n)
        remote(xland.at[s], xland.at[s], xs.at[i], xr.at[i], row, col).wait_recv()
        remote(gland.at[s], gland.at[s], gs.at[i], gr.at[i], row, col).wait_recv()
        x_copy(i).wait_send()
        g_copy(i).wait_send()

    with sc("xwait"):
        loop(1, n, x_finish)

    def keep(d):
        hid[rows_at(d * dl, dl), :] = xland[d]

    with sc("gains"):
        loop(0, n, keep)
        g_all = gland[...].astype(F32)
        for l in range(D.layers):
            g_rows = g_all[:, l, :]
            g_rows = jnp.concatenate([g_rows, jnp.zeros((128 - n, 128), F32)], axis=0) if n < 128 else g_rows
            g_cols = g_rows.T
            for d in range(n):
                gcol[l, d * dl : (d + 1) * dl, :] = jnp.broadcast_to(g_cols[:dl, d : d + 1], (dl, 128))

    blk = 64
    n_blk = D.d // blk

    def layer_norm(l):
        def add_up(i, acc):
            v = hid[rows_at(i * blk, blk), :].astype(F32)
            return acc + v.reshape(blk // 8, 8, tok).sum(axis=0)

        mean = lax.fori_loop(0, n_blk, add_up, jnp.zeros((8, tok), F32)).sum(axis=0, keepdims=True) / D.d

        def add_sq(i, acc):
            v = hid[rows_at(i * blk, blk), :].astype(F32) - mean
            return acc + (v * v).reshape(blk // 8, 8, tok).sum(axis=0)

        var = lax.fori_loop(0, n_blk, add_sq, jnp.zeros((8, tok), F32)).sum(axis=0, keepdims=True) / D.d
        scale = lax.rsqrt(var + LN_EPS)

        def write(i):
            rows = rows_at(i * blk, blk)
            g = gcol[l, rows, :]
            g = jnp.concatenate([g] * (tok // 128), axis=1)
            v = (hid[rows, :].astype(F32) - mean) * scale * g
            ht[x, rows, my_lanes] = v.astype(BF16)

        with sc(f"norm{l}"):
            loop(0, n_blk, write)

    d_low, d_high = pl.ds(0, D.d // 2), pl.ds(D.d // 2, D.d // 2)

    class Gather:
        def __init__(self, ref, tag):
            self.ref, self.tag, self.sends = ref, tag, []
            for i, c in ((0, right), (1, left), (2, twin)):
                self.send(i, ref(x, False, None), c)

        def send(self, i, ref, c):
            copy = remote(ref, ref, ags.at[self.tag, i], agr.at[self.tag, i], row, c)
            copy.start()
            self.sends.append(copy)

        def arrived(self, i, ref):
            remote(ref, ref, ags.at[self.tag, i], agr.at[self.tag, i], row, col).wait_recv()

        def pass_on(self):
            with sc(f"pass_on{self.tag}"):
                self.arrived(0, self.ref(xl_, False, None))
                self.send(3, self.ref(xl_, False, 0), right)
                self.send(4, self.ref(xl_, False, None), twin)
                self.arrived(1, self.ref(xr_, False, None))
                self.send(5, self.ref(xr_, False, 1), left)
                self.send(6, self.ref(xr_, False, None), twin)

        def own(self):
            self.arrived(2, self.ref(x, True, None))

        def near(self):
            with sc(f"near{self.tag}"):
                self.arrived(4, self.ref(xl_, True, None))
                self.arrived(6, self.ref(xr_, True, None))

        def pass_far(self):
            with sc(f"pass_far{self.tag}"):
                for part, i, j in ((0, 3, 7), (1, 5, 8)):
                    self.arrived(i, self.ref(xf_, False, part))
                    self.send(j, self.ref(xf_, False, part), twin)

        def far(self):
            with sc(f"far{self.tag}"):
                self.arrived(7, self.ref(xf_, True, 0))
                self.arrived(8, self.ref(xf_, True, 1))

        def finish(self):
            for c in self.sends:
                c.wait_send()

    def normed_of(buf):
        def ref(chip, other, part):
            rows = slice(None) if part is None else (d_low, d_high)[part]
            return buf.at[chip, rows, twin_lanes if other else my_lanes]

        return ref

    def kv_of(a):
        def ref(chip, other, part):
            h = D.seqs // 2
            span = pl.ds(a * D.seqs, D.seqs) if part is None else pl.ds(a * D.seqs + part * h, h)
            return kvland.at[chip * 2 + (1 - k if other else k), span]

        return ref

    half_dim = D.hd // 2

    def near3(i):
        return lax.rem(x + i + i // 2, n_x)

    def all4(i):
        return i

    def far1(i):
        return xf_

    def rope(p):
        lo_, hi_ = p[:half_dim], p[half_dim:]
        return jnp.concatenate([lo_ * cos_ref[...] - hi_ * sin_ref[...], hi_ * cos_ref[...] + lo_ * sin_ref[...]], axis=0)

    def project_q(l, a, seq_of, count):
        C = D.cfg[l]

        def body(i):
            s = seq_of(i)
            p = dot(wbuf[1, : C.q + D.kvp, :], ht[s]).astype(BF16).astype(F32)
            for h in range(C.heads):
                at = rows_at((a * D.seqs + s) * C.q + h * D.hd, D.hd)
                qt[at, :] = (rope(p[h * D.hd : (h + 1) * D.hd]) * D.hd**-0.5).astype(BF16)
            kvland[col, a * D.seqs + s] = p[C.q :].astype(BF16)

        with sc(f"q{l}{a}"):
            loop(0, count, body)

    def kv_copy(s, j, source):
        ref = kvland.at[source, s]
        return remote(ref, ref, kvs.at[s, j], kvr.at[s, j], row, lax.rem(col + j, n_col))

    def kv_send(seq_of, count):
        def body(i):
            s = seq_of(i)
            loop(1, n_col, lambda j: kv_copy(s, j, col).start())

        loop(0, count, body)

    def kv_arrive():
        def body(i):
            j = i // D.seqs + 1
            s = lax.rem(i, D.seqs)
            kv_copy(s, j, lax.rem(col + n_col - j, n_col)).wait_recv()
            kv_copy(s, j, col).wait_send()

        with sc("kvwait"):
            loop(0, D.seqs * (n_col - 1), body)

    def key_value(l, a):
        def body(i):
            s = a * D.seqs + i
            raw = kvland[:, s].reshape(n_col * D.kvp, D.seq)
            both = dot(perm_ref[...], raw)
            zeros = jnp.zeros((128 - D.hd, D.seq), F32)
            k_nat = jnp.concatenate([rope(both[: D.hd]), zeros], axis=0).T.astype(BF16)
            kn[s] = k_nat
            vt[s] = both[D.hd :].astype(BF16)
            if a == 0:
                kvbuf[l, 0, i] = k_nat
                kvbuf[l, 1, i] = jnp.concatenate([both[D.hd :], zeros], axis=0).T.astype(BF16)

        with sc(f"kv{l}{a}"):
            loop(0, D.seqs, body)

    qb = D.seq // 2

    def attention(l, a):
        C = D.cfg[l]

        pair = 2
        per = C.heads // pair

        def body(i):
            s, h0 = a * D.seqs + i // per, lax.rem(i, per) * pair
            q_rows = [rows_at(s * C.q + (h0 + e) * D.hd, D.hd) for e in range(pair)]
            o_rows = [rows_at(s * (C.q + C.f) + (h0 + e) * D.hd, D.hd) for e in range(pair)]
            for b in range(2):
                ext = (b + 1) * qb
                lanes = slice(b * qb, (b + 1) * qb)
                keys = lax.broadcasted_iota(jnp.int32, (ext, qb), 0)
                queries = lax.broadcasted_iota(jnp.int32, (ext, qb), 1) + b * qb
                scores = [dot(kn[s, :ext, : D.hd], qt[q_rows[e], lanes]) for e in range(pair)]
                for e in range(pair):
                    score = jnp.where(keys <= queries, scores[e], -1e30)
                    p = jnp.exp(score - jnp.max(score, axis=0, keepdims=True))
                    p = (p * (1.0 / jnp.sum(p, axis=0, keepdims=True))).astype(BF16)
                    jt[o_rows[e], lanes] = dot(vt[s, :, :ext], p).astype(BF16)

        with sc(f"attn{l}{a}"):
            loop(0, D.seqs * per, body)

    def gate_up(l, a, slot, j, seq_of, count):
        C = D.cfg[l]

        def body(i):
            s = seq_of(i)
            p = dot(wbuf[slot, : 2 * C.cw, :], ht[s])
            g = p[: C.cw].astype(BF16).astype(F32)
            u = p[C.cw :].astype(BF16).astype(F32)
            jt[rows_at((a * D.seqs + s) * (C.q + C.f) + C.q + j * C.cw, C.cw), :] = (g * jax.nn.sigmoid(g) * u).astype(BF16)

        loop(0, count, body)

    def gate_up_loop(l, a, seq_of, count, first, last, stop=None):
        C = D.cfg[l]
        stop = C.n_c if stop is None else stop
        have_chunk(l, min(last, stop - 1))

        def body(j):
            slot = lax.rem(j, 2)
            wait(w_fetch(l, "f", j, slot))

            @pl.when(j + 1 < stop)
            def _():
                start(w_fetch(l, "f", j + 1, 1 - slot))

            gate_up(l, a, slot, j, seq_of, count)

        with sc(f"gu{l}{a}"):
            loop(first, last, body)

    def have_chunk(l, j):
        C = D.cfg[l]
        have(l, "f", (j + 1) * C.cw // fch - 1)

    def load_q(l):
        have(l, "q", 0)
        copies = w_fetch(l, "q", 0, 1)
        start(copies)
        wait(copies)

    m = och * n_row
    m_low, m_high = pl.ds(0, m // 2), pl.ds(m // 2, m // 2)
    r_slots = twin_in.shape[0]
    r_step = 64

    def order(i):
        return lax.rem(x + lax.rem(2 + 3 * i, 4), n_x)

    class Reduce:
        def __init__(self, l):
            self.l, self.C, self.sends = l, D.cfg[l], {}

        def send(self, u, i, src, dst, c):
            copy = remote(src, dst, rss.at[u % r_slots, i], rsr.at[u % r_slots, i], row, c)
            copy.start()
            self.sends[u].append(copy)

        def arrived(self, u, i, ref):
            remote(ref, ref, rss.at[u % r_slots, i], rsr.at[u % r_slots, i], row, col).wait_recv()

        def twin_copy(self, u, i):
            us = u % r_slots
            return remote(ot.at[u % 2, order(i), :, twin_lanes], twin_in.at[us, i], rss.at[us, i], rsr.at[us, i], row, twin)

        def twin_done(self, u):
            loop(0, 4, lambda i: self.twin_copy(u, i).wait_send())

        def stage_a(self, u, a):
            C = self.C
            if u >= 2:
                self.twin_done(u - 2)
            if u >= r_slots - 1:
                for c in self.sends.pop(u - r_slots + 1):
                    c.wait_send()
            self.sends[u] = []
            R = C.q + C.f

            def body(i):
                s = order(i)
                ot[u % 2, s] = dot(wobuf[:, :R], jt[rows_at((a * D.seqs + s) * R, R), :]).astype(BF16)
                self.twin_copy(u, i).start()

            with sc(f"sa{self.l}_{u}"):
                loop(0, 4, body)

        def stage_b(self, u):
            us = u % r_slots

            def body(i):
                self.arrived(u, i, twin_in.at[us, i])
                s = order(i)

                def add(b):
                    at = rows_at(b * r_step, r_step)
                    twin_in[us, i, at, :] = (ot[u % 2, s, at, my_lanes].astype(F32) + twin_in[us, i, at, :].astype(F32)).astype(BF16)

                loop(0, m // r_step, add)

            with sc(f"sb{self.l}_{u}"):
                loop(0, 1, body)
                self.send(u, 4, twin_in.at[us, 0, m_low], far_in.at[us, m_low], right)
                self.send(u, 5, twin_in.at[us, 0, m_high], far_in.at[us, m_high], left)
                loop(1, 4, body)

        def stage_c(self, u):
            us = u % r_slots

            def add_far(i, base):
                def add(b):
                    at = rows_at(base + b * r_step, r_step)
                    twin_in[us, i, at, :] = (twin_in[us, i, at, :].astype(F32) + far_in[us, at, :].astype(F32)).astype(BF16)

                loop(0, m // 2 // r_step, add)

            with sc(f"sc{self.l}_{u}"):
                self.arrived(u, 4, far_in.at[us, m_low])
                add_far(1, 0)
                self.send(u, 6, twin_in.at[us, 1], near_in.at[us, 0], right)
                self.arrived(u, 5, far_in.at[us, m_high])
                add_far(3, m // 2)
                self.send(u, 7, twin_in.at[us, 3], near_in.at[us, 1], left)

        def add_update(self, j, total):
            step = min(r_step, och)
            for r in range(n_row):

                def add(b, r=r):
                    dst = rows_at(r * dr + (r + j) % D.n_o * och + b * step, step)
                    u = total(rows_at(r * och + b * step, step)).astype(BF16).astype(F32)
                    hid[dst, :] = (hid[dst, :].astype(F32) + u).astype(BF16)

                loop(0, och // step, add)

        def stage_d(self, u, j, a):
            us = u % r_slots

            def total(at):
                return twin_in[us, 2, at, :].astype(F32) + near_in[us, 0, at, :].astype(F32) + near_in[us, 1, at, :].astype(F32)

            with sc(f"sd{self.l}_{u}"):
                self.arrived(u, 6, near_in.at[us, 0])
                self.arrived(u, 7, near_in.at[us, 1])
                if self.C.split:

                    def save(b):
                        at = rows_at(b * r_step, r_step)
                        psum[a, j, at, :] = total(at).astype(BF16)

                    loop(0, m // r_step, save)
                    if a == 1:
                        remote(psum.at[1, j], pair_in.at[j], es.at[j], er.at[j], mate, col).start()
                else:
                    self.add_update(j, total)

        def stage_e(self, j):
            with sc(f"se{self.l}_{j}"):
                c = remote(psum.at[1, j], pair_in.at[j], es.at[j], er.at[j], mate, col)
                c.wait_recv()
                self.add_update(j, lambda at: psum[0, j, at, :].astype(F32) + pair_in[j, at, :].astype(F32))
                c.wait_send()

        def finish(self, units):
            with sc(f"rfin{self.l}"):
                for u in range(max(0, units - 2), units):
                    self.twin_done(u)
                for u in self.sends:
                    for c in self.sends[u]:
                        c.wait_send()

    o_started = set()

    def o_load(l, j, a):
        if (l, j, a) not in o_started:
            have(l, "o", j)
            start(o_fetch(l, j, j % 2))
            o_started.add((l, j, a))

    def o_use(l, j, a):
        C = D.cfg[l]
        with sc(f"ouse{l}_{j}"):
            o_load(l, j, a)
            wait(o_fetch(l, j, j % 2))
            R = C.q + C.f
            for r in range(n_row):
                wobuf[r * och : (r + 1) * och, :R] = wonat[j % 2, :R, r * och : (r + 1) * och].T

    layer_norm(0)
    g0 = Gather(normed_of(ht), 0)
    mine = ht.at[x, :, my_lanes]
    shared = g_h.at[x, :, my_lanes]
    to_mate = remote(mine, shared, ps, pr_, mate, col)
    to_mate.start()
    relay_to(1)
    mate_to(step(0, 5))
    peer_to(step(0, 5))
    g0.pass_on()
    with sc("mate"):
        to_mate.wait_recv()
    g1 = Gather(normed_of(g_h), 1)
    load_q(0)
    g0.own()
    g0.near()
    project_q(0, 0, near3, 3)
    relay_to(2)
    mate_to(step(0, 10))
    g0.pass_far()
    g0.far()
    project_q(0, 0, far1, 1)
    kv0 = Gather(kv_of(0), 2)
    relay_to(3)
    n_f = D.cfg[0].n_f
    f_started = set()

    def f_load(j):
        if j not in f_started:
            f_started.add(j)
            start(w_fetch(0, "f", j, j % 2))

    def h_copy(i):
        return pltpu.make_async_copy(g_h.at[i], ht.at[i], lh.at[i])

    have(0, "f", 0)
    f_load(0)
    gate_up_loop(0, 0, all4, 4, 0, 2, 2)
    relay_to(step(0, 4))
    for j in range(2, n_f):
        have(0, "f", j)
        f_load(j)
        with sc(f"gu0_{j}"):
            wait(w_fetch(0, "f", j, j % 2))
            gate_up(0, 0, j % 2, j, all4, 4)
        if j == max(2, n_f - 3):
            relay_to(step(0, 5))
            peer_to(step(0, 6))
            relay_to(step(0, 6))
            peer_to(step(0, 7))
    kv0.pass_on()
    g1.pass_on()
    for t in (7, 8):
        relay_to(step(0, t))
        peer_to(step(0, t + 1))
    relay_to(step(0, 9))
    peer_to(step(0, 10))
    relay_to(step(0, 10))
    peer_to(step(1, 4))
    mate_to(step(1, D.cfg[1].n_f - 2))
    g0.finish()
    to_mate.wait_send()
    g1.own()
    g1.near()
    loop(0, 3, lambda i: h_copy(near3(i)).start())
    kv0.pass_far()
    with sc("kv0wait"):
        kv0.own()
        kv0.near()
        kv0.far()
        kv0.finish()
    key_value(0, 0)
    attention(0, 0)

    red = Reduce(0)
    units = [(j, 0) for j in range(D.n_o - 1)] + [(j, 1) for j in range(D.n_o)] + [(D.n_o - 1, 0)]
    n_u = len(units)
    first = D.n_o - 1
    state = {"e": 0}

    def settle(count):
        while state["e"] < count:
            red.stage_e(state["e"])
            state["e"] += 1

    def unit(u):
        j, a = units[u]
        if u == 0 or units[u - 1][0] != j:
            o_use(0, j, a)
        red.stage_a(u, a)
        if u + 1 < n_u and units[u + 1][0] != j:
            o_load(0, *units[u + 1])
        if u >= 2:
            red.stage_c(u - 2)
        if u >= 3:
            red.stage_d(u - 3, *units[u - 3])
        red.stage_b(u)

    unit(0)
    g1.pass_far()
    unit(1)
    g1.far()
    h_copy(xf_).start()
    load_q(0)
    start(w_fetch(0, "f", 0, 0))
    loop(0, 3, lambda i: h_copy(near3(i)).wait())
    project_q(0, 1, near3, 3)
    h_copy(xf_).wait()
    project_q(0, 1, far1, 1)
    kv1 = Gather(kv_of(1), 3)
    parts = first - 2
    cuts = [n_f * i // parts for i in range(parts + 1)]
    for u in range(2, first):
        unit(u)
        if u == 2:
            kv1.pass_on()
        gate_up_loop(0, 1, all4, 4, cuts[u - 2], cuts[u - 1])
    kv1.pass_far()
    relay_to(step(1, 1))
    with sc("kv1wait"):
        kv1.own()
        kv1.near()
        kv1.far()
        kv1.finish()
    key_value(0, 1)
    attention(0, 1)
    g1.finish()
    relay_to(step(1, 2))
    peer_to(step(1, 5))
    n_f1 = D.cfg[1].n_f
    for u in range(first, n_u):
        unit(u)
        v = u - first
        if v in (0, 1, 2, 3):
            relay_to(step(1, min(v + 3, n_f1 - 2)))
            peer_to(step(1, min(v + 6, n_f1)))
        elif v == n_u - first - 1:
            peer_to(step(1, min(v + 5, n_f1)))
            relay_to(step(1, min(7, n_f1 - 2)))
            peer_to(step(1, n_f1))
    red.stage_c(n_u - 2)
    red.stage_d(n_u - 3, *units[n_u - 3])
    red.stage_c(n_u - 1)
    red.stage_d(n_u - 2, *units[n_u - 2])
    mate_to(step(1, n_f1))
    settle(D.n_o - 1)
    red.stage_d(n_u - 1, *units[n_u - 1])
    settle(D.n_o)
    red.finish(n_u)

    def y_copy_back(i):
        d = lax.rem(me + i, n)
        return remote(hid.at[rows_at(d * dl, dl), :], piece_of(y_out, me), xs.at[i], xr.at[i], d // n_col, lax.rem(d, n_col))

    own_y = pltpu.make_async_copy(hid.at[rows_at(me * dl, dl), :], piece_of(y_out, me), xr.at[0])

    def y_send_back(d):
        i = lax.rem(d - me + n, n)

        @pl.when(i == 0)
        def _():
            own_y.start()

        @pl.when(i != 0)
        def _():
            y_copy_back(i).start()

    def y_ready(low, high):
        def body(d):
            r, a = d // n_col, lax.rem(d, n_col) * dl
            first = lax.rem(a // och + D.n_o - lax.rem(r, D.n_o), D.n_o)
            second = lax.rem((a + dl - 1) // och + D.n_o - lax.rem(r, D.n_o), D.n_o)

            done = jnp.maximum(first, second)

            @pl.when((low <= done) & (done < high))
            def _():
                y_send_back(d)

        loop(0, n, body)

    for l in range(1, D.layers):
        C = D.cfg[l]
        layer_norm(l)
        g0 = Gather(normed_of(ht), 0)
        peer_to(step(l, C.n_f))
        mate_to(step(l, C.n_f))
        relay_to(step(l, min(8, C.n_f)))
        own1, near2 = (lambda i: x), (lambda i: lax.rem(x + 1 + 2 * i, n_x))
        n_mid = min(3, C.n_c - 1)

        def begin(seq_of, count):
            load_q(l)
            have_chunk(l, 0)
            start(w_fetch(l, "f", 0, 0))
            project_q(l, 0, seq_of, count)

        g0.own()
        begin(own1, 1)
        kv_send(own1, 1)
        gate_up_loop(l, 0, own1, 1, 0, n_mid, n_mid)
        relay_to(step(l, C.n_f))
        peer_to(step(l, C.n_f + 1))
        mate_to(step(l, C.n_f + 1))
        g0.pass_on()
        relay_to(step(l, C.n_f + 1))
        peer_to(step(l, C.n_f + 2))
        mate_to(step(l, C.n_f + 2))
        g0.near()
        begin(near2, 2)
        kv_send(near2, 2)
        gate_up_loop(l, 0, near2, 2, 0, n_mid)
        g0.pass_far()
        peer_to(step(l, C.n_f + 3))
        mate_to(step(l, C.n_f + 3))
        relay_to(step(l, C.n_f + 2))
        gate_up_loop(l, 0, near3, 3, n_mid, C.n_c)
        peer_to(step(l, C.n_f + 4))
        mate_to(step(l, C.n_f + 4))
        relay_to(step(l, C.n_f + 3))
        g0.far()
        begin(far1, 1)
        kv_send(far1, 1)
        gate_up_loop(l, 0, far1, 1, 0, C.n_c)
        peer_to(step(l, C.n_f + D.n_o))
        mate_to(step(l, C.n_f + D.n_o))
        relay_to(step(l, C.n_f + 4))
        g0.finish()
        kv_arrive()
        key_value(l, 0)
        attention(l, 0)
        red = Reduce(l)
        last = l + 1 == D.layers

        end = D.n_o - 1
        for j in range(D.n_o):
            o_use(l, j, 0)
            red.stage_a(j, 0)
            if j == 0:
                relay_to(step(l, C.n_f + D.n_o))
            if j < end:
                o_load(l, j + 1, 0)
            if 2 <= j:
                red.stage_c(j - 2)
            if 3 <= j:
                red.stage_d(j - 3, j - 3, 0)
            red.stage_b(j)
        red.stage_c(end - 1)
        red.stage_d(end - 2, end - 2, 0)
        red.stage_c(end)
        red.stage_d(end - 1, end - 1, 0)
        if last:
            with sc("send"):
                y_ready(0, end)
        red.stage_d(end, end, 0)
        if last:
            y_ready(end, end + 1)
        red.finish(D.n_o)

    def kv_back(i):
        r = lax.rem(row + i, n_row)
        pos = rows_at((r * n_col + col) * D.pos, D.pos)
        return kvbuf.at[:, :, :, pos, :], kv_out.at[:, :, pl.ds(row * D.seqs, D.seqs)], r

    src, dst, _ = kv_back(0)
    own_kv = pltpu.make_async_copy(src, dst, fl)
    own_kv.start()
    kv_sends = []
    for i in range(1, n_row):
        src, dst, r = kv_back(i)
        c = remote(src, dst, fs.at[i], fr.at[i], r, col)
        c.start()
        kv_sends.append(c)

    def y_finish(i):
        s = lax.rem(me + n - i, n)
        remote(piece_of(y_out, s), piece_of(y_out, s), xs.at[i], xr.at[i], row, col).wait_recv()
        y_copy_back(i).wait_send()

    with sc("ywait"):
        loop(1, n, y_finish)
        own_y.wait()
        own_kv.wait()
        for i in range(1, n_row):
            r = lax.rem(row + n_row - i, n_row)
            dst = kv_out.at[:, :, pl.ds(r * D.seqs, D.seqs)]
            remote(dst, dst, fs.at[i], fr.at[i], row, col).wait_recv()
        for c in kv_sends:
            c.wait_send()
        for c in y_sent:
            c.wait_send()


def solution(mesh):
    n_row, n_col = mesh.shape["row"], mesh.shape["col"]
    group = n_row * n_col
    act_spec = P("dp", None, ("row", "col"))
    weight_spec = P(None, "row", "col")

    def device_fn(x_loc, gain_loc, w_in_loc, w_kv_loc, w_out_loc):
        D = Dims()
        D.n_row, D.n_col = n_row, n_col
        n_batch, D.seq, D.dl = x_loc.shape
        D.layers, D.dr, e = w_in_loc.shape
        D.d = D.dl * group
        r_block = w_out_loc.shape[1]
        D.f = e - r_block
        D.q = r_block - D.f
        kv_local = w_kv_loc.shape[2]
        D.hd = kv_local * n_col // 2
        D.kvp = 32
        D.tok = n_batch * D.seq // group
        D.seqs = n_batch // n_row
        D.pos = D.seq // group
        D.fch = 128
        D.och = 128
        D.n_o = D.dr // D.och
        D.cfg = []
        for l in range(D.layers):
            C = Dims()
            C.split = l == 0
            parts = 2 if C.split else 1
            C.q, C.f = D.q // parts, D.f // parts
            C.heads, C.n_f = C.q // D.hd, C.f // D.fch
            C.cw = D.fch if C.split else 2 * D.fch
            C.n_c = C.f // C.cw
            D.cfg.append(C)
        assert D.seq == 2 * D.tok and D.seqs == n_col // 2 == n_row == 4

        half = D.hd // 2
        inv_freq = (np.float32(1.0) / (np.float32(10000.0) ** (np.arange(half, dtype=np.float32) * np.float32(2.0) / np.float32(D.hd)))).astype(np.float32)
        angles = (inv_freq[:, None] * np.arange(D.seq, dtype=np.float32)[None, :]).astype(np.float32)
        cos_t, sin_t = np.cos(angles).astype(np.float32), np.sin(angles).astype(np.float32)
        perm = np.zeros((2 * D.hd, n_col * D.kvp), np.float32)
        for i in range(2 * D.hd):
            perm[i, (i // kv_local) * D.kvp + i % kv_local] = 1.0

        x_t = x_loc.transpose(0, 2, 1)
        w_t = w_in_loc.transpose(0, 2, 1)
        wkv_t = jnp.pad(w_kv_loc.transpose(0, 2, 1), ((0, 0), (0, D.kvp - kv_local), (0, 0)))
        gains = jnp.pad(gain_loc, ((0, 16 - D.layers), (0, 128 - D.dl)))

        n_y = sum(12 + 6 * (C.n_f + D.n_o) for C in D.cfg)
        m = D.och * n_row
        sds = jax.ShapeDtypeStruct
        dma = pltpu.SemaphoreType.DMA
        out = pl.pallas_call(
            functools.partial(kernel, D),
            out_shape=(
                sds(x_t.shape, BF16),
                sds((D.layers, 2, n_batch, D.pos, 128), BF16),
                sds((D.layers, e, D.d), BF16),
                sds((D.layers, D.kvp, D.d), BF16),
                sds((D.layers, n_row, r_block, D.dr), BF16),
                sds((D.seqs, D.d, D.seq), BF16),
            ),
            in_specs=[ANY] * 5 + [VMEM] * 3,
            out_specs=(ANY,) * 6,
            scratch_shapes=[
                pltpu.VMEM((group, D.dl, D.tok), BF16),
                pltpu.VMEM((group, 16, 128), BF16),
                pltpu.VMEM((D.layers, D.d, 128), F32),
                pltpu.VMEM((D.d, D.tok), BF16),
                pltpu.VMEM((D.seqs, D.d, D.seq), BF16),
                pltpu.VMEM((2, max(4 * D.fch, D.q + D.kvp), D.d), BF16),
                pltpu.VMEM((2, r_block, m), BF16),
                pltpu.VMEM((m, r_block), BF16),
                pltpu.VMEM((D.seqs * D.q, D.seq), BF16),
                pltpu.VMEM((n_col, 2 * D.seqs, D.kvp, D.seq), BF16),
                pltpu.VMEM((2 * D.seqs, D.seq, 128), BF16),
                pltpu.VMEM((2 * D.seqs, D.hd, D.seq), BF16),
                pltpu.VMEM((D.layers, 2, D.seqs, D.seq, 128), BF16),
                pltpu.VMEM((D.seqs * r_block, D.seq), BF16),
                pltpu.VMEM((2, D.seqs, m, D.seq), BF16),
                pltpu.VMEM((5, 4, m, D.tok), BF16),
                pltpu.VMEM((5, m, D.tok), BF16),
                pltpu.VMEM((5, 2, m, D.tok), BF16),
                pltpu.VMEM((2, D.n_o, m, D.tok), BF16),
                pltpu.VMEM((D.n_o, m, D.tok), BF16),
                dma((group,)), dma((group,)), dma((group,)), dma((group,)),
                dma((n_y,)), dma((n_y,)),
                dma((4, 9)), dma((4, 9)), dma, dma,
                dma((D.seqs, n_col)), dma((D.seqs, n_col)),
                dma((5, 8)), dma((5, 8)),
                dma((D.n_o,)), dma((D.n_o,)),
                dma((2, 8)), dma((2, 8)), dma((D.seqs,)),
                dma((n_row,)), dma((n_row,)), dma,
            ],
            compiler_params=pltpu.CompilerParams(collective_id=0, has_side_effects=True, vmem_limit_bytes=67_000_000),
            name="two_layers",
        )(x_t, gains, w_t, wkv_t, w_out_loc, jnp.asarray(cos_t), jnp.asarray(sin_t), jnp.asarray(perm, BF16))
        return out[0].transpose(0, 2, 1), out[1][..., : D.hd]

    return jax.shard_map(device_fn, mesh=mesh, in_specs=(act_spec, P(None, ("row", "col")), weight_spec, weight_spec, P(None, "col", "row")), out_specs=(act_spec, P(None, None, "dp", ("row", "col"), None)), check_vma=False)
```

```python
import functools

import numpy as np

import jax
import jax.numpy as jnp
from jax import lax
from jax.experimental import pallas as pl
from jax.experimental.pallas import tpu as pltpu
from jax.sharding import PartitionSpec as P

LN_EPS = 1e-6
MESH = pl.DeviceIdType.MESH
ANY = pl.BlockSpec(memory_space=pl.ANY)
VMEM = pl.BlockSpec(memory_space=pltpu.VMEM)
F32, BF16 = jnp.float32, jnp.bfloat16


def dot(a, b):
    return jnp.dot(a, b, preferred_element_type=F32)


class Dims:
    pass


def rows_at(start, count, by=16):
    return pl.ds(start if isinstance(start, int) else pl.multiple_of(start, by), count)


def kernel(
    D,
    x_t, gains, w_t, wkv_t, w_o, cos_ref, sin_ref, perm_ref,
    y_out, kv_out, g_w, g_kv, g_wo, g_h,
    xland, gland, gcol, hid, ht, wbuf, wonat, wobuf, qt, kvland, kn, vt, kvbuf, jt, ot, twin_in, far_in, near_in, psum, pair_in,
    stage, hs, hr, xs, xr, gs, gr, ys, yr, ags, agr, ps, pr_, kvs, kvr, rss, rsr, es, er, lw, lo, lh, fs, fr, fl,
):
    sc = jax.named_scope
    row, col = lax.axis_index("row"), lax.axis_index("col")
    n_row, n_col, n = D.n_row, D.n_col, D.n_row * D.n_col
    n_x = n_col // 2
    me = row * n_col + col
    x, k = col // 2, lax.rem(col, 2)
    xr_, xl_, xf_ = lax.rem(x + 1, n_x), lax.rem(x + n_x - 1, n_x), lax.rem(x + 2, n_x)
    right, left, twin = xr_ * 2 + k, xl_ * 2 + k, x * 2 + 1 - k
    up, down, across = lax.rem(row + 1, n_row), lax.rem(row + n_row - 1, n_row), lax.rem(row + 2, n_row)
    half, mate = row // 2, n_row - 1 - row
    peer = row + 1 - 2 * lax.rem(row, 2)
    tok, dl, dr = D.tok, D.dl, D.dr
    och, fch = D.och, D.fch
    my_lanes = pl.ds(pl.multiple_of(k * tok, 128), tok)
    twin_lanes = pl.ds(pl.multiple_of((1 - k) * tok, 128), tok)

    def remote(src, dst, ssem, rsem, r, c):
        return pltpu.make_async_remote_copy(src_ref=src, dst_ref=dst, send_sem=ssem, recv_sem=rsem, device_id={"row": r, "col": c}, device_id_type=MESH)

    def loop(lo_, hi_, f):
        def body(i, carry):
            f(i)
            return carry

        lax.fori_loop(lo_, hi_, body, 0)

    barrier = pltpu.get_barrier_semaphore()

    def greet(i):
        d = lax.rem(me + i, n)
        pl.semaphore_signal(barrier, inc=1, device_id={"row": d // n_col, "col": lax.rem(d, n_col)}, device_id_type=MESH)

    with sc("barrier"):
        loop(1, n, greet)
        pl.semaphore_wait(barrier, n - 1)

    def piece_of(ref, d):
        return ref.at[d // 2, :, pl.ds(pl.multiple_of(lax.rem(d, 2) * tok, 128), tok)]

    def swap(from_piece, to_place, sends, recvs, tag):
        def index(src, dst):
            return lax.rem(dst - src + n, n)

        def start(d):
            r, c = d // n_col, lax.rem(d, n_col)
            i = index(me, d)
            other = lax.rem(c, 2) != k
            by_x = other & (c // 2 == xf_)
            by_y = other & (c // 2 != xf_) & (r == across)

            @pl.when(by_x)
            def _():
                remote(from_piece(d), stage.at[r], sends.at[i], hr.at[tag, r], row, left).start()

            @pl.when(by_y)
            def _():
                e = n_row + c // 2
                remote(from_piece(d), stage.at[e], sends.at[i], hr.at[tag, e], down, col).start()

            @pl.when((i != 0) & ~by_x & ~by_y)
            def _():
                remote(from_piece(d), to_place(me), sends.at[i], recvs.at[i], r, c).start()

        def pass_x(r):
            src, dst = row * n_col + right, r * n_col + xl_ * 2 + 1 - k
            return remote(stage.at[r], to_place(src), hs.at[tag, r], recvs.at[index(src, dst)], r, xl_ * 2 + 1 - k)

        def pass_y(e):
            c = lax.rem(x + e, n_x)
            src, dst = up * n_col + col, down * n_col + c * 2 + 1 - k
            at = n_row + c
            return remote(stage.at[at], to_place(src), hs.at[tag, at], recvs.at[index(src, dst)], down, c * 2 + 1 - k)

        def each_y(f):
            loop(0, n_x - 1, lambda i: f(i + i // 2))

        def arrive(at):
            remote(stage.at[at], stage.at[at], hs.at[tag, at], hr.at[tag, at], row, col).wait_recv()

        def hand_over():
            def one_x(r):
                arrive(r)
                pass_x(r).start()

            def one_y(e):
                arrive(n_row + lax.rem(x + e, n_x))
                pass_y(e).start()

            loop(0, n_row, one_x)
            each_y(one_y)

        def finish():
            def body(i):
                s = lax.rem(me + n - i, n)
                remote(to_place(s), to_place(s), sends.at[i], recvs.at[i], row, col).wait_recv()
                remote(from_piece(lax.rem(me + i, n)), to_place(me), sends.at[i], recvs.at[i], row, col).wait_send()

            loop(1, n, body)
            loop(0, n_row, lambda r: pass_x(r).wait_send())
            each_y(lambda e: pass_y(e).wait_send())

        return start, hand_over, finish

    x_start, x_hand_over, x_finish = swap(lambda d: piece_of(x_t, d), lambda s: xland.at[s], xs, xr, 0)

    def g_copy(i):
        d = lax.rem(me + i, n)
        return remote(gains, gland.at[me], gs.at[i], gr.at[i], d // n_col, lax.rem(d, n_col))

    own_x = pltpu.make_async_copy(piece_of(x_t, me), xland.at[me], xr.at[0])
    own_g = pltpu.make_async_copy(gains, gland.at[me], gr.at[0])
    own_x.start()
    own_g.start()
    def x_first(i):
        x_start(lax.rem(me + i, n))
        g_copy(i).start()

    loop(1, n, x_first)

    def own_lanes(r):
        return pl.ds(pl.multiple_of(r * dr, 128), dr)

    def o_lanes(j, r):
        return pl.ds(pl.multiple_of(lax.rem(r + j, D.n_o) * och, 128), och)

    steps = []
    for l, C in enumerate(D.cfg):
        steps += [(l, "q", 0)] + [(l, "f", j) for j in range(C.n_f)] + [(l, "o", j) for j in range(D.n_o)]
    n_steps = len(steps)
    step_of = {s: t for t, s in enumerate(steps)}

    def blocks(t, i):
        l, kind, j = steps[t]
        C = D.cfg[l]
        out = []

        def w_rows(a, m):
            at = rows_at(a, m)
            out.append((w_t.at[l, at, :], lambda r: g_w.at[l, at, own_lanes(r)]))

        def o_rows(a, m):
            at = rows_at(a, m)
            out.append((w_o.at[l, at, o_lanes(j, row)], lambda r: g_wo.at[l, r, at, o_lanes(j, r)]))

        def kv_rows(a, m):
            at = pl.ds(a, m)
            out.append((wkv_t.at[l, at, :], lambda r: g_kv.at[l, at, own_lanes(r)]))

        if kind == "q":
            for a in (0, C.q // 2):
                w_rows(i * C.q + a, C.q // 2)
            for a in (0, D.kvp // 2):
                kv_rows(a, D.kvp // 2)
        elif kind == "f":
            w_rows(D.q + i * C.f + j * fch, fch)
            w_rows(D.q + D.f + i * C.f + j * fch, fch)
        elif C.split:
            o_rows(i * C.q, C.q)
            o_rows(D.q + i * C.f, C.f)
        else:
            for a in (0, (D.q + D.f) // 2):
                o_rows(a, (D.q + D.f) // 2)
        return out

    base, n_sems = [], 0
    for l, kind, j in steps:
        base.append(n_sems)
        n_sems += 12 if kind == "q" else 6
    assert n_sems == ys.shape[0]
    y_sent = []

    def y_copy(t, i, kind, src, dst, r):
        at = base[t] + 3 * i + kind
        return remote(src, dst, ys.at[at], yr.at[at], r, col)

    def y_send(*args):
        c = y_copy(*args)
        c.start()
        y_sent.append(c)

    def issue_peer(t):
        for i, (src, place) in enumerate(blocks(t, half if D.cfg[steps[t][0]].split else 0)):
            y_send(t, i, 0, src, place(row), peer)

    def issue_mate(t):
        for i, (src, place) in enumerate(blocks(t, 1 - half if D.cfg[steps[t][0]].split else 0)):
            y_send(t, i, 1, src, place(row), mate)

    def relay(t):
        split = D.cfg[steps[t][0]].split
        with sc(f"relay{t}"):
            for i, (src, place) in enumerate(blocks(t, half if split else 0)):
                y_copy(t, i, 1, src, place(mate), mate).wait_recv()
                if split or i % 2 == 0:
                    y_send(t, i, 2, place(mate), place(mate), peer)
                if not split:
                    y_copy(t, i, 0, src, place(peer), peer).wait_recv()
                    if i % 2 == 1:
                        y_send(t, i, 2, place(peer), place(peer), mate)

    at = {"next": 0, "peer": 0, "mate": 0, "relay": 0}
    first_of = {l: min(t for t, st in enumerate(steps) if st[0] == l) for l in range(D.layers)}

    def step(l, j):
        return min(first_of[l] + j, first_of.get(l + 1, n_steps) - 1)

    def peer_to(t):
        while at["peer"] <= t:
            issue_peer(at["peer"])
            at["peer"] += 1

    def mate_to(t):
        while at["mate"] <= t:
            issue_mate(at["mate"])
            at["mate"] += 1

    def relay_to(t):
        assert t < at["peer"] and t < at["mate"]
        while at["relay"] <= t:
            relay(at["relay"])
            at["relay"] += 1

    def advance():
        t = at["next"]
        assert t < at["relay"], t
        rest = n_row - 1 - peer
        with sc(f"adv{t}"):
            split = D.cfg[steps[t][0]].split
            for i, (src, place) in enumerate(blocks(t, half if split else 0)):
                if split:
                    y_copy(t, i, 0, src, place(peer), peer).wait_recv()
                y_copy(t, i, 2, src, place(rest), rest).wait_recv()
            at["next"] = t + 1

    def have(*which):
        while at["next"] <= step_of[which]:
            advance()

    mate_to(1)
    peer_to(step(0, 3))

    def w_fetch(l, kind, j, slot):
        C = D.cfg[l]
        i = half if C.split else 0
        copies = []

        def fetch(src, dst):
            copies.append(pltpu.make_async_copy(src, dst, lw.at[slot, len(copies)]))

        def w_rows(a, m, at):
            a, at = rows_at(a, m), pl.ds(at, m)
            fetch(w_t.at[l, a, :], wbuf.at[slot, at, own_lanes(row)])
            for r in (up, down, across):
                fetch(g_w.at[l, a, own_lanes(r)], wbuf.at[slot, at, own_lanes(r)])

        if kind == "q":
            w_rows(i * C.q, C.q, 0)
            at = pl.ds(C.q, D.kvp)
            fetch(wkv_t.at[l], wbuf.at[slot, at, own_lanes(row)])
            for r in (up, down, across):
                fetch(g_kv.at[l, :, own_lanes(r)], wbuf.at[slot, at, own_lanes(r)])
        else:
            w_rows(D.q + i * C.f + j * C.cw, C.cw, 0)
            w_rows(D.q + D.f + i * C.f + j * C.cw, C.cw, C.cw)
        return copies

    def o_fetch(l, j, slot):
        C = D.cfg[l]
        copies = []

        def fetch(src, dst):
            copies.append(pltpu.make_async_copy(src, dst, lo.at[slot, len(copies)]))

        spans = ((half * C.q, 0, C.q), (D.q + half * C.f, C.q, C.f)) if C.split else ((0, 0, C.q + C.f),)
        for a, at, m in spans:
            a, at = rows_at(a, m), pl.ds(at, m)
            to = lambda r: pl.ds(pl.multiple_of(r * och, 128), och)
            fetch(w_o.at[l, a, o_lanes(j, row)], wonat.at[slot, at, to(row)])
            for r in (up, down, across):
                fetch(g_wo.at[l, r, a, o_lanes(j, r)], wonat.at[slot, at, to(r)])
        return copies

    def start(copies):
        for c in copies:
            c.start()

    def wait(copies):
        for c in copies:
            c.wait()

    own_x.wait()
    own_g.wait()

    def g_finish(i):
        s = lax.rem(me + n - i, n)
        remote(gland.at[s], gland.at[s], gs.at[i], gr.at[i], row, col).wait_recv()
        g_copy(i).wait_send()

    with sc("xwait"):
        x_hand_over()
        x_finish()
        loop(1, n, g_finish)

    def keep(d):
        hid[rows_at(d * dl, dl), :] = xland[d]

    with sc("gains"):
        loop(0, n, keep)
        g_all = gland[...].astype(F32)
        for l in range(D.layers):
            g_rows = g_all[:, l, :]
            g_rows = jnp.concatenate([g_rows, jnp.zeros((128 - n, 128), F32)], axis=0) if n < 128 else g_rows
            g_cols = g_rows.T
            for d in range(n):
                gcol[l, d * dl : (d + 1) * dl, :] = jnp.broadcast_to(g_cols[:dl, d : d + 1], (dl, 128))

    blk = 64
    n_blk = D.d // blk

    def layer_norm(l):
        def add_up(i, acc):
            v = hid[rows_at(i * blk, blk), :].astype(F32)
            return acc + v.reshape(blk // 8, 8, tok).sum(axis=0)

        mean = lax.fori_loop(0, n_blk, add_up, jnp.zeros((8, tok), F32)).sum(axis=0, keepdims=True) / D.d

        def add_sq(i, acc):
            v = hid[rows_at(i * blk, blk), :].astype(F32) - mean
            return acc + (v * v).reshape(blk // 8, 8, tok).sum(axis=0)

        var = lax.fori_loop(0, n_blk, add_sq, jnp.zeros((8, tok), F32)).sum(axis=0, keepdims=True) / D.d
        scale = lax.rsqrt(var + LN_EPS)

        def write(i):
            rows = rows_at(i * blk, blk)
            g = gcol[l, rows, :]
            g = jnp.concatenate([g] * (tok // 128), axis=1)
            v = (hid[rows, :].astype(F32) - mean) * scale * g
            ht[x, rows, my_lanes] = v.astype(BF16)

        with sc(f"norm{l}"):
            loop(0, n_blk, write)

    d_low, d_high = pl.ds(0, D.d // 2), pl.ds(D.d // 2, D.d // 2)

    class Gather:
        def __init__(self, ref, tag):
            self.ref, self.tag, self.sends = ref, tag, []
            for i, c in ((0, right), (1, left), (2, twin)):
                self.send(i, ref(x, False, None), c)

        def send(self, i, ref, c):
            copy = remote(ref, ref, ags.at[self.tag, i], agr.at[self.tag, i], row, c)
            copy.start()
            self.sends.append(copy)

        def arrived(self, i, ref):
            remote(ref, ref, ags.at[self.tag, i], agr.at[self.tag, i], row, col).wait_recv()

        def pass_on(self):
            with sc(f"pass_on{self.tag}"):
                self.arrived(0, self.ref(xl_, False, None))
                self.send(3, self.ref(xl_, False, 0), right)
                self.send(4, self.ref(xl_, False, None), twin)
                self.arrived(1, self.ref(xr_, False, None))
                self.send(5, self.ref(xr_, False, 1), left)
                self.send(6, self.ref(xr_, False, None), twin)

        def own(self):
            self.arrived(2, self.ref(x, True, None))

        def near(self):
            with sc(f"near{self.tag}"):
                self.arrived(4, self.ref(xl_, True, None))
                self.arrived(6, self.ref(xr_, True, None))

        def pass_far(self):
            with sc(f"pass_far{self.tag}"):
                for part, i, j in ((0, 3, 7), (1, 5, 8)):
                    self.arrived(i, self.ref(xf_, False, part))
                    self.send(j, self.ref(xf_, False, part), twin)

        def far(self):
            with sc(f"far{self.tag}"):
                self.arrived(7, self.ref(xf_, True, 0))
                self.arrived(8, self.ref(xf_, True, 1))

        def finish(self):
            for c in self.sends:
                c.wait_send()

    def normed_of(buf):
        def ref(chip, other, part):
            rows = slice(None) if part is None else (d_low, d_high)[part]
            return buf.at[chip, rows, twin_lanes if other else my_lanes]

        return ref

    def kv_of(a):
        def ref(chip, other, part):
            h = D.seqs // 2
            span = pl.ds(a * D.seqs, D.seqs) if part is None else pl.ds(a * D.seqs + part * h, h)
            return kvland.at[chip * 2 + (1 - k if other else k), span]

        return ref

    half_dim = D.hd // 2

    def near3(i):
        return lax.rem(x + i + i // 2, n_x)

    def all4(i):
        return i

    def far1(i):
        return xf_

    def rope(p):
        lo_, hi_ = p[:half_dim], p[half_dim:]
        return jnp.concatenate([lo_ * cos_ref[...] - hi_ * sin_ref[...], hi_ * cos_ref[...] + lo_ * sin_ref[...]], axis=0)

    def project_q(l, a, seq_of, count):
        C = D.cfg[l]

        def body(i):
            s = seq_of(i)
            p = dot(wbuf[1, : C.q + D.kvp, :], ht[s]).astype(BF16).astype(F32)
            for h in range(C.heads):
                at = rows_at((a * D.seqs + s) * C.q + h * D.hd, D.hd)
                qt[at, :] = (rope(p[h * D.hd : (h + 1) * D.hd]) * D.hd**-0.5).astype(BF16)
            kvland[col, a * D.seqs + s] = p[C.q :].astype(BF16)

        with sc(f"q{l}{a}"):
            loop(0, count, body)

    def kv_copy(s, j, source):
        ref = kvland.at[source, s]
        return remote(ref, ref, kvs.at[s, j], kvr.at[s, j], row, lax.rem(col + j, n_col))

    def kv_send(seq_of, count):
        def body(i):
            s = seq_of(i)
            loop(1, n_col, lambda j: kv_copy(s, j, col).start())

        loop(0, count, body)

    def kv_arrive():
        def body(i):
            j = i // D.seqs + 1
            s = lax.rem(i, D.seqs)
            kv_copy(s, j, lax.rem(col + n_col - j, n_col)).wait_recv()
            kv_copy(s, j, col).wait_send()

        with sc("kvwait"):
            loop(0, D.seqs * (n_col - 1), body)

    def key_value(l, a):
        def body(i):
            s = a * D.seqs + i
            raw = kvland[:, s].reshape(n_col * D.kvp, D.seq)
            both = dot(perm_ref[...], raw)
            zeros = jnp.zeros((128 - D.hd, D.seq), F32)
            k_nat = jnp.concatenate([rope(both[: D.hd]), zeros], axis=0).T.astype(BF16)
            kn[s] = k_nat
            vt[s] = both[D.hd :].astype(BF16)
            if a == 0:
                kvbuf[l, 0, i] = k_nat
                kvbuf[l, 1, i] = jnp.concatenate([both[D.hd :], zeros], axis=0).T.astype(BF16)

        with sc(f"kv{l}{a}"):
            loop(0, D.seqs, body)

    qb = D.seq // 2

    def attention(l, a):
        C = D.cfg[l]

        pair = 2
        per = C.heads // pair

        def body(i):
            s, h0 = a * D.seqs + i // per, lax.rem(i, per) * pair
            q_rows = [rows_at(s * C.q + (h0 + e) * D.hd, D.hd) for e in range(pair)]
            o_rows = [rows_at(s * (C.q + C.f) + (h0 + e) * D.hd, D.hd) for e in range(pair)]
            for b in range(2):
                ext = (b + 1) * qb
                lanes = slice(b * qb, (b + 1) * qb)
                keys = lax.broadcasted_iota(jnp.int32, (ext, qb), 0)
                queries = lax.broadcasted_iota(jnp.int32, (ext, qb), 1) + b * qb
                scores = [dot(kn[s, :ext, : D.hd], qt[q_rows[e], lanes]) for e in range(pair)]
                for e in range(pair):
                    score = jnp.where(keys <= queries, scores[e], -1e30)
                    p = jnp.exp(score - jnp.max(score, axis=0, keepdims=True))
                    p = (p * (1.0 / jnp.sum(p, axis=0, keepdims=True))).astype(BF16)
                    jt[o_rows[e], lanes] = dot(vt[s, :, :ext], p).astype(BF16)

        with sc(f"attn{l}{a}"):
            loop(0, D.seqs * per, body)

    def gate_up(l, a, slot, j, seq_of, count):
        C = D.cfg[l]

        def body(i):
            s = seq_of(i)
            p = dot(wbuf[slot, : 2 * C.cw, :], ht[s])
            g = p[: C.cw].astype(BF16).astype(F32)
            u = p[C.cw :].astype(BF16).astype(F32)
            jt[rows_at((a * D.seqs + s) * (C.q + C.f) + C.q + j * C.cw, C.cw), :] = (g * jax.nn.sigmoid(g) * u).astype(BF16)

        loop(0, count, body)

    def gate_up_loop(l, a, seq_of, count, first, last, stop=None):
        C = D.cfg[l]
        stop = C.n_c if stop is None else stop
        have_chunk(l, min(last, stop - 1))

        def body(j):
            slot = lax.rem(j, 2)
            wait(w_fetch(l, "f", j, slot))

            @pl.when(j + 1 < stop)
            def _():
                start(w_fetch(l, "f", j + 1, 1 - slot))

            gate_up(l, a, slot, j, seq_of, count)

        with sc(f"gu{l}{a}"):
            loop(first, last, body)

    def have_chunk(l, j):
        C = D.cfg[l]
        have(l, "f", (j + 1) * C.cw // fch - 1)

    def load_q(l):
        have(l, "q", 0)
        copies = w_fetch(l, "q", 0, 1)
        start(copies)
        wait(copies)

    m = och * n_row
    m_low, m_high = pl.ds(0, m // 2), pl.ds(m // 2, m // 2)
    r_slots = twin_in.shape[0]
    r_step = 64

    def order(i):
        return lax.rem(x + lax.rem(2 + 3 * i, 4), n_x)

    class Reduce:
        def __init__(self, l):
            self.l, self.C, self.sends = l, D.cfg[l], {}

        def send(self, u, i, src, dst, c):
            copy = remote(src, dst, rss.at[u % r_slots, i], rsr.at[u % r_slots, i], row, c)
            copy.start()
            self.sends[u].append(copy)

        def arrived(self, u, i, ref):
            remote(ref, ref, rss.at[u % r_slots, i], rsr.at[u % r_slots, i], row, col).wait_recv()

        def twin_copy(self, u, i):
            us = u % r_slots
            return remote(ot.at[u % 2, order(i), :, twin_lanes], twin_in.at[us, i], rss.at[us, i], rsr.at[us, i], row, twin)

        def twin_done(self, u):
            loop(0, 4, lambda i: self.twin_copy(u, i).wait_send())

        def stage_a(self, u, a):
            C = self.C
            if u >= 2:
                self.twin_done(u - 2)
            if u >= r_slots - 1:
                for c in self.sends.pop(u - r_slots + 1):
                    c.wait_send()
            self.sends[u] = []
            R = C.q + C.f

            def body(i):
                s = order(i)
                ot[u % 2, s] = dot(wobuf[:, :R], jt[rows_at((a * D.seqs + s) * R, R), :]).astype(BF16)
                self.twin_copy(u, i).start()

            with sc(f"sa{self.l}_{u}"):
                loop(0, 4, body)

        def stage_b(self, u):
            us = u % r_slots

            def body(i):
                self.arrived(u, i, twin_in.at[us, i])
                s = order(i)

                def add(b):
                    at = rows_at(b * r_step, r_step)
                    twin_in[us, i, at, :] = (ot[u % 2, s, at, my_lanes].astype(F32) + twin_in[us, i, at, :].astype(F32)).astype(BF16)

                loop(0, m // r_step, add)

            far = [
                remote(twin_in.at[us, 0, m_low], far_in.at[us, m_low], rss.at[us, 4], rsr.at[us, 4], row, right),
                remote(twin_in.at[us, 0, m_high], far_in.at[us, m_high], rss.at[us, 5], rsr.at[us, 5], row, left),
            ]
            self.sends[u] += far

            def each(i):
                body(i)

                @pl.when(i == 0)
                def _():
                    start(far)

            with sc(f"sb{self.l}_{u}"):
                loop(0, 4, each)

        def stage_c(self, u):
            us = u % r_slots

            def add_far(i, base):
                def add(b):
                    at = rows_at(base + b * r_step, r_step)
                    twin_in[us, i, at, :] = (twin_in[us, i, at, :].astype(F32) + far_in[us, at, :].astype(F32)).astype(BF16)

                loop(0, m // 2 // r_step, add)

            with sc(f"sc{self.l}_{u}"):
                self.arrived(u, 4, far_in.at[us, m_low])
                add_far(1, 0)
                self.send(u, 6, twin_in.at[us, 1], near_in.at[us, 0], right)
                self.arrived(u, 5, far_in.at[us, m_high])
                add_far(3, m // 2)
                self.send(u, 7, twin_in.at[us, 3], near_in.at[us, 1], left)

        def add_update(self, j, total):
            step = min(r_step, och)
            for r in range(n_row):

                def add(b, r=r):
                    dst = rows_at(r * dr + (r + j) % D.n_o * och + b * step, step)
                    u = total(rows_at(r * och + b * step, step)).astype(BF16).astype(F32)
                    hid[dst, :] = (hid[dst, :].astype(F32) + u).astype(BF16)

                loop(0, och // step, add)

        def stage_d(self, u, j, a):
            us = u % r_slots

            def total(at):
                return twin_in[us, 2, at, :].astype(F32) + near_in[us, 0, at, :].astype(F32) + near_in[us, 1, at, :].astype(F32)

            with sc(f"sd{self.l}_{u}"):
                self.arrived(u, 6, near_in.at[us, 0])
                self.arrived(u, 7, near_in.at[us, 1])
                if self.C.split:

                    def save(b):
                        at = rows_at(b * r_step, r_step)
                        psum[a, j, at, :] = total(at).astype(BF16)

                    loop(0, m // r_step, save)
                    if a == 1:
                        remote(psum.at[1, j], pair_in.at[j], es.at[j], er.at[j], mate, col).start()
                else:
                    self.add_update(j, total)

        def stage_e(self, j):
            with sc(f"se{self.l}_{j}"):
                c = remote(psum.at[1, j], pair_in.at[j], es.at[j], er.at[j], mate, col)
                c.wait_recv()
                self.add_update(j, lambda at: psum[0, j, at, :].astype(F32) + pair_in[j, at, :].astype(F32))
                c.wait_send()

        def finish(self, units):
            with sc(f"rfin{self.l}"):
                for u in range(max(0, units - 2), units):
                    self.twin_done(u)
                for u in self.sends:
                    for c in self.sends[u]:
                        c.wait_send()

    o_started = set()

    def o_load(l, j, a):
        if (l, j, a) not in o_started:
            have(l, "o", j)
            start(o_fetch(l, j, j % 2))
            o_started.add((l, j, a))

    def o_use(l, j, a):
        C = D.cfg[l]
        with sc(f"ouse{l}_{j}"):
            o_load(l, j, a)
            wait(o_fetch(l, j, j % 2))
            R = C.q + C.f
            for r in range(n_row):
                wobuf[r * och : (r + 1) * och, :R] = wonat[j % 2, :R, r * och : (r + 1) * och].T

    layer_norm(0)
    g0 = Gather(normed_of(ht), 0)
    mine = ht.at[x, :, my_lanes]
    shared = g_h.at[x, :, my_lanes]
    to_mate = remote(mine, shared, ps, pr_, mate, col)
    to_mate.start()
    relay_to(1)
    mate_to(step(0, 5))
    peer_to(step(0, 5))
    g0.pass_on()
    with sc("mate"):
        to_mate.wait_recv()
    g1 = Gather(normed_of(g_h), 1)
    load_q(0)
    g0.own()
    g0.near()
    project_q(0, 0, near3, 3)
    relay_to(2)
    mate_to(step(0, 10))
    g0.pass_far()
    g0.far()
    project_q(0, 0, far1, 1)
    kv0 = Gather(kv_of(0), 2)
    relay_to(3)
    n_f = D.cfg[0].n_f
    f_started = set()

    def f_load(j):
        if j not in f_started:
            f_started.add(j)
            start(w_fetch(0, "f", j, j % 2))

    def h_copy(i):
        return pltpu.make_async_copy(g_h.at[i], ht.at[i], lh.at[i])

    have(0, "f", 0)
    f_load(0)
    gate_up_loop(0, 0, all4, 4, 0, 2, 2)
    relay_to(step(0, 4))
    for j in range(2, n_f):
        have(0, "f", j)
        f_load(j)
        with sc(f"gu0_{j}"):
            wait(w_fetch(0, "f", j, j % 2))
            gate_up(0, 0, j % 2, j, all4, 4)
        if j == max(2, n_f - 3):
            relay_to(step(0, 5))
            peer_to(step(0, 6))
            relay_to(step(0, 6))
            peer_to(step(0, 7))
    kv0.pass_on()
    g1.pass_on()
    for t in (7, 8):
        relay_to(step(0, t))
        peer_to(step(0, t + 1))
    relay_to(step(0, 9))
    peer_to(step(0, 10))
    relay_to(step(0, 10))
    peer_to(step(1, 5))
    mate_to(step(1, D.cfg[1].n_f - 2))
    g0.finish()
    to_mate.wait_send()
    g1.own()
    g1.near()
    loop(0, 3, lambda i: h_copy(near3(i)).start())
    kv0.pass_far()
    with sc("kv0wait"):
        kv0.own()
        kv0.near()
        kv0.far()
        kv0.finish()
    key_value(0, 0)
    attention(0, 0)

    red = Reduce(0)
    units = [(j, 0) for j in range(D.n_o - 1)] + [(j, 1) for j in range(D.n_o)] + [(D.n_o - 1, 0)]
    n_u = len(units)
    first = D.n_o - 1
    state = {"e": 0}

    def settle(count):
        while state["e"] < count:
            red.stage_e(state["e"])
            state["e"] += 1

    def unit(u):
        j, a = units[u]
        if u == 0 or units[u - 1][0] != j:
            o_use(0, j, a)
        red.stage_a(u, a)
        if u + 1 < n_u and units[u + 1][0] != j:
            o_load(0, *units[u + 1])
        if u >= 2:
            red.stage_c(u - 2)
        if u >= 3:
            red.stage_d(u - 3, *units[u - 3])
        red.stage_b(u)

    unit(0)
    g1.pass_far()
    unit(1)
    g1.far()
    h_copy(xf_).start()
    load_q(0)
    start(w_fetch(0, "f", 0, 0))
    loop(0, 3, lambda i: h_copy(near3(i)).wait())
    h_copy(xf_).wait()
    project_q(0, 1, all4, 4)
    kv1 = Gather(kv_of(1), 3)
    parts = first - 2
    cuts = [n_f * i // parts for i in range(parts + 1)]
    for u in range(2, first):
        unit(u)
        if u == 2:
            kv1.pass_on()
        gate_up_loop(0, 1, all4, 4, cuts[u - 2], cuts[u - 1])
    kv1.pass_far()
    relay_to(step(1, 1))
    with sc("kv1wait"):
        kv1.own()
        kv1.near()
        kv1.far()
        kv1.finish()
    key_value(0, 1)
    attention(0, 1)
    g1.finish()
    relay_to(step(1, 2))
    peer_to(step(1, 7))
    n_f1 = D.cfg[1].n_f
    for u in range(first, n_u):
        unit(u)
        v = u - first
        if v in (0, 1, 2):
            relay_to(step(1, min(v + 3, n_f1 - 2)))
        if v == 1:
            peer_to(step(1, min(8, n_f1)))
        elif v == 4:
            relay_to(step(1, min(6, n_f1 - 2)))
            peer_to(step(1, min(9, n_f1)))
        elif v == 5:
            peer_to(step(1, n_f1))
    relay_to(step(1, min(6, n_f1 - 2)))
    peer_to(step(1, n_f1))
    red.stage_c(n_u - 2)
    red.stage_d(n_u - 3, *units[n_u - 3])
    red.stage_c(n_u - 1)
    red.stage_d(n_u - 2, *units[n_u - 2])
    mate_to(step(1, n_f1))
    settle(D.n_o - 1)
    red.stage_d(n_u - 1, *units[n_u - 1])
    settle(D.n_o)
    red.finish(n_u)

    def slice_of(d):
        return hid.at[rows_at(d * dl, dl), :]

    y_start, y_hand_over, y_finish = swap(slice_of, lambda s: piece_of(y_out, s), xs, xr, 1)
    own_y = pltpu.make_async_copy(slice_of(me), piece_of(y_out, me), xr.at[0])

    def y_send_back(d):
        @pl.when(d == me)
        def _():
            own_y.start()

        @pl.when(d != me)
        def _():
            y_start(d)

    def y_ready(low, high):
        def body(d):
            r, a = d // n_col, lax.rem(d, n_col) * dl
            first = lax.rem(a // och + D.n_o - lax.rem(r, D.n_o), D.n_o)
            second = lax.rem((a + dl - 1) // och + D.n_o - lax.rem(r, D.n_o), D.n_o)

            done = jnp.maximum(first, second)

            @pl.when((low <= done) & (done < high))
            def _():
                y_send_back(d)

        loop(0, n, body)

    for l in range(1, D.layers):
        C = D.cfg[l]
        layer_norm(l)
        g0 = Gather(normed_of(ht), 0)
        peer_to(step(l, C.n_f))
        mate_to(step(l, C.n_f))
        relay_to(step(l, min(8, C.n_f)))
        own1, near2 = (lambda i: x), (lambda i: lax.rem(x + 1 + 2 * i, n_x))
        n_mid = min(3, C.n_c - 1)

        def begin(seq_of, count):
            load_q(l)
            have_chunk(l, 0)
            start(w_fetch(l, "f", 0, 0))
            project_q(l, 0, seq_of, count)

        g0.own()
        begin(own1, 1)
        kv_send(own1, 1)
        gate_up_loop(l, 0, own1, 1, 0, n_mid, n_mid)
        relay_to(step(l, C.n_f))
        peer_to(step(l, C.n_f + 1))
        mate_to(step(l, C.n_f + 1))
        g0.pass_on()
        relay_to(step(l, C.n_f + 1))
        peer_to(step(l, C.n_f + 2))
        mate_to(step(l, C.n_f + 2))
        g0.near()
        begin(near2, 2)
        kv_send(near2, 2)
        gate_up_loop(l, 0, near2, 2, 0, n_mid)
        g0.pass_far()
        peer_to(step(l, C.n_f + 3))
        mate_to(step(l, C.n_f + 3))
        relay_to(step(l, C.n_f + 2))
        gate_up_loop(l, 0, near3, 3, n_mid, C.n_c)
        peer_to(step(l, C.n_f + 4))
        mate_to(step(l, C.n_f + 4))
        relay_to(step(l, C.n_f + 3))
        g0.far()
        begin(far1, 1)
        kv_send(far1, 1)
        gate_up_loop(l, 0, far1, 1, 0, C.n_c)
        peer_to(step(l, C.n_f + D.n_o))
        mate_to(step(l, C.n_f + D.n_o))
        relay_to(step(l, C.n_f + 4))
        g0.finish()
        kv_arrive()
        key_value(l, 0)
        attention(l, 0)
        red = Reduce(l)
        last = l + 1 == D.layers

        end = D.n_o - 1
        for j in range(D.n_o):
            o_use(l, j, 0)
            red.stage_a(j, 0)
            if j == 0:
                relay_to(step(l, C.n_f + D.n_o))
            if j < end:
                o_load(l, j + 1, 0)
            if 2 <= j:
                red.stage_c(j - 2)
            if 3 <= j:
                red.stage_d(j - 3, j - 3, 0)
            red.stage_b(j)
        red.stage_c(end - 1)
        red.stage_d(end - 2, end - 2, 0)
        red.stage_c(end)
        red.stage_d(end - 1, end - 1, 0)
        if last:
            with sc("send"):
                y_ready(0, end)
        red.stage_d(end, end, 0)
        if last:
            y_ready(end, end + 1)
        red.finish(D.n_o)

    def kv_back(i):
        r = lax.rem(row + i, n_row)
        pos = rows_at((r * n_col + col) * D.pos, D.pos)
        return kvbuf.at[:, :, :, pos, :], kv_out.at[:, :, pl.ds(row * D.seqs, D.seqs)], r

    src, dst, _ = kv_back(0)
    own_kv = pltpu.make_async_copy(src, dst, fl)
    own_kv.start()
    kv_sends = []
    for i in range(1, n_row):
        src, dst, r = kv_back(i)
        c = remote(src, dst, fs.at[i], fr.at[i], r, col)
        c.start()
        kv_sends.append(c)

    with sc("ywait"):
        y_hand_over()
        y_finish()
        own_y.wait()
        own_kv.wait()
        for i in range(1, n_row):
            r = lax.rem(row + n_row - i, n_row)
            dst = kv_out.at[:, :, pl.ds(r * D.seqs, D.seqs)]
            remote(dst, dst, fs.at[i], fr.at[i], row, col).wait_recv()
        for c in kv_sends:
            c.wait_send()
        for c in y_sent:
            c.wait_send()


def solution(mesh):
    n_row, n_col = mesh.shape["row"], mesh.shape["col"]
    group = n_row * n_col
    act_spec = P("dp", None, ("row", "col"))
    weight_spec = P(None, "row", "col")

    def device_fn(x_loc, gain_loc, w_in_loc, w_kv_loc, w_out_loc):
        D = Dims()
        D.n_row, D.n_col = n_row, n_col
        n_batch, D.seq, D.dl = x_loc.shape
        D.layers, D.dr, e = w_in_loc.shape
        D.d = D.dl * group
        r_block = w_out_loc.shape[1]
        D.f = e - r_block
        D.q = r_block - D.f
        kv_local = w_kv_loc.shape[2]
        D.hd = kv_local * n_col // 2
        D.kvp = 32
        D.tok = n_batch * D.seq // group
        D.seqs = n_batch // n_row
        D.pos = D.seq // group
        D.fch = 128
        D.och = 128
        D.n_o = D.dr // D.och
        D.cfg = []
        for l in range(D.layers):
            C = Dims()
            C.split = l == 0
            parts = 2 if C.split else 1
            C.q, C.f = D.q // parts, D.f // parts
            C.heads, C.n_f = C.q // D.hd, C.f // D.fch
            C.cw = D.fch if C.split else 2 * D.fch
            C.n_c = C.f // C.cw
            D.cfg.append(C)
        assert D.seq == 2 * D.tok and D.seqs == n_col // 2 == n_row == 4

        half = D.hd // 2
        inv_freq = (np.float32(1.0) / (np.float32(10000.0) ** (np.arange(half, dtype=np.float32) * np.float32(2.0) / np.float32(D.hd)))).astype(np.float32)
        angles = (inv_freq[:, None] * np.arange(D.seq, dtype=np.float32)[None, :]).astype(np.float32)
        cos_t, sin_t = np.cos(angles).astype(np.float32), np.sin(angles).astype(np.float32)
        perm = np.zeros((2 * D.hd, n_col * D.kvp), np.float32)
        for i in range(2 * D.hd):
            perm[i, (i // kv_local) * D.kvp + i % kv_local] = 1.0

        x_t = x_loc.transpose(0, 2, 1)
        w_t = w_in_loc.transpose(0, 2, 1)
        wkv_t = jnp.pad(w_kv_loc.transpose(0, 2, 1), ((0, 0), (0, D.kvp - kv_local), (0, 0)))
        gains = jnp.pad(gain_loc, ((0, 16 - D.layers), (0, 128 - D.dl)))

        n_y = sum(12 + 6 * (C.n_f + D.n_o) for C in D.cfg)
        m = D.och * n_row
        sds = jax.ShapeDtypeStruct
        dma = pltpu.SemaphoreType.DMA
        out = pl.pallas_call(
            functools.partial(kernel, D),
            out_shape=(
                sds(x_t.shape, BF16),
                sds((D.layers, 2, n_batch, D.pos, 128), BF16),
                sds((D.layers, e, D.d), BF16),
                sds((D.layers, D.kvp, D.d), BF16),
                sds((D.layers, n_row, r_block, D.dr), BF16),
                sds((D.seqs, D.d, D.seq), BF16),
            ),
            in_specs=[ANY] * 5 + [VMEM] * 3,
            out_specs=(ANY,) * 6,
            scratch_shapes=[
                pltpu.VMEM((group, D.dl, D.tok), BF16),
                pltpu.VMEM((group, 16, 128), BF16),
                pltpu.VMEM((D.layers, D.d, 128), F32),
                pltpu.VMEM((D.d, D.tok), BF16),
                pltpu.VMEM((D.seqs, D.d, D.seq), BF16),
                pltpu.VMEM((2, max(4 * D.fch, D.q + D.kvp), D.d), BF16),
                pltpu.VMEM((2, r_block, m), BF16),
                pltpu.VMEM((m, r_block), BF16),
                pltpu.VMEM((D.seqs * D.q, D.seq), BF16),
                pltpu.VMEM((n_col, 2 * D.seqs, D.kvp, D.seq), BF16),
                pltpu.VMEM((2 * D.seqs, D.seq, 128), BF16),
                pltpu.VMEM((2 * D.seqs, D.hd, D.seq), BF16),
                pltpu.VMEM((D.layers, 2, D.seqs, D.seq, 128), BF16),
                pltpu.VMEM((D.seqs * r_block, D.seq), BF16),
                pltpu.VMEM((2, D.seqs, m, D.seq), BF16),
                pltpu.VMEM((5, 4, m, D.tok), BF16),
                pltpu.VMEM((5, m, D.tok), BF16),
                pltpu.VMEM((5, 2, m, D.tok), BF16),
                pltpu.VMEM((2, D.n_o, m, D.tok), BF16),
                pltpu.VMEM((D.n_o, m, D.tok), BF16),
                pltpu.VMEM((n_row + n_col // 2, D.dl, D.tok), BF16), dma((2, n_row + n_col // 2)), dma((2, n_row + n_col // 2)),
                dma((group,)), dma((group,)), dma((group,)), dma((group,)),
                dma((n_y,)), dma((n_y,)),
                dma((4, 9)), dma((4, 9)), dma, dma,
                dma((D.seqs, n_col)), dma((D.seqs, n_col)),
                dma((5, 8)), dma((5, 8)),
                dma((D.n_o,)), dma((D.n_o,)),
                dma((2, 8)), dma((2, 8)), dma((D.seqs,)),
                dma((n_row,)), dma((n_row,)), dma,
            ],
            compiler_params=pltpu.CompilerParams(collective_id=0, has_side_effects=True, vmem_limit_bytes=67_000_000),
            name="two_layers",
        )(x_t, gains, w_t, wkv_t, w_out_loc, jnp.asarray(cos_t), jnp.asarray(sin_t), jnp.asarray(perm, BF16))
        return out[0].transpose(0, 2, 1), out[1][..., : D.hd]

    return jax.shard_map(device_fn, mesh=mesh, in_specs=(act_spec, P(None, ("row", "col")), weight_spec, weight_spec, P(None, "col", "row")), out_specs=(act_spec, P(None, None, "dp", ("row", "col"), None)), check_vma=False)
```

```python
import functools

import numpy as np

import jax
import jax.numpy as jnp
from jax import lax
from jax.experimental import pallas as pl
from jax.experimental.pallas import tpu as pltpu
from jax.sharding import PartitionSpec as P

LN_EPS = 1e-6
MESH = pl.DeviceIdType.MESH
ANY = pl.BlockSpec(memory_space=pl.ANY)
VMEM = pl.BlockSpec(memory_space=pltpu.VMEM)
F32, BF16 = jnp.float32, jnp.bfloat16


def dot(a, b):
    return jnp.dot(a, b, preferred_element_type=F32)


class Dims:
    pass


def rows_at(start, count, by=16):
    return pl.ds(start if isinstance(start, int) else pl.multiple_of(start, by), count)


def kernel(
    D,
    x_t, gains, w_t, wkv_t, w_o, cos_ref, sin_ref, perm_ref,
    y_out, kv_out, g_w, g_kv, g_wo, g_h,
    xland, gland, gcol, hid, ht, wbuf, wonat, wobuf, qt, kvland, kn, vt, kvbuf, jt, ot, twin_in, far_in, near_in, psum, pair_in,
    xs, xr, gs, gr, ys, yr, ags, agr, ps, pr_, kvs, kvr, rss, rsr, es, er, lw, lo, lh, fs, fr, fl,
):
    sc = jax.named_scope
    row, col = lax.axis_index("row"), lax.axis_index("col")
    n_row, n_col, n = D.n_row, D.n_col, D.n_row * D.n_col
    n_x = n_col // 2
    me = row * n_col + col
    x, k = col // 2, lax.rem(col, 2)
    xr_, xl_, xf_ = lax.rem(x + 1, n_x), lax.rem(x + n_x - 1, n_x), lax.rem(x + 2, n_x)
    right, left, twin = xr_ * 2 + k, xl_ * 2 + k, x * 2 + 1 - k
    up, down, across = lax.rem(row + 1, n_row), lax.rem(row + n_row - 1, n_row), lax.rem(row + 2, n_row)
    half, mate = row // 2, n_row - 1 - row
    peer = row + 1 - 2 * lax.rem(row, 2)
    tok, dl, dr = D.tok, D.dl, D.dr
    och, fch = D.och, D.fch
    my_lanes = pl.ds(pl.multiple_of(k * tok, 128), tok)
    twin_lanes = pl.ds(pl.multiple_of((1 - k) * tok, 128), tok)

    def remote(src, dst, ssem, rsem, r, c):
        return pltpu.make_async_remote_copy(src_ref=src, dst_ref=dst, send_sem=ssem, recv_sem=rsem, device_id={"row": r, "col": c}, device_id_type=MESH)

    def loop(lo_, hi_, f):
        def body(i, carry):
            f(i)
            return carry

        lax.fori_loop(lo_, hi_, body, 0)

    barrier = pltpu.get_barrier_semaphore()

    def greet(i):
        d = lax.rem(me + i, n)
        pl.semaphore_signal(barrier, inc=1, device_id={"row": d // n_col, "col": lax.rem(d, n_col)}, device_id_type=MESH)

    with sc("barrier"):
        loop(1, n, greet)
        pl.semaphore_wait(barrier, n - 1)

    def piece_of(ref, d):
        return ref.at[d // 2, :, pl.ds(pl.multiple_of(lax.rem(d, 2) * tok, 128), tok)]

    def x_copy(i):
        d = lax.rem(me + i, n)
        return remote(piece_of(x_t, d), xland.at[me], xs.at[i], xr.at[i], d // n_col, lax.rem(d, n_col))

    def g_copy(i):
        d = lax.rem(me + i, n)
        return remote(gains, gland.at[me], gs.at[i], gr.at[i], d // n_col, lax.rem(d, n_col))

    own_x = pltpu.make_async_copy(piece_of(x_t, me), xland.at[me], xr.at[0])
    own_g = pltpu.make_async_copy(gains, gland.at[me], gr.at[0])
    own_x.start()
    own_g.start()
    def x_first(i):
        x_copy(i).start()
        g_copy(i).start()

    loop(1, n, x_first)

    def own_lanes(r):
        return pl.ds(pl.multiple_of(r * dr, 128), dr)

    def o_lanes(j, r):
        return pl.ds(pl.multiple_of(lax.rem(r + j, D.n_o) * och, 128), och)

    steps = []
    for l, C in enumerate(D.cfg):
        steps += [(l, "q", 0)] + [(l, "f", j) for j in range(C.n_f)] + [(l, "o", j) for j in range(D.n_o)]
    n_steps = len(steps)
    step_of = {s: t for t, s in enumerate(steps)}

    def blocks(t, i):
        l, kind, j = steps[t]
        C = D.cfg[l]
        out = []

        def w_rows(a, m):
            at = rows_at(a, m)
            out.append((w_t.at[l, at, :], lambda r: g_w.at[l, at, own_lanes(r)]))

        def o_rows(a, m):
            at = rows_at(a, m)
            out.append((w_o.at[l, at, o_lanes(j, row)], lambda r: g_wo.at[l, r, at, o_lanes(j, r)]))

        def kv_rows(a, m):
            at = pl.ds(a, m)
            out.append((wkv_t.at[l, at, :], lambda r: g_kv.at[l, at, own_lanes(r)]))

        if kind == "q":
            for a in (0, C.q // 2):
                w_rows(i * C.q + a, C.q // 2)
            for a in (0, D.kvp // 2):
                kv_rows(a, D.kvp // 2)
        elif kind == "f":
            w_rows(D.q + i * C.f + j * fch, fch)
            w_rows(D.q + D.f + i * C.f + j * fch, fch)
        elif C.split:
            o_rows(i * C.q, C.q)
            o_rows(D.q + i * C.f, C.f)
        else:
            for a in (0, (D.q + D.f) // 2):
                o_rows(a, (D.q + D.f) // 2)
        return out

    base, n_sems = [], 0
    for l, kind, j in steps:
        base.append(n_sems)
        n_sems += 12 if kind == "q" else 6
    assert n_sems == ys.shape[0]
    y_sent = []

    def y_copy(t, i, kind, src, dst, r):
        at = base[t] + 3 * i + kind
        return remote(src, dst, ys.at[at], yr.at[at], r, col)

    def y_send(*args):
        c = y_copy(*args)
        c.start()
        y_sent.append(c)

    def issue_peer(t):
        for i, (src, place) in enumerate(blocks(t, half if D.cfg[steps[t][0]].split else 0)):
            y_send(t, i, 0, src, place(row), peer)

    def issue_mate(t):
        for i, (src, place) in enumerate(blocks(t, 1 - half if D.cfg[steps[t][0]].split else 0)):
            y_send(t, i, 1, src, place(row), mate)

    def relay(t):
        split = D.cfg[steps[t][0]].split
        with sc(f"relay{t}"):
            for i, (src, place) in enumerate(blocks(t, half if split else 0)):
                y_copy(t, i, 1, src, place(mate), mate).wait_recv()
                if split or i % 2 == 0:
                    y_send(t, i, 2, place(mate), place(mate), peer)
                if not split:
                    y_copy(t, i, 0, src, place(peer), peer).wait_recv()
                    if i % 2 == 1:
                        y_send(t, i, 2, place(peer), place(peer), mate)

    at = {"next": 0, "peer": 0, "mate": 0, "relay": 0}
    first_of = {l: min(t for t, st in enumerate(steps) if st[0] == l) for l in range(D.layers)}

    def step(l, j):
        return min(first_of[l] + j, first_of.get(l + 1, n_steps) - 1)

    def peer_to(t):
        while at["peer"] <= t:
            issue_peer(at["peer"])
            at["peer"] += 1

    def mate_to(t):
        while at["mate"] <= t:
            issue_mate(at["mate"])
            at["mate"] += 1

    def relay_to(t):
        assert t < at["peer"] and t < at["mate"]
        while at["relay"] <= t:
            relay(at["relay"])
            at["relay"] += 1

    def advance():
        t = at["next"]
        assert t < at["relay"], t
        rest = n_row - 1 - peer
        with sc(f"adv{t}"):
            split = D.cfg[steps[t][0]].split
            for i, (src, place) in enumerate(blocks(t, half if split else 0)):
                if split:
                    y_copy(t, i, 0, src, place(peer), peer).wait_recv()
                y_copy(t, i, 2, src, place(rest), rest).wait_recv()
            at["next"] = t + 1

    def have(*which):
        while at["next"] <= step_of[which]:
            advance()

    mate_to(1)
    peer_to(step(0, 3))

    def w_fetch(l, kind, j, slot):
        C = D.cfg[l]
        i = half if C.split else 0
        copies = []

        def fetch(src, dst):
            copies.append(pltpu.make_async_copy(src, dst, lw.at[slot, len(copies)]))

        def w_rows(a, m, at):
            a, at = rows_at(a, m), pl.ds(at, m)
            fetch(w_t.at[l, a, :], wbuf.at[slot, at, own_lanes(row)])
            for r in (up, down, across):
                fetch(g_w.at[l, a, own_lanes(r)], wbuf.at[slot, at, own_lanes(r)])

        if kind == "q":
            w_rows(i * C.q, C.q, 0)
            at = pl.ds(C.q, D.kvp)
            fetch(wkv_t.at[l], wbuf.at[slot, at, own_lanes(row)])
            for r in (up, down, across):
                fetch(g_kv.at[l, :, own_lanes(r)], wbuf.at[slot, at, own_lanes(r)])
        else:
            w_rows(D.q + i * C.f + j * C.cw, C.cw, 0)
            w_rows(D.q + D.f + i * C.f + j * C.cw, C.cw, C.cw)
        return copies

    def o_fetch(l, j, slot):
        C = D.cfg[l]
        copies = []

        def fetch(src, dst):
            copies.append(pltpu.make_async_copy(src, dst, lo.at[slot, len(copies)]))

        spans = ((half * C.q, 0, C.q), (D.q + half * C.f, C.q, C.f)) if C.split else ((0, 0, C.q + C.f),)
        for a, at, m in spans:
            a, at = rows_at(a, m), pl.ds(at, m)
            to = lambda r: pl.ds(pl.multiple_of(r * och, 128), och)
            fetch(w_o.at[l, a, o_lanes(j, row)], wonat.at[slot, at, to(row)])
            for r in (up, down, across):
                fetch(g_wo.at[l, r, a, o_lanes(j, r)], wonat.at[slot, at, to(r)])
        return copies

    def start(copies):
        for c in copies:
            c.start()

    def wait(copies):
        for c in copies:
            c.wait()

    own_x.wait()
    own_g.wait()

    def x_finish(i):
        s = lax.rem(me + n - i, n)
        remote(xland.at[s], xland.at[s], xs.at[i], xr.at[i], row, col).wait_recv()
        remote(gland.at[s], gland.at[s], gs.at[i], gr.at[i], row, col).wait_recv()
        x_copy(i).wait_send()
        g_copy(i).wait_send()

    with sc("xwait"):
        loop(1, n, x_finish)

    def keep(d):
        hid[rows_at(d * dl, dl), :] = xland[d]

    with sc("gains"):
        loop(0, n, keep)
        g_all = gland[...].astype(F32)
        for l in range(D.layers):
            g_rows = g_all[:, l, :]
            g_rows = jnp.concatenate([g_rows, jnp.zeros((128 - n, 128), F32)], axis=0) if n < 128 else g_rows
            g_cols = g_rows.T
            for d in range(n):
                gcol[l, d * dl : (d + 1) * dl, :] = jnp.broadcast_to(g_cols[:dl, d : d + 1], (dl, 128))

    blk = 64
    n_blk = D.d // blk

    def layer_norm(l):
        def add_up(i, acc):
            v = hid[rows_at(i * blk, blk), :].astype(F32)
            return acc + v.reshape(blk // 8, 8, tok).sum(axis=0)

        mean = lax.fori_loop(0, n_blk, add_up, jnp.zeros((8, tok), F32)).sum(axis=0, keepdims=True) / D.d

        def add_sq(i, acc):
            v = hid[rows_at(i * blk, blk), :].astype(F32) - mean
            return acc + (v * v).reshape(blk // 8, 8, tok).sum(axis=0)

        var = lax.fori_loop(0, n_blk, add_sq, jnp.zeros((8, tok), F32)).sum(axis=0, keepdims=True) / D.d
        scale = lax.rsqrt(var + LN_EPS)

        def write(i):
            rows = rows_at(i * blk, blk)
            g = gcol[l, rows, :]
            g = jnp.concatenate([g] * (tok // 128), axis=1)
            v = (hid[rows, :].astype(F32) - mean) * scale * g
            ht[x, rows, my_lanes] = v.astype(BF16)

        with sc(f"norm{l}"):
            loop(0, n_blk, write)

    d_low, d_high = pl.ds(0, D.d // 2), pl.ds(D.d // 2, D.d // 2)

    class Gather:
        def __init__(self, ref, tag):
            self.ref, self.tag, self.sends = ref, tag, []
            for i, c in ((0, right), (1, left), (2, twin)):
                self.send(i, ref(x, False, None), c)

        def send(self, i, ref, c):
            copy = remote(ref, ref, ags.at[self.tag, i], agr.at[self.tag, i], row, c)
            copy.start()
            self.sends.append(copy)

        def arrived(self, i, ref):
            remote(ref, ref, ags.at[self.tag, i], agr.at[self.tag, i], row, col).wait_recv()

        def pass_on(self):
            with sc(f"pass_on{self.tag}"):
                self.arrived(0, self.ref(xl_, False, None))
                self.send(3, self.ref(xl_, False, 0), right)
                self.send(4, self.ref(xl_, False, None), twin)
                self.arrived(1, self.ref(xr_, False, None))
                self.send(5, self.ref(xr_, False, 1), left)
                self.send(6, self.ref(xr_, False, None), twin)

        def own(self):
            self.arrived(2, self.ref(x, True, None))

        def near(self):
            with sc(f"near{self.tag}"):
                self.arrived(4, self.ref(xl_, True, None))
                self.arrived(6, self.ref(xr_, True, None))

        def pass_far(self):
            with sc(f"pass_far{self.tag}"):
                for part, i, j in ((0, 3, 7), (1, 5, 8)):
                    self.arrived(i, self.ref(xf_, False, part))
                    self.send(j, self.ref(xf_, False, part), twin)

        def far(self):
            with sc(f"far{self.tag}"):
                self.arrived(7, self.ref(xf_, True, 0))
                self.arrived(8, self.ref(xf_, True, 1))

        def finish(self):
            for c in self.sends:
                c.wait_send()

    def normed_of(buf):
        def ref(chip, other, part):
            rows = slice(None) if part is None else (d_low, d_high)[part]
            return buf.at[chip, rows, twin_lanes if other else my_lanes]

        return ref

    def kv_of(a):
        def ref(chip, other, part):
            h = D.seqs // 2
            span = pl.ds(a * D.seqs, D.seqs) if part is None else pl.ds(a * D.seqs + part * h, h)
            return kvland.at[chip * 2 + (1 - k if other else k), span]

        return ref

    half_dim = D.hd // 2

    def near3(i):
        return lax.rem(x + i + i // 2, n_x)

    def all4(i):
        return i

    def far1(i):
        return xf_

    def rope(p):
        lo_, hi_ = p[:half_dim], p[half_dim:]
        return jnp.concatenate([lo_ * cos_ref[...] - hi_ * sin_ref[...], hi_ * cos_ref[...] + lo_ * sin_ref[...]], axis=0)

    def project_q(l, a, seq_of, count):
        C = D.cfg[l]

        def body(i):
            s = seq_of(i)
            p = dot(wbuf[1, : C.q + D.kvp, :], ht[s]).astype(BF16).astype(F32)
            for h in range(C.heads):
                at = rows_at((a * D.seqs + s) * C.q + h * D.hd, D.hd)
                qt[at, :] = (rope(p[h * D.hd : (h + 1) * D.hd]) * D.hd**-0.5).astype(BF16)
            kvland[col, a * D.seqs + s] = p[C.q :].astype(BF16)

        with sc(f"q{l}{a}"):
            loop(0, count, body)

    def kv_copy(s, j, source):
        ref = kvland.at[source, s]
        return remote(ref, ref, kvs.at[s, j], kvr.at[s, j], row, lax.rem(col + j, n_col))

    def kv_send(seq_of, count):
        def body(i):
            s = seq_of(i)
            loop(1, n_col, lambda j: kv_copy(s, j, col).start())

        loop(0, count, body)

    def kv_arrive():
        def body(i):
            j = i // D.seqs + 1
            s = lax.rem(i, D.seqs)
            kv_copy(s, j, lax.rem(col + n_col - j, n_col)).wait_recv()
            kv_copy(s, j, col).wait_send()

        with sc("kvwait"):
            loop(0, D.seqs * (n_col - 1), body)

    def key_value(l, a):
        def body(i):
            s = a * D.seqs + i
            raw = kvland[:, s].reshape(n_col * D.kvp, D.seq)
            both = dot(perm_ref[...], raw)
            zeros = jnp.zeros((128 - D.hd, D.seq), F32)
            k_nat = jnp.concatenate([rope(both[: D.hd]), zeros], axis=0).T.astype(BF16)
            kn[s] = k_nat
            vt[s] = both[D.hd :].astype(BF16)
            if a == 0:
                kvbuf[l, 0, i] = k_nat
                kvbuf[l, 1, i] = jnp.concatenate([both[D.hd :], zeros], axis=0).T.astype(BF16)

        with sc(f"kv{l}{a}"):
            loop(0, D.seqs, body)

    qb = D.seq // 2

    def attention(l, a):
        C = D.cfg[l]

        pair = 2
        per = C.heads // pair

        def body(i):
            s, h0 = a * D.seqs + i // per, lax.rem(i, per) * pair
            q_rows = [rows_at(s * C.q + (h0 + e) * D.hd, D.hd) for e in range(pair)]
            o_rows = [rows_at(s * (C.q + C.f) + (h0 + e) * D.hd, D.hd) for e in range(pair)]
            for b in range(2):
                ext = (b + 1) * qb
                lanes = slice(b * qb, (b + 1) * qb)
                keys = lax.broadcasted_iota(jnp.int32, (ext, qb), 0)
                queries = lax.broadcasted_iota(jnp.int32, (ext, qb), 1) + b * qb
                scores = [dot(kn[s, :ext, : D.hd], qt[q_rows[e], lanes]) for e in range(pair)]
                for e in range(pair):
                    score = jnp.where(keys <= queries, scores[e], -1e30)
                    p = jnp.exp(score - jnp.max(score, axis=0, keepdims=True))
                    p = (p * (1.0 / jnp.sum(p, axis=0, keepdims=True))).astype(BF16)
                    jt[o_rows[e], lanes] = dot(vt[s, :, :ext], p).astype(BF16)

        with sc(f"attn{l}{a}"):
            loop(0, D.seqs * per, body)

    def gate_up(l, a, slot, j, seq_of, count):
        C = D.cfg[l]

        def body(i):
            s = seq_of(i)
            p = dot(wbuf[slot, : 2 * C.cw, :], ht[s])
            g = p[: C.cw].astype(BF16).astype(F32)
            u = p[C.cw :].astype(BF16).astype(F32)
            jt[rows_at((a * D.seqs + s) * (C.q + C.f) + C.q + j * C.cw, C.cw), :] = (g * jax.nn.sigmoid(g) * u).astype(BF16)

        loop(0, count, body)

    def gate_up_loop(l, a, seq_of, count, first, last, stop=None):
        C = D.cfg[l]
        stop = C.n_c if stop is None else stop
        have_chunk(l, min(last, stop - 1))

        def body(j):
            slot = lax.rem(j, 2)
            wait(w_fetch(l, "f", j, slot))

            @pl.when(j + 1 < stop)
            def _():
                start(w_fetch(l, "f", j + 1, 1 - slot))

            gate_up(l, a, slot, j, seq_of, count)

        with sc(f"gu{l}{a}"):
            loop(first, last, body)

    def have_chunk(l, j):
        C = D.cfg[l]
        have(l, "f", (j + 1) * C.cw // fch - 1)

    def load_q(l):
        have(l, "q", 0)
        copies = w_fetch(l, "q", 0, 1)
        start(copies)
        wait(copies)

    m = och * n_row
    m_low, m_high = pl.ds(0, m // 2), pl.ds(m // 2, m // 2)
    r_slots = twin_in.shape[0]
    r_step = 64

    def order(i):
        return lax.rem(x + lax.rem(2 + 3 * i, 4), n_x)

    class Reduce:
        def __init__(self, l):
            self.l, self.C, self.sends = l, D.cfg[l], {}

        def send(self, u, i, src, dst, c):
            copy = remote(src, dst, rss.at[u % r_slots, i], rsr.at[u % r_slots, i], row, c)
            copy.start()
            self.sends[u].append(copy)

        def arrived(self, u, i, ref):
            remote(ref, ref, rss.at[u % r_slots, i], rsr.at[u % r_slots, i], row, col).wait_recv()

        def twin_copy(self, u, i):
            us = u % r_slots
            return remote(ot.at[u % 2, order(i), :, twin_lanes], twin_in.at[us, i], rss.at[us, i], rsr.at[us, i], row, twin)

        def twin_done(self, u):
            loop(0, 4, lambda i: self.twin_copy(u, i).wait_send())

        def stage_a(self, u, a):
            C = self.C
            if u >= 2:
                self.twin_done(u - 2)
            if u >= r_slots - 1:
                for c in self.sends.pop(u - r_slots + 1):
                    c.wait_send()
            self.sends[u] = []
            R = C.q + C.f

            def body(i):
                s = order(i)
                ot[u % 2, s] = dot(wobuf[:, :R], jt[rows_at((a * D.seqs + s) * R, R), :]).astype(BF16)
                self.twin_copy(u, i).start()

            with sc(f"sa{self.l}_{u}"):
                loop(0, 4, body)

        def stage_b(self, u):
            us = u % r_slots

            def body(i):
                self.arrived(u, i, twin_in.at[us, i])
                s = order(i)

                def add(b):
                    at = rows_at(b * r_step, r_step)
                    twin_in[us, i, at, :] = (ot[u % 2, s, at, my_lanes].astype(F32) + twin_in[us, i, at, :].astype(F32)).astype(BF16)

                loop(0, m // r_step, add)

            far = [
                remote(twin_in.at[us, 0, m_low], far_in.at[us, m_low], rss.at[us, 4], rsr.at[us, 4], row, right),
                remote(twin_in.at[us, 0, m_high], far_in.at[us, m_high], rss.at[us, 5], rsr.at[us, 5], row, left),
            ]
            self.sends[u] += far

            def each(i):
                body(i)

                @pl.when(i == 0)
                def _():
                    start(far)

            with sc(f"sb{self.l}_{u}"):
                loop(0, 4, each)

        def stage_c(self, u):
            us = u % r_slots

            def add_far(i, base):
                def add(b):
                    at = rows_at(base + b * r_step, r_step)
                    twin_in[us, i, at, :] = (twin_in[us, i, at, :].astype(F32) + far_in[us, at, :].astype(F32)).astype(BF16)

                loop(0, m // 2 // r_step, add)

            with sc(f"sc{self.l}_{u}"):
                self.arrived(u, 4, far_in.at[us, m_low])
                add_far(1, 0)
                self.send(u, 6, twin_in.at[us, 1], near_in.at[us, 0], right)
                self.arrived(u, 5, far_in.at[us, m_high])
                add_far(3, m // 2)
                self.send(u, 7, twin_in.at[us, 3], near_in.at[us, 1], left)

        def add_update(self, j, total):
            step = min(r_step, och)
            for r in range(n_row):

                def add(b, r=r):
                    dst = rows_at(r * dr + (r + j) % D.n_o * och + b * step, step)
                    u = total(rows_at(r * och + b * step, step)).astype(BF16).astype(F32)
                    hid[dst, :] = (hid[dst, :].astype(F32) + u).astype(BF16)

                loop(0, och // step, add)

        def stage_d(self, u, j, a):
            us = u % r_slots

            def total(at):
                return twin_in[us, 2, at, :].astype(F32) + near_in[us, 0, at, :].astype(F32) + near_in[us, 1, at, :].astype(F32)

            with sc(f"sd{self.l}_{u}"):
                self.arrived(u, 6, near_in.at[us, 0])
                self.arrived(u, 7, near_in.at[us, 1])
                if self.C.split:

                    def save(b):
                        at = rows_at(b * r_step, r_step)
                        psum[a, j, at, :] = total(at).astype(BF16)

                    loop(0, m // r_step, save)
                    if a == 1:
                        remote(psum.at[1, j], pair_in.at[j], es.at[j], er.at[j], mate, col).start()
                else:
                    self.add_update(j, total)

        def stage_e(self, j):
            with sc(f"se{self.l}_{j}"):
                c = remote(psum.at[1, j], pair_in.at[j], es.at[j], er.at[j], mate, col)
                c.wait_recv()
                self.add_update(j, lambda at: psum[0, j, at, :].astype(F32) + pair_in[j, at, :].astype(F32))
                c.wait_send()

        def finish(self, units):
            with sc(f"rfin{self.l}"):
                for u in range(max(0, units - 2), units):
                    self.twin_done(u)
                for u in self.sends:
                    for c in self.sends[u]:
                        c.wait_send()

    o_started = set()

    def o_load(l, j, a):
        if (l, j, a) not in o_started:
            have(l, "o", j)
            start(o_fetch(l, j, j % 2))
            o_started.add((l, j, a))

    def o_use(l, j, a):
        C = D.cfg[l]
        with sc(f"ouse{l}_{j}"):
            o_load(l, j, a)
            wait(o_fetch(l, j, j % 2))
            R = C.q + C.f
            for r in range(n_row):
                wobuf[r * och : (r + 1) * och, :R] = wonat[j % 2, :R, r * och : (r + 1) * och].T

    layer_norm(0)
    g0 = Gather(normed_of(ht), 0)
    mine = ht.at[x, :, my_lanes]
    shared = g_h.at[x, :, my_lanes]
    to_mate = remote(mine, shared, ps, pr_, mate, col)
    to_mate.start()
    relay_to(1)
    mate_to(step(0, 5))
    peer_to(step(0, 5))
    g0.pass_on()
    with sc("mate"):
        to_mate.wait_recv()
    g1 = Gather(normed_of(g_h), 1)
    load_q(0)
    g0.own()
    g0.near()
    project_q(0, 0, near3, 3)
    relay_to(2)
    mate_to(step(0, 10))
    g0.pass_far()
    g0.far()
    project_q(0, 0, far1, 1)
    kv0 = Gather(kv_of(0), 2)
    relay_to(3)
    n_f = D.cfg[0].n_f
    f_started = set()

    def f_load(j):
        if j not in f_started:
            f_started.add(j)
            start(w_fetch(0, "f", j, j % 2))

    def h_copy(i):
        return pltpu.make_async_copy(g_h.at[i], ht.at[i], lh.at[i])

    have(0, "f", 0)
    f_load(0)
    gate_up_loop(0, 0, all4, 4, 0, 2, 2)
    relay_to(step(0, 4))
    for j in range(2, n_f):
        have(0, "f", j)
        f_load(j)
        with sc(f"gu0_{j}"):
            wait(w_fetch(0, "f", j, j % 2))
            gate_up(0, 0, j % 2, j, all4, 4)
        if j == max(2, n_f - 3):
            relay_to(step(0, 5))
            peer_to(step(0, 6))
            relay_to(step(0, 6))
            peer_to(step(0, 7))
    kv0.pass_on()
    g1.pass_on()
    for t in (7, 8):
        relay_to(step(0, t))
        peer_to(step(0, t + 1))
    relay_to(step(0, 9))
    peer_to(step(0, 10))
    relay_to(step(0, 10))
    peer_to(step(1, 5))
    mate_to(step(1, D.cfg[1].n_f - 2))
    g0.finish()
    to_mate.wait_send()
    g1.own()
    g1.near()
    loop(0, 3, lambda i: h_copy(near3(i)).start())
    kv0.pass_far()
    with sc("kv0wait"):
        kv0.own()
        kv0.near()
        kv0.far()
        kv0.finish()
    key_value(0, 0)
    attention(0, 0)

    red = Reduce(0)
    units = [(j, 0) for j in range(D.n_o - 1)] + [(j, 1) for j in range(D.n_o)] + [(D.n_o - 1, 0)]
    n_u = len(units)
    first = D.n_o - 1
    state = {"e": 0}

    def settle(count):
        while state["e"] < count:
            red.stage_e(state["e"])
            state["e"] += 1

    def unit(u):
        j, a = units[u]
        if u == 0 or units[u - 1][0] != j:
            o_use(0, j, a)
        red.stage_a(u, a)
        if u + 1 < n_u and units[u + 1][0] != j:
            o_load(0, *units[u + 1])
        if u >= 2:
            red.stage_c(u - 2)
        if u >= 3:
            red.stage_d(u - 3, *units[u - 3])
        red.stage_b(u)

    unit(0)
    g1.pass_far()
    unit(1)
    g1.far()
    h_copy(xf_).start()
    load_q(0)
    start(w_fetch(0, "f", 0, 0))
    loop(0, 3, lambda i: h_copy(near3(i)).wait())
    h_copy(xf_).wait()
    project_q(0, 1, all4, 4)
    kv1 = Gather(kv_of(1), 3)
    parts = first - 2
    cuts = [n_f * i // parts for i in range(parts + 1)]
    for u in range(2, first):
        unit(u)
        if u == 2:
            kv1.pass_on()
        gate_up_loop(0, 1, all4, 4, cuts[u - 2], cuts[u - 1])
    kv1.pass_far()
    relay_to(step(1, 1))
    with sc("kv1wait"):
        kv1.own()
        kv1.near()
        kv1.far()
        kv1.finish()
    key_value(0, 1)
    attention(0, 1)
    g1.finish()
    relay_to(step(1, 2))
    peer_to(step(1, 7))
    n_f1 = D.cfg[1].n_f
    for u in range(first, n_u):
        unit(u)
        v = u - first
        if v in (0, 1, 2):
            relay_to(step(1, min(v + 3, n_f1 - 2)))
        if v == 1:
            peer_to(step(1, min(8, n_f1)))
        elif v == 4:
            relay_to(step(1, min(6, n_f1 - 2)))
            peer_to(step(1, min(9, n_f1)))
        elif v == 5:
            peer_to(step(1, n_f1))
    relay_to(step(1, min(6, n_f1 - 2)))
    peer_to(step(1, n_f1))
    red.stage_c(n_u - 2)
    red.stage_d(n_u - 3, *units[n_u - 3])
    red.stage_c(n_u - 1)
    red.stage_d(n_u - 2, *units[n_u - 2])
    mate_to(step(1, n_f1))
    settle(D.n_o - 1)
    red.stage_d(n_u - 1, *units[n_u - 1])
    settle(D.n_o)
    red.finish(n_u)

    def slice_of(d):
        return hid.at[rows_at(d * dl, dl), :]

    own_y = pltpu.make_async_copy(slice_of(me), piece_of(y_out, me), xr.at[0])

    def y_copy_back(i):
        d = lax.rem(me + i, n)
        return remote(slice_of(d), piece_of(y_out, me), xs.at[i], xr.at[i], d // n_col, lax.rem(d, n_col))

    def y_send_back(i):
        @pl.when(i == 0)
        def _():
            own_y.start()

        @pl.when(i != 0)
        def _():
            y_copy_back(i).start()

    def y_finish(i):
        s = lax.rem(me + n - i, n)
        remote(piece_of(y_out, s), piece_of(y_out, s), xs.at[i], xr.at[i], row, col).wait_recv()
        y_copy_back(i).wait_send()

    def y_ready(low, high):
        def body(i):
            d = lax.rem(me + i, n)
            r, a = d // n_col, lax.rem(d, n_col) * dl
            first = lax.rem(a // och + D.n_o - lax.rem(r, D.n_o), D.n_o)
            second = lax.rem((a + dl - 1) // och + D.n_o - lax.rem(r, D.n_o), D.n_o)

            done = jnp.maximum(first, second)

            @pl.when((low <= done) & (done < high))
            def _():
                y_send_back(i)

        loop(0, n, body)

    for l in range(1, D.layers):
        C = D.cfg[l]
        layer_norm(l)
        g0 = Gather(normed_of(ht), 0)
        peer_to(step(l, C.n_f))
        mate_to(step(l, C.n_f))
        relay_to(step(l, min(8, C.n_f)))
        own1, near2 = (lambda i: x), (lambda i: lax.rem(x + 1 + 2 * i, n_x))
        n_mid = min(3, C.n_c - 1)

        def begin(seq_of, count):
            load_q(l)
            have_chunk(l, 0)
            start(w_fetch(l, "f", 0, 0))
            project_q(l, 0, seq_of, count)

        g0.own()
        begin(own1, 1)
        kv_send(own1, 1)
        gate_up_loop(l, 0, own1, 1, 0, n_mid, n_mid)
        relay_to(step(l, C.n_f))
        peer_to(step(l, C.n_f + 2))
        mate_to(step(l, C.n_f + 2))
        g0.pass_on()
        g0.near()
        begin(near2, 2)
        kv_send(near2, 2)
        gate_up_loop(l, 0, near2, 2, 0, n_mid)
        g0.pass_far()
        relay_to(step(l, C.n_f + 1))
        peer_to(step(l, C.n_f + 4))
        mate_to(step(l, C.n_f + 4))
        gate_up_loop(l, 0, near3, 3, n_mid, C.n_c)
        relay_to(step(l, C.n_f + 2))
        g0.far()
        begin(far1, 1)
        kv_send(far1, 1)
        gate_up_loop(l, 0, far1, 1, 0, C.n_c)
        peer_to(step(l, C.n_f + D.n_o))
        mate_to(step(l, C.n_f + D.n_o))
        relay_to(step(l, C.n_f + 3))
        g0.finish()
        kv_arrive()
        key_value(l, 0)
        attention(l, 0)
        relay_to(step(l, C.n_f + 4))
        red = Reduce(l)
        last = l + 1 == D.layers

        end = D.n_o - 1
        for j in range(D.n_o):
            o_use(l, j, 0)
            red.stage_a(j, 0)
            if j == 0:
                relay_to(step(l, C.n_f + D.n_o))
            if j < end:
                o_load(l, j + 1, 0)
            if 2 <= j:
                red.stage_c(j - 2)
            if 3 <= j:
                red.stage_d(j - 3, j - 3, 0)
            red.stage_b(j)
        red.stage_c(end - 1)
        red.stage_d(end - 2, end - 2, 0)
        red.stage_c(end)
        red.stage_d(end - 1, end - 1, 0)
        if last:
            with sc("send"):
                y_ready(0, end)
        red.stage_d(end, end, 0)
        if last:
            y_ready(end, end + 1)
        red.finish(D.n_o)

    def kv_back(i):
        r = lax.rem(row + i, n_row)
        pos = rows_at((r * n_col + col) * D.pos, D.pos)
        return kvbuf.at[:, :, :, pos, :], kv_out.at[:, :, pl.ds(row * D.seqs, D.seqs)], r

    src, dst, _ = kv_back(0)
    own_kv = pltpu.make_async_copy(src, dst, fl)
    own_kv.start()
    kv_sends = []
    for i in range(1, n_row):
        src, dst, r = kv_back(i)
        c = remote(src, dst, fs.at[i], fr.at[i], r, col)
        c.start()
        kv_sends.append(c)

    with sc("ywait"):
        loop(1, n, y_finish)
        own_y.wait()
        own_kv.wait()
        for i in range(1, n_row):
            r = lax.rem(row + n_row - i, n_row)
            dst = kv_out.at[:, :, pl.ds(r * D.seqs, D.seqs)]
            remote(dst, dst, fs.at[i], fr.at[i], row, col).wait_recv()
        for c in kv_sends:
            c.wait_send()
        for c in y_sent:
            c.wait_send()


def solution(mesh):
    n_row, n_col = mesh.shape["row"], mesh.shape["col"]
    group = n_row * n_col
    act_spec = P("dp", None, ("row", "col"))
    weight_spec = P(None, "row", "col")

    def device_fn(x_loc, gain_loc, w_in_loc, w_kv_loc, w_out_loc):
        D = Dims()
        D.n_row, D.n_col = n_row, n_col
        n_batch, D.seq, D.dl = x_loc.shape
        D.layers, D.dr, e = w_in_loc.shape
        D.d = D.dl * group
        r_block = w_out_loc.shape[1]
        D.f = e - r_block
        D.q = r_block - D.f
        kv_local = w_kv_loc.shape[2]
        D.hd = kv_local * n_col // 2
        D.kvp = 32
        D.tok = n_batch * D.seq // group
        D.seqs = n_batch // n_row
        D.pos = D.seq // group
        D.fch = 128
        D.och = 128
        D.n_o = D.dr // D.och
        D.cfg = []
        for l in range(D.layers):
            C = Dims()
            C.split = l == 0
            parts = 2 if C.split else 1
            C.q, C.f = D.q // parts, D.f // parts
            C.heads, C.n_f = C.q // D.hd, C.f // D.fch
            C.cw = D.fch if C.split else 2 * D.fch
            C.n_c = C.f // C.cw
            D.cfg.append(C)
        assert D.seq == 2 * D.tok and D.seqs == n_col // 2 == n_row == 4

        half = D.hd // 2
        inv_freq = (np.float32(1.0) / (np.float32(10000.0) ** (np.arange(half, dtype=np.float32) * np.float32(2.0) / np.float32(D.hd)))).astype(np.float32)
        angles = (inv_freq[:, None] * np.arange(D.seq, dtype=np.float32)[None, :]).astype(np.float32)
        cos_t, sin_t = np.cos(angles).astype(np.float32), np.sin(angles).astype(np.float32)
        perm = np.zeros((2 * D.hd, n_col * D.kvp), np.float32)
        for i in range(2 * D.hd):
            perm[i, (i // kv_local) * D.kvp + i % kv_local] = 1.0

        x_t = x_loc.transpose(0, 2, 1)
        w_t = w_in_loc.transpose(0, 2, 1)
        wkv_t = jnp.pad(w_kv_loc.transpose(0, 2, 1), ((0, 0), (0, D.kvp - kv_local), (0, 0)))
        gains = jnp.pad(gain_loc, ((0, 16 - D.layers), (0, 128 - D.dl)))

        n_y = sum(12 + 6 * (C.n_f + D.n_o) for C in D.cfg)
        m = D.och * n_row
        sds = jax.ShapeDtypeStruct
        dma = pltpu.SemaphoreType.DMA
        out = pl.pallas_call(
            functools.partial(kernel, D),
            out_shape=(
                sds(x_t.shape, BF16),
                sds((D.layers, 2, n_batch, D.pos, 128), BF16),
                sds((D.layers, e, D.d), BF16),
                sds((D.layers, D.kvp, D.d), BF16),
                sds((D.layers, n_row, r_block, D.dr), BF16),
                sds((D.seqs, D.d, D.seq), BF16),
            ),
            in_specs=[ANY] * 5 + [VMEM] * 3,
            out_specs=(ANY,) * 6,
            scratch_shapes=[
                pltpu.VMEM((group, D.dl, D.tok), BF16),
                pltpu.VMEM((group, 16, 128), BF16),
                pltpu.VMEM((D.layers, D.d, 128), F32),
                pltpu.VMEM((D.d, D.tok), BF16),
                pltpu.VMEM((D.seqs, D.d, D.seq), BF16),
                pltpu.VMEM((2, max(4 * D.fch, D.q + D.kvp), D.d), BF16),
                pltpu.VMEM((2, r_block, m), BF16),
                pltpu.VMEM((m, r_block), BF16),
                pltpu.VMEM((D.seqs * D.q, D.seq), BF16),
                pltpu.VMEM((n_col, 2 * D.seqs, D.kvp, D.seq), BF16),
                pltpu.VMEM((2 * D.seqs, D.seq, 128), BF16),
                pltpu.VMEM((2 * D.seqs, D.hd, D.seq), BF16),
                pltpu.VMEM((D.layers, 2, D.seqs, D.seq, 128), BF16),
                pltpu.VMEM((D.seqs * r_block, D.seq), BF16),
                pltpu.VMEM((2, D.seqs, m, D.seq), BF16),
                pltpu.VMEM((5, 4, m, D.tok), BF16),
                pltpu.VMEM((5, m, D.tok), BF16),
                pltpu.VMEM((5, 2, m, D.tok), BF16),
                pltpu.VMEM((2, D.n_o, m, D.tok), BF16),
                pltpu.VMEM((D.n_o, m, D.tok), BF16),
                dma((group,)), dma((group,)), dma((group,)), dma((group,)),
                dma((n_y,)), dma((n_y,)),
                dma((4, 9)), dma((4, 9)), dma, dma,
                dma((D.seqs, n_col)), dma((D.seqs, n_col)),
                dma((5, 8)), dma((5, 8)),
                dma((D.n_o,)), dma((D.n_o,)),
                dma((2, 8)), dma((2, 8)), dma((D.seqs,)),
                dma((n_row,)), dma((n_row,)), dma,
            ],
            compiler_params=pltpu.CompilerParams(collective_id=0, has_side_effects=True, vmem_limit_bytes=67_000_000),
            name="two_layers",
        )(x_t, gains, w_t, wkv_t, w_out_loc, jnp.asarray(cos_t), jnp.asarray(sin_t), jnp.asarray(perm, BF16))
        return out[0].transpose(0, 2, 1), out[1][..., : D.hd]

    return jax.shard_map(device_fn, mesh=mesh, in_specs=(act_spec, P(None, ("row", "col")), weight_spec, weight_spec, P(None, "col", "row")), out_specs=(act_spec, P(None, None, "dp", ("row", "col"), None)), check_vma=False)
```

```python
import functools

import numpy as np

import jax
import jax.numpy as jnp
from jax import lax
from jax.experimental import pallas as pl
from jax.experimental.pallas import tpu as pltpu
from jax.sharding import PartitionSpec as P

LN_EPS = 1e-6
MESH = pl.DeviceIdType.MESH
ANY = pl.BlockSpec(memory_space=pl.ANY)
VMEM = pl.BlockSpec(memory_space=pltpu.VMEM)
F32, BF16 = jnp.float32, jnp.bfloat16


def dot(a, b):
    return jnp.dot(a, b, preferred_element_type=F32)


class Dims:
    pass


def rows_at(start, count, by=16):
    return pl.ds(start if isinstance(start, int) else pl.multiple_of(start, by), count)


def kernel(
    D,
    x_t, gains, w_t, wkv_t, w_o, cos_ref, sin_ref, perm_ref,
    y_out, kv_out, g_w, g_kv, g_wo, g_h,
    xland, gland, gcol, hid, ht, wbuf, wonat, wobuf, qt, kvland, kn, vt, kvbuf, jt, ot, twin_in, far_in, near_in, psum, pair_in,
    xs, xr, gs, gr, ys, yr, ags, agr, ps, pr_, kvs, kvr, rss, rsr, es, er, lw, lo, lh, fs, fr, fl,
):
    sc = jax.named_scope
    row, col = lax.axis_index("row"), lax.axis_index("col")
    n_row, n_col, n = D.n_row, D.n_col, D.n_row * D.n_col
    n_x = n_col // 2
    me = row * n_col + col
    x, k = col // 2, lax.rem(col, 2)
    xr_, xl_, xf_ = lax.rem(x + 1, n_x), lax.rem(x + n_x - 1, n_x), lax.rem(x + 2, n_x)
    right, left, twin = xr_ * 2 + k, xl_ * 2 + k, x * 2 + 1 - k
    up, down, across = lax.rem(row + 1, n_row), lax.rem(row + n_row - 1, n_row), lax.rem(row + 2, n_row)
    half, mate = row // 2, n_row - 1 - row
    peer = row + 1 - 2 * lax.rem(row, 2)
    tok, dl, dr = D.tok, D.dl, D.dr
    och, fch = D.och, D.fch
    my_lanes = pl.ds(pl.multiple_of(k * tok, 128), tok)
    twin_lanes = pl.ds(pl.multiple_of((1 - k) * tok, 128), tok)

    def remote(src, dst, ssem, rsem, r, c):
        return pltpu.make_async_remote_copy(src_ref=src, dst_ref=dst, send_sem=ssem, recv_sem=rsem, device_id={"row": r, "col": c}, device_id_type=MESH)

    def loop(lo_, hi_, f):
        def body(i, carry):
            f(i)
            return carry

        lax.fori_loop(lo_, hi_, body, 0)

    barrier = pltpu.get_barrier_semaphore()

    def greet(i):
        d = lax.rem(me + i, n)
        pl.semaphore_signal(barrier, inc=1, device_id={"row": d // n_col, "col": lax.rem(d, n_col)}, device_id_type=MESH)

    with sc("barrier"):
        loop(1, n, greet)
        pl.semaphore_wait(barrier, n - 1)

    def piece_of(ref, d):
        return ref.at[d // 2, :, pl.ds(pl.multiple_of(lax.rem(d, 2) * tok, 128), tok)]

    def x_copy(i):
        d = lax.rem(me + i, n)
        return remote(piece_of(x_t, d), xland.at[me], xs.at[i], xr.at[i], d // n_col, lax.rem(d, n_col))

    def g_copy(i):
        d = lax.rem(me + i, n)
        return remote(gains, gland.at[me], gs.at[i], gr.at[i], d // n_col, lax.rem(d, n_col))

    own_x = pltpu.make_async_copy(piece_of(x_t, me), xland.at[me], xr.at[0])
    own_g = pltpu.make_async_copy(gains, gland.at[me], gr.at[0])
    own_x.start()
    own_g.start()
    def x_first(i):
        x_copy(i).start()
        g_copy(i).start()

    loop(1, n, x_first)

    def own_lanes(r):
        return pl.ds(pl.multiple_of(r * dr, 128), dr)

    def o_lanes(j, r):
        return pl.ds(pl.multiple_of(lax.rem(r + j, D.n_o) * och, 128), och)

    steps = []
    for l, C in enumerate(D.cfg):
        steps += [(l, "q", 0)] + [(l, "f", j) for j in range(C.n_f)] + [(l, "o", j) for j in range(D.n_o)]
    n_steps = len(steps)
    step_of = {s: t for t, s in enumerate(steps)}

    def blocks(t, i):
        l, kind, j = steps[t]
        C = D.cfg[l]
        out = []

        def w_rows(a, m):
            at = rows_at(a, m)
            out.append((w_t.at[l, at, :], lambda r: g_w.at[l, at, own_lanes(r)]))

        def o_rows(a, m):
            at = rows_at(a, m)
            out.append((w_o.at[l, at, o_lanes(j, row)], lambda r: g_wo.at[l, r, at, o_lanes(j, r)]))

        def kv_rows(a, m):
            at = pl.ds(a, m)
            out.append((wkv_t.at[l, at, :], lambda r: g_kv.at[l, at, own_lanes(r)]))

        if kind == "q":
            for a in (0, C.q // 2):
                w_rows(i * C.q + a, C.q // 2)
            for a in (0, D.kvp // 2):
                kv_rows(a, D.kvp // 2)
        elif kind == "f":
            w_rows(D.q + i * C.f + j * fch, fch)
            w_rows(D.q + D.f + i * C.f + j * fch, fch)
        elif C.split:
            o_rows(i * C.q, C.q)
            o_rows(D.q + i * C.f, C.f)
        else:
            for a in (0, (D.q + D.f) // 2):
                o_rows(a, (D.q + D.f) // 2)
        return out

    base, n_sems = [], 0
    for l, kind, j in steps:
        base.append(n_sems)
        n_sems += 12 if kind == "q" else 6
    assert n_sems == ys.shape[0]
    y_sent = []

    def y_copy(t, i, kind, src, dst, r):
        at = base[t] + 3 * i + kind
        return remote(src, dst, ys.at[at], yr.at[at], r, col)

    def y_send(*args):
        c = y_copy(*args)
        c.start()
        y_sent.append(c)

    def issue_peer(t):
        for i, (src, place) in enumerate(blocks(t, half if D.cfg[steps[t][0]].split else 0)):
            y_send(t, i, 0, src, place(row), peer)

    def issue_mate(t):
        for i, (src, place) in enumerate(blocks(t, 1 - half if D.cfg[steps[t][0]].split else 0)):
            y_send(t, i, 1, src, place(row), mate)

    def relay(t):
        split = D.cfg[steps[t][0]].split
        with sc(f"relay{t}"):
            for i, (src, place) in enumerate(blocks(t, half if split else 0)):
                y_copy(t, i, 1, src, place(mate), mate).wait_recv()
                if split or i % 2 == 0:
                    y_send(t, i, 2, place(mate), place(mate), peer)
                if not split:
                    y_copy(t, i, 0, src, place(peer), peer).wait_recv()
                    if i % 2 == 1:
                        y_send(t, i, 2, place(peer), place(peer), mate)

    at = {"next": 0, "peer": 0, "mate": 0, "relay": 0}
    first_of = {l: min(t for t, st in enumerate(steps) if st[0] == l) for l in range(D.layers)}

    def step(l, j):
        return min(first_of[l] + j, first_of.get(l + 1, n_steps) - 1)

    def peer_to(t):
        while at["peer"] <= t:
            issue_peer(at["peer"])
            at["peer"] += 1

    def mate_to(t):
        while at["mate"] <= t:
            issue_mate(at["mate"])
            at["mate"] += 1

    def relay_to(t):
        assert t < at["peer"] and t < at["mate"]
        while at["relay"] <= t:
            relay(at["relay"])
            at["relay"] += 1

    def advance():
        t = at["next"]
        assert t < at["relay"], t
        rest = n_row - 1 - peer
        with sc(f"adv{t}"):
            split = D.cfg[steps[t][0]].split
            for i, (src, place) in enumerate(blocks(t, half if split else 0)):
                if split:
                    y_copy(t, i, 0, src, place(peer), peer).wait_recv()
                y_copy(t, i, 2, src, place(rest), rest).wait_recv()
            at["next"] = t + 1

    def have(*which):
        while at["next"] <= step_of[which]:
            advance()

    mate_to(1)
    peer_to(step(0, 3))

    def w_fetch(l, kind, j, slot):
        C = D.cfg[l]
        i = half if C.split else 0
        copies = []

        def fetch(src, dst):
            copies.append(pltpu.make_async_copy(src, dst, lw.at[slot, len(copies)]))

        def w_rows(a, m, at):
            a, at = rows_at(a, m), pl.ds(at, m)
            fetch(w_t.at[l, a, :], wbuf.at[slot, at, own_lanes(row)])
            for r in (up, down, across):
                fetch(g_w.at[l, a, own_lanes(r)], wbuf.at[slot, at, own_lanes(r)])

        if kind == "q":
            w_rows(i * C.q, C.q, 0)
            at = pl.ds(C.q, D.kvp)
            fetch(wkv_t.at[l], wbuf.at[slot, at, own_lanes(row)])
            for r in (up, down, across):
                fetch(g_kv.at[l, :, own_lanes(r)], wbuf.at[slot, at, own_lanes(r)])
        else:
            w_rows(D.q + i * C.f + j * C.cw, C.cw, 0)
            w_rows(D.q + D.f + i * C.f + j * C.cw, C.cw, C.cw)
        return copies

    def o_fetch(l, j, slot):
        C = D.cfg[l]
        copies = []

        def fetch(src, dst):
            copies.append(pltpu.make_async_copy(src, dst, lo.at[slot, len(copies)]))

        spans = ((half * C.q, 0, C.q), (D.q + half * C.f, C.q, C.f)) if C.split else ((0, 0, C.q + C.f),)
        for a, at, m in spans:
            a, at = rows_at(a, m), pl.ds(at, m)
            to = lambda r: pl.ds(pl.multiple_of(r * och, 128), och)
            fetch(w_o.at[l, a, o_lanes(j, row)], wonat.at[slot, at, to(row)])
            for r in (up, down, across):
                fetch(g_wo.at[l, r, a, o_lanes(j, r)], wonat.at[slot, at, to(r)])
        return copies

    def start(copies):
        for c in copies:
            c.start()

    def wait(copies):
        for c in copies:
            c.wait()

    own_x.wait()
    own_g.wait()

    def x_finish(i):
        s = lax.rem(me + n - i, n)
        remote(xland.at[s], xland.at[s], xs.at[i], xr.at[i], row, col).wait_recv()
        remote(gland.at[s], gland.at[s], gs.at[i], gr.at[i], row, col).wait_recv()
        x_copy(i).wait_send()
        g_copy(i).wait_send()

    with sc("xwait"):
        loop(1, n, x_finish)

    def keep(d):
        hid[rows_at(d * dl, dl), :] = xland[d]

    with sc("gains"):
        loop(0, n, keep)
        g_all = gland[...].astype(F32)
        for l in range(D.layers):
            g_rows = g_all[:, l, :]
            g_rows = jnp.concatenate([g_rows, jnp.zeros((128 - n, 128), F32)], axis=0) if n < 128 else g_rows
            g_cols = g_rows.T
            for d in range(n):
                gcol[l, d * dl : (d + 1) * dl, :] = jnp.broadcast_to(g_cols[:dl, d : d + 1], (dl, 128))

    blk = 64
    n_blk = D.d // blk

    def layer_norm(l):
        def add_up(i, acc):
            v = hid[rows_at(i * blk, blk), :].astype(F32)
            return acc + v.reshape(blk // 8, 8, tok).sum(axis=0)

        mean = lax.fori_loop(0, n_blk, add_up, jnp.zeros((8, tok), F32)).sum(axis=0, keepdims=True) / D.d

        def add_sq(i, acc):
            v = hid[rows_at(i * blk, blk), :].astype(F32) - mean
            return acc + (v * v).reshape(blk // 8, 8, tok).sum(axis=0)

        var = lax.fori_loop(0, n_blk, add_sq, jnp.zeros((8, tok), F32)).sum(axis=0, keepdims=True) / D.d
        scale = lax.rsqrt(var + LN_EPS)

        def write(i):
            rows = rows_at(i * blk, blk)
            g = gcol[l, rows, :]
            g = jnp.concatenate([g] * (tok // 128), axis=1)
            v = (hid[rows, :].astype(F32) - mean) * scale * g
            ht[x, rows, my_lanes] = v.astype(BF16)

        with sc(f"norm{l}"):
            loop(0, n_blk, write)

    d_low, d_high = pl.ds(0, D.d // 2), pl.ds(D.d // 2, D.d // 2)

    class Gather:
        def __init__(self, ref, tag):
            self.ref, self.tag, self.sends = ref, tag, []
            for i, part, c in ((0, 0, right), (1, 0, left), (2, None, twin), (9, 1, right), (10, 1, left)):
                self.send(i, ref(x, False, part), c)

        def send(self, i, ref, c):
            copy = remote(ref, ref, ags.at[self.tag, i], agr.at[self.tag, i], row, c)
            copy.start()
            self.sends.append(copy)

        def arrived(self, i, ref):
            remote(ref, ref, ags.at[self.tag, i], agr.at[self.tag, i], row, col).wait_recv()

        def pass_low(self):
            with sc(f"pass_low{self.tag}"):
                self.arrived(0, self.ref(xl_, False, 0))
                self.send(3, self.ref(xl_, False, 0), right)
                self.send(4, self.ref(xl_, False, 0), twin)
                self.arrived(1, self.ref(xr_, False, 0))
                self.send(6, self.ref(xr_, False, 0), twin)

        def pass_on(self):
            with sc(f"pass_on{self.tag}"):
                self.arrived(10, self.ref(xr_, False, 1))
                self.send(5, self.ref(xr_, False, 1), left)
                self.send(12, self.ref(xr_, False, 1), twin)
                self.arrived(9, self.ref(xl_, False, 1))
                self.send(11, self.ref(xl_, False, 1), twin)

        def own(self):
            with sc(f"own{self.tag}"):
                self.arrived(2, self.ref(x, True, None))

        def near(self):
            with sc(f"near{self.tag}"):
                self.arrived(4, self.ref(xl_, True, 0))
                self.arrived(6, self.ref(xr_, True, 0))
                self.arrived(12, self.ref(xr_, True, 1))
                self.arrived(11, self.ref(xl_, True, 1))

        def pass_far(self):
            with sc(f"pass_far{self.tag}"):
                for part, i, j in ((0, 3, 7), (1, 5, 8)):
                    self.arrived(i, self.ref(xf_, False, part))
                    self.send(j, self.ref(xf_, False, part), twin)

        def far(self):
            with sc(f"far{self.tag}"):
                self.arrived(7, self.ref(xf_, True, 0))
                self.arrived(8, self.ref(xf_, True, 1))

        def finish(self):
            for c in self.sends:
                c.wait_send()

    def normed_of(buf):
        def ref(chip, other, part):
            rows = slice(None) if part is None else (d_low, d_high)[part]
            return buf.at[chip, rows, twin_lanes if other else my_lanes]

        return ref

    def kv_of(a):
        def ref(chip, other, part):
            h = D.seqs // 2
            span = pl.ds(a * D.seqs, D.seqs) if part is None else pl.ds(a * D.seqs + part * h, h)
            return kvland.at[chip * 2 + (1 - k if other else k), span]

        return ref

    half_dim = D.hd // 2

    def near3(i):
        return lax.rem(x + i + i // 2, n_x)

    def all4(i):
        return i

    def far1(i):
        return xf_

    def rope(p):
        lo_, hi_ = p[:half_dim], p[half_dim:]
        return jnp.concatenate([lo_ * cos_ref[...] - hi_ * sin_ref[...], hi_ * cos_ref[...] + lo_ * sin_ref[...]], axis=0)

    def project_q(l, a, seq_of, count):
        C = D.cfg[l]

        def body(i):
            s = seq_of(i)
            p = dot(wbuf[1, : C.q + D.kvp, :], ht[s]).astype(BF16).astype(F32)
            for h in range(C.heads):
                at = rows_at((a * D.seqs + s) * C.q + h * D.hd, D.hd)
                qt[at, :] = (rope(p[h * D.hd : (h + 1) * D.hd]) * D.hd**-0.5).astype(BF16)
            kvland[col, a * D.seqs + s] = p[C.q :].astype(BF16)

        with sc(f"q{l}{a}"):
            loop(0, count, body)

    def kv_copy(s, j, source):
        ref = kvland.at[source, s]
        return remote(ref, ref, kvs.at[s, j], kvr.at[s, j], row, lax.rem(col + j, n_col))

    def kv_send(seq_of, count):
        def body(i):
            s = seq_of(i)
            loop(1, n_col, lambda j: kv_copy(s, j, col).start())

        loop(0, count, body)

    def kv_arrive():
        def body(i):
            j = i // D.seqs + 1
            s = lax.rem(i, D.seqs)
            kv_copy(s, j, lax.rem(col + n_col - j, n_col)).wait_recv()
            kv_copy(s, j, col).wait_send()

        with sc("kvwait"):
            loop(0, D.seqs * (n_col - 1), body)

    def key_value(l, a):
        def body(i):
            s = a * D.seqs + i
            raw = kvland[:, s].reshape(n_col * D.kvp, D.seq)
            both = dot(perm_ref[...], raw)
            zeros = jnp.zeros((128 - D.hd, D.seq), F32)
            k_nat = jnp.concatenate([rope(both[: D.hd]), zeros], axis=0).T.astype(BF16)
            kn[s] = k_nat
            vt[s] = both[D.hd :].astype(BF16)
            if a == 0:
                kvbuf[l, 0, i] = k_nat
                kvbuf[l, 1, i] = jnp.concatenate([both[D.hd :], zeros], axis=0).T.astype(BF16)

        with sc(f"kv{l}{a}"):
            loop(0, D.seqs, body)

    qb = D.seq // 2

    def attention(l, a):
        C = D.cfg[l]

        pair = 2
        per = C.heads // pair

        def body(i):
            s, h0 = a * D.seqs + i // per, lax.rem(i, per) * pair
            q_rows = [rows_at(s * C.q + (h0 + e) * D.hd, D.hd) for e in range(pair)]
            o_rows = [rows_at(s * (C.q + C.f) + (h0 + e) * D.hd, D.hd) for e in range(pair)]
            for b in range(2):
                ext = (b + 1) * qb
                lanes = slice(b * qb, (b + 1) * qb)
                keys = lax.broadcasted_iota(jnp.int32, (ext, qb), 0)
                queries = lax.broadcasted_iota(jnp.int32, (ext, qb), 1) + b * qb
                scores = [dot(kn[s, :ext, : D.hd], qt[q_rows[e], lanes]) for e in range(pair)]
                for e in range(pair):
                    score = jnp.where(keys <= queries, scores[e], -1e30)
                    p = jnp.exp(score - jnp.max(score, axis=0, keepdims=True))
                    p = (p * (1.0 / jnp.sum(p, axis=0, keepdims=True))).astype(BF16)
                    jt[o_rows[e], lanes] = dot(vt[s, :, :ext], p).astype(BF16)

        with sc(f"attn{l}{a}"):
            loop(0, D.seqs * per, body)

    def gate_up(l, a, slot, j, seq_of, count):
        C = D.cfg[l]

        def body(i):
            s = seq_of(i)
            p = dot(wbuf[slot, : 2 * C.cw, :], ht[s])
            g = p[: C.cw].astype(BF16).astype(F32)
            u = p[C.cw :].astype(BF16).astype(F32)
            jt[rows_at((a * D.seqs + s) * (C.q + C.f) + C.q + j * C.cw, C.cw), :] = (g * jax.nn.sigmoid(g) * u).astype(BF16)

        loop(0, count, body)

    def gate_up_loop(l, a, seq_of, count, first, last, stop=None):
        C = D.cfg[l]
        stop = C.n_c if stop is None else stop
        have_chunk(l, min(last, stop - 1))

        def body(j):
            slot = lax.rem(j, 2)
            wait(w_fetch(l, "f", j, slot))

            @pl.when(j + 1 < stop)
            def _():
                start(w_fetch(l, "f", j + 1, 1 - slot))

            gate_up(l, a, slot, j, seq_of, count)

        with sc(f"gu{l}{a}"):
            loop(first, last, body)

    def have_chunk(l, j):
        C = D.cfg[l]
        have(l, "f", (j + 1) * C.cw // fch - 1)

    def load_q(l):
        have(l, "q", 0)
        copies = w_fetch(l, "q", 0, 1)
        start(copies)
        wait(copies)

    m = och * n_row
    m_low, m_high = pl.ds(0, m // 2), pl.ds(m // 2, m // 2)
    r_slots = twin_in.shape[0]
    r_step = 64

    def order(i):
        return lax.rem(x + lax.rem(2 + 3 * i, 4), n_x)

    class Reduce:
        def __init__(self, l):
            self.l, self.C, self.sends = l, D.cfg[l], {}

        def send(self, u, i, src, dst, c):
            copy = remote(src, dst, rss.at[u % r_slots, i], rsr.at[u % r_slots, i], row, c)
            copy.start()
            self.sends[u].append(copy)

        def arrived(self, u, i, ref):
            remote(ref, ref, rss.at[u % r_slots, i], rsr.at[u % r_slots, i], row, col).wait_recv()

        def twin_copy(self, u, i):
            us = u % r_slots
            return remote(ot.at[u % 2, order(i), :, twin_lanes], twin_in.at[us, i], rss.at[us, i], rsr.at[us, i], row, twin)

        def twin_done(self, u):
            loop(0, 4, lambda i: self.twin_copy(u, i).wait_send())

        def stage_a(self, u, a):
            C = self.C
            if u >= 2:
                self.twin_done(u - 2)
            if u >= r_slots - 1:
                for c in self.sends.pop(u - r_slots + 1):
                    c.wait_send()
            self.sends[u] = []
            R = C.q + C.f

            def body(i):
                s = order(i)
                ot[u % 2, s] = dot(wobuf[:, :R], jt[rows_at((a * D.seqs + s) * R, R), :]).astype(BF16)
                self.twin_copy(u, i).start()

            with sc(f"sa{self.l}_{u}"):
                loop(0, 4, body)

        def stage_b(self, u):
            us = u % r_slots

            def body(i):
                self.arrived(u, i, twin_in.at[us, i])
                s = order(i)

                def add(b):
                    at = rows_at(b * r_step, r_step)
                    twin_in[us, i, at, :] = (ot[u % 2, s, at, my_lanes].astype(F32) + twin_in[us, i, at, :].astype(F32)).astype(BF16)

                loop(0, m // r_step, add)

            far = [
                remote(twin_in.at[us, 0, m_low], far_in.at[us, m_low], rss.at[us, 4], rsr.at[us, 4], row, right),
                remote(twin_in.at[us, 0, m_high], far_in.at[us, m_high], rss.at[us, 5], rsr.at[us, 5], row, left),
            ]
            self.sends[u] += far

            def each(i):
                body(i)

                @pl.when(i == 0)
                def _():
                    start(far)

            with sc(f"sb{self.l}_{u}"):
                loop(0, 4, each)

        def stage_c(self, u):
            us = u % r_slots

            def add_far(i, base):
                def add(b):
                    at = rows_at(base + b * r_step, r_step)
                    twin_in[us, i, at, :] = (twin_in[us, i, at, :].astype(F32) + far_in[us, at, :].astype(F32)).astype(BF16)

                loop(0, m // 2 // r_step, add)

            with sc(f"sc{self.l}_{u}"):
                self.arrived(u, 4, far_in.at[us, m_low])
                add_far(1, 0)
                self.send(u, 6, twin_in.at[us, 1], near_in.at[us, 0], right)
                self.arrived(u, 5, far_in.at[us, m_high])
                add_far(3, m // 2)
                self.send(u, 7, twin_in.at[us, 3], near_in.at[us, 1], left)

        def add_update(self, j, total):
            step = min(r_step, och)
            for r in range(n_row):

                def add(b, r=r):
                    dst = rows_at(r * dr + (r + j) % D.n_o * och + b * step, step)
                    u = total(rows_at(r * och + b * step, step)).astype(BF16).astype(F32)
                    hid[dst, :] = (hid[dst, :].astype(F32) + u).astype(BF16)

                loop(0, och // step, add)

        def stage_d(self, u, j, a):
            us = u % r_slots

            def total(at):
                return twin_in[us, 2, at, :].astype(F32) + near_in[us, 0, at, :].astype(F32) + near_in[us, 1, at, :].astype(F32)

            with sc(f"sd{self.l}_{u}"):
                self.arrived(u, 6, near_in.at[us, 0])
                self.arrived(u, 7, near_in.at[us, 1])
                if self.C.split:

                    def save(b):
                        at = rows_at(b * r_step, r_step)
                        psum[a, j, at, :] = total(at).astype(BF16)

                    loop(0, m // r_step, save)
                    if a == 1:
                        remote(psum.at[1, j], pair_in.at[j], es.at[j], er.at[j], mate, col).start()
                else:
                    self.add_update(j, total)

        def stage_e(self, j):
            with sc(f"se{self.l}_{j}"):
                c = remote(psum.at[1, j], pair_in.at[j], es.at[j], er.at[j], mate, col)
                c.wait_recv()
                self.add_update(j, lambda at: psum[0, j, at, :].astype(F32) + pair_in[j, at, :].astype(F32))
                c.wait_send()

        def finish(self, units):
            with sc(f"rfin{self.l}"):
                for u in range(max(0, units - 2), units):
                    self.twin_done(u)
                for u in self.sends:
                    for c in self.sends[u]:
                        c.wait_send()

    o_started = set()

    def o_load(l, j, a):
        if (l, j, a) not in o_started:
            have(l, "o", j)
            start(o_fetch(l, j, j % 2))
            o_started.add((l, j, a))

    def o_use(l, j, a):
        C = D.cfg[l]
        with sc(f"ouse{l}_{j}"):
            o_load(l, j, a)
            wait(o_fetch(l, j, j % 2))
            R = C.q + C.f
            for r in range(n_row):
                wobuf[r * och : (r + 1) * och, :R] = wonat[j % 2, :R, r * och : (r + 1) * och].T

    layer_norm(0)
    g0 = Gather(normed_of(ht), 0)
    mine = ht.at[x, :, my_lanes]
    shared = g_h.at[x, :, my_lanes]
    to_mate = remote(mine, shared, ps, pr_, mate, col)
    to_mate.start()
    relay_to(1)
    mate_to(step(0, 5))
    peer_to(step(0, 5))
    g0.pass_low()
    g0.pass_on()
    with sc("mate"):
        to_mate.wait_recv()
    g1 = Gather(normed_of(g_h), 1)
    load_q(0)
    g0.own()
    g0.near()
    project_q(0, 0, near3, 3)
    relay_to(2)
    mate_to(step(0, 10))
    g0.pass_far()
    g0.far()
    project_q(0, 0, far1, 1)
    kv0 = Gather(kv_of(0), 2)
    relay_to(3)
    n_f = D.cfg[0].n_f
    f_started = set()

    def f_load(j):
        if j not in f_started:
            f_started.add(j)
            start(w_fetch(0, "f", j, j % 2))

    def h_copy(i):
        return pltpu.make_async_copy(g_h.at[i], ht.at[i], lh.at[i])

    have(0, "f", 0)
    f_load(0)
    gate_up_loop(0, 0, all4, 4, 0, 2, 2)
    relay_to(step(0, 4))
    for j in range(2, n_f):
        have(0, "f", j)
        f_load(j)
        with sc(f"gu0_{j}"):
            wait(w_fetch(0, "f", j, j % 2))
            gate_up(0, 0, j % 2, j, all4, 4)
        if j == max(2, n_f - 3):
            g1.pass_low()
            relay_to(step(0, 5))
            peer_to(step(0, 6))
            relay_to(step(0, 6))
            peer_to(step(0, 7))
    kv0.pass_low()
    kv0.pass_on()
    g1.pass_on()
    for t in (7, 8):
        relay_to(step(0, t))
        peer_to(step(0, t + 1))
    relay_to(step(0, 9))
    peer_to(step(0, 10))
    relay_to(step(0, 10))
    peer_to(step(1, 5))
    mate_to(step(1, D.cfg[1].n_f - 2))
    g0.finish()
    to_mate.wait_send()
    g1.own()
    g1.near()
    loop(0, 3, lambda i: h_copy(near3(i)).start())
    kv0.pass_far()
    with sc("kv0wait"):
        kv0.own()
        kv0.near()
        kv0.far()
        kv0.finish()
    key_value(0, 0)
    attention(0, 0)

    red = Reduce(0)
    units = [(j, 0) for j in range(D.n_o - 1)] + [(j, 1) for j in range(D.n_o)] + [(D.n_o - 1, 0)]
    n_u = len(units)
    first = D.n_o - 1
    state = {"e": 0}

    def settle(count):
        while state["e"] < count:
            red.stage_e(state["e"])
            state["e"] += 1

    def unit(u):
        j, a = units[u]
        if u == 0 or units[u - 1][0] != j:
            o_use(0, j, a)
        red.stage_a(u, a)
        if u + 1 < n_u and units[u + 1][0] != j:
            o_load(0, *units[u + 1])
        if u >= 2:
            red.stage_c(u - 2)
        if u >= 3:
            red.stage_d(u - 3, *units[u - 3])
        red.stage_b(u)

    unit(0)
    g1.pass_far()
    unit(1)
    g1.far()
    h_copy(xf_).start()
    load_q(0)
    start(w_fetch(0, "f", 0, 0))
    loop(0, 3, lambda i: h_copy(near3(i)).wait())
    h_copy(xf_).wait()
    project_q(0, 1, all4, 4)
    kv1 = Gather(kv_of(1), 3)
    parts = first - 2
    cuts = [n_f * i // parts for i in range(parts + 1)]
    for u in range(2, first):
        unit(u)
        if u == 2:
            kv1.pass_low()
            kv1.pass_on()
        gate_up_loop(0, 1, all4, 4, cuts[u - 2], cuts[u - 1])
    kv1.pass_far()
    relay_to(step(1, 1))
    with sc("kv1wait"):
        kv1.own()
        kv1.near()
        kv1.far()
        kv1.finish()
    key_value(0, 1)
    attention(0, 1)
    g1.finish()
    relay_to(step(1, 2))
    peer_to(step(1, 7))
    n_f1 = D.cfg[1].n_f
    for u in range(first, n_u):
        unit(u)
        v = u - first
        if v in (0, 1, 2):
            relay_to(step(1, min(v + 3, n_f1 - 2)))
        if v == 1:
            peer_to(step(1, min(8, n_f1)))
        elif v == 4:
            relay_to(step(1, min(6, n_f1 - 2)))
            peer_to(step(1, min(9, n_f1)))
        elif v == 5:
            peer_to(step(1, n_f1))
    relay_to(step(1, min(6, n_f1 - 2)))
    peer_to(step(1, n_f1))
    red.stage_c(n_u - 2)
    red.stage_d(n_u - 3, *units[n_u - 3])
    red.stage_c(n_u - 1)
    red.stage_d(n_u - 2, *units[n_u - 2])
    mate_to(step(1, n_f1))
    settle(D.n_o - 1)
    red.stage_d(n_u - 1, *units[n_u - 1])
    settle(D.n_o)
    red.finish(n_u)

    def slice_of(d):
        return hid.at[rows_at(d * dl, dl), :]

    own_y = pltpu.make_async_copy(slice_of(me), piece_of(y_out, me), xr.at[0])

    def y_copy_back(i):
        d = lax.rem(me + i, n)
        return remote(slice_of(d), piece_of(y_out, me), xs.at[i], xr.at[i], d // n_col, lax.rem(d, n_col))

    def y_send_back(i):
        @pl.when(i == 0)
        def _():
            own_y.start()

        @pl.when(i != 0)
        def _():
            y_copy_back(i).start()

    def y_finish(i):
        s = lax.rem(me + n - i, n)
        remote(piece_of(y_out, s), piece_of(y_out, s), xs.at[i], xr.at[i], row, col).wait_recv()
        y_copy_back(i).wait_send()

    def y_ready(low, high):
        def body(i):
            d = lax.rem(me + i, n)
            r, a = d // n_col, lax.rem(d, n_col) * dl
            first = lax.rem(a // och + D.n_o - lax.rem(r, D.n_o), D.n_o)
            second = lax.rem((a + dl - 1) // och + D.n_o - lax.rem(r, D.n_o), D.n_o)

            done = jnp.maximum(first, second)

            @pl.when((low <= done) & (done < high))
            def _():
                y_send_back(i)

        loop(0, n, body)

    for l in range(1, D.layers):
        C = D.cfg[l]
        layer_norm(l)
        g0 = Gather(normed_of(ht), 0)
        peer_to(step(l, C.n_f))
        mate_to(step(l, C.n_f))
        relay_to(step(l, min(8, C.n_f)))
        own1, near2 = (lambda i: x), (lambda i: lax.rem(x + 1 + 2 * i, n_x))
        n_mid = min(3, C.n_c - 1)

        def begin(seq_of, count):
            load_q(l)
            have_chunk(l, 0)
            start(w_fetch(l, "f", 0, 0))
            project_q(l, 0, seq_of, count)

        g0.own()
        begin(own1, 1)
        kv_send(own1, 1)
        relay_to(step(l, C.n_f))
        peer_to(step(l, C.n_f + 2))
        mate_to(step(l, C.n_f + 2))
        g0.pass_low()
        gate_up_loop(l, 0, own1, 1, 0, C.n_c)
        g0.pass_on()
        g0.near()
        begin(near2, 2)
        kv_send(near2, 2)
        gate_up_loop(l, 0, near2, 2, 0, n_mid)
        g0.pass_far()
        relay_to(step(l, C.n_f + 1))
        peer_to(step(l, C.n_f + 4))
        mate_to(step(l, C.n_f + 4))
        gate_up_loop(l, 0, near2, 2, n_mid, C.n_c)
        relay_to(step(l, C.n_f + 2))
        g0.far()
        begin(far1, 1)
        kv_send(far1, 1)
        gate_up_loop(l, 0, far1, 1, 0, C.n_c)
        peer_to(step(l, C.n_f + D.n_o))
        mate_to(step(l, C.n_f + D.n_o))
        relay_to(step(l, C.n_f + 3))
        g0.finish()
        kv_arrive()
        key_value(l, 0)
        attention(l, 0)
        relay_to(step(l, C.n_f + 4))
        red = Reduce(l)
        last = l + 1 == D.layers

        end = D.n_o - 1
        for j in range(D.n_o):
            o_use(l, j, 0)
            red.stage_a(j, 0)
            if j == 0:
                relay_to(step(l, C.n_f + D.n_o))
            if j < end:
                o_load(l, j + 1, 0)
            if 2 <= j:
                red.stage_c(j - 2)
            if 3 <= j:
                red.stage_d(j - 3, j - 3, 0)
            red.stage_b(j)
        red.stage_c(end - 1)
        red.stage_d(end - 2, end - 2, 0)
        red.stage_c(end)
        red.stage_d(end - 1, end - 1, 0)
        if last:
            with sc("send"):
                y_ready(0, end)
        red.stage_d(end, end, 0)
        if last:
            y_ready(end, end + 1)
        red.finish(D.n_o)

    def kv_back(i):
        r = lax.rem(row + i, n_row)
        pos = rows_at((r * n_col + col) * D.pos, D.pos)
        return kvbuf.at[:, :, :, pos, :], kv_out.at[:, :, pl.ds(row * D.seqs, D.seqs)], r

    src, dst, _ = kv_back(0)
    own_kv = pltpu.make_async_copy(src, dst, fl)
    own_kv.start()
    kv_sends = []
    for i in range(1, n_row):
        src, dst, r = kv_back(i)
        c = remote(src, dst, fs.at[i], fr.at[i], r, col)
        c.start()
        kv_sends.append(c)

    with sc("ywait"):
        loop(1, n, y_finish)
        own_y.wait()
        own_kv.wait()
        for i in range(1, n_row):
            r = lax.rem(row + n_row - i, n_row)
            dst = kv_out.at[:, :, pl.ds(r * D.seqs, D.seqs)]
            remote(dst, dst, fs.at[i], fr.at[i], row, col).wait_recv()
        for c in kv_sends:
            c.wait_send()
        for c in y_sent:
            c.wait_send()


def solution(mesh):
    n_row, n_col = mesh.shape["row"], mesh.shape["col"]
    group = n_row * n_col
    act_spec = P("dp", None, ("row", "col"))
    weight_spec = P(None, "row", "col")

    def device_fn(x_loc, gain_loc, w_in_loc, w_kv_loc, w_out_loc):
        D = Dims()
        D.n_row, D.n_col = n_row, n_col
        n_batch, D.seq, D.dl = x_loc.shape
        D.layers, D.dr, e = w_in_loc.shape
        D.d = D.dl * group
        r_block = w_out_loc.shape[1]
        D.f = e - r_block
        D.q = r_block - D.f
        kv_local = w_kv_loc.shape[2]
        D.hd = kv_local * n_col // 2
        D.kvp = 32
        D.tok = n_batch * D.seq // group
        D.seqs = n_batch // n_row
        D.pos = D.seq // group
        D.fch = 128
        D.och = 128
        D.n_o = D.dr // D.och
        D.cfg = []
        for l in range(D.layers):
            C = Dims()
            C.split = l == 0
            parts = 2 if C.split else 1
            C.q, C.f = D.q // parts, D.f // parts
            C.heads, C.n_f = C.q // D.hd, C.f // D.fch
            C.cw = D.fch if C.split else 2 * D.fch
            C.n_c = C.f // C.cw
            D.cfg.append(C)
        assert D.seq == 2 * D.tok and D.seqs == n_col // 2 == n_row == 4

        half = D.hd // 2
        inv_freq = (np.float32(1.0) / (np.float32(10000.0) ** (np.arange(half, dtype=np.float32) * np.float32(2.0) / np.float32(D.hd)))).astype(np.float32)
        angles = (inv_freq[:, None] * np.arange(D.seq, dtype=np.float32)[None, :]).astype(np.float32)
        cos_t, sin_t = np.cos(angles).astype(np.float32), np.sin(angles).astype(np.float32)
        perm = np.zeros((2 * D.hd, n_col * D.kvp), np.float32)
        for i in range(2 * D.hd):
            perm[i, (i // kv_local) * D.kvp + i % kv_local] = 1.0

        x_t = x_loc.transpose(0, 2, 1)
        w_t = w_in_loc.transpose(0, 2, 1)
        wkv_t = jnp.pad(w_kv_loc.transpose(0, 2, 1), ((0, 0), (0, D.kvp - kv_local), (0, 0)))
        gains = jnp.pad(gain_loc, ((0, 16 - D.layers), (0, 128 - D.dl)))

        n_y = sum(12 + 6 * (C.n_f + D.n_o) for C in D.cfg)
        m = D.och * n_row
        sds = jax.ShapeDtypeStruct
        dma = pltpu.SemaphoreType.DMA
        out = pl.pallas_call(
            functools.partial(kernel, D),
            out_shape=(
                sds(x_t.shape, BF16),
                sds((D.layers, 2, n_batch, D.pos, 128), BF16),
                sds((D.layers, e, D.d), BF16),
                sds((D.layers, D.kvp, D.d), BF16),
                sds((D.layers, n_row, r_block, D.dr), BF16),
                sds((D.seqs, D.d, D.seq), BF16),
            ),
            in_specs=[ANY] * 5 + [VMEM] * 3,
            out_specs=(ANY,) * 6,
            scratch_shapes=[
                pltpu.VMEM((group, D.dl, D.tok), BF16),
                pltpu.VMEM((group, 16, 128), BF16),
                pltpu.VMEM((D.layers, D.d, 128), F32),
                pltpu.VMEM((D.d, D.tok), BF16),
                pltpu.VMEM((D.seqs, D.d, D.seq), BF16),
                pltpu.VMEM((2, max(4 * D.fch, D.q + D.kvp), D.d), BF16),
                pltpu.VMEM((2, r_block, m), BF16),
                pltpu.VMEM((m, r_block), BF16),
                pltpu.VMEM((D.seqs * D.q, D.seq), BF16),
                pltpu.VMEM((n_col, 2 * D.seqs, D.kvp, D.seq), BF16),
                pltpu.VMEM((2 * D.seqs, D.seq, 128), BF16),
                pltpu.VMEM((2 * D.seqs, D.hd, D.seq), BF16),
                pltpu.VMEM((D.layers, 2, D.seqs, D.seq, 128), BF16),
                pltpu.VMEM((D.seqs * r_block, D.seq), BF16),
                pltpu.VMEM((2, D.seqs, m, D.seq), BF16),
                pltpu.VMEM((5, 4, m, D.tok), BF16),
                pltpu.VMEM((5, m, D.tok), BF16),
                pltpu.VMEM((5, 2, m, D.tok), BF16),
                pltpu.VMEM((2, D.n_o, m, D.tok), BF16),
                pltpu.VMEM((D.n_o, m, D.tok), BF16),
                dma((group,)), dma((group,)), dma((group,)), dma((group,)),
                dma((n_y,)), dma((n_y,)),
                dma((4, 13)), dma((4, 13)), dma, dma,
                dma((D.seqs, n_col)), dma((D.seqs, n_col)),
                dma((5, 8)), dma((5, 8)),
                dma((D.n_o,)), dma((D.n_o,)),
                dma((2, 8)), dma((2, 8)), dma((D.seqs,)),
                dma((n_row,)), dma((n_row,)), dma,
            ],
            compiler_params=pltpu.CompilerParams(collective_id=0, has_side_effects=True, vmem_limit_bytes=67_000_000),
            name="two_layers",
        )(x_t, gains, w_t, wkv_t, w_out_loc, jnp.asarray(cos_t), jnp.asarray(sin_t), jnp.asarray(perm, BF16))
        return out[0].transpose(0, 2, 1), out[1][..., : D.hd]

    return jax.shard_map(device_fn, mesh=mesh, in_specs=(act_spec, P(None, ("row", "col")), weight_spec, weight_spec, P(None, "col", "row")), out_specs=(act_spec, P(None, None, "dp", ("row", "col"), None)), check_vma=False)
```

```python
import functools

import numpy as np

import jax
import jax.numpy as jnp
from jax import lax
from jax.experimental import pallas as pl
from jax.experimental.pallas import tpu as pltpu
from jax.sharding import PartitionSpec as P

LN_EPS = 1e-6
MESH = pl.DeviceIdType.MESH
ANY = pl.BlockSpec(memory_space=pl.ANY)
VMEM = pl.BlockSpec(memory_space=pltpu.VMEM)
F32, BF16 = jnp.float32, jnp.bfloat16


def dot(a, b):
    return jnp.dot(a, b, preferred_element_type=F32)


class Dims:
    pass


def rows_at(start, count, by=16):
    return pl.ds(start if isinstance(start, int) else pl.multiple_of(start, by), count)


def kernel(
    D,
    x_t, gains, w_t, wkv_t, w_o, cos_ref, sin_ref, perm_ref,
    y_out, kv_out, g_w, g_kv, g_wo, g_h,
    xland, gland, gcol, hid, ht, wbuf, wonat, wobuf, qt, kvland, kn, vt, kvbuf, jt, ot, twin_in, far_in, near_in, psum, pair_in,
    xs, xr, gs, gr, ys, yr, ags, agr, ps, pr_, kvs, kvr, rss, rsr, es, er, lw, lo, lh, fs, fr, fl,
):
    sc = jax.named_scope
    row, col = lax.axis_index("row"), lax.axis_index("col")
    n_row, n_col, n = D.n_row, D.n_col, D.n_row * D.n_col
    n_x = n_col // 2
    me = row * n_col + col
    x, k = col // 2, lax.rem(col, 2)
    xr_, xl_, xf_ = lax.rem(x + 1, n_x), lax.rem(x + n_x - 1, n_x), lax.rem(x + 2, n_x)
    right, left, twin = xr_ * 2 + k, xl_ * 2 + k, x * 2 + 1 - k
    up, down, across = lax.rem(row + 1, n_row), lax.rem(row + n_row - 1, n_row), lax.rem(row + 2, n_row)
    half, mate = row // 2, n_row - 1 - row
    peer = row + 1 - 2 * lax.rem(row, 2)
    tok, dl, dr = D.tok, D.dl, D.dr
    och, fch = D.och, D.fch
    my_lanes = pl.ds(pl.multiple_of(k * tok, 128), tok)
    twin_lanes = pl.ds(pl.multiple_of((1 - k) * tok, 128), tok)

    def remote(src, dst, ssem, rsem, r, c):
        return pltpu.make_async_remote_copy(src_ref=src, dst_ref=dst, send_sem=ssem, recv_sem=rsem, device_id={"row": r, "col": c}, device_id_type=MESH)

    def loop(lo_, hi_, f):
        def body(i, carry):
            f(i)
            return carry

        lax.fori_loop(lo_, hi_, body, 0)

    barrier = pltpu.get_barrier_semaphore()

    def greet(i):
        d = lax.rem(me + i, n)
        pl.semaphore_signal(barrier, inc=1, device_id={"row": d // n_col, "col": lax.rem(d, n_col)}, device_id_type=MESH)

    with sc("barrier"):
        loop(1, n, greet)
        pl.semaphore_wait(barrier, n - 1)

    def piece_of(ref, d):
        return ref.at[d // 2, :, pl.ds(pl.multiple_of(lax.rem(d, 2) * tok, 128), tok)]

    def x_copy(i):
        d = lax.rem(me + i, n)
        return remote(piece_of(x_t, d), xland.at[me], xs.at[i], xr.at[i], d // n_col, lax.rem(d, n_col))

    def g_copy(i):
        d = lax.rem(me + i, n)
        return remote(gains, gland.at[me], gs.at[i], gr.at[i], d // n_col, lax.rem(d, n_col))

    own_x = pltpu.make_async_copy(piece_of(x_t, me), xland.at[me], xr.at[0])
    own_g = pltpu.make_async_copy(gains, gland.at[me], gr.at[0])
    own_x.start()
    own_g.start()
    def x_first(i):
        x_copy(i).start()
        g_copy(i).start()

    loop(1, n, x_first)

    def own_lanes(r):
        return pl.ds(pl.multiple_of(r * dr, 128), dr)

    def o_lanes(j, r):
        return pl.ds(pl.multiple_of(lax.rem(r + j, D.n_o) * och, 128), och)

    steps = []
    for l, C in enumerate(D.cfg):
        steps += [(l, "q", 0)] + [(l, "f", j) for j in range(C.n_f)] + [(l, "o", j) for j in range(D.n_o)]
    n_steps = len(steps)
    step_of = {s: t for t, s in enumerate(steps)}

    def blocks(t, i):
        l, kind, j = steps[t]
        C = D.cfg[l]
        out = []

        def w_rows(a, m):
            at = rows_at(a, m)
            out.append((w_t.at[l, at, :], lambda r: g_w.at[l, at, own_lanes(r)]))

        def o_rows(a, m):
            at = rows_at(a, m)
            out.append((w_o.at[l, at, o_lanes(j, row)], lambda r: g_wo.at[l, r, at, o_lanes(j, r)]))

        def kv_rows(a, m):
            at = pl.ds(a, m)
            out.append((wkv_t.at[l, at, :], lambda r: g_kv.at[l, at, own_lanes(r)]))

        if kind == "q":
            for a in (0, C.q // 2):
                w_rows(i * C.q + a, C.q // 2)
            for a in (0, D.kvp // 2):
                kv_rows(a, D.kvp // 2)
        elif kind == "f":
            w_rows(D.q + i * C.f + j * fch, fch)
            w_rows(D.q + D.f + i * C.f + j * fch, fch)
        elif C.split:
            o_rows(i * C.q, C.q)
            o_rows(D.q + i * C.f, C.f)
        else:
            for a in (0, (D.q + D.f) // 2):
                o_rows(a, (D.q + D.f) // 2)
        return out

    base, n_sems = [], 0
    for l, kind, j in steps:
        base.append(n_sems)
        n_sems += 12 if kind == "q" else 6
    assert n_sems == ys.shape[0]
    y_sent = []

    def y_copy(t, i, kind, src, dst, r):
        at = base[t] + 3 * i + kind
        return remote(src, dst, ys.at[at], yr.at[at], r, col)

    def y_send(*args):
        c = y_copy(*args)
        c.start()
        y_sent.append(c)

    def issue_peer(t):
        for i, (src, place) in enumerate(blocks(t, half if D.cfg[steps[t][0]].split else 0)):
            y_send(t, i, 0, src, place(row), peer)

    def issue_mate(t):
        for i, (src, place) in enumerate(blocks(t, 1 - half if D.cfg[steps[t][0]].split else 0)):
            y_send(t, i, 1, src, place(row), mate)

    def relay(t):
        split = D.cfg[steps[t][0]].split
        with sc(f"relay{t}"):
            for i, (src, place) in enumerate(blocks(t, half if split else 0)):
                y_copy(t, i, 1, src, place(mate), mate).wait_recv()
                if split or i % 2 == 0:
                    y_send(t, i, 2, place(mate), place(mate), peer)
                if not split:
                    y_copy(t, i, 0, src, place(peer), peer).wait_recv()
                    if i % 2 == 1:
                        y_send(t, i, 2, place(peer), place(peer), mate)

    at = {"next": 0, "peer": 0, "mate": 0, "relay": 0}
    first_of = {l: min(t for t, st in enumerate(steps) if st[0] == l) for l in range(D.layers)}

    def step(l, j):
        return min(first_of[l] + j, first_of.get(l + 1, n_steps) - 1)

    def peer_to(t):
        while at["peer"] <= t:
            issue_peer(at["peer"])
            at["peer"] += 1

    def mate_to(t):
        while at["mate"] <= t:
            issue_mate(at["mate"])
            at["mate"] += 1

    def relay_to(t):
        assert t < at["peer"] and t < at["mate"]
        while at["relay"] <= t:
            relay(at["relay"])
            at["relay"] += 1

    def advance():
        t = at["next"]
        assert t < at["relay"], t
        rest = n_row - 1 - peer
        with sc(f"adv{t}"):
            split = D.cfg[steps[t][0]].split
            for i, (src, place) in enumerate(blocks(t, half if split else 0)):
                if split:
                    y_copy(t, i, 0, src, place(peer), peer).wait_recv()
                y_copy(t, i, 2, src, place(rest), rest).wait_recv()
            at["next"] = t + 1

    def have(*which):
        while at["next"] <= step_of[which]:
            advance()

    mate_to(1)
    peer_to(step(0, 3))

    def w_fetch(l, kind, j, slot):
        C = D.cfg[l]
        i = half if C.split else 0
        copies = []

        def fetch(src, dst):
            copies.append(pltpu.make_async_copy(src, dst, lw.at[slot, len(copies)]))

        def w_rows(a, m, at):
            a, at = rows_at(a, m), pl.ds(at, m)
            fetch(w_t.at[l, a, :], wbuf.at[slot, at, own_lanes(row)])
            for r in (up, down, across):
                fetch(g_w.at[l, a, own_lanes(r)], wbuf.at[slot, at, own_lanes(r)])

        if kind == "q":
            w_rows(i * C.q, C.q, 0)
            at = pl.ds(C.q, D.kvp)
            fetch(wkv_t.at[l], wbuf.at[slot, at, own_lanes(row)])
            for r in (up, down, across):
                fetch(g_kv.at[l, :, own_lanes(r)], wbuf.at[slot, at, own_lanes(r)])
        else:
            w_rows(D.q + i * C.f + j * C.cw, C.cw, 0)
            w_rows(D.q + D.f + i * C.f + j * C.cw, C.cw, C.cw)
        return copies

    def o_fetch(l, j, slot):
        C = D.cfg[l]
        copies = []

        def fetch(src, dst):
            copies.append(pltpu.make_async_copy(src, dst, lo.at[slot, len(copies)]))

        spans = ((half * C.q, 0, C.q), (D.q + half * C.f, C.q, C.f)) if C.split else ((0, 0, C.q + C.f),)
        for a, at, m in spans:
            a, at = rows_at(a, m), pl.ds(at, m)
            to = lambda r: pl.ds(pl.multiple_of(r * och, 128), och)
            fetch(w_o.at[l, a, o_lanes(j, row)], wonat.at[slot, at, to(row)])
            for r in (up, down, across):
                fetch(g_wo.at[l, r, a, o_lanes(j, r)], wonat.at[slot, at, to(r)])
        return copies

    def start(copies):
        for c in copies:
            c.start()

    def wait(copies):
        for c in copies:
            c.wait()

    own_x.wait()
    own_g.wait()

    def x_finish(i):
        s = lax.rem(me + n - i, n)
        remote(xland.at[s], xland.at[s], xs.at[i], xr.at[i], row, col).wait_recv()
        remote(gland.at[s], gland.at[s], gs.at[i], gr.at[i], row, col).wait_recv()
        x_copy(i).wait_send()
        g_copy(i).wait_send()

    with sc("xwait"):
        loop(1, n, x_finish)

    def keep(d):
        hid[rows_at(d * dl, dl), :] = xland[d]

    with sc("gains"):
        loop(0, n, keep)
        g_all = gland[...].astype(F32)
        for l in range(D.layers):
            g_rows = g_all[:, l, :]
            g_rows = jnp.concatenate([g_rows, jnp.zeros((128 - n, 128), F32)], axis=0) if n < 128 else g_rows
            g_cols = g_rows.T
            for d in range(n):
                gcol[l, d * dl : (d + 1) * dl, :] = jnp.broadcast_to(g_cols[:dl, d : d + 1], (dl, 128))

    blk = 64
    n_blk = D.d // blk

    def layer_norm(l):
        def add_up(i, acc):
            v = hid[rows_at(i * blk, blk), :].astype(F32)
            return acc + v.reshape(blk // 8, 8, tok).sum(axis=0)

        mean = lax.fori_loop(0, n_blk, add_up, jnp.zeros((8, tok), F32)).sum(axis=0, keepdims=True) / D.d

        def add_sq(i, acc):
            v = hid[rows_at(i * blk, blk), :].astype(F32) - mean
            return acc + (v * v).reshape(blk // 8, 8, tok).sum(axis=0)

        var = lax.fori_loop(0, n_blk, add_sq, jnp.zeros((8, tok), F32)).sum(axis=0, keepdims=True) / D.d
        scale = lax.rsqrt(var + LN_EPS)

        def write(i):
            rows = rows_at(i * blk, blk)
            g = gcol[l, rows, :]
            g = jnp.concatenate([g] * (tok // 128), axis=1)
            v = (hid[rows, :].astype(F32) - mean) * scale * g
            ht[x, rows, my_lanes] = v.astype(BF16)

        with sc(f"norm{l}"):
            loop(0, n_blk, write)

    d_low, d_high = pl.ds(0, D.d // 2), pl.ds(D.d // 2, D.d // 2)

    class Gather:
        def __init__(self, ref, tag):
            self.ref, self.tag, self.sends = ref, tag, []
            for i, part, c in ((0, 0, right), (1, 0, left), (2, None, twin), (9, 1, right), (10, 1, left)):
                self.send(i, ref(x, False, part), c)

        def send(self, i, ref, c):
            copy = remote(ref, ref, ags.at[self.tag, i], agr.at[self.tag, i], row, c)
            copy.start()
            self.sends.append(copy)

        def arrived(self, i, ref):
            remote(ref, ref, ags.at[self.tag, i], agr.at[self.tag, i], row, col).wait_recv()

        def pass_low(self):
            with sc(f"pass_low{self.tag}"):
                self.arrived(0, self.ref(xl_, False, 0))
                self.send(3, self.ref(xl_, False, 0), right)
                self.send(4, self.ref(xl_, False, 0), twin)
                self.arrived(1, self.ref(xr_, False, 0))
                self.send(6, self.ref(xr_, False, 0), twin)

        def pass_on(self):
            with sc(f"pass_on{self.tag}"):
                self.arrived(10, self.ref(xr_, False, 1))
                self.send(5, self.ref(xr_, False, 1), left)
                self.send(12, self.ref(xr_, False, 1), twin)
                self.arrived(9, self.ref(xl_, False, 1))
                self.send(11, self.ref(xl_, False, 1), twin)

        def own(self):
            with sc(f"own{self.tag}"):
                self.arrived(2, self.ref(x, True, None))

        def near(self):
            with sc(f"near{self.tag}"):
                self.arrived(4, self.ref(xl_, True, 0))
                self.arrived(6, self.ref(xr_, True, 0))
                self.arrived(12, self.ref(xr_, True, 1))
                self.arrived(11, self.ref(xl_, True, 1))

        def pass_far(self):
            with sc(f"pass_far{self.tag}"):
                for part, i, j in ((0, 3, 7), (1, 5, 8)):
                    self.arrived(i, self.ref(xf_, False, part))
                    self.send(j, self.ref(xf_, False, part), twin)

        def far(self):
            with sc(f"far{self.tag}"):
                self.arrived(7, self.ref(xf_, True, 0))
                self.arrived(8, self.ref(xf_, True, 1))

        def finish(self):
            for c in self.sends:
                c.wait_send()

    def normed_of(buf):
        def ref(chip, other, part):
            rows = slice(None) if part is None else (d_low, d_high)[part]
            return buf.at[chip, rows, twin_lanes if other else my_lanes]

        return ref

    def kv_of(a):
        def ref(chip, other, part):
            h = D.seqs // 2
            span = pl.ds(a * D.seqs, D.seqs) if part is None else pl.ds(a * D.seqs + part * h, h)
            return kvland.at[chip * 2 + (1 - k if other else k), span]

        return ref

    half_dim = D.hd // 2

    def near3(i):
        return lax.rem(x + i + i // 2, n_x)

    def all4(i):
        return i

    def far1(i):
        return xf_

    def rope(p):
        lo_, hi_ = p[:half_dim], p[half_dim:]
        return jnp.concatenate([lo_ * cos_ref[...] - hi_ * sin_ref[...], hi_ * cos_ref[...] + lo_ * sin_ref[...]], axis=0)

    def project_q(l, a, seq_of, count):
        C = D.cfg[l]

        def body(i):
            s = seq_of(i)
            p = dot(wbuf[1, : C.q + D.kvp, :], ht[s]).astype(BF16).astype(F32)
            for h in range(C.heads):
                at = rows_at((a * D.seqs + s) * C.q + h * D.hd, D.hd)
                qt[at, :] = (rope(p[h * D.hd : (h + 1) * D.hd]) * D.hd**-0.5).astype(BF16)
            kvland[col, a * D.seqs + s] = p[C.q :].astype(BF16)

        with sc(f"q{l}{a}"):
            loop(0, count, body)

    def kv_copy(s, j, source):
        ref = kvland.at[source, s]
        return remote(ref, ref, kvs.at[s, j], kvr.at[s, j], row, lax.rem(col + j, n_col))

    def kv_send(seq_of, count):
        def body(i):
            s = seq_of(i)
            loop(1, n_col, lambda j: kv_copy(s, j, col).start())

        loop(0, count, body)

    def kv_arrive():
        def body(i):
            j = i // D.seqs + 1
            s = lax.rem(i, D.seqs)
            kv_copy(s, j, lax.rem(col + n_col - j, n_col)).wait_recv()
            kv_copy(s, j, col).wait_send()

        with sc("kvwait"):
            loop(0, D.seqs * (n_col - 1), body)

    def key_value(l, a):
        def body(i):
            s = a * D.seqs + i
            raw = kvland[:, s].reshape(n_col * D.kvp, D.seq)
            both = dot(perm_ref[...], raw)
            zeros = jnp.zeros((128 - D.hd, D.seq), F32)
            k_nat = jnp.concatenate([rope(both[: D.hd]), zeros], axis=0).T.astype(BF16)
            kn[s] = k_nat
            vt[s] = both[D.hd :].astype(BF16)
            if a == 0:
                kvbuf[l, 0, i] = k_nat
                kvbuf[l, 1, i] = jnp.concatenate([both[D.hd :], zeros], axis=0).T.astype(BF16)

        with sc(f"kv{l}{a}"):
            loop(0, D.seqs, body)

    qb = D.seq // 2

    def attention(l, a):
        C = D.cfg[l]

        pair = 2
        per = C.heads // pair

        def body(i):
            s, h0 = a * D.seqs + i // per, lax.rem(i, per) * pair
            q_rows = [rows_at(s * C.q + (h0 + e) * D.hd, D.hd) for e in range(pair)]
            o_rows = [rows_at(s * (C.q + C.f) + (h0 + e) * D.hd, D.hd) for e in range(pair)]
            for b in range(2):
                ext = (b + 1) * qb
                lanes = slice(b * qb, (b + 1) * qb)
                keys = lax.broadcasted_iota(jnp.int32, (ext, qb), 0)
                queries = lax.broadcasted_iota(jnp.int32, (ext, qb), 1) + b * qb
                scores = [dot(kn[s, :ext, : D.hd], qt[q_rows[e], lanes]) for e in range(pair)]
                for e in range(pair):
                    score = jnp.where(keys <= queries, scores[e], -1e30)
                    p = jnp.exp(score - jnp.max(score, axis=0, keepdims=True))
                    p = (p * (1.0 / jnp.sum(p, axis=0, keepdims=True))).astype(BF16)
                    jt[o_rows[e], lanes] = dot(vt[s, :, :ext], p).astype(BF16)

        with sc(f"attn{l}{a}"):
            loop(0, D.seqs * per, body)

    def gate_up(l, a, slot, j, seq_of, count):
        C = D.cfg[l]

        def body(i):
            s = seq_of(i)
            p = dot(wbuf[slot, : 2 * C.cw, :], ht[s])
            g = p[: C.cw].astype(BF16).astype(F32)
            u = p[C.cw :].astype(BF16).astype(F32)
            jt[rows_at((a * D.seqs + s) * (C.q + C.f) + C.q + j * C.cw, C.cw), :] = (g * jax.nn.sigmoid(g) * u).astype(BF16)

        loop(0, count, body)

    def gate_up_loop(l, a, seq_of, count, first, last, stop=None):
        C = D.cfg[l]
        stop = C.n_c if stop is None else stop
        have_chunk(l, min(last, stop - 1))

        def body(j):
            slot = lax.rem(j, 2)
            wait(w_fetch(l, "f", j, slot))

            @pl.when(j + 1 < stop)
            def _():
                start(w_fetch(l, "f", j + 1, 1 - slot))

            gate_up(l, a, slot, j, seq_of, count)

        with sc(f"gu{l}{a}"):
            loop(first, last, body)

    def have_chunk(l, j):
        C = D.cfg[l]
        have(l, "f", (j + 1) * C.cw // fch - 1)

    def load_q(l):
        have(l, "q", 0)
        copies = w_fetch(l, "q", 0, 1)
        start(copies)
        wait(copies)

    m = och * n_row
    m_low, m_high = pl.ds(0, m // 2), pl.ds(m // 2, m // 2)
    r_slots = twin_in.shape[0]
    r_step = 64

    def order(i):
        return lax.rem(x + lax.rem(2 + 3 * i, 4), n_x)

    class Reduce:
        def __init__(self, l):
            self.l, self.C, self.sends = l, D.cfg[l], {}

        def send(self, u, i, src, dst, c):
            copy = remote(src, dst, rss.at[u % r_slots, i], rsr.at[u % r_slots, i], row, c)
            copy.start()
            self.sends[u].append(copy)

        def arrived(self, u, i, ref):
            remote(ref, ref, rss.at[u % r_slots, i], rsr.at[u % r_slots, i], row, col).wait_recv()

        def twin_copy(self, u, i):
            us = u % r_slots
            return remote(ot.at[u % 2, order(i), :, twin_lanes], twin_in.at[us, i], rss.at[us, i], rsr.at[us, i], row, twin)

        def twin_done(self, u):
            loop(0, 4, lambda i: self.twin_copy(u, i).wait_send())

        def stage_a(self, u, a):
            C = self.C
            if u >= 2:
                self.twin_done(u - 2)
            if u >= r_slots - 1:
                for c in self.sends.pop(u - r_slots + 1):
                    c.wait_send()
            self.sends[u] = []
            R = C.q + C.f

            def body(i):
                s = order(i)
                ot[u % 2, s] = dot(wobuf[:, :R], jt[rows_at((a * D.seqs + s) * R, R), :]).astype(BF16)
                self.twin_copy(u, i).start()

            with sc(f"sa{self.l}_{u}"):
                loop(0, 4, body)

        def stage_b(self, u):
            us = u % r_slots

            def body(i):
                self.arrived(u, i, twin_in.at[us, i])
                s = order(i)

                def add(b):
                    at = rows_at(b * r_step, r_step)
                    twin_in[us, i, at, :] = (ot[u % 2, s, at, my_lanes].astype(F32) + twin_in[us, i, at, :].astype(F32)).astype(BF16)

                loop(0, m // r_step, add)

            far = [
                remote(twin_in.at[us, 0, m_low], far_in.at[us, m_low], rss.at[us, 4], rsr.at[us, 4], row, right),
                remote(twin_in.at[us, 0, m_high], far_in.at[us, m_high], rss.at[us, 5], rsr.at[us, 5], row, left),
            ]
            self.sends[u] += far

            def each(i):
                body(i)

                @pl.when(i == 0)
                def _():
                    start(far)

            with sc(f"sb{self.l}_{u}"):
                loop(0, 4, each)

        def stage_c(self, u):
            us = u % r_slots

            def add_far(i, base):
                def add(b):
                    at = rows_at(base + b * r_step, r_step)
                    twin_in[us, i, at, :] = (twin_in[us, i, at, :].astype(F32) + far_in[us, at, :].astype(F32)).astype(BF16)

                loop(0, m // 2 // r_step, add)

            with sc(f"sc{self.l}_{u}"):
                self.arrived(u, 4, far_in.at[us, m_low])
                add_far(1, 0)
                self.send(u, 6, twin_in.at[us, 1], near_in.at[us, 0], right)
                self.arrived(u, 5, far_in.at[us, m_high])
                add_far(3, m // 2)
                self.send(u, 7, twin_in.at[us, 3], near_in.at[us, 1], left)

        def add_update(self, j, total):
            step = min(r_step, och)
            for r in range(n_row):

                def add(b, r=r):
                    dst = rows_at(r * dr + (r + j) % D.n_o * och + b * step, step)
                    u = total(rows_at(r * och + b * step, step)).astype(BF16).astype(F32)
                    hid[dst, :] = (hid[dst, :].astype(F32) + u).astype(BF16)

                loop(0, och // step, add)

        def stage_d(self, u, j, a):
            us = u % r_slots

            def total(at):
                return twin_in[us, 2, at, :].astype(F32) + near_in[us, 0, at, :].astype(F32) + near_in[us, 1, at, :].astype(F32)

            with sc(f"sd{self.l}_{u}"):
                self.arrived(u, 6, near_in.at[us, 0])
                self.arrived(u, 7, near_in.at[us, 1])
                if self.C.split:

                    def save(b):
                        at = rows_at(b * r_step, r_step)
                        psum[a, j, at, :] = total(at).astype(BF16)

                    loop(0, m // r_step, save)
                    if a == 1:
                        remote(psum.at[1, j], pair_in.at[j], es.at[j], er.at[j], mate, col).start()
                else:
                    self.add_update(j, total)

        def stage_e(self, j):
            with sc(f"se{self.l}_{j}"):
                c = remote(psum.at[1, j], pair_in.at[j], es.at[j], er.at[j], mate, col)
                c.wait_recv()
                self.add_update(j, lambda at: psum[0, j, at, :].astype(F32) + pair_in[j, at, :].astype(F32))
                c.wait_send()

        def finish(self, units):
            with sc(f"rfin{self.l}"):
                for u in range(max(0, units - 2), units):
                    self.twin_done(u)
                for u in self.sends:
                    for c in self.sends[u]:
                        c.wait_send()

    o_started = set()

    def o_load(l, j, a):
        if (l, j, a) not in o_started:
            have(l, "o", j)
            start(o_fetch(l, j, j % 2))
            o_started.add((l, j, a))

    def o_use(l, j, a):
        C = D.cfg[l]
        with sc(f"ouse{l}_{j}"):
            o_load(l, j, a)
            wait(o_fetch(l, j, j % 2))
            R = C.q + C.f
            for r in range(n_row):
                wobuf[r * och : (r + 1) * och, :R] = wonat[j % 2, :R, r * och : (r + 1) * och].T

    layer_norm(0)
    g0 = Gather(normed_of(ht), 0)
    mine = ht.at[x, :, my_lanes]
    shared = g_h.at[x, :, my_lanes]
    to_mate = remote(mine, shared, ps, pr_, mate, col)
    to_mate.start()
    relay_to(1)
    mate_to(step(0, 5))
    peer_to(step(0, 5))
    g0.pass_low()
    g0.pass_on()
    with sc("mate"):
        to_mate.wait_recv()
    g1 = Gather(normed_of(g_h), 1)
    load_q(0)
    g0.own()
    g0.near()
    project_q(0, 0, near3, 3)
    relay_to(2)
    mate_to(step(0, 10))
    g0.pass_far()
    g0.far()
    project_q(0, 0, far1, 1)
    kv0 = Gather(kv_of(0), 2)
    relay_to(3)
    n_f = D.cfg[0].n_f
    f_started = set()

    def f_load(j):
        if j not in f_started:
            f_started.add(j)
            start(w_fetch(0, "f", j, j % 2))

    def h_copy(i):
        return pltpu.make_async_copy(g_h.at[i], ht.at[i], lh.at[i])

    have(0, "f", 0)
    f_load(0)
    gate_up_loop(0, 0, all4, 4, 0, 2, 2)
    relay_to(step(0, 4))
    for j in range(2, n_f):
        have(0, "f", j)
        f_load(j)
        with sc(f"gu0_{j}"):
            wait(w_fetch(0, "f", j, j % 2))
            gate_up(0, 0, j % 2, j, all4, 4)
        if j == max(2, n_f - 3):
            relay_to(step(0, 5))
            peer_to(step(0, 6))
            relay_to(step(0, 6))
            peer_to(step(0, 7))
    kv0.pass_low()
    kv0.pass_on()
    g1.pass_low()
    g1.pass_on()
    for t in (7, 8):
        relay_to(step(0, t))
        peer_to(step(0, t + 1))
    relay_to(step(0, 9))
    peer_to(step(0, 10))
    relay_to(step(0, 10))
    peer_to(step(1, 5))
    mate_to(step(1, D.cfg[1].n_f - 2))
    g0.finish()
    to_mate.wait_send()
    g1.own()
    g1.near()
    loop(0, 3, lambda i: h_copy(near3(i)).start())
    kv0.pass_far()
    with sc("kv0wait"):
        kv0.own()
        kv0.near()
        kv0.far()
        kv0.finish()
    key_value(0, 0)
    attention(0, 0)

    red = Reduce(0)
    units = [(j, 0) for j in range(D.n_o - 1)] + [(j, 1) for j in range(D.n_o)] + [(D.n_o - 1, 0)]
    n_u = len(units)
    first = D.n_o - 1
    state = {"e": 0}

    def settle(count):
        while state["e"] < count:
            red.stage_e(state["e"])
            state["e"] += 1

    def unit(u):
        j, a = units[u]
        if u == 0 or units[u - 1][0] != j:
            o_use(0, j, a)
        red.stage_a(u, a)
        if u + 1 < n_u and units[u + 1][0] != j:
            o_load(0, *units[u + 1])
        if u >= 2:
            red.stage_c(u - 2)
        if u >= 3:
            red.stage_d(u - 3, *units[u - 3])
        red.stage_b(u)

    unit(0)
    g1.pass_far()
    unit(1)
    g1.far()
    h_copy(xf_).start()
    load_q(0)
    start(w_fetch(0, "f", 0, 0))
    loop(0, 3, lambda i: h_copy(near3(i)).wait())
    h_copy(xf_).wait()
    project_q(0, 1, all4, 4)
    kv1 = Gather(kv_of(1), 3)
    parts = first - 2
    cuts = [n_f * i // parts for i in range(parts + 1)]
    for u in range(2, first):
        unit(u)
        if u == 2:
            kv1.pass_low()
            kv1.pass_on()
        gate_up_loop(0, 1, all4, 4, cuts[u - 2], cuts[u - 1])
    kv1.pass_far()
    relay_to(step(1, 1))
    with sc("kv1wait"):
        kv1.own()
        kv1.near()
        kv1.far()
        kv1.finish()
    key_value(0, 1)
    attention(0, 1)
    g1.finish()
    relay_to(step(1, 2))
    peer_to(step(1, 7))
    n_f1 = D.cfg[1].n_f
    for u in range(first, n_u):
        unit(u)
        v = u - first
        if v in (0, 1, 2):
            relay_to(step(1, min(v + 3, n_f1 - 2)))
        if v == 1:
            peer_to(step(1, min(8, n_f1)))
        elif v == 4:
            relay_to(step(1, min(6, n_f1 - 2)))
            peer_to(step(1, min(9, n_f1)))
        elif v == 5:
            peer_to(step(1, n_f1))
    relay_to(step(1, min(6, n_f1 - 2)))
    peer_to(step(1, n_f1))
    red.stage_c(n_u - 2)
    red.stage_d(n_u - 3, *units[n_u - 3])
    red.stage_c(n_u - 1)
    red.stage_d(n_u - 2, *units[n_u - 2])
    mate_to(step(1, n_f1))
    settle(D.n_o - 1)
    red.stage_d(n_u - 1, *units[n_u - 1])
    settle(D.n_o)
    red.finish(n_u)

    def slice_of(d):
        return hid.at[rows_at(d * dl, dl), :]

    own_y = pltpu.make_async_copy(slice_of(me), piece_of(y_out, me), xr.at[0])

    def y_copy_back(i):
        d = lax.rem(me + i, n)
        return remote(slice_of(d), piece_of(y_out, me), xs.at[i], xr.at[i], d // n_col, lax.rem(d, n_col))

    def y_send_back(i):
        @pl.when(i == 0)
        def _():
            own_y.start()

        @pl.when(i != 0)
        def _():
            y_copy_back(i).start()

    def y_finish(i):
        s = lax.rem(me + n - i, n)
        remote(piece_of(y_out, s), piece_of(y_out, s), xs.at[i], xr.at[i], row, col).wait_recv()
        y_copy_back(i).wait_send()

    def y_ready(low, high):
        def body(i):
            d = lax.rem(me + i, n)
            r, a = d // n_col, lax.rem(d, n_col) * dl
            first = lax.rem(a // och + D.n_o - lax.rem(r, D.n_o), D.n_o)
            second = lax.rem((a + dl - 1) // och + D.n_o - lax.rem(r, D.n_o), D.n_o)

            done = jnp.maximum(first, second)

            @pl.when((low <= done) & (done < high))
            def _():
                y_send_back(i)

        loop(0, n, body)

    for l in range(1, D.layers):
        C = D.cfg[l]
        layer_norm(l)
        g0 = Gather(normed_of(ht), 0)
        peer_to(step(l, C.n_f))
        mate_to(step(l, C.n_f))
        relay_to(step(l, min(8, C.n_f)))
        own1, near2 = (lambda i: x), (lambda i: lax.rem(x + 1 + 2 * i, n_x))
        n_mid = min(3, C.n_c - 1)

        def begin(seq_of, count):
            load_q(l)
            have_chunk(l, 0)
            start(w_fetch(l, "f", 0, 0))
            project_q(l, 0, seq_of, count)

        g0.own()
        begin(own1, 1)
        kv_send(own1, 1)
        gate_up_loop(l, 0, own1, 1, 0, n_mid, n_mid)
        g0.pass_low()
        relay_to(step(l, C.n_f))
        peer_to(step(l, C.n_f + 2))
        mate_to(step(l, C.n_f + 2))
        g0.pass_on()
        g0.near()
        begin(near2, 2)
        kv_send(near2, 2)
        gate_up_loop(l, 0, near2, 2, 0, n_mid)
        g0.pass_far()
        relay_to(step(l, C.n_f + 1))
        peer_to(step(l, C.n_f + 4))
        mate_to(step(l, C.n_f + 4))
        gate_up_loop(l, 0, near3, 3, n_mid, C.n_c)
        relay_to(step(l, C.n_f + 2))
        g0.far()
        begin(far1, 1)
        kv_send(far1, 1)
        gate_up_loop(l, 0, far1, 1, 0, C.n_c)
        peer_to(step(l, C.n_f + D.n_o))
        mate_to(step(l, C.n_f + D.n_o))
        relay_to(step(l, C.n_f + 3))
        g0.finish()
        kv_arrive()
        key_value(l, 0)
        attention(l, 0)
        relay_to(step(l, C.n_f + 4))
        red = Reduce(l)
        last = l + 1 == D.layers

        end = D.n_o - 1
        for j in range(D.n_o):
            o_use(l, j, 0)
            red.stage_a(j, 0)
            if j == 1:
                relay_to(step(l, C.n_f + D.n_o))
            if j < end:
                o_load(l, j + 1, 0)
            if 2 <= j:
                red.stage_c(j - 2)
            if 3 <= j:
                red.stage_d(j - 3, j - 3, 0)
            red.stage_b(j)
        red.stage_c(end - 1)
        red.stage_d(end - 2, end - 2, 0)
        red.stage_c(end)
        red.stage_d(end - 1, end - 1, 0)
        if last:
            with sc("send"):
                y_ready(0, end)
        red.stage_d(end, end, 0)
        if last:
            y_ready(end, end + 1)
        red.finish(D.n_o)

    def kv_back(i):
        r = lax.rem(row + i, n_row)
        pos = rows_at((r * n_col + col) * D.pos, D.pos)
        return kvbuf.at[:, :, :, pos, :], kv_out.at[:, :, pl.ds(row * D.seqs, D.seqs)], r

    src, dst, _ = kv_back(0)
    own_kv = pltpu.make_async_copy(src, dst, fl)
    own_kv.start()
    kv_sends = []
    for i in range(1, n_row):
        src, dst, r = kv_back(i)
        c = remote(src, dst, fs.at[i], fr.at[i], r, col)
        c.start()
        kv_sends.append(c)

    with sc("ywait"):
        loop(1, n, y_finish)
        own_y.wait()
        own_kv.wait()
        for i in range(1, n_row):
            r = lax.rem(row + n_row - i, n_row)
            dst = kv_out.at[:, :, pl.ds(r * D.seqs, D.seqs)]
            remote(dst, dst, fs.at[i], fr.at[i], row, col).wait_recv()
        for c in kv_sends:
            c.wait_send()
        for c in y_sent:
            c.wait_send()


def solution(mesh):
    n_row, n_col = mesh.shape["row"], mesh.shape["col"]
    group = n_row * n_col
    act_spec = P("dp", None, ("row", "col"))
    weight_spec = P(None, "row", "col")

    def device_fn(x_loc, gain_loc, w_in_loc, w_kv_loc, w_out_loc):
        D = Dims()
        D.n_row, D.n_col = n_row, n_col
        n_batch, D.seq, D.dl = x_loc.shape
        D.layers, D.dr, e = w_in_loc.shape
        D.d = D.dl * group
        r_block = w_out_loc.shape[1]
        D.f = e - r_block
        D.q = r_block - D.f
        kv_local = w_kv_loc.shape[2]
        D.hd = kv_local * n_col // 2
        D.kvp = 32
        D.tok = n_batch * D.seq // group
        D.seqs = n_batch // n_row
        D.pos = D.seq // group
        D.fch = 128
        D.och = 128
        D.n_o = D.dr // D.och
        D.cfg = []
        for l in range(D.layers):
            C = Dims()
            C.split = l == 0
            parts = 2 if C.split else 1
            C.q, C.f = D.q // parts, D.f // parts
            C.heads, C.n_f = C.q // D.hd, C.f // D.fch
            C.cw = D.fch if C.split else 2 * D.fch
            C.n_c = C.f // C.cw
            D.cfg.append(C)
        assert D.seq == 2 * D.tok and D.seqs == n_col // 2 == n_row == 4

        half = D.hd // 2
        inv_freq = (np.float32(1.0) / (np.float32(10000.0) ** (np.arange(half, dtype=np.float32) * np.float32(2.0) / np.float32(D.hd)))).astype(np.float32)
        angles = (inv_freq[:, None] * np.arange(D.seq, dtype=np.float32)[None, :]).astype(np.float32)
        cos_t, sin_t = np.cos(angles).astype(np.float32), np.sin(angles).astype(np.float32)
        perm = np.zeros((2 * D.hd, n_col * D.kvp), np.float32)
        for i in range(2 * D.hd):
            perm[i, (i // kv_local) * D.kvp + i % kv_local] = 1.0

        x_t = x_loc.transpose(0, 2, 1)
        w_t = w_in_loc.transpose(0, 2, 1)
        wkv_t = jnp.pad(w_kv_loc.transpose(0, 2, 1), ((0, 0), (0, D.kvp - kv_local), (0, 0)))
        gains = jnp.pad(gain_loc, ((0, 16 - D.layers), (0, 128 - D.dl)))

        n_y = sum(12 + 6 * (C.n_f + D.n_o) for C in D.cfg)
        m = D.och * n_row
        sds = jax.ShapeDtypeStruct
        dma = pltpu.SemaphoreType.DMA
        out = pl.pallas_call(
            functools.partial(kernel, D),
            out_shape=(
                sds(x_t.shape, BF16),
                sds((D.layers, 2, n_batch, D.pos, 128), BF16),
                sds((D.layers, e, D.d), BF16),
                sds((D.layers, D.kvp, D.d), BF16),
                sds((D.layers, n_row, r_block, D.dr), BF16),
                sds((D.seqs, D.d, D.seq), BF16),
            ),
            in_specs=[ANY] * 5 + [VMEM] * 3,
            out_specs=(ANY,) * 6,
            scratch_shapes=[
                pltpu.VMEM((group, D.dl, D.tok), BF16),
                pltpu.VMEM((group, 16, 128), BF16),
                pltpu.VMEM((D.layers, D.d, 128), F32),
                pltpu.VMEM((D.d, D.tok), BF16),
                pltpu.VMEM((D.seqs, D.d, D.seq), BF16),
                pltpu.VMEM((2, max(4 * D.fch, D.q + D.kvp), D.d), BF16),
                pltpu.VMEM((2, r_block, m), BF16),
                pltpu.VMEM((m, r_block), BF16),
                pltpu.VMEM((D.seqs * D.q, D.seq), BF16),
                pltpu.VMEM((n_col, 2 * D.seqs, D.kvp, D.seq), BF16),
                pltpu.VMEM((2 * D.seqs, D.seq, 128), BF16),
                pltpu.VMEM((2 * D.seqs, D.hd, D.seq), BF16),
                pltpu.VMEM((D.layers, 2, D.seqs, D.seq, 128), BF16),
                pltpu.VMEM((D.seqs * r_block, D.seq), BF16),
                pltpu.VMEM((2, D.seqs, m, D.seq), BF16),
                pltpu.VMEM((5, 4, m, D.tok), BF16),
                pltpu.VMEM((5, m, D.tok), BF16),
                pltpu.VMEM((5, 2, m, D.tok), BF16),
                pltpu.VMEM((2, D.n_o, m, D.tok), BF16),
                pltpu.VMEM((D.n_o, m, D.tok), BF16),
                dma((group,)), dma((group,)), dma((group,)), dma((group,)),
                dma((n_y,)), dma((n_y,)),
                dma((4, 13)), dma((4, 13)), dma, dma,
                dma((D.seqs, n_col)), dma((D.seqs, n_col)),
                dma((5, 8)), dma((5, 8)),
                dma((D.n_o,)), dma((D.n_o,)),
                dma((2, 8)), dma((2, 8)), dma((D.seqs,)),
                dma((n_row,)), dma((n_row,)), dma,
            ],
            compiler_params=pltpu.CompilerParams(collective_id=0, has_side_effects=True, vmem_limit_bytes=67_000_000),
            name="two_layers",
        )(x_t, gains, w_t, wkv_t, w_out_loc, jnp.asarray(cos_t), jnp.asarray(sin_t), jnp.asarray(perm, BF16))
        return out[0].transpose(0, 2, 1), out[1][..., : D.hd]

    return jax.shard_map(device_fn, mesh=mesh, in_specs=(act_spec, P(None, ("row", "col")), weight_spec, weight_spec, P(None, "col", "row")), out_specs=(act_spec, P(None, None, "dp", ("row", "col"), None)), check_vma=False)
```

```python
import functools

import numpy as np

import jax
import jax.numpy as jnp
from jax import lax
from jax.experimental import pallas as pl
from jax.experimental.pallas import tpu as pltpu
from jax.sharding import PartitionSpec as P

LN_EPS = 1e-6
MESH = pl.DeviceIdType.MESH
ANY = pl.BlockSpec(memory_space=pl.ANY)
VMEM = pl.BlockSpec(memory_space=pltpu.VMEM)
F32, BF16 = jnp.float32, jnp.bfloat16


def dot(a, b):
    return jnp.dot(a, b, preferred_element_type=F32)


class Dims:
    pass


def rows_at(start, count, by=16):
    return pl.ds(start if isinstance(start, int) else pl.multiple_of(start, by), count)


def kernel(
    D,
    x_t, gains, w_t, wkv_t, w_o, cos_ref, sin_ref, perm_ref,
    y_out, kv_out, g_w, g_kv, g_wo, g_h,
    xland, gland, gcol, hid, ht, wbuf, wonat, wobuf, qt, kvland, kn, vt, kvbuf, jt, ot, twin_in, far_in, near_in, psum, pair_in,
    xs, xr, gs, gr, ys, yr, ags, agr, ps, pr_, kvs, kvr, rss, rsr, es, er, lw, lo, lh, fs, fr, fl,
):
    sc = jax.named_scope
    row, col = lax.axis_index("row"), lax.axis_index("col")
    n_row, n_col, n = D.n_row, D.n_col, D.n_row * D.n_col
    n_x = n_col // 2
    me = row * n_col + col
    x, k = col // 2, lax.rem(col, 2)
    xr_, xl_, xf_ = lax.rem(x + 1, n_x), lax.rem(x + n_x - 1, n_x), lax.rem(x + 2, n_x)
    right, left, twin = xr_ * 2 + k, xl_ * 2 + k, x * 2 + 1 - k
    up, down, across = lax.rem(row + 1, n_row), lax.rem(row + n_row - 1, n_row), lax.rem(row + 2, n_row)
    half, mate = row // 2, n_row - 1 - row
    peer = row + 1 - 2 * lax.rem(row, 2)
    tok, dl, dr = D.tok, D.dl, D.dr
    och, fch = D.och, D.fch
    my_lanes = pl.ds(pl.multiple_of(k * tok, 128), tok)
    twin_lanes = pl.ds(pl.multiple_of((1 - k) * tok, 128), tok)

    def remote(src, dst, ssem, rsem, r, c):
        return pltpu.make_async_remote_copy(src_ref=src, dst_ref=dst, send_sem=ssem, recv_sem=rsem, device_id={"row": r, "col": c}, device_id_type=MESH)

    def loop(lo_, hi_, f):
        def body(i, carry):
            f(i)
            return carry

        lax.fori_loop(lo_, hi_, body, 0)

    barrier = pltpu.get_barrier_semaphore()

    def greet(i):
        d = lax.rem(me + i, n)
        pl.semaphore_signal(barrier, inc=1, device_id={"row": d // n_col, "col": lax.rem(d, n_col)}, device_id_type=MESH)

    with sc("barrier"):
        loop(1, n, greet)
        pl.semaphore_wait(barrier, n - 1)

    def piece_of(ref, d):
        return ref.at[d // 2, :, pl.ds(pl.multiple_of(lax.rem(d, 2) * tok, 128), tok)]

    def x_copy(i):
        d = lax.rem(me + i, n)
        return remote(piece_of(x_t, d), xland.at[me], xs.at[i], xr.at[i], d // n_col, lax.rem(d, n_col))

    def g_copy(i):
        d = lax.rem(me + i, n)
        return remote(gains, gland.at[me], gs.at[i], gr.at[i], d // n_col, lax.rem(d, n_col))

    own_x = pltpu.make_async_copy(piece_of(x_t, me), xland.at[me], xr.at[0])
    own_g = pltpu.make_async_copy(gains, gland.at[me], gr.at[0])
    own_x.start()
    own_g.start()
    def x_first(i):
        x_copy(i).start()
        g_copy(i).start()

    loop(1, n, x_first)

    def own_lanes(r):
        return pl.ds(pl.multiple_of(r * dr, 128), dr)

    def o_lanes(j, r):
        return pl.ds(pl.multiple_of(lax.rem(r + j, D.n_o) * och, 128), och)

    steps = []
    for l, C in enumerate(D.cfg):
        steps += [(l, "q", 0)] + [(l, "f", j) for j in range(C.n_f)] + [(l, "o", j) for j in range(D.n_o)]
    n_steps = len(steps)
    step_of = {s: t for t, s in enumerate(steps)}

    def blocks(t, i):
        l, kind, j = steps[t]
        C = D.cfg[l]
        out = []

        def w_rows(a, m):
            at = rows_at(a, m)
            out.append((w_t.at[l, at, :], lambda r: g_w.at[l, at, own_lanes(r)]))

        def o_rows(a, m):
            at = rows_at(a, m)
            out.append((w_o.at[l, at, o_lanes(j, row)], lambda r: g_wo.at[l, r, at, o_lanes(j, r)]))

        def kv_rows(a, m):
            at = pl.ds(a, m)
            out.append((wkv_t.at[l, at, :], lambda r: g_kv.at[l, at, own_lanes(r)]))

        if kind == "q":
            for a in (0, C.q // 2):
                w_rows(i * C.q + a, C.q // 2)
            for a in (0, D.kvp // 2):
                kv_rows(a, D.kvp // 2)
        elif kind == "f":
            w_rows(D.q + i * C.f + j * fch, fch)
            w_rows(D.q + D.f + i * C.f + j * fch, fch)
        elif C.split:
            o_rows(i * C.q, C.q)
            o_rows(D.q + i * C.f, C.f)
        else:
            for a in (0, (D.q + D.f) // 2):
                o_rows(a, (D.q + D.f) // 2)
        return out

    base, n_sems = [], 0
    for l, kind, j in steps:
        base.append(n_sems)
        n_sems += 12 if kind == "q" else 6
    assert n_sems == ys.shape[0]
    y_sent = []

    def y_copy(t, i, kind, src, dst, r):
        at = base[t] + 3 * i + kind
        return remote(src, dst, ys.at[at], yr.at[at], r, col)

    def y_send(*args):
        c = y_copy(*args)
        c.start()
        y_sent.append(c)

    def issue_peer(t):
        for i, (src, place) in enumerate(blocks(t, half if D.cfg[steps[t][0]].split else 0)):
            y_send(t, i, 0, src, place(row), peer)

    def issue_mate(t):
        for i, (src, place) in enumerate(blocks(t, 1 - half if D.cfg[steps[t][0]].split else 0)):
            y_send(t, i, 1, src, place(row), mate)

    def relay(t):
        split = D.cfg[steps[t][0]].split
        with sc(f"relay{t}"):
            for i, (src, place) in enumerate(blocks(t, half if split else 0)):
                y_copy(t, i, 1, src, place(mate), mate).wait_recv()
                if split or i % 2 == 0:
                    y_send(t, i, 2, place(mate), place(mate), peer)
                if not split:
                    y_copy(t, i, 0, src, place(peer), peer).wait_recv()
                    if i % 2 == 1:
                        y_send(t, i, 2, place(peer), place(peer), mate)

    at = {"next": 0, "peer": 0, "mate": 0, "relay": 0}
    first_of = {l: min(t for t, st in enumerate(steps) if st[0] == l) for l in range(D.layers)}

    def step(l, j):
        return min(first_of[l] + j, first_of.get(l + 1, n_steps) - 1)

    def peer_to(t):
        while at["peer"] <= t:
            issue_peer(at["peer"])
            at["peer"] += 1

    def mate_to(t):
        while at["mate"] <= t:
            issue_mate(at["mate"])
            at["mate"] += 1

    def relay_to(t):
        assert t < at["peer"] and t < at["mate"]
        while at["relay"] <= t:
            relay(at["relay"])
            at["relay"] += 1

    def advance():
        t = at["next"]
        assert t < at["relay"], t
        rest = n_row - 1 - peer
        with sc(f"adv{t}"):
            split = D.cfg[steps[t][0]].split
            for i, (src, place) in enumerate(blocks(t, half if split else 0)):
                if split:
                    y_copy(t, i, 0, src, place(peer), peer).wait_recv()
                y_copy(t, i, 2, src, place(rest), rest).wait_recv()
            at["next"] = t + 1

    def have(*which):
        while at["next"] <= step_of[which]:
            advance()

    mate_to(1)
    peer_to(step(0, 3))

    def w_fetch(l, kind, j, slot):
        C = D.cfg[l]
        i = half if C.split else 0
        copies = []

        def fetch(src, dst):
            copies.append(pltpu.make_async_copy(src, dst, lw.at[slot, len(copies)]))

        def w_rows(a, m, at):
            a, at = rows_at(a, m), pl.ds(at, m)
            fetch(w_t.at[l, a, :], wbuf.at[slot, at, own_lanes(row)])
            for r in (up, down, across):
                fetch(g_w.at[l, a, own_lanes(r)], wbuf.at[slot, at, own_lanes(r)])

        if kind == "q":
            w_rows(i * C.q, C.q, 0)
            at = pl.ds(C.q, D.kvp)
            fetch(wkv_t.at[l], wbuf.at[slot, at, own_lanes(row)])
            for r in (up, down, across):
                fetch(g_kv.at[l, :, own_lanes(r)], wbuf.at[slot, at, own_lanes(r)])
        else:
            w_rows(D.q + i * C.f + j * C.cw, C.cw, 0)
            w_rows(D.q + D.f + i * C.f + j * C.cw, C.cw, C.cw)
        return copies

    def o_fetch(l, j, slot):
        C = D.cfg[l]
        copies = []

        def fetch(src, dst):
            copies.append(pltpu.make_async_copy(src, dst, lo.at[slot, len(copies)]))

        spans = ((half * C.q, 0, C.q), (D.q + half * C.f, C.q, C.f)) if C.split else ((0, 0, C.q + C.f),)
        for a, at, m in spans:
            a, at = rows_at(a, m), pl.ds(at, m)
            to = lambda r: pl.ds(pl.multiple_of(r * och, 128), och)
            fetch(w_o.at[l, a, o_lanes(j, row)], wonat.at[slot, at, to(row)])
            for r in (up, down, across):
                fetch(g_wo.at[l, r, a, o_lanes(j, r)], wonat.at[slot, at, to(r)])
        return copies

    def start(copies):
        for c in copies:
            c.start()

    def wait(copies):
        for c in copies:
            c.wait()

    own_x.wait()
    own_g.wait()

    def x_finish(i):
        s = lax.rem(me + n - i, n)
        remote(xland.at[s], xland.at[s], xs.at[i], xr.at[i], row, col).wait_recv()
        remote(gland.at[s], gland.at[s], gs.at[i], gr.at[i], row, col).wait_recv()
        x_copy(i).wait_send()
        g_copy(i).wait_send()

    with sc("xwait"):
        loop(1, n, x_finish)

    def keep(d):
        hid[rows_at(d * dl, dl), :] = xland[d]

    with sc("gains"):
        loop(0, n, keep)
        g_all = gland[...].astype(F32)
        for l in range(D.layers):
            g_rows = g_all[:, l, :]
            g_rows = jnp.concatenate([g_rows, jnp.zeros((128 - n, 128), F32)], axis=0) if n < 128 else g_rows
            g_cols = g_rows.T
            for d in range(n):
                gcol[l, d * dl : (d + 1) * dl, :] = jnp.broadcast_to(g_cols[:dl, d : d + 1], (dl, 128))

    blk = 64
    n_blk = D.d // blk

    def layer_norm(l):
        def add_up(i, acc):
            v = hid[rows_at(i * blk, blk), :].astype(F32)
            return acc + v.reshape(blk // 8, 8, tok).sum(axis=0)

        mean = lax.fori_loop(0, n_blk, add_up, jnp.zeros((8, tok), F32)).sum(axis=0, keepdims=True) / D.d

        def add_sq(i, acc):
            v = hid[rows_at(i * blk, blk), :].astype(F32) - mean
            return acc + (v * v).reshape(blk // 8, 8, tok).sum(axis=0)

        var = lax.fori_loop(0, n_blk, add_sq, jnp.zeros((8, tok), F32)).sum(axis=0, keepdims=True) / D.d
        scale = lax.rsqrt(var + LN_EPS)

        def write(i):
            rows = rows_at(i * blk, blk)
            g = gcol[l, rows, :]
            g = jnp.concatenate([g] * (tok // 128), axis=1)
            v = (hid[rows, :].astype(F32) - mean) * scale * g
            ht[x, rows, my_lanes] = v.astype(BF16)

        with sc(f"norm{l}"):
            loop(0, n_blk, write)

    d_low, d_high = pl.ds(0, D.d // 2), pl.ds(D.d // 2, D.d // 2)

    class Gather:
        def __init__(self, ref, tag):
            self.ref, self.tag, self.sends = ref, tag, []
            for i, part, c in ((0, 0, right), (1, 0, left), (2, None, twin), (9, 1, right), (10, 1, left)):
                self.send(i, ref(x, False, part), c)

        def send(self, i, ref, c):
            copy = remote(ref, ref, ags.at[self.tag, i], agr.at[self.tag, i], row, c)
            copy.start()
            self.sends.append(copy)

        def arrived(self, i, ref):
            remote(ref, ref, ags.at[self.tag, i], agr.at[self.tag, i], row, col).wait_recv()

        def pass_low(self):
            with sc(f"pass_low{self.tag}"):
                self.arrived(0, self.ref(xl_, False, 0))
                self.send(3, self.ref(xl_, False, 0), right)
                self.send(4, self.ref(xl_, False, 0), twin)
                self.arrived(1, self.ref(xr_, False, 0))
                self.send(6, self.ref(xr_, False, 0), twin)

        def pass_on(self):
            with sc(f"pass_on{self.tag}"):
                self.arrived(10, self.ref(xr_, False, 1))
                self.send(5, self.ref(xr_, False, 1), left)
                self.send(12, self.ref(xr_, False, 1), twin)
                self.arrived(9, self.ref(xl_, False, 1))
                self.send(11, self.ref(xl_, False, 1), twin)

        def own(self):
            with sc(f"own{self.tag}"):
                self.arrived(2, self.ref(x, True, None))

        def near(self):
            with sc(f"near{self.tag}"):
                self.arrived(4, self.ref(xl_, True, 0))
                self.arrived(6, self.ref(xr_, True, 0))
                self.arrived(12, self.ref(xr_, True, 1))
                self.arrived(11, self.ref(xl_, True, 1))

        def pass_far(self):
            with sc(f"pass_far{self.tag}"):
                for part, i, j in ((0, 3, 7), (1, 5, 8)):
                    self.arrived(i, self.ref(xf_, False, part))
                    self.send(j, self.ref(xf_, False, part), twin)

        def far(self):
            with sc(f"far{self.tag}"):
                self.arrived(7, self.ref(xf_, True, 0))
                self.arrived(8, self.ref(xf_, True, 1))

        def finish(self):
            for c in self.sends:
                c.wait_send()

    def normed_of(buf):
        def ref(chip, other, part):
            rows = slice(None) if part is None else (d_low, d_high)[part]
            return buf.at[chip, rows, twin_lanes if other else my_lanes]

        return ref

    def kv_of(a):
        def ref(chip, other, part):
            h = D.seqs // 2
            span = pl.ds(a * D.seqs, D.seqs) if part is None else pl.ds(a * D.seqs + part * h, h)
            return kvland.at[chip * 2 + (1 - k if other else k), span]

        return ref

    half_dim = D.hd // 2

    def near3(i):
        return lax.rem(x + i + i // 2, n_x)

    def all4(i):
        return i

    def far1(i):
        return xf_

    def rope(p):
        lo_, hi_ = p[:half_dim], p[half_dim:]
        return jnp.concatenate([lo_ * cos_ref[...] - hi_ * sin_ref[...], hi_ * cos_ref[...] + lo_ * sin_ref[...]], axis=0)

    def project_q(l, a, seq_of, count):
        C = D.cfg[l]

        def body(i):
            s = seq_of(i)
            p = dot(wbuf[1, : C.q + D.kvp, :], ht[s]).astype(BF16).astype(F32)
            for h in range(C.heads):
                at = rows_at((a * D.seqs + s) * C.q + h * D.hd, D.hd)
                qt[at, :] = (rope(p[h * D.hd : (h + 1) * D.hd]) * D.hd**-0.5).astype(BF16)
            kvland[col, a * D.seqs + s] = p[C.q :].astype(BF16)

        with sc(f"q{l}{a}"):
            loop(0, count, body)

    def kv_copy(s, j, source):
        ref = kvland.at[source, s]
        return remote(ref, ref, kvs.at[s, j], kvr.at[s, j], row, lax.rem(col + j, n_col))

    def kv_send(seq_of, count):
        def body(i):
            s = seq_of(i)
            loop(1, n_col, lambda j: kv_copy(s, j, col).start())

        loop(0, count, body)

    def kv_arrive():
        def body(i):
            j = i // D.seqs + 1
            s = lax.rem(i, D.seqs)
            kv_copy(s, j, lax.rem(col + n_col - j, n_col)).wait_recv()
            kv_copy(s, j, col).wait_send()

        with sc("kvwait"):
            loop(0, D.seqs * (n_col - 1), body)

    def key_value(l, a):
        def body(i):
            s = a * D.seqs + i
            raw = kvland[:, s].reshape(n_col * D.kvp, D.seq)
            both = dot(perm_ref[...], raw)
            zeros = jnp.zeros((128 - D.hd, D.seq), F32)
            k_nat = jnp.concatenate([rope(both[: D.hd]), zeros], axis=0).T.astype(BF16)
            kn[s] = k_nat
            vt[s] = both[D.hd :].astype(BF16)
            if a == 0:
                kvbuf[l, 0, i] = k_nat
                kvbuf[l, 1, i] = jnp.concatenate([both[D.hd :], zeros], axis=0).T.astype(BF16)

        with sc(f"kv{l}{a}"):
            loop(0, D.seqs, body)

    qb = D.seq // 2

    def attention(l, a):
        C = D.cfg[l]

        pair = 2
        per = C.heads // pair

        def body(i):
            s, h0 = a * D.seqs + i // per, lax.rem(i, per) * pair
            q_rows = [rows_at(s * C.q + (h0 + e) * D.hd, D.hd) for e in range(pair)]
            o_rows = [rows_at(s * (C.q + C.f) + (h0 + e) * D.hd, D.hd) for e in range(pair)]
            for b in range(2):
                ext = (b + 1) * qb
                lanes = slice(b * qb, (b + 1) * qb)
                keys = lax.broadcasted_iota(jnp.int32, (ext, qb), 0)
                queries = lax.broadcasted_iota(jnp.int32, (ext, qb), 1) + b * qb
                scores = [dot(kn[s, :ext, : D.hd], qt[q_rows[e], lanes]) for e in range(pair)]
                for e in range(pair):
                    score = jnp.where(keys <= queries, scores[e], -1e30)
                    p = jnp.exp(score - jnp.max(score, axis=0, keepdims=True))
                    p = (p * (1.0 / jnp.sum(p, axis=0, keepdims=True))).astype(BF16)
                    jt[o_rows[e], lanes] = dot(vt[s, :, :ext], p).astype(BF16)

        with sc(f"attn{l}{a}"):
            loop(0, D.seqs * per, body)

    def gate_up(l, a, slot, j, seq_of, count):
        C = D.cfg[l]

        def body(i):
            s = seq_of(i)
            p = dot(wbuf[slot, : 2 * C.cw, :], ht[s])
            g = p[: C.cw].astype(BF16).astype(F32)
            u = p[C.cw :].astype(BF16).astype(F32)
            jt[rows_at((a * D.seqs + s) * (C.q + C.f) + C.q + j * C.cw, C.cw), :] = (g * jax.nn.sigmoid(g) * u).astype(BF16)

        loop(0, count, body)

    def gate_up_loop(l, a, seq_of, count, first, last, stop=None):
        C = D.cfg[l]
        stop = C.n_c if stop is None else stop
        have_chunk(l, min(last, stop - 1))

        def body(j):
            slot = lax.rem(j, 2)
            wait(w_fetch(l, "f", j, slot))

            @pl.when(j + 1 < stop)
            def _():
                start(w_fetch(l, "f", j + 1, 1 - slot))

            gate_up(l, a, slot, j, seq_of, count)

        with sc(f"gu{l}{a}"):
            loop(first, last, body)

    def have_chunk(l, j):
        C = D.cfg[l]
        have(l, "f", (j + 1) * C.cw // fch - 1)

    def load_q(l):
        have(l, "q", 0)
        copies = w_fetch(l, "q", 0, 1)
        start(copies)
        wait(copies)

    m = och * n_row
    m_low, m_high = pl.ds(0, m // 2), pl.ds(m // 2, m // 2)
    r_slots = twin_in.shape[0]
    r_step = 64

    def order(i):
        return lax.rem(x + lax.rem(2 + 3 * i, 4), n_x)

    class Reduce:
        def __init__(self, l):
            self.l, self.C, self.sends = l, D.cfg[l], {}

        def send(self, u, i, src, dst, c):
            copy = remote(src, dst, rss.at[u % r_slots, i], rsr.at[u % r_slots, i], row, c)
            copy.start()
            self.sends[u].append(copy)

        def arrived(self, u, i, ref):
            remote(ref, ref, rss.at[u % r_slots, i], rsr.at[u % r_slots, i], row, col).wait_recv()

        def twin_copy(self, u, i):
            us = u % r_slots
            return remote(ot.at[u % 2, order(i), :, twin_lanes], twin_in.at[us, i], rss.at[us, i], rsr.at[us, i], row, twin)

        def twin_done(self, u):
            loop(0, 4, lambda i: self.twin_copy(u, i).wait_send())

        def stage_a(self, u, a):
            C = self.C
            if u >= 2:
                self.twin_done(u - 2)
            if u >= r_slots - 1:
                for c in self.sends.pop(u - r_slots + 1):
                    c.wait_send()
            self.sends[u] = []
            R = C.q + C.f

            def body(i):
                s = order(i)
                ot[u % 2, s] = dot(wobuf[:, :R], jt[rows_at((a * D.seqs + s) * R, R), :]).astype(BF16)
                self.twin_copy(u, i).start()

            with sc(f"sa{self.l}_{u}"):
                loop(0, 4, body)

        def stage_b(self, u):
            us = u % r_slots

            def body(i):
                self.arrived(u, i, twin_in.at[us, i])
                s = order(i)

                def add(b):
                    at = rows_at(b * r_step, r_step)
                    twin_in[us, i, at, :] = (ot[u % 2, s, at, my_lanes].astype(F32) + twin_in[us, i, at, :].astype(F32)).astype(BF16)

                loop(0, m // r_step, add)

            far = [
                remote(twin_in.at[us, 0, m_low], far_in.at[us, m_low], rss.at[us, 4], rsr.at[us, 4], row, right),
                remote(twin_in.at[us, 0, m_high], far_in.at[us, m_high], rss.at[us, 5], rsr.at[us, 5], row, left),
            ]
            self.sends[u] += far

            def each(i):
                body(i)

                @pl.when(i == 0)
                def _():
                    start(far)

            with sc(f"sb{self.l}_{u}"):
                loop(0, 4, each)

        def stage_c(self, u):
            us = u % r_slots

            def add_far(i, base):
                def add(b):
                    at = rows_at(base + b * r_step, r_step)
                    twin_in[us, i, at, :] = (twin_in[us, i, at, :].astype(F32) + far_in[us, at, :].astype(F32)).astype(BF16)

                loop(0, m // 2 // r_step, add)

            with sc(f"sc{self.l}_{u}"):
                self.arrived(u, 4, far_in.at[us, m_low])
                add_far(1, 0)
                self.send(u, 6, twin_in.at[us, 1], near_in.at[us, 0], right)
                self.arrived(u, 5, far_in.at[us, m_high])
                add_far(3, m // 2)
                self.send(u, 7, twin_in.at[us, 3], near_in.at[us, 1], left)

        def add_update(self, j, total):
            step = min(r_step, och)
            for r in range(n_row):

                def add(b, r=r):
                    dst = rows_at(r * dr + (r + j) % D.n_o * och + b * step, step)
                    u = total(rows_at(r * och + b * step, step)).astype(BF16).astype(F32)
                    hid[dst, :] = (hid[dst, :].astype(F32) + u).astype(BF16)

                loop(0, och // step, add)

        def stage_d(self, u, j, a):
            us = u % r_slots

            def total(at):
                return twin_in[us, 2, at, :].astype(F32) + near_in[us, 0, at, :].astype(F32) + near_in[us, 1, at, :].astype(F32)

            with sc(f"sd{self.l}_{u}"):
                self.arrived(u, 6, near_in.at[us, 0])
                self.arrived(u, 7, near_in.at[us, 1])
                if self.C.split:

                    def save(b):
                        at = rows_at(b * r_step, r_step)
                        psum[a, j, at, :] = total(at).astype(BF16)

                    loop(0, m // r_step, save)
                    if a == 1:
                        remote(psum.at[1, j], pair_in.at[j], es.at[j], er.at[j], mate, col).start()
                else:
                    self.add_update(j, total)

        def stage_e(self, j):
            with sc(f"se{self.l}_{j}"):
                c = remote(psum.at[1, j], pair_in.at[j], es.at[j], er.at[j], mate, col)
                c.wait_recv()
                self.add_update(j, lambda at: psum[0, j, at, :].astype(F32) + pair_in[j, at, :].astype(F32))
                c.wait_send()

        def finish(self, units):
            with sc(f"rfin{self.l}"):
                for u in range(max(0, units - 2), units):
                    self.twin_done(u)
                for u in self.sends:
                    for c in self.sends[u]:
                        c.wait_send()

    o_started = set()

    def o_load(l, j, a):
        if (l, j, a) not in o_started:
            have(l, "o", j)
            start(o_fetch(l, j, j % 2))
            o_started.add((l, j, a))

    def o_use(l, j, a):
        C = D.cfg[l]
        with sc(f"ouse{l}_{j}"):
            o_load(l, j, a)
            wait(o_fetch(l, j, j % 2))
            R = C.q + C.f
            for r in range(n_row):
                wobuf[r * och : (r + 1) * och, :R] = wonat[j % 2, :R, r * och : (r + 1) * och].T

    layer_norm(0)
    g0 = Gather(normed_of(ht), 0)
    mine = ht.at[x, :, my_lanes]
    shared = g_h.at[x, :, my_lanes]
    to_mate = remote(mine, shared, ps, pr_, mate, col)
    to_mate.start()
    relay_to(1)
    mate_to(step(0, 5))
    peer_to(step(0, 5))
    g0.pass_low()
    g0.pass_on()
    with sc("mate"):
        to_mate.wait_recv()
    g1 = Gather(normed_of(g_h), 1)
    load_q(0)
    g0.own()
    g0.near()
    project_q(0, 0, near3, 3)
    relay_to(2)
    mate_to(step(0, 10))
    g0.pass_far()
    g0.far()
    project_q(0, 0, far1, 1)
    kv0 = Gather(kv_of(0), 2)
    relay_to(3)
    n_f = D.cfg[0].n_f
    f_started = set()

    def f_load(j):
        if j not in f_started:
            f_started.add(j)
            start(w_fetch(0, "f", j, j % 2))

    def h_copy(i):
        return pltpu.make_async_copy(g_h.at[i], ht.at[i], lh.at[i])

    have(0, "f", 0)
    f_load(0)
    gate_up_loop(0, 0, all4, 4, 0, 2, 2)
    relay_to(step(0, 4))
    for j in range(2, n_f):
        have(0, "f", j)
        f_load(j)
        with sc(f"gu0_{j}"):
            wait(w_fetch(0, "f", j, j % 2))
            gate_up(0, 0, j % 2, j, all4, 4)
        if j == max(2, n_f - 3):
            relay_to(step(0, 5))
            peer_to(step(0, 6))
            relay_to(step(0, 6))
            peer_to(step(0, 7))
    kv0.pass_low()
    kv0.pass_on()
    g1.pass_low()
    g1.pass_on()
    for t in (7, 8):
        relay_to(step(0, t))
        peer_to(step(0, t + 1))
    relay_to(step(0, 9))
    peer_to(step(0, 10))
    relay_to(step(0, 10))
    peer_to(step(1, 5))
    mate_to(step(1, D.cfg[1].n_f - 2))
    g0.finish()
    to_mate.wait_send()
    g1.own()
    g1.near()
    loop(0, 3, lambda i: h_copy(near3(i)).start())
    kv0.pass_far()
    with sc("kv0wait"):
        kv0.own()
        kv0.near()
        kv0.far()
        kv0.finish()
    key_value(0, 0)
    attention(0, 0)

    red = Reduce(0)
    units = [(j, 0) for j in range(D.n_o - 1)] + [(j, 1) for j in range(D.n_o)] + [(D.n_o - 1, 0)]
    n_u = len(units)
    first = D.n_o - 1
    state = {"e": 0}

    def settle(count):
        while state["e"] < count:
            red.stage_e(state["e"])
            state["e"] += 1

    def unit(u):
        j, a = units[u]
        if u == 0 or units[u - 1][0] != j:
            o_use(0, j, a)
        red.stage_a(u, a)
        if u + 1 < n_u and units[u + 1][0] != j:
            o_load(0, *units[u + 1])
        if u >= 2:
            red.stage_c(u - 2)
        if u >= 3:
            red.stage_d(u - 3, *units[u - 3])
        red.stage_b(u)

    unit(0)
    g1.pass_far()
    unit(1)
    g1.far()
    h_copy(xf_).start()
    load_q(0)
    start(w_fetch(0, "f", 0, 0))
    loop(0, 3, lambda i: h_copy(near3(i)).wait())
    h_copy(xf_).wait()
    project_q(0, 1, all4, 4)
    kv1 = Gather(kv_of(1), 3)
    parts = first - 2
    cuts = [n_f * i // parts for i in range(parts + 1)]
    for u in range(2, first):
        unit(u)
        if u == 2:
            kv1.pass_low()
            kv1.pass_on()
        gate_up_loop(0, 1, all4, 4, cuts[u - 2], cuts[u - 1])
    kv1.pass_far()
    relay_to(step(1, 1))
    with sc("kv1wait"):
        kv1.own()
        kv1.near()
        kv1.far()
        kv1.finish()
    key_value(0, 1)
    attention(0, 1)
    g1.finish()
    relay_to(step(1, 2))
    peer_to(step(1, 7))
    n_f1 = D.cfg[1].n_f
    for u in range(first, n_u):
        unit(u)
        v = u - first
        if v in (0, 1, 2):
            relay_to(step(1, min(v + 3, n_f1 - 2)))
        if v == 1:
            peer_to(step(1, min(8, n_f1)))
        elif v == 4:
            peer_to(step(1, min(9, n_f1)))
    red.stage_c(n_u - 2)
    relay_to(step(1, min(6, n_f1 - 2)))
    peer_to(step(1, n_f1))
    red.stage_d(n_u - 3, *units[n_u - 3])
    red.stage_c(n_u - 1)
    red.stage_d(n_u - 2, *units[n_u - 2])
    mate_to(step(1, n_f1))
    settle(D.n_o - 1)
    red.stage_d(n_u - 1, *units[n_u - 1])
    settle(D.n_o)
    red.finish(n_u)

    def slice_of(d):
        return hid.at[rows_at(d * dl, dl), :]

    own_y = pltpu.make_async_copy(slice_of(me), piece_of(y_out, me), xr.at[0])

    def y_copy_back(i):
        d = lax.rem(me + i, n)
        return remote(slice_of(d), piece_of(y_out, me), xs.at[i], xr.at[i], d // n_col, lax.rem(d, n_col))

    def y_send_back(i):
        @pl.when(i == 0)
        def _():
            own_y.start()

        @pl.when(i != 0)
        def _():
            y_copy_back(i).start()

    def y_finish(i):
        s = lax.rem(me + n - i, n)
        remote(piece_of(y_out, s), piece_of(y_out, s), xs.at[i], xr.at[i], row, col).wait_recv()
        y_copy_back(i).wait_send()

    def y_ready(low, high):
        def body(i):
            d = lax.rem(me + i, n)
            r, a = d // n_col, lax.rem(d, n_col) * dl
            first = lax.rem(a // och + D.n_o - lax.rem(r, D.n_o), D.n_o)
            second = lax.rem((a + dl - 1) // och + D.n_o - lax.rem(r, D.n_o), D.n_o)

            done = jnp.maximum(first, second)

            @pl.when((low <= done) & (done < high))
            def _():
                y_send_back(i)

        loop(0, n, body)

    for l in range(1, D.layers):
        C = D.cfg[l]
        layer_norm(l)
        g0 = Gather(normed_of(ht), 0)
        peer_to(step(l, C.n_f))
        mate_to(step(l, C.n_f))
        relay_to(step(l, min(8, C.n_f)))
        own1, near2 = (lambda i: x), (lambda i: lax.rem(x + 1 + 2 * i, n_x))
        n_mid = min(3, C.n_c - 1)

        def begin(seq_of, count):
            load_q(l)
            have_chunk(l, 0)
            start(w_fetch(l, "f", 0, 0))
            project_q(l, 0, seq_of, count)

        g0.own()
        begin(own1, 1)
        gate_up_loop(l, 0, own1, 1, 0, n_mid, n_mid)
        g0.pass_low()
        relay_to(step(l, C.n_f))
        peer_to(step(l, C.n_f + 2))
        mate_to(step(l, C.n_f + 2))
        g0.pass_on()
        g0.near()
        begin(near2, 2)
        gate_up_loop(l, 0, near2, 2, 0, n_mid)
        g0.pass_far()
        kv_send(near3, 3)
        relay_to(step(l, C.n_f + 1))
        peer_to(step(l, C.n_f + 4))
        mate_to(step(l, C.n_f + 4))
        gate_up_loop(l, 0, near3, 3, n_mid, C.n_c)
        relay_to(step(l, C.n_f + 2))
        g0.far()
        begin(far1, 1)
        kv_send(far1, 1)
        gate_up_loop(l, 0, far1, 1, 0, C.n_c)
        peer_to(step(l, C.n_f + D.n_o))
        mate_to(step(l, C.n_f + D.n_o))
        relay_to(step(l, C.n_f + 3))
        g0.finish()
        kv_arrive()
        key_value(l, 0)
        o_load(l, 0, 0)
        attention(l, 0)
        relay_to(step(l, C.n_f + 4))
        red = Reduce(l)
        last = l + 1 == D.layers

        end = D.n_o - 1
        for j in range(D.n_o):
            o_use(l, j, 0)
            red.stage_a(j, 0)
            if j == 1:
                relay_to(step(l, C.n_f + D.n_o))
            if j < end:
                o_load(l, j + 1, 0)
            if 2 <= j:
                red.stage_c(j - 2)
            if 3 <= j:
                red.stage_d(j - 3, j - 3, 0)
            red.stage_b(j)
        red.stage_c(end - 1)
        red.stage_d(end - 2, end - 2, 0)
        red.stage_c(end)
        red.stage_d(end - 1, end - 1, 0)
        if last:
            with sc("send"):
                y_ready(0, end)
        red.stage_d(end, end, 0)
        if last:
            y_ready(end, end + 1)
        red.finish(D.n_o)

    def kv_back(i):
        r = lax.rem(row + i, n_row)
        pos = rows_at((r * n_col + col) * D.pos, D.pos)
        return kvbuf.at[:, :, :, pos, :], kv_out.at[:, :, pl.ds(row * D.seqs, D.seqs)], r

    src, dst, _ = kv_back(0)
    own_kv = pltpu.make_async_copy(src, dst, fl)
    own_kv.start()
    kv_sends = []
    for i in range(1, n_row):
        src, dst, r = kv_back(i)
        c = remote(src, dst, fs.at[i], fr.at[i], r, col)
        c.start()
        kv_sends.append(c)

    with sc("ywait"):
        loop(1, n, y_finish)
        own_y.wait()
        own_kv.wait()
        for i in range(1, n_row):
            r = lax.rem(row + n_row - i, n_row)
            dst = kv_out.at[:, :, pl.ds(r * D.seqs, D.seqs)]
            remote(dst, dst, fs.at[i], fr.at[i], row, col).wait_recv()
        for c in kv_sends:
            c.wait_send()
        for c in y_sent:
            c.wait_send()


def solution(mesh):
    n_row, n_col = mesh.shape["row"], mesh.shape["col"]
    group = n_row * n_col
    act_spec = P("dp", None, ("row", "col"))
    weight_spec = P(None, "row", "col")

    def device_fn(x_loc, gain_loc, w_in_loc, w_kv_loc, w_out_loc):
        D = Dims()
        D.n_row, D.n_col = n_row, n_col
        n_batch, D.seq, D.dl = x_loc.shape
        D.layers, D.dr, e = w_in_loc.shape
        D.d = D.dl * group
        r_block = w_out_loc.shape[1]
        D.f = e - r_block
        D.q = r_block - D.f
        kv_local = w_kv_loc.shape[2]
        D.hd = kv_local * n_col // 2
        D.kvp = 32
        D.tok = n_batch * D.seq // group
        D.seqs = n_batch // n_row
        D.pos = D.seq // group
        D.fch = 128
        D.och = 128
        D.n_o = D.dr // D.och
        D.cfg = []
        for l in range(D.layers):
            C = Dims()
            C.split = l == 0
            parts = 2 if C.split else 1
            C.q, C.f = D.q // parts, D.f // parts
            C.heads, C.n_f = C.q // D.hd, C.f // D.fch
            C.cw = D.fch if C.split else 2 * D.fch
            C.n_c = C.f // C.cw
            D.cfg.append(C)
        assert D.seq == 2 * D.tok and D.seqs == n_col // 2 == n_row == 4

        half = D.hd // 2
        inv_freq = (np.float32(1.0) / (np.float32(10000.0) ** (np.arange(half, dtype=np.float32) * np.float32(2.0) / np.float32(D.hd)))).astype(np.float32)
        angles = (inv_freq[:, None] * np.arange(D.seq, dtype=np.float32)[None, :]).astype(np.float32)
        cos_t, sin_t = np.cos(angles).astype(np.float32), np.sin(angles).astype(np.float32)
        perm = np.zeros((2 * D.hd, n_col * D.kvp), np.float32)
        for i in range(2 * D.hd):
            perm[i, (i // kv_local) * D.kvp + i % kv_local] = 1.0

        x_t = x_loc.transpose(0, 2, 1)
        w_t = w_in_loc.transpose(0, 2, 1)
        wkv_t = jnp.pad(w_kv_loc.transpose(0, 2, 1), ((0, 0), (0, D.kvp - kv_local), (0, 0)))
        gains = jnp.pad(gain_loc, ((0, 16 - D.layers), (0, 128 - D.dl)))

        n_y = sum(12 + 6 * (C.n_f + D.n_o) for C in D.cfg)
        m = D.och * n_row
        sds = jax.ShapeDtypeStruct
        dma = pltpu.SemaphoreType.DMA
        out = pl.pallas_call(
            functools.partial(kernel, D),
            out_shape=(
                sds(x_t.shape, BF16),
                sds((D.layers, 2, n_batch, D.pos, 128), BF16),
                sds((D.layers, e, D.d), BF16),
                sds((D.layers, D.kvp, D.d), BF16),
                sds((D.layers, n_row, r_block, D.dr), BF16),
                sds((D.seqs, D.d, D.seq), BF16),
            ),
            in_specs=[ANY] * 5 + [VMEM] * 3,
            out_specs=(ANY,) * 6,
            scratch_shapes=[
                pltpu.VMEM((group, D.dl, D.tok), BF16),
                pltpu.VMEM((group, 16, 128), BF16),
                pltpu.VMEM((D.layers, D.d, 128), F32),
                pltpu.VMEM((D.d, D.tok), BF16),
                pltpu.VMEM((D.seqs, D.d, D.seq), BF16),
                pltpu.VMEM((2, max(4 * D.fch, D.q + D.kvp), D.d), BF16),
                pltpu.VMEM((2, r_block, m), BF16),
                pltpu.VMEM((m, r_block), BF16),
                pltpu.VMEM((D.seqs * D.q, D.seq), BF16),
                pltpu.VMEM((n_col, 2 * D.seqs, D.kvp, D.seq), BF16),
                pltpu.VMEM((2 * D.seqs, D.seq, 128), BF16),
                pltpu.VMEM((2 * D.seqs, D.hd, D.seq), BF16),
                pltpu.VMEM((D.layers, 2, D.seqs, D.seq, 128), BF16),
                pltpu.VMEM((D.seqs * r_block, D.seq), BF16),
                pltpu.VMEM((2, D.seqs, m, D.seq), BF16),
                pltpu.VMEM((5, 4, m, D.tok), BF16),
                pltpu.VMEM((5, m, D.tok), BF16),
                pltpu.VMEM((5, 2, m, D.tok), BF16),
                pltpu.VMEM((2, D.n_o, m, D.tok), BF16),
                pltpu.VMEM((D.n_o, m, D.tok), BF16),
                dma((group,)), dma((group,)), dma((group,)), dma((group,)),
                dma((n_y,)), dma((n_y,)),
                dma((4, 13)), dma((4, 13)), dma, dma,
                dma((D.seqs, n_col)), dma((D.seqs, n_col)),
                dma((5, 8)), dma((5, 8)),
                dma((D.n_o,)), dma((D.n_o,)),
                dma((2, 8)), dma((2, 8)), dma((D.seqs,)),
                dma((n_row,)), dma((n_row,)), dma,
            ],
            compiler_params=pltpu.CompilerParams(collective_id=0, has_side_effects=True, vmem_limit_bytes=67_000_000),
            name="two_layers",
        )(x_t, gains, w_t, wkv_t, w_out_loc, jnp.asarray(cos_t), jnp.asarray(sin_t), jnp.asarray(perm, BF16))
        return out[0].transpose(0, 2, 1), out[1][..., : D.hd]

    return jax.shard_map(device_fn, mesh=mesh, in_specs=(act_spec, P(None, ("row", "col")), weight_spec, weight_spec, P(None, "col", "row")), out_specs=(act_spec, P(None, None, "dp", ("row", "col"), None)), check_vma=False)
```

```python
import functools

import numpy as np

import jax
import jax.numpy as jnp
from jax import lax
from jax.experimental import pallas as pl
from jax.experimental.pallas import tpu as pltpu
from jax.sharding import PartitionSpec as P

LN_EPS = 1e-6
MESH = pl.DeviceIdType.MESH
ANY = pl.BlockSpec(memory_space=pl.ANY)
VMEM = pl.BlockSpec(memory_space=pltpu.VMEM)
F32, BF16 = jnp.float32, jnp.bfloat16


def dot(a, b):
    return jnp.dot(a, b, preferred_element_type=F32)


class Dims:
    pass


def rows_at(start, count, by=16):
    return pl.ds(start if isinstance(start, int) else pl.multiple_of(start, by), count)


def kernel(
    D,
    x_t, gains, w_t, wkv_t, w_o, cos_ref, sin_ref, perm_ref,
    y_out, kv_out, g_w, g_kv, g_wo, g_h,
    xland, gland, gcol, hid, ht, wbuf, wonat, wobuf, qt, kvland, kn, vt, kvbuf, jt, ot, twin_in, far_in, near_in, psum, pair_in,
    xs, xr, gs, gr, ys, yr, ags, agr, ps, pr_, kvs, kvr, rss, rsr, es, er, lw, lo, lh, fs, fr, fl,
):
    sc = jax.named_scope
    row, col = lax.axis_index("row"), lax.axis_index("col")
    n_row, n_col, n = D.n_row, D.n_col, D.n_row * D.n_col
    n_x = n_col // 2
    me = row * n_col + col
    x, k = col // 2, lax.rem(col, 2)
    xr_, xl_, xf_ = lax.rem(x + 1, n_x), lax.rem(x + n_x - 1, n_x), lax.rem(x + 2, n_x)
    right, left, twin = xr_ * 2 + k, xl_ * 2 + k, x * 2 + 1 - k
    up, down, across = lax.rem(row + 1, n_row), lax.rem(row + n_row - 1, n_row), lax.rem(row + 2, n_row)
    half, mate = row // 2, n_row - 1 - row
    peer = row + 1 - 2 * lax.rem(row, 2)
    tok, dl, dr = D.tok, D.dl, D.dr
    och, fch = D.och, D.fch
    my_lanes = pl.ds(pl.multiple_of(k * tok, 128), tok)
    twin_lanes = pl.ds(pl.multiple_of((1 - k) * tok, 128), tok)

    def remote(src, dst, ssem, rsem, r, c):
        return pltpu.make_async_remote_copy(src_ref=src, dst_ref=dst, send_sem=ssem, recv_sem=rsem, device_id={"row": r, "col": c}, device_id_type=MESH)

    def loop(lo_, hi_, f):
        def body(i, carry):
            f(i)
            return carry

        lax.fori_loop(lo_, hi_, body, 0)

    barrier = pltpu.get_barrier_semaphore()

    def greet(i):
        d = lax.rem(me + i, n)
        pl.semaphore_signal(barrier, inc=1, device_id={"row": d // n_col, "col": lax.rem(d, n_col)}, device_id_type=MESH)

    with sc("barrier"):
        loop(1, n, greet)
        pl.semaphore_wait(barrier, n - 1)

    def piece_of(ref, d):
        return ref.at[d // 2, :, pl.ds(pl.multiple_of(lax.rem(d, 2) * tok, 128), tok)]

    def x_copy(i):
        d = lax.rem(me + i, n)
        return remote(piece_of(x_t, d), xland.at[me], xs.at[i], xr.at[i], d // n_col, lax.rem(d, n_col))

    def g_copy(i):
        d = lax.rem(me + i, n)
        return remote(gains, gland.at[me], gs.at[i], gr.at[i], d // n_col, lax.rem(d, n_col))

    own_x = pltpu.make_async_copy(piece_of(x_t, me), xland.at[me], xr.at[0])
    own_g = pltpu.make_async_copy(gains, gland.at[me], gr.at[0])
    own_x.start()
    own_g.start()
    def x_first(i):
        x_copy(i).start()
        g_copy(i).start()

    loop(1, n, x_first)

    def own_lanes(r):
        return pl.ds(pl.multiple_of(r * dr, 128), dr)

    def o_lanes(j, r):
        return pl.ds(pl.multiple_of(lax.rem(r + j, D.n_o) * och, 128), och)

    steps = []
    for l, C in enumerate(D.cfg):
        steps += [(l, "q", 0)] + [(l, "f", j) for j in range(C.n_f)] + [(l, "o", j) for j in range(D.n_o)]
    n_steps = len(steps)
    step_of = {s: t for t, s in enumerate(steps)}

    def blocks(t, i):
        l, kind, j = steps[t]
        C = D.cfg[l]
        out = []

        def w_rows(a, m):
            at = rows_at(a, m)
            out.append((w_t.at[l, at, :], lambda r: g_w.at[l, at, own_lanes(r)]))

        def o_rows(a, m):
            at = rows_at(a, m)
            out.append((w_o.at[l, at, o_lanes(j, row)], lambda r: g_wo.at[l, r, at, o_lanes(j, r)]))

        def kv_rows(a, m):
            at = pl.ds(a, m)
            out.append((wkv_t.at[l, at, :], lambda r: g_kv.at[l, at, own_lanes(r)]))

        if kind == "q":
            for a in (0, C.q // 2):
                w_rows(i * C.q + a, C.q // 2)
            for a in (0, D.kvp // 2):
                kv_rows(a, D.kvp // 2)
        elif kind == "f":
            w_rows(D.q + i * C.f + j * fch, fch)
            w_rows(D.q + D.f + i * C.f + j * fch, fch)
        elif C.split:
            o_rows(i * C.q, C.q)
            o_rows(D.q + i * C.f, C.f)
        else:
            for a in (0, (D.q + D.f) // 2):
                o_rows(a, (D.q + D.f) // 2)
        return out

    base, n_sems = [], 0
    for l, kind, j in steps:
        base.append(n_sems)
        n_sems += 12 if kind == "q" else 6
    assert n_sems == ys.shape[0]
    y_sent = []

    def y_copy(t, i, kind, src, dst, r):
        at = base[t] + 3 * i + kind
        return remote(src, dst, ys.at[at], yr.at[at], r, col)

    def y_send(*args):
        c = y_copy(*args)
        c.start()
        y_sent.append(c)

    def issue_peer(t):
        for i, (src, place) in enumerate(blocks(t, half if D.cfg[steps[t][0]].split else 0)):
            y_send(t, i, 0, src, place(row), peer)

    def issue_mate(t):
        for i, (src, place) in enumerate(blocks(t, 1 - half if D.cfg[steps[t][0]].split else 0)):
            y_send(t, i, 1, src, place(row), mate)

    def relay(t):
        split = D.cfg[steps[t][0]].split
        with sc(f"relay{t}"):
            for i, (src, place) in enumerate(blocks(t, half if split else 0)):
                y_copy(t, i, 1, src, place(mate), mate).wait_recv()
                if split or i % 2 == 0:
                    y_send(t, i, 2, place(mate), place(mate), peer)
                if not split:
                    y_copy(t, i, 0, src, place(peer), peer).wait_recv()
                    if i % 2 == 1:
                        y_send(t, i, 2, place(peer), place(peer), mate)

    at = {"next": 0, "peer": 0, "mate": 0, "relay": 0}
    first_of = {l: min(t for t, st in enumerate(steps) if st[0] == l) for l in range(D.layers)}

    def step(l, j):
        return min(first_of[l] + j, first_of.get(l + 1, n_steps) - 1)

    def peer_to(t):
        while at["peer"] <= t:
            issue_peer(at["peer"])
            at["peer"] += 1

    def mate_to(t):
        while at["mate"] <= t:
            issue_mate(at["mate"])
            at["mate"] += 1

    def relay_to(t):
        assert t < at["peer"] and t < at["mate"]
        while at["relay"] <= t:
            relay(at["relay"])
            at["relay"] += 1

    def advance():
        t = at["next"]
        assert t < at["relay"], t
        rest = n_row - 1 - peer
        with sc(f"adv{t}"):
            split = D.cfg[steps[t][0]].split
            for i, (src, place) in enumerate(blocks(t, half if split else 0)):
                if split:
                    y_copy(t, i, 0, src, place(peer), peer).wait_recv()
                y_copy(t, i, 2, src, place(rest), rest).wait_recv()
            at["next"] = t + 1

    def have(*which):
        while at["next"] <= step_of[which]:
            advance()

    mate_to(1)
    peer_to(step(0, 3))

    def w_fetch(l, kind, j, slot):
        C = D.cfg[l]
        i = half if C.split else 0
        copies = []

        def fetch(src, dst):
            copies.append(pltpu.make_async_copy(src, dst, lw.at[slot, len(copies)]))

        def w_rows(a, m, at):
            a, at = rows_at(a, m), pl.ds(at, m)
            fetch(w_t.at[l, a, :], wbuf.at[slot, at, own_lanes(row)])
            for r in (up, down, across):
                fetch(g_w.at[l, a, own_lanes(r)], wbuf.at[slot, at, own_lanes(r)])

        if kind == "q":
            w_rows(i * C.q, C.q, 0)
            at = pl.ds(C.q, D.kvp)
            fetch(wkv_t.at[l], wbuf.at[slot, at, own_lanes(row)])
            for r in (up, down, across):
                fetch(g_kv.at[l, :, own_lanes(r)], wbuf.at[slot, at, own_lanes(r)])
        else:
            w_rows(D.q + i * C.f + j * C.cw, C.cw, 0)
            w_rows(D.q + D.f + i * C.f + j * C.cw, C.cw, C.cw)
        return copies

    def o_fetch(l, j, slot):
        C = D.cfg[l]
        copies = []

        def fetch(src, dst):
            copies.append(pltpu.make_async_copy(src, dst, lo.at[slot, len(copies)]))

        spans = ((half * C.q, 0, C.q), (D.q + half * C.f, C.q, C.f)) if C.split else ((0, 0, C.q + C.f),)
        for a, at, m in spans:
            a, at = rows_at(a, m), pl.ds(at, m)
            to = lambda r: pl.ds(pl.multiple_of(r * och, 128), och)
            fetch(w_o.at[l, a, o_lanes(j, row)], wonat.at[slot, at, to(row)])
            for r in (up, down, across):
                fetch(g_wo.at[l, r, a, o_lanes(j, r)], wonat.at[slot, at, to(r)])
        return copies

    def start(copies):
        for c in copies:
            c.start()

    def wait(copies):
        for c in copies:
            c.wait()

    own_x.wait()
    own_g.wait()

    def x_finish(i):
        s = lax.rem(me + n - i, n)
        remote(xland.at[s], xland.at[s], xs.at[i], xr.at[i], row, col).wait_recv()
        remote(gland.at[s], gland.at[s], gs.at[i], gr.at[i], row, col).wait_recv()
        x_copy(i).wait_send()
        g_copy(i).wait_send()

    with sc("xwait"):
        loop(1, n, x_finish)

    def keep(d):
        hid[rows_at(d * dl, dl), :] = xland[d]

    with sc("gains"):
        loop(0, n, keep)
        g_all = gland[...].astype(F32)
        for l in range(D.layers):
            g_rows = g_all[:, l, :]
            g_rows = jnp.concatenate([g_rows, jnp.zeros((128 - n, 128), F32)], axis=0) if n < 128 else g_rows
            g_cols = g_rows.T
            for d in range(n):
                gcol[l, d * dl : (d + 1) * dl, :] = jnp.broadcast_to(g_cols[:dl, d : d + 1], (dl, 128))

    blk = 64
    n_blk = D.d // blk

    def layer_norm(l):
        def add_up(i, acc):
            v = hid[rows_at(i * blk, blk), :].astype(F32)
            return acc + v.reshape(blk // 8, 8, tok).sum(axis=0)

        mean = lax.fori_loop(0, n_blk, add_up, jnp.zeros((8, tok), F32)).sum(axis=0, keepdims=True) / D.d

        def add_sq(i, acc):
            v = hid[rows_at(i * blk, blk), :].astype(F32) - mean
            return acc + (v * v).reshape(blk // 8, 8, tok).sum(axis=0)

        var = lax.fori_loop(0, n_blk, add_sq, jnp.zeros((8, tok), F32)).sum(axis=0, keepdims=True) / D.d
        scale = lax.rsqrt(var + LN_EPS)

        def write(i):
            rows = rows_at(i * blk, blk)
            g = gcol[l, rows, :]
            g = jnp.concatenate([g] * (tok // 128), axis=1)
            v = (hid[rows, :].astype(F32) - mean) * scale * g
            ht[x, rows, my_lanes] = v.astype(BF16)

        with sc(f"norm{l}"):
            loop(0, n_blk, write)

    d_low, d_high = pl.ds(0, D.d // 2), pl.ds(D.d // 2, D.d // 2)

    class Gather:
        def __init__(self, ref, tag):
            self.ref, self.tag, self.sends = ref, tag, []
            for i, part, c in ((0, 0, right), (1, 0, left), (2, None, twin), (9, 1, right), (10, 1, left)):
                self.send(i, ref(x, False, part), c)

        def send(self, i, ref, c):
            copy = remote(ref, ref, ags.at[self.tag, i], agr.at[self.tag, i], row, c)
            copy.start()
            self.sends.append(copy)

        def arrived(self, i, ref):
            remote(ref, ref, ags.at[self.tag, i], agr.at[self.tag, i], row, col).wait_recv()

        def pass_low(self):
            with sc(f"pass_low{self.tag}"):
                self.arrived(0, self.ref(xl_, False, 0))
                self.send(3, self.ref(xl_, False, 0), right)
                self.send(4, self.ref(xl_, False, 0), twin)
                self.arrived(1, self.ref(xr_, False, 0))
                self.send(6, self.ref(xr_, False, 0), twin)

        def pass_on(self):
            with sc(f"pass_on{self.tag}"):
                self.arrived(10, self.ref(xr_, False, 1))
                self.send(5, self.ref(xr_, False, 1), left)
                self.send(12, self.ref(xr_, False, 1), twin)
                self.arrived(9, self.ref(xl_, False, 1))
                self.send(11, self.ref(xl_, False, 1), twin)

        def own(self):
            with sc(f"own{self.tag}"):
                self.arrived(2, self.ref(x, True, None))

        def near(self):
            with sc(f"near{self.tag}"):
                self.arrived(4, self.ref(xl_, True, 0))
                self.arrived(6, self.ref(xr_, True, 0))
                self.arrived(12, self.ref(xr_, True, 1))
                self.arrived(11, self.ref(xl_, True, 1))

        def pass_far(self):
            with sc(f"pass_far{self.tag}"):
                for part, i, j in ((0, 3, 7), (1, 5, 8)):
                    self.arrived(i, self.ref(xf_, False, part))
                    self.send(j, self.ref(xf_, False, part), twin)

        def far(self):
            with sc(f"far{self.tag}"):
                self.arrived(7, self.ref(xf_, True, 0))
                self.arrived(8, self.ref(xf_, True, 1))

        def finish(self):
            for c in self.sends:
                c.wait_send()

    def normed_of(buf):
        def ref(chip, other, part):
            rows = slice(None) if part is None else (d_low, d_high)[part]
            return buf.at[chip, rows, twin_lanes if other else my_lanes]

        return ref

    def kv_of(a):
        def ref(chip, other, part):
            h = D.seqs // 2
            span = pl.ds(a * D.seqs, D.seqs) if part is None else pl.ds(a * D.seqs + part * h, h)
            return kvland.at[chip * 2 + (1 - k if other else k), span]

        return ref

    half_dim = D.hd // 2

    def near3(i):
        return lax.rem(x + i + i // 2, n_x)

    def all4(i):
        return i

    def far1(i):
        return xf_

    def rope(p):
        lo_, hi_ = p[:half_dim], p[half_dim:]
        return jnp.concatenate([lo_ * cos_ref[...] - hi_ * sin_ref[...], hi_ * cos_ref[...] + lo_ * sin_ref[...]], axis=0)

    def project_q(l, a, seq_of, count):
        C = D.cfg[l]

        def body(i):
            s = seq_of(i)
            p = dot(wbuf[1, : C.q + D.kvp, :], ht[s]).astype(BF16).astype(F32)
            for h in range(C.heads):
                at = rows_at((a * D.seqs + s) * C.q + h * D.hd, D.hd)
                qt[at, :] = (rope(p[h * D.hd : (h + 1) * D.hd]) * D.hd**-0.5).astype(BF16)
            kvland[col, a * D.seqs + s] = p[C.q :].astype(BF16)

        with sc(f"q{l}{a}"):
            loop(0, count, body)

    def kv_copy(s, j, source):
        ref = kvland.at[source, s]
        return remote(ref, ref, kvs.at[s, j], kvr.at[s, j], row, lax.rem(col + j, n_col))

    def kv_send(seq_of, count):
        def body(i):
            s = seq_of(i)
            loop(1, n_col, lambda j: kv_copy(s, j, col).start())

        loop(0, count, body)

    def kv_arrive():
        def body(i):
            j = i // D.seqs + 1
            s = lax.rem(i, D.seqs)
            kv_copy(s, j, lax.rem(col + n_col - j, n_col)).wait_recv()
            kv_copy(s, j, col).wait_send()

        with sc("kvwait"):
            loop(0, D.seqs * (n_col - 1), body)

    def key_value(l, a):
        def body(i):
            s = a * D.seqs + i
            raw = kvland[:, s].reshape(n_col * D.kvp, D.seq)
            both = dot(perm_ref[...], raw)
            zeros = jnp.zeros((128 - D.hd, D.seq), F32)
            k_nat = jnp.concatenate([rope(both[: D.hd]), zeros], axis=0).T.astype(BF16)
            kn[s] = k_nat
            vt[s] = both[D.hd :].astype(BF16)
            if a == 0:
                kvbuf[l, 0, i] = k_nat
                kvbuf[l, 1, i] = jnp.concatenate([both[D.hd :], zeros], axis=0).T.astype(BF16)

        with sc(f"kv{l}{a}"):
            loop(0, D.seqs, body)

    qb = D.seq // 2

    def attention(l, a):
        C = D.cfg[l]

        pair = 2
        per = C.heads // pair

        def body(i):
            s, h0 = a * D.seqs + i // per, lax.rem(i, per) * pair
            q_rows = [rows_at(s * C.q + (h0 + e) * D.hd, D.hd) for e in range(pair)]
            o_rows = [rows_at(s * (C.q + C.f) + (h0 + e) * D.hd, D.hd) for e in range(pair)]
            for b in range(2):
                ext = (b + 1) * qb
                lanes = slice(b * qb, (b + 1) * qb)
                keys = lax.broadcasted_iota(jnp.int32, (ext, qb), 0)
                queries = lax.broadcasted_iota(jnp.int32, (ext, qb), 1) + b * qb
                scores = [dot(kn[s, :ext, : D.hd], qt[q_rows[e], lanes]) for e in range(pair)]
                for e in range(pair):
                    score = jnp.where(keys <= queries, scores[e], -1e30)
                    p = jnp.exp(score - jnp.max(score, axis=0, keepdims=True))
                    p = (p * (1.0 / jnp.sum(p, axis=0, keepdims=True))).astype(BF16)
                    jt[o_rows[e], lanes] = dot(vt[s, :, :ext], p).astype(BF16)

        with sc(f"attn{l}{a}"):
            loop(0, D.seqs * per, body)

    def gate_up(l, a, slot, j, seq_of, count):
        C = D.cfg[l]

        def body(i):
            s = seq_of(i)
            p = dot(wbuf[slot, : 2 * C.cw, :], ht[s])
            g = p[: C.cw].astype(BF16).astype(F32)
            u = p[C.cw :].astype(BF16).astype(F32)
            jt[rows_at((a * D.seqs + s) * (C.q + C.f) + C.q + j * C.cw, C.cw), :] = (g * jax.nn.sigmoid(g) * u).astype(BF16)

        loop(0, count, body)

    def gate_up_loop(l, a, seq_of, count, first, last, stop=None):
        C = D.cfg[l]
        stop = C.n_c if stop is None else stop
        have_chunk(l, min(last, stop - 1))

        def body(j):
            slot = lax.rem(j, 2)
            wait(w_fetch(l, "f", j, slot))

            @pl.when(j + 1 < stop)
            def _():
                start(w_fetch(l, "f", j + 1, 1 - slot))

            gate_up(l, a, slot, j, seq_of, count)

        with sc(f"gu{l}{a}"):
            loop(first, last, body)

    def have_chunk(l, j):
        C = D.cfg[l]
        have(l, "f", (j + 1) * C.cw // fch - 1)

    def load_q(l):
        have(l, "q", 0)
        copies = w_fetch(l, "q", 0, 1)
        start(copies)
        wait(copies)

    m = och * n_row
    m_low, m_high = pl.ds(0, m // 2), pl.ds(m // 2, m // 2)
    r_slots = twin_in.shape[0]
    r_step = 64

    def order(i):
        return lax.rem(x + lax.rem(2 + 3 * i, 4), n_x)

    class Reduce:
        def __init__(self, l):
            self.l, self.C, self.sends = l, D.cfg[l], {}

        def send(self, u, i, src, dst, c):
            copy = remote(src, dst, rss.at[u % r_slots, i], rsr.at[u % r_slots, i], row, c)
            copy.start()
            self.sends[u].append(copy)

        def arrived(self, u, i, ref):
            remote(ref, ref, rss.at[u % r_slots, i], rsr.at[u % r_slots, i], row, col).wait_recv()

        def twin_copy(self, u, i):
            us = u % r_slots
            return remote(ot.at[u % 2, order(i), :, twin_lanes], twin_in.at[us, i], rss.at[us, i], rsr.at[us, i], row, twin)

        def twin_done(self, u):
            loop(0, 4, lambda i: self.twin_copy(u, i).wait_send())

        def stage_a(self, u, a):
            C = self.C
            if u >= 2:
                self.twin_done(u - 2)
            if u >= r_slots - 1:
                for c in self.sends.pop(u - r_slots + 1):
                    c.wait_send()
            self.sends[u] = []
            R = C.q + C.f

            def body(i):
                s = order(i)
                ot[u % 2, s] = dot(wobuf[:, :R], jt[rows_at((a * D.seqs + s) * R, R), :]).astype(BF16)
                self.twin_copy(u, i).start()

            with sc(f"sa{self.l}_{u}"):
                loop(0, 4, body)

        def stage_b(self, u):
            us = u % r_slots

            def body(i):
                self.arrived(u, i, twin_in.at[us, i])
                s = order(i)

                def add(b):
                    at = rows_at(b * r_step, r_step)
                    twin_in[us, i, at, :] = (ot[u % 2, s, at, my_lanes].astype(F32) + twin_in[us, i, at, :].astype(F32)).astype(BF16)

                loop(0, m // r_step, add)

            far = [
                remote(twin_in.at[us, 0, m_low], far_in.at[us, m_low], rss.at[us, 4], rsr.at[us, 4], row, right),
                remote(twin_in.at[us, 0, m_high], far_in.at[us, m_high], rss.at[us, 5], rsr.at[us, 5], row, left),
            ]
            self.sends[u] += far

            def each(i):
                body(i)

                @pl.when(i == 0)
                def _():
                    start(far)

            with sc(f"sb{self.l}_{u}"):
                loop(0, 4, each)

        def stage_c(self, u):
            us = u % r_slots

            def add_far(i, base):
                def add(b):
                    at = rows_at(base + b * r_step, r_step)
                    twin_in[us, i, at, :] = (twin_in[us, i, at, :].astype(F32) + far_in[us, at, :].astype(F32)).astype(BF16)

                loop(0, m // 2 // r_step, add)

            with sc(f"sc{self.l}_{u}"):
                self.arrived(u, 4, far_in.at[us, m_low])
                add_far(1, 0)
                self.send(u, 6, twin_in.at[us, 1], near_in.at[us, 0], right)
                self.arrived(u, 5, far_in.at[us, m_high])
                add_far(3, m // 2)
                self.send(u, 7, twin_in.at[us, 3], near_in.at[us, 1], left)

        def add_update(self, j, total):
            step = min(r_step, och)
            for r in range(n_row):

                def add(b, r=r):
                    dst = rows_at(r * dr + (r + j) % D.n_o * och + b * step, step)
                    u = total(rows_at(r * och + b * step, step)).astype(BF16).astype(F32)
                    hid[dst, :] = (hid[dst, :].astype(F32) + u).astype(BF16)

                loop(0, och // step, add)

        def stage_d(self, u, j, a):
            us = u % r_slots

            def total(at):
                return twin_in[us, 2, at, :].astype(F32) + near_in[us, 0, at, :].astype(F32) + near_in[us, 1, at, :].astype(F32)

            with sc(f"sd{self.l}_{u}"):
                self.arrived(u, 6, near_in.at[us, 0])
                self.arrived(u, 7, near_in.at[us, 1])
                if self.C.split:

                    def save(b):
                        at = rows_at(b * r_step, r_step)
                        psum[a, j, at, :] = total(at).astype(BF16)

                    loop(0, m // r_step, save)
                    if a == 1:
                        remote(psum.at[1, j], pair_in.at[j], es.at[j], er.at[j], mate, col).start()
                else:
                    self.add_update(j, total)

        def stage_e(self, j):
            with sc(f"se{self.l}_{j}"):
                c = remote(psum.at[1, j], pair_in.at[j], es.at[j], er.at[j], mate, col)
                c.wait_recv()
                self.add_update(j, lambda at: psum[0, j, at, :].astype(F32) + pair_in[j, at, :].astype(F32))
                c.wait_send()

        def finish(self, units):
            with sc(f"rfin{self.l}"):
                for u in range(max(0, units - 2), units):
                    self.twin_done(u)
                for u in self.sends:
                    for c in self.sends[u]:
                        c.wait_send()

    o_started = set()

    def o_load(l, j, a):
        if (l, j, a) not in o_started:
            have(l, "o", j)
            start(o_fetch(l, j, j % 2))
            o_started.add((l, j, a))

    def o_use(l, j, a):
        C = D.cfg[l]
        with sc(f"ouse{l}_{j}"):
            o_load(l, j, a)
            wait(o_fetch(l, j, j % 2))
            R = C.q + C.f
            for r in range(n_row):
                wobuf[r * och : (r + 1) * och, :R] = wonat[j % 2, :R, r * och : (r + 1) * och].T

    layer_norm(0)
    g0 = Gather(normed_of(ht), 0)
    mine = ht.at[x, :, my_lanes]
    shared = g_h.at[x, :, my_lanes]
    to_mate = remote(mine, shared, ps, pr_, mate, col)
    to_mate.start()
    relay_to(1)
    mate_to(step(0, 5))
    peer_to(step(0, 5))
    g0.pass_low()
    g0.pass_on()
    with sc("mate"):
        to_mate.wait_recv()
    g1 = Gather(normed_of(g_h), 1)
    load_q(0)
    g0.own()
    g0.near()
    project_q(0, 0, near3, 3)
    relay_to(2)
    mate_to(step(0, 10))
    g0.pass_far()
    g0.far()
    project_q(0, 0, far1, 1)
    kv0 = Gather(kv_of(0), 2)
    relay_to(3)
    n_f = D.cfg[0].n_f
    f_started = set()

    def f_load(j):
        if j not in f_started:
            f_started.add(j)
            start(w_fetch(0, "f", j, j % 2))

    def h_copy(i):
        return pltpu.make_async_copy(g_h.at[i], ht.at[i], lh.at[i])

    have(0, "f", 0)
    f_load(0)
    gate_up_loop(0, 0, all4, 4, 0, 2, 2)
    relay_to(step(0, 4))
    for j in range(2, n_f):
        have(0, "f", j)
        f_load(j)
        with sc(f"gu0_{j}"):
            wait(w_fetch(0, "f", j, j % 2))
            gate_up(0, 0, j % 2, j, all4, 4)
        if j == max(2, n_f - 3):
            relay_to(step(0, 5))
            peer_to(step(0, 6))
            relay_to(step(0, 6))
            peer_to(step(0, 7))
    kv0.pass_low()
    kv0.pass_on()
    g1.pass_low()
    g1.pass_on()
    for t in (7, 8):
        relay_to(step(0, t))
        peer_to(step(0, t + 1))
    relay_to(step(0, 9))
    peer_to(step(0, 10))
    relay_to(step(0, 10))
    peer_to(step(1, 5))
    mate_to(step(1, D.cfg[1].n_f - 2))
    g0.finish()
    to_mate.wait_send()
    g1.own()
    g1.near()
    loop(0, 3, lambda i: h_copy(near3(i)).start())
    kv0.pass_far()
    with sc("kv0wait"):
        kv0.own()
        kv0.near()
        kv0.far()
        kv0.finish()
    key_value(0, 0)
    attention(0, 0)

    red = Reduce(0)
    units = [(j, 0) for j in range(D.n_o - 1)] + [(j, 1) for j in range(D.n_o)] + [(D.n_o - 1, 0)]
    n_u = len(units)
    first = D.n_o - 1
    state = {"e": 0}

    def settle(count):
        while state["e"] < count:
            red.stage_e(state["e"])
            state["e"] += 1

    def unit(u):
        j, a = units[u]
        if u == 0 or units[u - 1][0] != j:
            o_use(0, j, a)
        red.stage_a(u, a)
        if u + 1 < n_u and units[u + 1][0] != j:
            o_load(0, *units[u + 1])
        if u >= 2:
            red.stage_c(u - 2)
        if u >= 3:
            red.stage_d(u - 3, *units[u - 3])
        red.stage_b(u)

    unit(0)
    g1.pass_far()
    unit(1)
    g1.far()
    h_copy(xf_).start()
    load_q(0)
    start(w_fetch(0, "f", 0, 0))
    loop(0, 3, lambda i: h_copy(near3(i)).wait())
    h_copy(xf_).wait()
    project_q(0, 1, all4, 4)
    kv1 = Gather(kv_of(1), 3)
    parts = first - 2
    cuts = [n_f * i // parts for i in range(parts + 1)]
    for u in range(2, first):
        unit(u)
        if u == 2:
            kv1.pass_low()
            kv1.pass_on()
        gate_up_loop(0, 1, all4, 4, cuts[u - 2], cuts[u - 1])
    kv1.pass_far()
    relay_to(step(1, 0))
    with sc("kv1wait"):
        kv1.own()
        kv1.near()
        kv1.far()
        kv1.finish()
    key_value(0, 1)
    attention(0, 1)
    g1.finish()
    peer_to(step(1, 7))
    n_f1 = D.cfg[1].n_f
    for u in range(first, n_u):
        unit(u)
        v = u - first
        if v in (0, 1, 2, 3):
            relay_to(step(1, min(v + 2, n_f1 - 2)))
        if v == 1:
            peer_to(step(1, min(8, n_f1)))
        elif v == 4:
            peer_to(step(1, min(9, n_f1)))
    red.stage_c(n_u - 2)
    relay_to(step(1, min(6, n_f1 - 2)))
    peer_to(step(1, n_f1))
    red.stage_d(n_u - 3, *units[n_u - 3])
    red.stage_c(n_u - 1)
    red.stage_d(n_u - 2, *units[n_u - 2])
    mate_to(step(1, n_f1))
    settle(D.n_o - 1)
    red.stage_d(n_u - 1, *units[n_u - 1])
    settle(D.n_o)
    red.finish(n_u)

    def slice_of(d):
        return hid.at[rows_at(d * dl, dl), :]

    own_y = pltpu.make_async_copy(slice_of(me), piece_of(y_out, me), xr.at[0])

    def y_copy_back(i):
        d = lax.rem(me + i, n)
        return remote(slice_of(d), piece_of(y_out, me), xs.at[i], xr.at[i], d // n_col, lax.rem(d, n_col))

    def y_send_back(i):
        @pl.when(i == 0)
        def _():
            own_y.start()

        @pl.when(i != 0)
        def _():
            y_copy_back(i).start()

    def y_finish(i):
        s = lax.rem(me + n - i, n)
        remote(piece_of(y_out, s), piece_of(y_out, s), xs.at[i], xr.at[i], row, col).wait_recv()
        y_copy_back(i).wait_send()

    def y_ready(low, high):
        def body(i):
            d = lax.rem(me + i, n)
            r, a = d // n_col, lax.rem(d, n_col) * dl
            first = lax.rem(a // och + D.n_o - lax.rem(r, D.n_o), D.n_o)
            second = lax.rem((a + dl - 1) // och + D.n_o - lax.rem(r, D.n_o), D.n_o)

            done = jnp.maximum(first, second)

            @pl.when((low <= done) & (done < high))
            def _():
                y_send_back(i)

        loop(0, n, body)

    for l in range(1, D.layers):
        C = D.cfg[l]
        layer_norm(l)
        g0 = Gather(normed_of(ht), 0)
        peer_to(step(l, C.n_f))
        mate_to(step(l, C.n_f))
        relay_to(step(l, min(8, C.n_f)))
        own1, near2 = (lambda i: x), (lambda i: lax.rem(x + 1 + 2 * i, n_x))
        n_mid = min(3, C.n_c - 1)

        def begin(seq_of, count):
            load_q(l)
            have_chunk(l, 0)
            start(w_fetch(l, "f", 0, 0))
            project_q(l, 0, seq_of, count)

        g0.own()
        begin(own1, 1)
        gate_up_loop(l, 0, own1, 1, 0, n_mid, n_mid)
        g0.pass_low()
        relay_to(step(l, C.n_f))
        peer_to(step(l, C.n_f + 2))
        mate_to(step(l, C.n_f + 2))
        g0.pass_on()
        g0.near()
        begin(near2, 2)
        gate_up_loop(l, 0, near2, 2, 0, n_mid)
        g0.pass_far()
        kv_send(near3, 3)
        relay_to(step(l, C.n_f + 1))
        peer_to(step(l, C.n_f + 4))
        mate_to(step(l, C.n_f + 4))
        gate_up_loop(l, 0, near3, 3, n_mid, C.n_c)
        relay_to(step(l, C.n_f + 2))
        g0.far()
        begin(far1, 1)
        kv_send(far1, 1)
        gate_up_loop(l, 0, far1, 1, 0, C.n_c)
        peer_to(step(l, C.n_f + D.n_o))
        mate_to(step(l, C.n_f + D.n_o))
        relay_to(step(l, C.n_f + 3))
        g0.finish()
        kv_arrive()
        key_value(l, 0)
        o_load(l, 0, 0)
        attention(l, 0)
        relay_to(step(l, C.n_f + 4))
        red = Reduce(l)
        last = l + 1 == D.layers

        end = D.n_o - 1
        for j in range(D.n_o):
            o_use(l, j, 0)
            red.stage_a(j, 0)
            if j == 1:
                relay_to(step(l, C.n_f + D.n_o))
            if j < end:
                o_load(l, j + 1, 0)
            if 2 <= j:
                red.stage_c(j - 2)
            if 3 <= j:
                red.stage_d(j - 3, j - 3, 0)
            red.stage_b(j)
        red.stage_c(end - 1)
        red.stage_d(end - 2, end - 2, 0)
        red.stage_c(end)
        red.stage_d(end - 1, end - 1, 0)
        if last:
            with sc("send"):
                y_ready(0, end)
        red.stage_d(end, end, 0)
        if last:
            y_ready(end, end + 1)
        red.finish(D.n_o)

    def kv_back(i):
        r = lax.rem(row + i, n_row)
        pos = rows_at((r * n_col + col) * D.pos, D.pos)
        return kvbuf.at[:, :, :, pos, :], kv_out.at[:, :, pl.ds(row * D.seqs, D.seqs)], r

    src, dst, _ = kv_back(0)
    own_kv = pltpu.make_async_copy(src, dst, fl)
    own_kv.start()
    kv_sends = []
    for i in range(1, n_row):
        src, dst, r = kv_back(i)
        c = remote(src, dst, fs.at[i], fr.at[i], r, col)
        c.start()
        kv_sends.append(c)

    with sc("ywait"):
        loop(1, n, y_finish)
        own_y.wait()
        own_kv.wait()
        for i in range(1, n_row):
            r = lax.rem(row + n_row - i, n_row)
            dst = kv_out.at[:, :, pl.ds(r * D.seqs, D.seqs)]
            remote(dst, dst, fs.at[i], fr.at[i], row, col).wait_recv()
        for c in kv_sends:
            c.wait_send()
        for c in y_sent:
            c.wait_send()


def solution(mesh):
    n_row, n_col = mesh.shape["row"], mesh.shape["col"]
    group = n_row * n_col
    act_spec = P("dp", None, ("row", "col"))
    weight_spec = P(None, "row", "col")

    def device_fn(x_loc, gain_loc, w_in_loc, w_kv_loc, w_out_loc):
        D = Dims()
        D.n_row, D.n_col = n_row, n_col
        n_batch, D.seq, D.dl = x_loc.shape
        D.layers, D.dr, e = w_in_loc.shape
        D.d = D.dl * group
        r_block = w_out_loc.shape[1]
        D.f = e - r_block
        D.q = r_block - D.f
        kv_local = w_kv_loc.shape[2]
        D.hd = kv_local * n_col // 2
        D.kvp = 32
        D.tok = n_batch * D.seq // group
        D.seqs = n_batch // n_row
        D.pos = D.seq // group
        D.fch = 128
        D.och = 128
        D.n_o = D.dr // D.och
        D.cfg = []
        for l in range(D.layers):
            C = Dims()
            C.split = l == 0
            parts = 2 if C.split else 1
            C.q, C.f = D.q // parts, D.f // parts
            C.heads, C.n_f = C.q // D.hd, C.f // D.fch
            C.cw = D.fch if C.split else 2 * D.fch
            C.n_c = C.f // C.cw
            D.cfg.append(C)
        assert D.seq == 2 * D.tok and D.seqs == n_col // 2 == n_row == 4

        half = D.hd // 2
        inv_freq = (np.float32(1.0) / (np.float32(10000.0) ** (np.arange(half, dtype=np.float32) * np.float32(2.0) / np.float32(D.hd)))).astype(np.float32)
        angles = (inv_freq[:, None] * np.arange(D.seq, dtype=np.float32)[None, :]).astype(np.float32)
        cos_t, sin_t = np.cos(angles).astype(np.float32), np.sin(angles).astype(np.float32)
        perm = np.zeros((2 * D.hd, n_col * D.kvp), np.float32)
        for i in range(2 * D.hd):
            perm[i, (i // kv_local) * D.kvp + i % kv_local] = 1.0

        x_t = x_loc.transpose(0, 2, 1)
        w_t = w_in_loc.transpose(0, 2, 1)
        wkv_t = jnp.pad(w_kv_loc.transpose(0, 2, 1), ((0, 0), (0, D.kvp - kv_local), (0, 0)))
        gains = jnp.pad(gain_loc, ((0, 16 - D.layers), (0, 128 - D.dl)))

        n_y = sum(12 + 6 * (C.n_f + D.n_o) for C in D.cfg)
        m = D.och * n_row
        sds = jax.ShapeDtypeStruct
        dma = pltpu.SemaphoreType.DMA
        out = pl.pallas_call(
            functools.partial(kernel, D),
            out_shape=(
                sds(x_t.shape, BF16),
                sds((D.layers, 2, n_batch, D.pos, 128), BF16),
                sds((D.layers, e, D.d), BF16),
                sds((D.layers, D.kvp, D.d), BF16),
                sds((D.layers, n_row, r_block, D.dr), BF16),
                sds((D.seqs, D.d, D.seq), BF16),
            ),
            in_specs=[ANY] * 5 + [VMEM] * 3,
            out_specs=(ANY,) * 6,
            scratch_shapes=[
                pltpu.VMEM((group, D.dl, D.tok), BF16),
                pltpu.VMEM((group, 16, 128), BF16),
                pltpu.VMEM((D.layers, D.d, 128), F32),
                pltpu.VMEM((D.d, D.tok), BF16),
                pltpu.VMEM((D.seqs, D.d, D.seq), BF16),
                pltpu.VMEM((2, max(4 * D.fch, D.q + D.kvp), D.d), BF16),
                pltpu.VMEM((2, r_block, m), BF16),
                pltpu.VMEM((m, r_block), BF16),
                pltpu.VMEM((D.seqs * D.q, D.seq), BF16),
                pltpu.VMEM((n_col, 2 * D.seqs, D.kvp, D.seq), BF16),
                pltpu.VMEM((2 * D.seqs, D.seq, 128), BF16),
                pltpu.VMEM((2 * D.seqs, D.hd, D.seq), BF16),
                pltpu.VMEM((D.layers, 2, D.seqs, D.seq, 128), BF16),
                pltpu.VMEM((D.seqs * r_block, D.seq), BF16),
                pltpu.VMEM((2, D.seqs, m, D.seq), BF16),
                pltpu.VMEM((5, 4, m, D.tok), BF16),
                pltpu.VMEM((5, m, D.tok), BF16),
                pltpu.VMEM((5, 2, m, D.tok), BF16),
                pltpu.VMEM((2, D.n_o, m, D.tok), BF16),
                pltpu.VMEM((D.n_o, m, D.tok), BF16),
                dma((group,)), dma((group,)), dma((group,)), dma((group,)),
                dma((n_y,)), dma((n_y,)),
                dma((4, 13)), dma((4, 13)), dma, dma,
                dma((D.seqs, n_col)), dma((D.seqs, n_col)),
                dma((5, 8)), dma((5, 8)),
                dma((D.n_o,)), dma((D.n_o,)),
                dma((2, 8)), dma((2, 8)), dma((D.seqs,)),
                dma((n_row,)), dma((n_row,)), dma,
            ],
            compiler_params=pltpu.CompilerParams(collective_id=0, has_side_effects=True, vmem_limit_bytes=67_000_000),
            name="two_layers",
        )(x_t, gains, w_t, wkv_t, w_out_loc, jnp.asarray(cos_t), jnp.asarray(sin_t), jnp.asarray(perm, BF16))
        return out[0].transpose(0, 2, 1), out[1][..., : D.hd]

    return jax.shard_map(device_fn, mesh=mesh, in_specs=(act_spec, P(None, ("row", "col")), weight_spec, weight_spec, P(None, "col", "row")), out_specs=(act_spec, P(None, None, "dp", ("row", "col"), None)), check_vma=False)
```
